32 devices in a mesh: seq: 8 (over y, x, core), head: 4 (over z).
Axes of the slice: x: 2, y: 2, z: 4, core: 2. Of those that a mesh axis runs over, the one named last changes fastest.
Arguments:
- queries: bfloat16 [1024, 8192], P('seq', 'head'), may hold values from -2.5 to 2.5
- keys: bfloat16 [1024, 8192], P('seq', 'head'), may hold values from -2.5 to 2.5
- values: bfloat16 [1024, 4096], P('seq', 'head'), may hold values from -2.5 to 2.5
- out_grad: bfloat16 [1024, 4096], P('seq', 'head'), may hold values from -2.5 to 2.5
- log_gate: float32 [64, 1024], P('head', 'seq'), may hold values from -1 to 0
- level_weight: float32 [6, 64, 1024], P(None, 'head', 'seq'), may hold values from 0.25 to 2
- doc_start: int32 [1024], P('seq'), may hold values 0 or 1
Outputs:
- grad_queries: bfloat16 [1024, 8192], P('seq', 'head')
- grad_keys: bfloat16 [1024, 8192], P('seq', 'head')
- grad_values: bfloat16 [1024, 4096], P('seq', 'head')
- grad_level_weight: float32 [6, 64, 1024], P(None, 'head', 'seq')
- grad_log_gate: float32 [64, 1024], P('head', 'seq')
The draws below stay inside these ranges and needn't reach their ends.
All inputs are finite; a program needn't handle non-finite values. No bound on the sum of `doc_start` on one device may be relied on, other than what follows from the above.
Results may differ from the reference program's by a relative error of at most 0.0027.
Values sent between devices are 32-bit elements; how exact they have to be, the bound alone decides.
A program may use at most 128 MiB of HBM per device.

```python
import math
import jax
import jax.numpy as jnp
from jax import lax

HEAD_COUNT = 64
DK = 128
DV = 64
NL = 6
SPAN = 64
TOK_DEV = 128
TOKEN_COUNT = 1024
SPANS = 16


def draw_log_gate(key, part):
    every_key = jax.random.split(key, 7)
    slow_share = 0.5
    sluggish_head = jax.random.uniform(every_key[0], (HEAD_COUNT, 1)) < slow_share
    fast_rate = jnp.exp(jax.random.uniform(every_key[1], (HEAD_COUNT, 1), minval=jnp.log(0.02), maxval=jnp.log(0.05)))
    slow_rate = jnp.exp(jax.random.uniform(every_key[2], (HEAD_COUNT, 1), minval=jnp.log(0.1), maxval=jnp.log(0.56))) / TOKEN_COUNT
    block_count = TOKEN_COUNT // TOK_DEV
    block_factor = jnp.exp(jax.random.uniform(every_key[3], (HEAD_COUNT, block_count), minval=jnp.log(0.5), maxval=jnp.log(2.0)))
    block_factor = jnp.repeat(block_factor, TOK_DEV, axis=1)
    rough = jax.random.uniform(every_key[4], (HEAD_COUNT, TOKEN_COUNT), minval=0.5, maxval=2.0)
    decay_speed = jnp.where(sluggish_head, slow_rate, fast_rate * block_factor) * rough
    spike_position = jax.random.randint(every_key[5], (3,), 0, TOKEN_COUNT)
    spike_struck = jnp.any(jnp.arange(TOKEN_COUNT)[None, :] == spike_position[:, None], axis=0)
    spike_length = jnp.log(1.0 - jax.random.uniform(every_key[6], (HEAD_COUNT, 1), minval=0.2, maxval=0.4))
    spike_event = jnp.where(sluggish_head & spike_struck[None, :], spike_length, 0.0)
    return (spike_event - decay_speed).astype(jnp.float32)


def place_ends(values, rng, smallest, top_value):
    spot = [jax.random.randint(jax.random.fold_in(rng, axis), (), 0, length) for axis, length in enumerate(values.shape)]
    longest = values.shape.index(max(values.shape))
    neighbour = spot[:longest] + [(spot[longest] + 1) % values.shape[longest]] + spot[longest + 1:]
    return values.at[tuple(spot)].set(smallest).at[tuple(neighbour)].set(top_value)


def block_scale(key, dims, cuts, smallest, largest):
    loudness, own = 1.0, jax.random.fold_in(key, 6)
    for dim, shards_of in cuts:
        draws = jnp.exp(jax.random.uniform(jax.random.fold_in(own, dim), (shards_of,), jnp.float32, smallest / len(cuts), largest / len(cuts)))
        loudness = loudness * jnp.repeat(draws, dims[dim] // shards_of).reshape([-1 if axis == dim else 1 for axis in range(len(dims))])
    return loudness


def scatter_about(rng, extent, deviation, reach, shards=(), dtype=jnp.bfloat16):
    result = jax.random.normal(rng, extent, jnp.float32) * deviation
    if len(shards) > 0:
        result = block_scale(rng, extent, shards, -0.22, 0.18) * result
    return jnp.clip(result, min=-reach, max=reach).astype(dtype)


def setup_inputs(seed: int = 0) -> dict:
    key_of = jax.random.split(jax.random.key(seed), 8)
    return {
        "queries": scatter_about(key_of[0], (TOKEN_COUNT, HEAD_COUNT * DK), 0.16, 2.5, ((0, 8), (1, 4))),
        "keys": scatter_about(key_of[1], (TOKEN_COUNT, HEAD_COUNT * DK), 0.16, 2.5, ((0, 8), (1, 4))),
        "values": scatter_about(key_of[2], (TOKEN_COUNT, HEAD_COUNT * DV), 0.16, 2.5, ((0, 8), (1, 4))),
        "out_grad": scatter_about(key_of[3], (TOKEN_COUNT, HEAD_COUNT * DV), 0.16, 2.5, ((0, 8), (1, 4))),
        "log_gate": draw_log_gate(jax.random.fold_in(key_of[7], 71), 0),
        "level_weight": jnp.clip(jnp.exp(math.log(2.0) - 2.0794415 * jax.random.uniform(key_of[5], (NL, HEAD_COUNT, TOKEN_COUNT), jnp.float32) ** block_scale(key_of[5], (NL, HEAD_COUNT, TOKEN_COUNT), ((1, 4), (2, 8)), -0.2, 0.2)), 0.25, 2.0),
        "doc_start": place_ends((jax.random.randint(key_of[6], (TOKEN_COUNT,), 0, TOK_DEV * 8) < 1).astype(jnp.int32), jax.random.fold_in(key_of[6], 1), 0, 1),
    }


exact_mode = lax.Precision.HIGHEST

def group_sums(span_log, span_dead, width):
    groups = span_log.shape[0] // width
    logs = span_log.reshape(groups, width)
    deads = span_dead.reshape(groups, width)
    return (jnp.cumsum(logs, axis=1), jnp.cumsum(deads, axis=1), logs, deads)

def fenwick_pull(states, span_log, span_dead):
    total = states.shape[1]
    rows = states.shape[2]
    cols = states.shape[3]
    pieces = [jnp.zeros((total, rows, cols), jnp.float32)]
    for level in range(1, NL - 1):
        width = 2 ** (level - 1)
        groups = total // (2 * width)
        cum_log, cum_dead, logs, deads = group_sums(span_log, span_dead, 2 * width)
        source = states[level].reshape(groups, 2 * width, rows, cols)[:, :width]
        reach_log = cum_log[:, width - 1:2 * width - 1]
        reach_dead = cum_dead[:, width - 1:2 * width - 1]
        same = reach_dead[:, :, None] == cum_dead[:, None, :width]
        gap = reach_log[:, :, None] - cum_log[:, None, :width]
        weight = jnp.where(same, jnp.exp(jnp.where(same, gap, 0.0)), 0.0)
        pulled = jnp.einsum('gis,gsde->gide', weight, source, precision=exact_mode)
        pieces.append(jnp.concatenate([jnp.zeros_like(pulled), pulled], axis=1).reshape(total, rows, cols))
    width = 2 ** (NL - 2)
    groups = total // width
    cum_log, cum_dead, logs, deads = group_sums(span_log, span_dead, width)
    source = states[NL - 1].reshape(groups, width, rows, cols)
    end_same = cum_dead[:, -1:] == cum_dead
    end_weight = jnp.where(end_same, jnp.exp(jnp.where(end_same, cum_log[:, -1:] - cum_log, 0.0)), 0.0)
    block_total = jnp.einsum('gs,gsde->gde', end_weight, source, precision=exact_mode)
    block_decay = jnp.exp(cum_log[:, -1]) * (cum_dead[:, -1] == 0).astype(jnp.float32)

    def carry_step(carry, inputs):
        decay_now, total_now = inputs
        return (decay_now * carry + total_now, carry)
    _, entering = lax.scan(carry_step, jnp.zeros((rows, cols), jnp.float32), (block_decay, block_total))
    lead = jnp.exp(cum_log - logs) * (cum_dead - deads == 0).astype(jnp.float32)
    pieces.append((lead[:, :, None, None] * entering[:, None]).reshape(total, rows, cols))
    return jnp.stack(pieces)

def head_pass(query_h, key_h, value_h, grad_h, gate_h, weight_h, start_all):
    positions = jnp.arange(SPAN)
    causal = positions[:, None] >= positions[None, :]
    cum_gate = jnp.cumsum(gate_h, axis=1)
    cum_reset = jnp.cumsum(start_all, axis=1)
    valid = causal[None] & (cum_reset[:, :, None] == cum_reset[:, None, :])
    gap = cum_gate[:, :, None] - cum_gate[:, None, :]
    decay_in = jnp.where(valid, jnp.exp(jnp.where(valid, gap, 0.0)), 0.0)
    from_start = jnp.exp(cum_gate) * (cum_reset == 0).astype(jnp.float32)
    to_end = jnp.exp(cum_gate[:, -1:] - cum_gate) * (cum_reset == cum_reset[:, -1:]).astype(jnp.float32)
    span_log = cum_gate[:, -1]
    span_dead = (cum_reset[:, -1] > 0).astype(jnp.int32)
    query_f = query_h.astype(jnp.float32)
    key_f = key_h.astype(jnp.float32)
    value_f = value_h.astype(jnp.float32)
    grad_f = grad_h.astype(jnp.float32)
    scores = jnp.einsum('ctd,csd->cts', query_f, key_f, precision=exact_mode)
    grad_dot = jnp.einsum('cte,cse->cts', grad_f, value_f, precision=exact_mode)
    weighted = decay_in * weight_h[0][:, :, None]
    prob_mix = (weighted * scores).astype(jnp.bfloat16)
    grad_mix = (weighted * grad_dot).astype(jnp.bfloat16)
    intra = lax.optimization_barrier(jnp.sum(decay_in * scores * grad_dot, axis=2))
    end_col = to_end[:, :, None]
    span_state = jnp.einsum('csd,cse->cde', key_f * end_col, value_f, precision=exact_mode)
    forward = fenwick_pull(jnp.broadcast_to(span_state[None], (NL,) + span_state.shape), span_log, span_dead)
    query_state = jnp.einsum('ctd,lcde->lcte', query_f, forward, precision=exact_mode)
    lam_start = weight_h * from_start[None]
    out_in = jnp.einsum('lcte,lct->cte', query_state, lam_start, precision=exact_mode)
    level_in = jnp.einsum('lcte,cte->lct', query_state, grad_f, precision=exact_mode) * from_start[None]
    grad_weighted = lam_start[:, :, :, None] * grad_f[None]
    query_in = jnp.einsum('lcte,lcde->ctd', grad_weighted, forward, precision=exact_mode)
    out_loc = jnp.einsum('cts,cse->cte', prob_mix.astype(jnp.float32), value_f, precision=exact_mode)
    query_loc = jnp.einsum('cts,csd->ctd', grad_mix.astype(jnp.float32), key_f, precision=exact_mode)
    outputs = out_loc + out_in
    grad_query = (query_loc + query_in).astype(jnp.bfloat16)
    level_zero = (jnp.arange(NL) == 0).astype(jnp.float32)
    grad_level = level_in + level_zero[:, None, None] * intra[None]
    lam_query = lam_start[:, :, :, None] * query_f[None]
    back_local = jnp.einsum('lctd,cte->lcde', lam_query, grad_f, precision=exact_mode)
    backward = fenwick_pull(back_local[:, ::-1], span_log[::-1], span_dead[::-1])[:, ::-1]
    back_sum = lax.optimization_barrier(jnp.sum(backward, axis=0))
    key_in = jnp.einsum('cse,cde->csd', value_f * end_col, back_sum, precision=exact_mode)
    value_in = jnp.einsum('csd,cde->cse', key_f * end_col, back_sum, precision=exact_mode)
    key_loc = jnp.einsum('cts,ctd->csd', grad_mix.astype(jnp.float32), query_f, precision=exact_mode)
    value_loc = jnp.einsum('cts,cte->cse', prob_mix.astype(jnp.float32), grad_f, precision=exact_mode)
    value_grad = value_loc + value_in
    drift = lax.optimization_barrier(jnp.sum(grad_f * outputs, axis=2)) - lax.optimization_barrier(jnp.sum(value_f * value_grad, axis=2))
    return (grad_query, (key_loc + key_in).astype(jnp.bfloat16), value_grad.astype(jnp.bfloat16), grad_level, drift)

def reference(queries, keys, values, out_grad, log_gate, level_weight, doc_start):
    query_all = queries.reshape(SPANS, SPAN, HEAD_COUNT, DK).transpose(2, 0, 1, 3)
    key_all = keys.reshape(SPANS, SPAN, HEAD_COUNT, DK).transpose(2, 0, 1, 3)
    value_all = values.reshape(SPANS, SPAN, HEAD_COUNT, DV).transpose(2, 0, 1, 3)
    grad_all = out_grad.reshape(SPANS, SPAN, HEAD_COUNT, DV).transpose(2, 0, 1, 3)
    gate_all = log_gate.reshape(HEAD_COUNT, SPANS, SPAN)
    start_all = doc_start.reshape(SPANS, SPAN)
    weight_all = level_weight.reshape(NL, HEAD_COUNT, SPANS, SPAN).transpose(1, 0, 2, 3)

    def one_head(inputs):
        query_h, key_h, value_h, grad_h, gate_h, weight_h = inputs
        return head_pass(query_h, key_h, value_h, grad_h, gate_h, weight_h, start_all)
    results = lax.map(one_head, (query_all, key_all, value_all, grad_all, gate_all, weight_all))
    grad_query, grad_key, grad_value, grad_level, drift = results
    grad_queries = grad_query.transpose(1, 2, 0, 3).reshape(TOKEN_COUNT, HEAD_COUNT * DK)
    grad_keys = grad_key.transpose(1, 2, 0, 3).reshape(TOKEN_COUNT, HEAD_COUNT * DK)
    grad_values = grad_value.transpose(1, 2, 0, 3).reshape(TOKEN_COUNT, HEAD_COUNT * DV)
    grad_level_weight = grad_level.transpose(1, 0, 2, 3).reshape(NL, HEAD_COUNT, TOKEN_COUNT)
    drift_term = drift.reshape(HEAD_COUNT, TOKEN_COUNT)
    tail = lax.cumsum(drift_term, axis=1, reverse=True)
    squares = jnp.sum(tail * tail)
    factor = jnp.minimum(1.0, lax.rsqrt(squares / (HEAD_COUNT * TOKEN_COUNT) + 1e-06))
    return (grad_queries, grad_keys, grad_values, grad_level_weight, tail * factor)
```

```python
import functools

import jax
import jax.numpy as jnp
from jax import lax
from jax.experimental import pallas as pl
from jax.experimental.pallas import tpu as pltpu
from jax.sharding import PartitionSpec as P

SPAN = 64
F32 = jnp.float32
BF16 = jnp.bfloat16
NN = (((1,), (0,)), ((), ()))
NT = (((1,), (1,)), ((), ()))
TN = (((0,), (0,)), ((), ()))
MESH = pl.DeviceIdType.MESH


def dot(a, b, dims):
    return lax.dot_general(a, b, dims, preferred_element_type=F32)


def split(x):
    high = x.astype(BF16)
    return high, (x - high.astype(F32)).astype(BF16)


def dot_fine(x, b, dims):
    high, low = split(x)
    return dot(high, b, dims) + dot(low, b, dims)


def span_level(a, b, levels):
    return 0 if a == b else min(levels - 1, (a ^ b).bit_length())


def kernel(
    seq_count,
    head_count,
    q_ref,
    k_ref,
    v_ref,
    g_ref,
    lg_ref,
    lw_ref,
    ds_ref,
    gq_ref,
    gk_ref,
    gv_ref,
    gl_ref,
    gg_ref,
    cum_s,
    col_s,
    lead_s,
    tail_s,
    bias_s,
    vt_s,
    gt_s,
    vg_s,
    gq_s,
    gk_s,
    drift_s,
    coef_s,
    state_s,
    back_s,
    lvl,
    got_s,
    got_u,
    sum_s,
    sum_u,
    dec,
    got_dec,
    tot,
    sq,
    lvl_send,
    lvl_recv,
    fwd_send,
    fwd_recv,
    s_send,
    s_recv,
    u_send,
    u_recv,
    d_send,
    d_recv,
    t_send,
    t_recv,
    q_send,
    q_recv,
):
    tok = q_ref.shape[0]
    heads = lg_ref.shape[0]
    levels = lw_ref.shape[0]
    dk = q_ref.shape[1] // heads
    dv = v_ref.shape[1] // heads
    group = dk // dv
    pairs = heads // group
    spans = tok // SPAN
    span_bits = spans.bit_length() - 1
    bits = seq_count.bit_length() - 1
    half = heads // 2
    cross = [min(span_bits + 1 + b, levels - 1) for b in range(bits)]
    slots = sorted(set(cross))
    place = lax.axis_index("seq")
    row = lax.axis_index("head")
    bit = [(place // (1 << b)) % 2 for b in range(bits)]
    peer = [place + (1 - 2 * bit[b]) * (1 << b) for b in range(bits)]
    want_s = [(place // (2 << b)) != (seq_count // (2 << b)) - 1 for b in range(bits)]
    mine = bit[0] * half
    theirs = (1 - bit[0]) * half

    barrier = pltpu.get_barrier_semaphore()
    for o in range(1, seq_count):
        pl.semaphore_signal(
            barrier, inc=1, device_id={"seq": (place + o) % seq_count}, device_id_type=MESH
        )
    for o in range(1, head_count):
        pl.semaphore_signal(
            barrier, inc=1, device_id={"head": (row + o) % head_count}, device_id_type=MESH
        )

    rows_i = lax.broadcasted_iota(jnp.int32, (tok, tok), 0)
    cols_i = lax.broadcasted_iota(jnp.int32, (tok, tok), 1)
    tri = (rows_i <= cols_i).astype(F32)
    starts = jnp.broadcast_to(ds_ref[...].astype(F32), (8, tok))
    both = jnp.concatenate([lg_ref[...], starts], axis=0)
    cum_all = lax.dot_general(
        both, tri, NN, precision=lax.Precision.HIGHEST, preferred_element_type=F32
    )
    cum_t = jnp.transpose(cum_all)
    cum = cum_all[:heads]
    reset = cum_all[heads : heads + 1]
    reset_col = cum_t[:, heads : heads + 1]
    bias_s[...] = jnp.where((rows_i <= cols_i) & (reset == reset_col), 0.0, -1e30)
    end = cum[:, tok - 1 : tok]
    reset_end = reset[:, tok - 1 : tok]
    cum_s[...] = cum
    lead_s[...] = jnp.where(reset == 0, jnp.exp(cum), 0.0)
    tail_s[...] = jnp.where(reset == reset_end, jnp.exp(end - cum), 0.0)
    dec[0] = jnp.broadcast_to(jnp.where(reset_end == 0, jnp.exp(end), 0.0), (heads, dk))
    for h in range(heads):
        col_s[h] = jnp.broadcast_to(cum_t[:, h : h + 1], (tok, tok))

    def states(p, _):
        lanes = pl.ds(pl.multiple_of(p * dk, dk), dk)
        vt = jnp.transpose(v_ref[:, lanes].astype(F32))
        gt = jnp.transpose(g_ref[:, lanes].astype(F32))
        vt_s[p] = vt.astype(BF16)
        gt_s[p] = gt.astype(BF16)
        for i in range(group):
            h = p * group + i
            wide = pl.ds(pl.multiple_of(h * dk, dk), dk)
            part = slice(i * dv, (i + 1) * dv)
            tail = tail_s[pl.ds(h, 1), :]
            lead = lead_s[pl.ds(h, 1), :]
            state_s[h] = dot_fine(vt[part] * tail, k_ref[:, wide], NN)
            gw = jnp.concatenate(
                [gt[part] * (lead * lw_ref[l, pl.ds(h, 1), :]) for l in slots], axis=0
            )
            back = dot_fine(gw, q_ref[:, wide], NN)
            for n in range(len(slots)):
                back_s[n, h] = back[n * dv : (n + 1) * dv]
        return 0

    lax.fori_loop(0, pairs, states, 0, unroll=2)
    pl.semaphore_wait(barrier, seq_count - 1 + head_count - 1)

    def slot(b):
        return slots.index(cross[b])

    def remote(src, dst, send, recv, b):
        return pltpu.make_async_remote_copy(
            src_ref=src,
            dst_ref=dst,
            send_sem=send,
            recv_sem=recv,
            device_id={"seq": peer[b]},
            device_id_type=MESH,
        )

    own = pl.ds(mine, half)
    other = pl.ds(theirs, half)

    def u_copy(b, j):
        src = back_s.at[slot(j), other] if b == 0 else sum_u.at[b, j]
        return remote(src, got_u.at[b, j], u_send.at[b, j], u_recv.at[b, j], b)

    def s_copy(b):
        src = state_s.at[other] if b == 0 else sum_s.at[b]
        return remote(src, got_s.at[b], s_send.at[b], s_recv.at[b], b)

    def d_copy(b):
        return remote(dec.at[b], got_dec.at[b], d_send.at[b], d_recv.at[b], b)

    def level_copy(b, low):
        if b == 0:
            src = state_s if low else back_s.at[slot(0)]
            return [
                remote(src.at[part], lvl.at[0, part], lvl_send.at[0, n], lvl_recv.at[0, n], 0)
                for n, part in enumerate((other, own))
            ]
        src = sum_s.at[b] if low else sum_u.at[b, b]
        return [remote(src, lvl.at[b, own], lvl_send.at[b, 0], lvl_recv.at[b, 0], b)]

    def level_wait(b, n):
        part = other if n == 1 else own
        return remote(
            lvl.at[b, part], lvl.at[b, part], lvl_send.at[b, n], lvl_recv.at[b, n], b
        )

    def forward_copy(b, part):
        return remote(lvl.at[b, part], lvl.at[b, part], fwd_send.at[b], fwd_recv.at[b], 0)

    def land(b):
        up_summed = (bit[b] == 1) & want_s[b]

        @pl.when(jnp.logical_not(up_summed))
        def _():
            level_wait(b, 0).wait_recv()

        if b > 0:
            forward_copy(b, own).start()

    def begin(b):
        d_copy(b).start()

        early = 0 if b in (0, bits - 1) else 1

        @pl.when((bit[b] == 0) & (want_s[b] | (early == 0)))
        def _():
            for c in level_copy(b, True):
                c.start()

        if b < bits - 1:

            @pl.when((bit[b] == 1) & want_s[b])
            def _():
                s_copy(b).start()

            for j in range(b + 1, bits):

                @pl.when(bit[j] == 1)
                def _(j=j):
                    u_copy(b, j).start()

        if early == 0:

            @pl.when(bit[b] == 1)
            def _():
                for c in level_copy(b, False):
                    c.start()

    def begin_late(b):
        if b in (0, bits - 1):
            return

        @pl.when((bit[b] == 0) & jnp.logical_not(want_s[b]))
        def _():
            for c in level_copy(b, True):
                c.start()

        @pl.when(bit[b] == 1)
        def _():
            for c in level_copy(b, False):
                c.start()

    def join(b):
        d_copy(b).wait_recv()
        up = bit[b].astype(F32)
        got = got_dec[b]
        now = dec[b]
        dec[b + 1] = got * now
        if b == bits - 1:
            return
        base_s = state_s.at[own] if b == 0 else sum_s.at[b]

        @pl.when(want_s[b])
        def _():
            @pl.when(bit[b] == 1)
            def _():
                level_wait(b, 0).wait_recv()

                def body(i, _):
                    d = dec[b, pl.ds(mine + i, 1), :]
                    sum_s[b + 1, i] = d * lvl[b, mine + i] + base_s[i]
                    return 0

                lax.fori_loop(0, half, body, 0, unroll=True)

            @pl.when(bit[b] == 0)
            def _():
                s_copy(b).wait_recv()

                def body(i, _):
                    d = got_dec[b, pl.ds(mine + i, 1), :]
                    sum_s[b + 1, i] = d * base_s[i] + got_s[b, i]
                    return 0

                lax.fori_loop(0, half, body, 0, unroll=True)

        for j in range(b + 1, bits):
            base_u = back_s.at[slot(j), own] if b == 0 else sum_u.at[b, j]

            @pl.when(bit[j] == 1)
            def _(j=j, base_u=base_u):
                u_copy(b, j).wait_recv()

                def body(i, _):
                    d0 = dec[b, pl.ds(mine + i, 1), :]
                    d1 = got_dec[b, pl.ds(mine + i, 1), :]
                    a = up * d1 + (1.0 - up)
                    c = (1.0 - up) * d0 + up
                    sum_u[b + 1, j, i] = a * base_u[i] + c * got_u[b, j, i]
                    return 0

                lax.fori_loop(0, half, body, 0, unroll=True)

    span_of = lax.broadcasted_iota(jnp.int32, (1, tok), 1) // SPAN

    def local(p, _):
        vt = vt_s[p]
        gt = gt_s[p]
        lanes = pl.ds(pl.multiple_of(p * dk, dk), dk)
        v_blk = v_ref[:, lanes]
        for i in range(group):
            h = p * group + i
            wide = pl.ds(pl.multiple_of(h * dk, dk), dk)
            part = slice(i * dv, (i + 1) * dv)
            q = q_ref[:, wide]
            k = k_ref[:, wide]
            score = dot(k, q, NT)
            pair = dot(v_blk[:, part], gt[part], NN)
            decay = jnp.exp((cum_s[pl.ds(h, 1), :] - col_s[h]) + bias_s[...])
            seen = decay * score
            both_p = seen * pair
            gains = [lw_ref[l, pl.ds(h, 1), :] for l in range(span_bits + 1)]
            level_rows = [jnp.zeros((1, tok), F32) for _ in range(span_bits + 1)]
            mixed, graded = [], []
            for cs in range(spans):
                rows = slice(cs * SPAN, (cs + 1) * SPAN)
                total = jnp.sum(both_p[rows], axis=0, keepdims=True)
                gain = jnp.zeros((1, tok), F32)
                for ct in range(cs, spans):
                    l = span_level(cs, ct, levels)
                    hit = span_of == ct
                    gain = jnp.where(hit, gains[l], gain)
                    level_rows[l] = level_rows[l] + jnp.where(hit, total, 0.0)
                mixed.append(seen[rows] * gain)
                graded.append(decay[rows] * gain * pair[rows])
            mix = jnp.concatenate(mixed, axis=0).astype(BF16)
            grade = jnp.concatenate(graded, axis=0).astype(BF16)
            for l in range(span_bits + 1):
                gl_ref[l, pl.ds(h, 1), :] = level_rows[l]
            drift_s[pl.ds(h, 1), :] = jnp.sum(mix.astype(F32) * pair, axis=0, keepdims=True)
            vg_s[p, part] = dot(gt[part], mix, NT)
            gk_s[h] = dot(grade, q, NN)
            gq_s[h] = dot(grade, k, TN)
        return 0

    begin(0)
    lax.fori_loop(0, pairs // 4, local, 0, unroll=2)
    join(0)
    if bits > 1:
        begin(1)
    lax.fori_loop(pairs // 4, pairs, local, 0, unroll=2)
    for b in range(1, bits):
        join(b)
        if b + 1 < bits:
            begin(b + 1)
        begin_late(b)
        land(b - 1)
    land(bits - 1)

    inner_f = jnp.ones((heads, dk), F32)
    inner_b = jnp.ones((heads, dk), F32)
    for b in range(bits):
        up = bit[b].astype(F32)
        got = got_dec[b]
        coef_s[0, b] = inner_f * up
        coef_s[1, b] = inner_b * (1.0 - up)
        inner_f = inner_f * (up * got + (1.0 - up))
        inner_b = inner_b * ((1.0 - up) * got + up)
    level_wait(0, 1).wait_recv()
    for b in range(1, bits):
        forward_copy(b, other).wait_recv()

    def finish(p, _):
        lanes = pl.ds(pl.multiple_of(p * dk, dk), dk)
        vt = vt_s[p].astype(F32)
        gt = gt_s[p].astype(F32)
        vg_all = []
        for i in range(group):
            h = p * group + i
            wide = pl.ds(pl.multiple_of(h * dk, dk), dk)
            part = slice(i * dv, (i + 1) * dv)
            q = q_ref[:, wide]
            k = k_ref[:, wide]
            tail = tail_s[pl.ds(h, 1), :]
            lead = lead_s[pl.ds(h, 1), :]
            blocks = [lvl[b, h] for b in range(bits)]
            entering = []
            for n in range(len(slots)):
                terms = [
                    coef_s[0, b, pl.ds(h, 1), :] * blocks[b] for b in range(bits) if slot(b) == n
                ]
                entering.append(functools.reduce(jnp.add, terms))
            entering = jnp.concatenate(entering, axis=0)
            after = functools.reduce(
                jnp.add, [coef_s[1, b, pl.ds(h, 1), :] * blocks[b] for b in range(bits)]
            )
            e_high, e_low = split(entering)
            seen = dot(e_high, q, NT) + dot(e_low, q, NT)
            drift = drift_s[pl.ds(h, 1), :]
            gws = []
            for n, l in enumerate(slots):
                gain = lw_ref[l, pl.ds(h, 1), :]
                level = lead * jnp.sum(
                    seen[n * dv : (n + 1) * dv] * gt[part], axis=0, keepdims=True
                )
                gl_ref[l, pl.ds(h, 1), :] = level
                drift = drift + gain * level
                gws.append(gt[part] * (lead * gain))
            gw, gw_low = split(jnp.concatenate(gws, axis=0))
            gq_in = dot(gw, e_high, TN) + dot(gw, e_low, TN) + dot(gw_low, e_high, TN)
            gq_ref[:, wide] = (gq_s[h] + gq_in).astype(BF16)
            a_high, a_low = split(after)
            tv, tv_low = split(vt[part] * tail)
            gk_in = dot(tv, a_high, TN) + dot(tv, a_low, TN) + dot(tv_low, a_high, TN)
            gk_ref[:, wide] = (gk_s[h] + gk_in).astype(BF16)
            vg = vg_s[p, part] + tail * (dot(a_high, k, NT) + dot(a_low, k, NT))
            drift_s[pl.ds(h, 1), :] = drift - jnp.sum(vg * vt[part], axis=0, keepdims=True)
            vg_all.append(vg)
        gv_ref[:, lanes] = jnp.transpose(jnp.concatenate(vg_all, axis=0)).astype(BF16)
        return 0

    lax.fori_loop(0, pairs, finish, 0, unroll=2)
    for l in range(levels):
        if l > span_bits and l not in slots:
            gl_ref[l] = jnp.zeros((heads, tok), F32)

    later = (rows_i >= cols_i).astype(F32)
    local_tail = lax.dot_general(
        drift_s[...], later, NN, precision=lax.Precision.HIGHEST, preferred_element_type=F32
    )
    lane = lax.broadcasted_iota(jnp.int32, (heads, tok), 1)
    first = local_tail[:, 0:1]
    plain = jnp.sum(local_tail, axis=1, keepdims=True)
    square = jnp.sum(local_tail * local_tail, axis=1, keepdims=True)
    tot[place] = jnp.where(lane == 0, first, jnp.where(lane == 1, plain, square))

    def tot_copy(o, slot_at):
        return pltpu.make_async_remote_copy(
            src_ref=tot.at[place],
            dst_ref=tot.at[slot_at],
            send_sem=t_send.at[o],
            recv_sem=t_recv.at[slot_at],
            device_id={"seq": (place + o) % seq_count},
            device_id_type=MESH,
        )

    for o in range(1, seq_count):
        tot_copy(o, place).start()
    for o in range(1, seq_count):
        tot_copy(o, (place + o) % seq_count).wait_recv()
    after_total = jnp.zeros((heads, 1), F32)
    my_later = jnp.zeros((heads, 1), F32)
    energy = jnp.zeros((heads, 1), F32)
    for d in reversed(range(seq_count)):
        piece = tot[d]
        my_later = my_later + jnp.where(place == d, 1.0, 0.0) * after_total
        energy = energy + (
            piece[:, 2:3] + after_total * (2.0 * piece[:, 1:2] + tok * after_total)
        )
        after_total = after_total + piece[:, 0:1]
    energy = jnp.sum(jnp.broadcast_to(energy, (heads, dk)), axis=0, keepdims=True)
    sq[row] = jnp.broadcast_to(energy, (8, dk))

    def sq_copy(o, slot_at):
        return pltpu.make_async_remote_copy(
            src_ref=sq.at[row],
            dst_ref=sq.at[slot_at],
            send_sem=q_send.at[o],
            recv_sem=q_recv.at[slot_at],
            device_id={"head": (row + o) % head_count},
            device_id_type=MESH,
        )

    for o in range(1, head_count):
        sq_copy(o, row).start()
    for o in range(1, head_count):
        sq_copy(o, (row + o) % head_count).wait_recv()
    whole = sq[0]
    for r in range(1, head_count):
        whole = whole + sq[r]
    count = heads * tok * seq_count * head_count
    factor = jnp.minimum(1.0, lax.rsqrt(whole[0:1] / count + 1e-6))
    gg_ref[...] = (local_tail + my_later) * factor

    for b in range(bits):
        d_copy(b).wait_send()
        for n in range(2 if b == 0 else 1):
            level_wait(b, n).wait_send()
        if b > 0:
            forward_copy(b, own).wait_send()
        if b < bits - 1:

            @pl.when((bit[b] == 1) & want_s[b])
            def _(b=b):
                s_copy(b).wait_send()

            for j in range(b + 1, bits):

                @pl.when(bit[j] == 1)
                def _(b=b, j=j):
                    u_copy(b, j).wait_send()

    for o in range(1, seq_count):
        tot_copy(o, place).wait_send()
    for o in range(1, head_count):
        sq_copy(o, row).wait_send()


def write_out(count, *refs):
    sems = refs[-1]
    copies = [
        pltpu.make_async_copy(refs[i], refs[count + i], sems.at[i]) for i in range(count)
    ]
    for c in copies:
        c.start()
    for c in copies:
        c.wait()


def shards(seq_count, head_count, queries, keys, values, out_grad, log_gate, level_weight, doc_start):
    tok = queries.shape[0]
    heads = log_gate.shape[0]
    levels = level_weight.shape[0]
    dk = queries.shape[1] // heads
    dv = values.shape[1] // heads
    group = dk // dv
    pairs = heads // group
    bits = seq_count.bit_length() - 1
    half = heads // 2
    span_bits = (tok // SPAN).bit_length() - 1
    slots = len({min(span_bits + 1 + b, levels - 1) for b in range(bits)})
    dma = pltpu.SemaphoreType.DMA
    vmem = pltpu.VMEM
    block = (dv, dk)
    scratch = [
        vmem((heads, tok), F32),
        vmem((heads, tok, tok), F32),
        vmem((heads, tok), F32),
        vmem((heads, tok), F32),
        vmem((tok, tok), F32),
        vmem((pairs, group * dv, tok), BF16),
        vmem((pairs, group * dv, tok), BF16),
        vmem((pairs, group * dv, tok), F32),
        vmem((heads, tok, dk), F32),
        vmem((heads, tok, dk), F32),
        vmem((heads, tok), F32),
        vmem((2, bits, heads, dk), F32),
        vmem((heads,) + block, F32),
        vmem((slots, heads) + block, F32),
        vmem((bits, heads) + block, F32),
        vmem((bits, half) + block, F32),
        vmem((bits, bits, half) + block, F32),
        vmem((bits, half) + block, F32),
        vmem((bits, bits, half) + block, F32),
        vmem((bits + 1, heads, dk), F32),
        vmem((bits, heads, dk), F32),
        vmem((seq_count, heads, tok), F32),
        vmem((head_count, 8, dk), F32),
        dma((bits, 2)),
        dma((bits, 2)),
        dma((bits,)),
        dma((bits,)),
        dma((bits,)),
        dma((bits,)),
        dma((bits, bits)),
        dma((bits, bits)),
        dma((bits,)),
        dma((bits,)),
        dma((seq_count,)),
        dma((seq_count,)),
        dma((head_count,)),
        dma((head_count,)),
    ]
    spec = pl.BlockSpec(memory_space=pltpu.VMEM)
    outs = [
        (queries.shape, BF16),
        (keys.shape, BF16),
        (values.shape, BF16),
        (level_weight.shape, F32),
        (log_gate.shape, F32),
    ]
    results = pl.pallas_call(
        functools.partial(kernel, seq_count, head_count),
        out_shape=tuple(vmem(shape, dtype) for shape, dtype in outs),
        in_specs=[spec] * 7,
        out_specs=(spec,) * 5,
        scratch_shapes=scratch,
        compiler_params=pltpu.CompilerParams(collective_id=0, has_side_effects=True),
    )(queries, keys, values, out_grad, log_gate, level_weight, doc_start.reshape(1, tok))
    count = len(outs)
    return pl.pallas_call(
        functools.partial(write_out, count),
        out_shape=tuple(jax.ShapeDtypeStruct(shape, dtype) for shape, dtype in outs),
        in_specs=[spec] * count,
        out_specs=(pl.BlockSpec(memory_space=pltpu.HBM),) * count,
        scratch_shapes=[dma((count,))],
    )(*[pltpu.with_memory_space_constraint(r, pltpu.VMEM) for r in results])


def solution(mesh):
    return jax.shard_map(
        functools.partial(shards, mesh.shape["seq"], mesh.shape["head"]),
        mesh=mesh,
        in_specs=(
            P("seq", "head"),
            P("seq", "head"),
            P("seq", "head"),
            P("seq", "head"),
            P("head", "seq"),
            P(None, "head", "seq"),
            P("seq"),
        ),
        out_specs=(
            P("seq", "head"),
            P("seq", "head"),
            P("seq", "head"),
            P(None, "head", "seq"),
            P("head", "seq"),
        ),
        check_vma=False,
    )
```

```python
import functools

import jax
import jax.numpy as jnp
from jax import lax
from jax.experimental import pallas as pl
from jax.experimental.pallas import tpu as pltpu
from jax.sharding import PartitionSpec as P

SPAN = 64
F32 = jnp.float32
BF16 = jnp.bfloat16
NN = (((1,), (0,)), ((), ()))
NT = (((1,), (1,)), ((), ()))
TN = (((0,), (0,)), ((), ()))
MESH = pl.DeviceIdType.MESH


def dot(a, b, dims):
    return lax.dot_general(a, b, dims, preferred_element_type=F32)


def split(x):
    high = x.astype(BF16)
    return high, (x - high.astype(F32)).astype(BF16)


def dot_fine(x, b, dims):
    high, low = split(x)
    return dot(high, b, dims) + dot(low, b, dims)


def span_level(a, b, levels):
    return 0 if a == b else min(levels - 1, (a ^ b).bit_length())


def kernel(
    seq_count,
    head_count,
    q_ref,
    k_ref,
    v_ref,
    g_ref,
    lg_ref,
    lw_ref,
    ds_ref,
    gq_ref,
    gk_ref,
    gv_ref,
    gl_ref,
    gg_ref,
    cum_s,
    col_s,
    lead_s,
    tail_s,
    bias_s,
    vt_s,
    gt_s,
    vg_s,
    gq_s,
    gk_s,
    drift_s,
    coef_s,
    state_s,
    back_s,
    lvl,
    got_s,
    got_u,
    sum_s,
    sum_u,
    dec,
    got_dec,
    tot,
    sq,
    lvl_send,
    lvl_recv,
    fwd_send,
    fwd_recv,
    s_send,
    s_recv,
    u_send,
    u_recv,
    d_send,
    d_recv,
    t_send,
    t_recv,
    q_send,
    q_recv,
):
    tok = q_ref.shape[0]
    heads = lg_ref.shape[0]
    levels = lw_ref.shape[0]
    dk = q_ref.shape[1] // heads
    dv = v_ref.shape[1] // heads
    group = dk // dv
    pairs = heads // group
    spans = tok // SPAN
    span_bits = spans.bit_length() - 1
    bits = seq_count.bit_length() - 1
    half = heads // 2
    cross = [min(span_bits + 1 + b, levels - 1) for b in range(bits)]
    slots = sorted(set(cross))
    place = lax.axis_index("seq")
    row = lax.axis_index("head")
    bit = [(place // (1 << b)) % 2 for b in range(bits)]
    peer = [place + (1 - 2 * bit[b]) * (1 << b) for b in range(bits)]
    want_s = [(place // (2 << b)) != (seq_count // (2 << b)) - 1 for b in range(bits)]
    mine = bit[0] * half
    theirs = (1 - bit[0]) * half

    barrier = pltpu.get_barrier_semaphore()
    for o in range(1, seq_count):
        pl.semaphore_signal(
            barrier, inc=1, device_id={"seq": (place + o) % seq_count}, device_id_type=MESH
        )
    for o in range(1, head_count):
        pl.semaphore_signal(
            barrier, inc=1, device_id={"head": (row + o) % head_count}, device_id_type=MESH
        )

    rows_i = lax.broadcasted_iota(jnp.int32, (tok, tok), 0)
    cols_i = lax.broadcasted_iota(jnp.int32, (tok, tok), 1)
    tri = (rows_i <= cols_i).astype(F32)
    starts = jnp.broadcast_to(ds_ref[...].astype(F32), (8, tok))
    both = jnp.concatenate([lg_ref[...], starts], axis=0)
    cum_all = lax.dot_general(
        both, tri, NN, precision=lax.Precision.HIGHEST, preferred_element_type=F32
    )
    cum_t = jnp.transpose(cum_all)
    cum = cum_all[:heads]
    reset = cum_all[heads : heads + 1]
    reset_col = cum_t[:, heads : heads + 1]
    bias_s[...] = jnp.where((rows_i <= cols_i) & (reset == reset_col), 0.0, -1e30)
    end = cum[:, tok - 1 : tok]
    reset_end = reset[:, tok - 1 : tok]
    cum_s[...] = cum
    lead_s[...] = jnp.where(reset == 0, jnp.exp(cum), 0.0)
    tail_s[...] = jnp.where(reset == reset_end, jnp.exp(end - cum), 0.0)
    dec[0] = jnp.broadcast_to(jnp.where(reset_end == 0, jnp.exp(end), 0.0), (heads, dk))
    for h in range(heads):
        col_s[h] = jnp.broadcast_to(cum_t[:, h : h + 1], (tok, tok))

    def states(p, _):
        lanes = pl.ds(pl.multiple_of(p * dk, dk), dk)
        vt = jnp.transpose(v_ref[:, lanes].astype(F32))
        gt = jnp.transpose(g_ref[:, lanes].astype(F32))
        vt_s[p] = vt.astype(BF16)
        gt_s[p] = gt.astype(BF16)
        for i in range(group):
            h = p * group + i
            wide = pl.ds(pl.multiple_of(h * dk, dk), dk)
            part = slice(i * dv, (i + 1) * dv)
            tail = tail_s[pl.ds(h, 1), :]
            lead = lead_s[pl.ds(h, 1), :]
            state_s[h] = dot_fine(vt[part] * tail, k_ref[:, wide], NN)
            gw = jnp.concatenate(
                [gt[part] * (lead * lw_ref[l, pl.ds(h, 1), :]) for l in slots], axis=0
            )
            back = dot_fine(gw, q_ref[:, wide], NN)
            for n in range(len(slots)):
                back_s[n, h] = back[n * dv : (n + 1) * dv]
        return 0

    lax.fori_loop(0, pairs, states, 0, unroll=2)
    pl.semaphore_wait(barrier, seq_count - 1 + head_count - 1)

    def slot(b):
        return slots.index(cross[b])

    def remote(src, dst, send, recv, b):
        return pltpu.make_async_remote_copy(
            src_ref=src,
            dst_ref=dst,
            send_sem=send,
            recv_sem=recv,
            device_id={"seq": peer[b]},
            device_id_type=MESH,
        )

    own = pl.ds(mine, half)
    other = pl.ds(theirs, half)

    def u_copy(b, j):
        src = back_s.at[slot(j), other] if b == 0 else sum_u.at[b, j]
        return remote(src, got_u.at[b, j], u_send.at[b, j], u_recv.at[b, j], b)

    def s_copy(b):
        src = state_s.at[other] if b == 0 else sum_s.at[b]
        return remote(src, got_s.at[b], s_send.at[b], s_recv.at[b], b)

    def d_copy(b):
        return remote(dec.at[b], got_dec.at[b], d_send.at[b], d_recv.at[b], b)

    def level_copy(b, low):
        if b == 0:
            src = state_s if low else back_s.at[slot(0)]
            return [
                remote(src.at[part], lvl.at[0, part], lvl_send.at[0, n], lvl_recv.at[0, n], 0)
                for n, part in enumerate((other, own))
            ]
        src = sum_s.at[b] if low else sum_u.at[b, b]
        return [remote(src, lvl.at[b, own], lvl_send.at[b, 0], lvl_recv.at[b, 0], b)]

    def level_wait(b, n):
        part = other if n == 1 else own
        return remote(
            lvl.at[b, part], lvl.at[b, part], lvl_send.at[b, n], lvl_recv.at[b, n], b
        )

    def forward_copy(b, part):
        return remote(lvl.at[b, part], lvl.at[b, part], fwd_send.at[b], fwd_recv.at[b], 0)

    def land(b):
        up_summed = (bit[b] == 1) & want_s[b]

        @pl.when(jnp.logical_not(up_summed))
        def _():
            level_wait(b, 0).wait_recv()

        if b > 0:
            forward_copy(b, own).start()

    def begin(b):
        d_copy(b).start()

        early = 0 if b in (0, bits - 1) else 1

        @pl.when((bit[b] == 0) & (want_s[b] | (early == 0)))
        def _():
            for c in level_copy(b, True):
                c.start()

        if b < bits - 1:

            @pl.when((bit[b] == 1) & want_s[b])
            def _():
                s_copy(b).start()

            for j in range(b + 1, bits):

                @pl.when(bit[j] == 1)
                def _(j=j):
                    u_copy(b, j).start()

        if early == 0:

            @pl.when(bit[b] == 1)
            def _():
                for c in level_copy(b, False):
                    c.start()

    def begin_late(b):
        if b in (0, bits - 1):
            return

        @pl.when((bit[b] == 0) & jnp.logical_not(want_s[b]))
        def _():
            for c in level_copy(b, True):
                c.start()

        @pl.when(bit[b] == 1)
        def _():
            for c in level_copy(b, False):
                c.start()

    def join(b):
        d_copy(b).wait_recv()
        up = bit[b].astype(F32)
        got = got_dec[b]
        now = dec[b]
        dec[b + 1] = got * now
        if b == bits - 1:
            return
        base_s = state_s.at[own] if b == 0 else sum_s.at[b]

        @pl.when(want_s[b])
        def _():
            @pl.when(bit[b] == 1)
            def _():
                level_wait(b, 0).wait_recv()

                def body(i, _):
                    d = dec[b, pl.ds(mine + i, 1), :]
                    sum_s[b + 1, i] = d * lvl[b, mine + i] + base_s[i]
                    return 0

                lax.fori_loop(0, half, body, 0, unroll=True)

            @pl.when(bit[b] == 0)
            def _():
                s_copy(b).wait_recv()

                def body(i, _):
                    d = got_dec[b, pl.ds(mine + i, 1), :]
                    sum_s[b + 1, i] = d * base_s[i] + got_s[b, i]
                    return 0

                lax.fori_loop(0, half, body, 0, unroll=True)

        for j in range(b + 1, bits):
            base_u = back_s.at[slot(j), own] if b == 0 else sum_u.at[b, j]

            @pl.when(bit[j] == 1)
            def _(j=j, base_u=base_u):
                u_copy(b, j).wait_recv()

                def body(i, _):
                    d0 = dec[b, pl.ds(mine + i, 1), :]
                    d1 = got_dec[b, pl.ds(mine + i, 1), :]
                    a = up * d1 + (1.0 - up)
                    c = (1.0 - up) * d0 + up
                    sum_u[b + 1, j, i] = a * base_u[i] + c * got_u[b, j, i]
                    return 0

                lax.fori_loop(0, half, body, 0, unroll=True)

    span_of = lax.broadcasted_iota(jnp.int32, (1, tok), 1) // SPAN

    def local(p, _):
        vt = vt_s[p]
        gt = gt_s[p]
        lanes = pl.ds(pl.multiple_of(p * dk, dk), dk)
        v_blk = v_ref[:, lanes]
        for i in range(group):
            h = p * group + i
            wide = pl.ds(pl.multiple_of(h * dk, dk), dk)
            part = slice(i * dv, (i + 1) * dv)
            q = q_ref[:, wide]
            k = k_ref[:, wide]
            score = dot(k, q, NT)
            pair = dot(v_blk[:, part], gt[part], NN)
            decay = jnp.exp((cum_s[pl.ds(h, 1), :] - col_s[h]) + bias_s[...])
            seen = decay * score
            both_p = seen * pair
            gains = [lw_ref[l, pl.ds(h, 1), :] for l in range(span_bits + 1)]
            level_rows = [jnp.zeros((1, tok), F32) for _ in range(span_bits + 1)]
            mixed, graded = [], []
            for cs in range(spans):
                rows = slice(cs * SPAN, (cs + 1) * SPAN)
                total = jnp.sum(both_p[rows], axis=0, keepdims=True)
                gain = jnp.zeros((1, tok), F32)
                for ct in range(cs, spans):
                    l = span_level(cs, ct, levels)
                    hit = span_of == ct
                    gain = jnp.where(hit, gains[l], gain)
                    level_rows[l] = level_rows[l] + jnp.where(hit, total, 0.0)
                mixed.append(seen[rows] * gain)
                graded.append(decay[rows] * gain * pair[rows])
            mix = jnp.concatenate(mixed, axis=0).astype(BF16)
            grade = jnp.concatenate(graded, axis=0).astype(BF16)
            for l in range(span_bits + 1):
                gl_ref[l, pl.ds(h, 1), :] = level_rows[l]
            drift_s[pl.ds(h, 1), :] = jnp.sum(mix.astype(F32) * pair, axis=0, keepdims=True)
            vg_s[p, part] = dot(gt[part], mix, NT)
            gk_s[h] = dot(grade, q, NN)
            gq_s[h] = dot(grade, k, TN)
        return 0

    begin(0)
    lax.fori_loop(0, pairs // 4, local, 0, unroll=2)
    join(0)
    if bits > 1:
        begin(1)
    lax.fori_loop(pairs // 4, pairs, local, 0, unroll=2)
    for b in range(1, bits):
        join(b)
        if b + 1 < bits:
            begin(b + 1)
        begin_late(b)
        land(b - 1)
    land(bits - 1)

    inner_f = jnp.ones((heads, dk), F32)
    inner_b = jnp.ones((heads, dk), F32)
    for b in range(bits):
        up = bit[b].astype(F32)
        got = got_dec[b]
        coef_s[0, b] = inner_f * up
        coef_s[1, b] = inner_b * (1.0 - up)
        inner_f = inner_f * (up * got + (1.0 - up))
        inner_b = inner_b * ((1.0 - up) * got + up)
    level_wait(0, 1).wait_recv()
    for b in range(1, bits):
        forward_copy(b, other).wait_recv()

    def finish(p, _):
        lanes = pl.ds(pl.multiple_of(p * dk, dk), dk)
        vt = vt_s[p].astype(F32)
        gt = gt_s[p].astype(F32)
        vg_all = []
        for i in range(group):
            h = p * group + i
            wide = pl.ds(pl.multiple_of(h * dk, dk), dk)
            part = slice(i * dv, (i + 1) * dv)
            q = q_ref[:, wide]
            k = k_ref[:, wide]
            tail = tail_s[pl.ds(h, 1), :]
            lead = lead_s[pl.ds(h, 1), :]
            blocks = [lvl[b, h] for b in range(bits)]
            entering = []
            for n in range(len(slots)):
                terms = [
                    coef_s[0, b, pl.ds(h, 1), :] * blocks[b] for b in range(bits) if slot(b) == n
                ]
                entering.append(functools.reduce(jnp.add, terms))
            entering = jnp.concatenate(entering, axis=0)
            after = functools.reduce(
                jnp.add, [coef_s[1, b, pl.ds(h, 1), :] * blocks[b] for b in range(bits)]
            )
            e_high, e_low = split(entering)
            seen = dot(e_high, q, NT) + dot(e_low, q, NT)
            drift = drift_s[pl.ds(h, 1), :]
            gws = []
            for n, l in enumerate(slots):
                gain = lw_ref[l, pl.ds(h, 1), :]
                level = lead * jnp.sum(
                    seen[n * dv : (n + 1) * dv] * gt[part], axis=0, keepdims=True
                )
                gl_ref[l, pl.ds(h, 1), :] = level
                drift = drift + gain * level
                gws.append(gt[part] * (lead * gain))
            gw, gw_low = split(jnp.concatenate(gws, axis=0))
            gq_in = dot(gw, e_high, TN) + dot(gw, e_low, TN) + dot(gw_low, e_high, TN)
            gq_ref[:, wide] = (gq_s[h] + gq_in).astype(BF16)
            a_high, a_low = split(after)
            tv, tv_low = split(vt[part] * tail)
            gk_in = dot(tv, a_high, TN) + dot(tv, a_low, TN) + dot(tv_low, a_high, TN)
            gk_ref[:, wide] = (gk_s[h] + gk_in).astype(BF16)
            vg = vg_s[p, part] + tail * (dot(a_high, k, NT) + dot(a_low, k, NT))
            drift_s[pl.ds(h, 1), :] = drift - jnp.sum(vg * vt[part], axis=0, keepdims=True)
            vg_all.append(vg)
        gv_ref[:, lanes] = jnp.transpose(jnp.concatenate(vg_all, axis=0)).astype(BF16)
        return 0

    lax.fori_loop(0, pairs, finish, 0, unroll=2)
    for l in range(levels):
        if l > span_bits and l not in slots:
            gl_ref[l] = jnp.zeros((heads, tok), F32)

    later = (rows_i >= cols_i).astype(F32)
    local_tail = lax.dot_general(
        drift_s[...], later, NN, precision=lax.Precision.HIGHEST, preferred_element_type=F32
    )
    lane = lax.broadcasted_iota(jnp.int32, (heads, tok), 1)
    first = local_tail[:, 0:1]
    plain = jnp.sum(local_tail, axis=1, keepdims=True)
    square = jnp.sum(local_tail * local_tail, axis=1, keepdims=True)
    tot[place] = jnp.where(lane == 0, first, jnp.where(lane == 1, plain, square))

    def tot_copy(o, slot_at):
        return pltpu.make_async_remote_copy(
            src_ref=tot.at[place],
            dst_ref=tot.at[slot_at],
            send_sem=t_send.at[o],
            recv_sem=t_recv.at[slot_at],
            device_id={"seq": (place + o) % seq_count},
            device_id_type=MESH,
        )

    for o in range(1, seq_count):
        tot_copy(o, place).start()
    for o in range(1, seq_count):
        tot_copy(o, (place + o) % seq_count).wait_recv()
    after_total = jnp.zeros((heads, 1), F32)
    my_later = jnp.zeros((heads, 1), F32)
    energy = jnp.zeros((heads, 1), F32)
    for d in reversed(range(seq_count)):
        piece = tot[d]
        my_later = my_later + jnp.where(place == d, 1.0, 0.0) * after_total
        energy = energy + (
            piece[:, 2:3] + after_total * (2.0 * piece[:, 1:2] + tok * after_total)
        )
        after_total = after_total + piece[:, 0:1]
    energy = jnp.sum(jnp.broadcast_to(energy, (heads, dk)), axis=0, keepdims=True)
    sq[row] = jnp.broadcast_to(energy, (8, dk))

    def sq_copy(o, slot_at):
        return pltpu.make_async_remote_copy(
            src_ref=sq.at[row],
            dst_ref=sq.at[slot_at],
            send_sem=q_send.at[o],
            recv_sem=q_recv.at[slot_at],
            device_id={"head": (row + o) % head_count},
            device_id_type=MESH,
        )

    for o in range(1, head_count):
        sq_copy(o, row).start()
    for o in range(1, head_count):
        sq_copy(o, (row + o) % head_count).wait_recv()
    whole = sq[0]
    for r in range(1, head_count):
        whole = whole + sq[r]
    count = heads * tok * seq_count * head_count
    factor = jnp.minimum(1.0, lax.rsqrt(whole[0:1] / count + 1e-6))
    gg_ref[...] = (local_tail + my_later) * factor

    for b in range(bits):
        d_copy(b).wait_send()
        for n in range(2 if b == 0 else 1):
            level_wait(b, n).wait_send()
        if b > 0:
            forward_copy(b, own).wait_send()
        if b < bits - 1:

            @pl.when((bit[b] == 1) & want_s[b])
            def _(b=b):
                s_copy(b).wait_send()

            for j in range(b + 1, bits):

                @pl.when(bit[j] == 1)
                def _(b=b, j=j):
                    u_copy(b, j).wait_send()

    for o in range(1, seq_count):
        tot_copy(o, place).wait_send()
    for o in range(1, head_count):
        sq_copy(o, row).wait_send()


def chunked_kernel(
    seq_count,
    head_count,
    q_ref,
    k_ref,
    v_ref,
    g_ref,
    lg_ref,
    lw_ref,
    ds_ref,
    gq_ref,
    gk_ref,
    gv_ref,
    gl_ref,
    gg_ref,
    cum_s,
    col_s,
    lead_s,
    tail_s,
    bias_s,
    vt_s,
    gt_s,
    vg_s,
    gq_s,
    gk_s,
    drift_s,
    coef_s,
    mix_s,
    st,
    got_a,
    got_b,
    sum_a,
    sum_b,
    sum_q,
    lvl,
    decs,
    tot,
    sq,
    a_send,
    a_recv,
    b_send,
    b_recv,
    p_send,
    p_recv,
    xa_send,
    xa_recv,
    xb_send,
    xb_recv,
    y_send,
    y_recv,
    f_send,
    f_recv,
    d_send,
    d_recv,
    t_send,
    t_recv,
    q_send,
    q_recv,
):
    tok = q_ref.shape[0]
    heads = lg_ref.shape[0]
    levels = lw_ref.shape[0]
    dk = q_ref.shape[1] // heads
    dv = v_ref.shape[1] // heads
    group = dk // dv
    pairs = heads // group
    spans = tok // SPAN
    span_bits = spans.bit_length() - 1
    bits = seq_count.bit_length() - 1
    half = heads // 2
    chunks = half // group
    cross = [min(span_bits + 1 + b, levels - 1) for b in range(bits)]
    slots = sorted(set(cross))
    kind = [1 + slots.index(l) for l in cross]
    place = lax.axis_index("seq")
    row = lax.axis_index("head")
    core, x, y = [(place // (1 << b)) % 2 for b in range(bits)]
    peer = [place + (1 - 2 * u) * (1 << b) for b, u in enumerate((core, x, y))]
    first_chip = (1 - x) * (1 - y)
    second_chip = x * (1 - y)
    mine = core * half
    theirs = (1 - core) * half

    barrier = pltpu.get_barrier_semaphore()
    for o in range(1, seq_count):
        pl.semaphore_signal(
            barrier, inc=1, device_id={"seq": (place + o) % seq_count}, device_id_type=MESH
        )
    for o in range(1, head_count):
        pl.semaphore_signal(
            barrier, inc=1, device_id={"head": (row + o) % head_count}, device_id_type=MESH
        )

    rows_i = lax.broadcasted_iota(jnp.int32, (tok, tok), 0)
    cols_i = lax.broadcasted_iota(jnp.int32, (tok, tok), 1)
    tri = (rows_i <= cols_i).astype(F32)
    starts = jnp.broadcast_to(ds_ref[...].astype(F32), (8, tok))
    both = jnp.concatenate([lg_ref[...], starts], axis=0)
    cum_all = lax.dot_general(
        both, tri, NN, precision=lax.Precision.HIGHEST, preferred_element_type=F32
    )
    cum_t = jnp.transpose(
        jnp.concatenate([cum_all, jnp.zeros((dk - heads - 8, tok), F32)], axis=0)
    )
    cum = cum_all[:heads]
    reset = cum_all[heads : heads + 1]
    reset_col = cum_t[:, heads : heads + 1]
    bias_s[...] = jnp.where((rows_i <= cols_i) & (reset == reset_col), 0.0, -1e30)
    end = cum[:, tok - 1 : tok]
    reset_end = reset[:, tok - 1 : tok]
    cum_s[...] = cum
    lead_s[...] = jnp.where(reset == 0, jnp.exp(cum), 0.0)
    tail_s[...] = jnp.where(reset == reset_end, jnp.exp(end - cum), 0.0)
    lane_row = lax.broadcasted_iota(jnp.int32, (1, dk), 1)
    end_row = jnp.where(lane_row < heads, cum_t[tok - 1 : tok, :], 0.0)
    decs[place] = jnp.where(reset_end == 0, jnp.exp(end_row), 0.0)
    for h in range(heads):
        col_s[h] = jnp.broadcast_to(cum_t[:, h : h + 1], (tok, tok))

    def states(p, _):
        lanes = pl.ds(pl.multiple_of(p * dk, dk), dk)
        vt = jnp.transpose(v_ref[:, lanes].astype(F32))
        gt = jnp.transpose(g_ref[:, lanes].astype(F32))
        vt_s[p] = vt.astype(BF16)
        gt_s[p] = gt.astype(BF16)
        for i in range(group):
            h = p * group + i
            wide = pl.ds(pl.multiple_of(h * dk, dk), dk)
            part = slice(i * dv, (i + 1) * dv)
            tail = tail_s[pl.ds(h, 1), :]
            lead = lead_s[pl.ds(h, 1), :]
            st[0, h] = dot_fine(vt[part] * tail, k_ref[:, wide], NN)
            gw = jnp.concatenate(
                [gt[part] * (lead * lw_ref[l, pl.ds(h, 1), :]) for l in slots], axis=0
            )
            back = dot_fine(gw, q_ref[:, wide], NN)
            for n in range(len(slots)):
                st[1 + n, h] = back[n * dv : (n + 1) * dv]
        return 0

    lax.fori_loop(0, pairs, states, 0, unroll=2)
    pl.semaphore_wait(barrier, seq_count - 1 + head_count - 1)

    def remote(src, dst, send, recv, b):
        return pltpu.make_async_remote_copy(
            src_ref=src,
            dst_ref=dst,
            send_sem=send,
            recv_sem=recv,
            device_id={"seq": peer[b]},
            device_id_type=MESH,
        )

    def of(base, c):
        return pl.ds(base + c * group, group)

    def at(c):
        return pl.ds(c * group, group)

    kind_a = y * kind[2]
    kind_b = x * kind[1]
    slot_out = bits - (bits - 1) * first_chip
    slot_in = bits - (bits - 1) * second_chip

    def dec_copy(o, slot_at):
        return pltpu.make_async_remote_copy(
            src_ref=decs.at[place],
            dst_ref=decs.at[slot_at],
            send_sem=d_send.at[o],
            recv_sem=d_recv.at[slot_at],
            device_id={"seq": (place + o) % seq_count},
            device_id_type=MESH,
        )

    def a_copy(c):
        return remote(
            st.at[kind_a, of(theirs, c)], got_a.at[at(c)], a_send.at[c], a_recv.at[c], 0
        )

    def b_copy(c):
        return remote(
            st.at[kind_b, of(theirs, c)], got_b.at[at(c)], b_send.at[c], b_recv.at[c], 0
        )

    def p_copy():
        return remote(st.at[core * kind[0]], lvl.at[0], p_send.at[0], p_recv.at[0], 0)

    def xa_copy(c):
        return remote(
            sum_a.at[at(c)], lvl.at[slot_out, of(mine, c)], xa_send.at[c], xa_recv.at[c], 1
        )

    def xb_copy(c):
        return remote(sum_b.at[at(c)], lvl.at[1, of(mine, c)], xb_send.at[c], xb_recv.at[c], 1)

    def y_copy(c):
        return remote(sum_q.at[at(c)], lvl.at[2, of(mine, c)], y_send.at[c], y_recv.at[c], 2)

    def f_copy(j, base, c):
        part = lvl.at[j, of(base, c)]
        return remote(part, part, f_send.at[j - 1, c], f_recv.at[j - 1, c], 0)

    for o in range(1, seq_count):
        dec_copy(o, place).start()
    for c in range(chunks):
        a_copy(c).start()

    @pl.when(first_chip == 0)
    def _():
        for c in range(chunks):
            b_copy(c).start()

    p_copy().start()

    span_of = lax.broadcasted_iota(jnp.int32, (1, tok), 1) // SPAN

    def local(p, _):
        vt = vt_s[p]
        gt = gt_s[p]
        lanes = pl.ds(pl.multiple_of(p * dk, dk), dk)
        v_blk = v_ref[:, lanes]
        for i in range(group):
            h = p * group + i
            wide = pl.ds(pl.multiple_of(h * dk, dk), dk)
            part = slice(i * dv, (i + 1) * dv)
            q = q_ref[:, wide]
            k = k_ref[:, wide]
            score = dot(k, q, NT)
            pair = dot(v_blk[:, part], gt[part], NN)
            decay = jnp.exp((cum_s[pl.ds(h, 1), :] - col_s[h]) + bias_s[...])
            seen = decay * score
            both_p = seen * pair
            gains = [lw_ref[l, pl.ds(h, 1), :] for l in range(span_bits + 1)]
            level_rows = [jnp.zeros((1, tok), F32) for _ in range(span_bits + 1)]
            mixed, graded = [], []
            for cs in range(spans):
                rows = slice(cs * SPAN, (cs + 1) * SPAN)
                total = jnp.sum(both_p[rows], axis=0, keepdims=True)
                gain = jnp.zeros((1, tok), F32)
                for ct in range(cs, spans):
                    l = span_level(cs, ct, levels)
                    hit = span_of == ct
                    gain = jnp.where(hit, gains[l], gain)
                    level_rows[l] = level_rows[l] + jnp.where(hit, total, 0.0)
                mixed.append(seen[rows] * gain)
                graded.append(decay[rows] * gain * pair[rows])
            mix = jnp.concatenate(mixed, axis=0).astype(BF16)
            grade = jnp.concatenate(graded, axis=0).astype(BF16)
            for l in range(span_bits + 1):
                gl_ref[l, pl.ds(h, 1), :] = level_rows[l]
            drift_s[pl.ds(h, 1), :] = jnp.sum(mix.astype(F32) * pair, axis=0, keepdims=True)
            vg_s[p, part] = dot(gt[part], mix, NT)
            gk_s[h] = dot(grade, q, NN)
            gq_s[h] = dot(grade, k, TN)
        return 0

    def decay_of(device):
        return decs[device]

    def wait_dec(device):
        dec_copy((device + seq_count - place) % seq_count, device).wait_recv()

    def spread(device_rows):
        t = jnp.transpose(
            jnp.concatenate(
                device_rows + [jnp.zeros((8 - len(device_rows), dk), F32)], axis=0
            )
        )
        return [
            jnp.broadcast_to(t[:heads, n : n + 1], (heads, dk)) for n in range(len(device_rows))
        ]

    def weigh(n, swap, own, got):
        w = (swap % 2).astype(F32)
        mix_s[n, 0] = own * (1.0 - w) + w
        mix_s[n, 1] = got * w + (1.0 - w)

    def combine(n, c, own_at, got_at, put):
        for i in range(group):
            r = c * group + i
            ca = mix_s[n, 0, pl.ds(mine + r, 1), :]
            cb = mix_s[n, 1, pl.ds(mine + r, 1), :]
            put[r] = ca * own_at(r) + cb * got_at(r)

    lax.fori_loop(0, 2, local, 0, unroll=2)

    dec_recv = [peer[0], peer[1], peer[1] + 1 - 2 * core]
    wait_dec(dec_recv[0])
    d_self, d_pair = spread([decay_of(place), decay_of(dec_recv[0])])
    weigh(0, core + y, d_pair, d_self)
    weigh(1, core + x, d_pair, d_self)
    for c in range(chunks):
        a_copy(c).wait_recv()
        combine(0, c, lambda r: st[kind_a, mine + r], lambda r: got_a[r], sum_a)
        xa_copy(c).start()

    @pl.when(first_chip == 0)
    def _():
        for c in range(chunks):
            b_copy(c).wait_recv()
            combine(1, c, lambda r: st[kind_b, mine + r], lambda r: got_b[r], sum_b)
            xb_copy(c).start()

    lax.fori_loop(2, pairs - 2, local, 0, unroll=2)

    for n in (1, 2):
        wait_dec(dec_recv[n])
    side, other_side = spread([decay_of(dec_recv[1]), decay_of(dec_recv[2])])
    d_side = side * other_side
    weigh(2, x + y, d_side, d_self * d_pair)
    inner_f = jnp.ones((heads, dk), F32)
    inner_b = jnp.ones((heads, dk), F32)
    for b, (u, got) in enumerate(((core, d_pair), (x, d_side), (y, None))):
        up = u.astype(F32)
        coef_s[0, b] = inner_f * up
        coef_s[1, b] = inner_b * (1.0 - up)
        if got is not None:
            inner_f = inner_f * (up * got + (1.0 - up))
            inner_b = inner_b * ((1.0 - up) * got + up)

    for c in range(chunks):
        xa_copy(c).wait_recv()
        combine(2, c, lambda r: sum_a[r], lambda r: lvl[slot_in, mine + r], sum_q)
        y_copy(c).start()

        @pl.when(second_chip == 1)
        def _(c=c):
            f_copy(1, mine, c).start()

        if c == 0:
            lax.fori_loop(pairs - 2, pairs, local, 0, unroll=2)

    def finish(p, _):
        lanes = pl.ds(pl.multiple_of(p * dk, dk), dk)
        vt = vt_s[p].astype(F32)
        gt = gt_s[p].astype(F32)
        vg_all = []
        for i in range(group):
            h = p * group + i
            wide = pl.ds(pl.multiple_of(h * dk, dk), dk)
            part = slice(i * dv, (i + 1) * dv)
            q = q_ref[:, wide]
            k = k_ref[:, wide]
            tail = tail_s[pl.ds(h, 1), :]
            lead = lead_s[pl.ds(h, 1), :]
            blocks = [lvl[b, h] for b in range(bits)]
            entering = []
            for n in range(len(slots)):
                terms = [
                    coef_s[0, b, pl.ds(h, 1), :] * blocks[b]
                    for b in range(bits)
                    if kind[b] == 1 + n
                ]
                entering.append(functools.reduce(jnp.add, terms))
            entering = jnp.concatenate(entering, axis=0)
            after = functools.reduce(
                jnp.add, [coef_s[1, b, pl.ds(h, 1), :] * blocks[b] for b in range(bits)]
            )
            e_high, e_low = split(entering)
            seen = dot(e_high, q, NT) + dot(e_low, q, NT)
            drift = drift_s[pl.ds(h, 1), :]
            gws = []
            for n, l in enumerate(slots):
                gain = lw_ref[l, pl.ds(h, 1), :]
                level = lead * jnp.sum(
                    seen[n * dv : (n + 1) * dv] * gt[part], axis=0, keepdims=True
                )
                gl_ref[l, pl.ds(h, 1), :] = level
                drift = drift + gain * level
                gws.append(gt[part] * (lead * gain))
            gw, gw_low = split(jnp.concatenate(gws, axis=0))
            gq_in = dot(gw, e_high, TN) + dot(gw, e_low, TN) + dot(gw_low, e_high, TN)
            gq_ref[:, wide] = (gq_s[h] + gq_in).astype(BF16)
            a_high, a_low = split(after)
            tv, tv_low = split(vt[part] * tail)
            gk_in = dot(tv, a_high, TN) + dot(tv, a_low, TN) + dot(tv_low, a_high, TN)
            gk_ref[:, wide] = (gk_s[h] + gk_in).astype(BF16)
            vg = vg_s[p, part] + tail * (dot(a_high, k, NT) + dot(a_low, k, NT))
            drift_s[pl.ds(h, 1), :] = drift - jnp.sum(vg * vt[part], axis=0, keepdims=True)
            vg_all.append(vg)
        gv_ref[:, lanes] = jnp.transpose(jnp.concatenate(vg_all, axis=0)).astype(BF16)
        return 0

    def finish_chunk(c):
        if c == 0:
            p_copy().wait_recv()
        for j in (1, 2):
            f_copy(j, theirs, c).wait_recv()
        lax.fori_loop(0, 2, lambda i, _: finish(c + i * chunks, 0), 0, unroll=2)

    for c in range(chunks):

        @pl.when(second_chip == 0)
        def _(c=c):
            xb_copy(c).wait_recv()
            f_copy(1, mine, c).start()

        y_copy(c).wait_recv()
        f_copy(2, mine, c).start()
        if c > 0:
            finish_chunk(c - 1)
    finish_chunk(chunks - 1)
    for l in range(levels):
        if l > span_bits and l not in slots:
            gl_ref[l] = jnp.zeros((heads, tok), F32)

    later = (rows_i >= cols_i).astype(F32)
    local_tail = lax.dot_general(
        drift_s[...], later, NN, precision=lax.Precision.HIGHEST, preferred_element_type=F32
    )
    lane = lax.broadcasted_iota(jnp.int32, (heads, tok), 1)
    first = local_tail[:, 0:1]
    plain = jnp.sum(local_tail, axis=1, keepdims=True)
    square = jnp.sum(local_tail * local_tail, axis=1, keepdims=True)
    tot[place] = jnp.where(lane == 0, first, jnp.where(lane == 1, plain, square))

    def tot_copy(o, slot_at):
        return pltpu.make_async_remote_copy(
            src_ref=tot.at[place],
            dst_ref=tot.at[slot_at],
            send_sem=t_send.at[o],
            recv_sem=t_recv.at[slot_at],
            device_id={"seq": (place + o) % seq_count},
            device_id_type=MESH,
        )

    for o in range(1, seq_count):
        tot_copy(o, place).start()
    for o in range(1, seq_count):
        tot_copy(o, (place + o) % seq_count).wait_recv()
    after_total = jnp.zeros((heads, 1), F32)
    my_later = jnp.zeros((heads, 1), F32)
    energy = jnp.zeros((heads, 1), F32)
    for d in reversed(range(seq_count)):
        piece = tot[d]
        my_later = my_later + jnp.where(place == d, 1.0, 0.0) * after_total
        energy = energy + (
            piece[:, 2:3] + after_total * (2.0 * piece[:, 1:2] + tok * after_total)
        )
        after_total = after_total + piece[:, 0:1]
    energy = jnp.sum(jnp.broadcast_to(energy, (heads, dk)), axis=0, keepdims=True)
    sq[row] = jnp.broadcast_to(energy, (8, dk))

    def sq_copy(o, slot_at):
        return pltpu.make_async_remote_copy(
            src_ref=sq.at[row],
            dst_ref=sq.at[slot_at],
            send_sem=q_send.at[o],
            recv_sem=q_recv.at[slot_at],
            device_id={"head": (row + o) % head_count},
            device_id_type=MESH,
        )

    for o in range(1, head_count):
        sq_copy(o, row).start()
    for o in range(1, head_count):
        sq_copy(o, (row + o) % head_count).wait_recv()
    whole = sq[0]
    for r in range(1, head_count):
        whole = whole + sq[r]
    count = heads * tok * seq_count * head_count
    factor = jnp.minimum(1.0, lax.rsqrt(whole[0:1] / count + 1e-6))
    gg_ref[...] = (local_tail + my_later) * factor

    for o in range(1, seq_count):
        dec_copy(o, place).wait_send()

        @pl.when((place + o) % seq_count != dec_recv[0])
        def _(o=o):
            device = (place + o) % seq_count

            @pl.when((device != dec_recv[1]) & (device != dec_recv[2]))
            def _():
                wait_dec(device)

    p_copy().wait_send()
    for c in range(chunks):
        a_copy(c).wait_send()
        xa_copy(c).wait_send()
        y_copy(c).wait_send()
        for j in (1, 2):
            f_copy(j, mine, c).wait_send()

    @pl.when(first_chip == 0)
    def _():
        for c in range(chunks):
            b_copy(c).wait_send()
            xb_copy(c).wait_send()

    for o in range(1, seq_count):
        tot_copy(o, place).wait_send()
    for o in range(1, head_count):
        sq_copy(o, row).wait_send()


def write_out(count, *refs):
    sems = refs[-1]
    copies = [
        pltpu.make_async_copy(refs[i], refs[count + i], sems.at[i]) for i in range(count)
    ]
    for c in copies:
        c.start()
    for c in copies:
        c.wait()


def shards(seq_count, head_count, queries, keys, values, out_grad, log_gate, level_weight, doc_start):
    tok = queries.shape[0]
    heads = log_gate.shape[0]
    levels = level_weight.shape[0]
    dk = queries.shape[1] // heads
    dv = values.shape[1] // heads
    group = dk // dv
    pairs = heads // group
    bits = seq_count.bit_length() - 1
    half = heads // 2
    span_bits = (tok // SPAN).bit_length() - 1
    slots = len({min(span_bits + 1 + b, levels - 1) for b in range(bits)})
    dma = pltpu.SemaphoreType.DMA
    vmem = pltpu.VMEM
    block = (dv, dk)
    scratch = [
        vmem((heads, tok), F32),
        vmem((heads, tok, tok), F32),
        vmem((heads, tok), F32),
        vmem((heads, tok), F32),
        vmem((tok, tok), F32),
        vmem((pairs, group * dv, tok), BF16),
        vmem((pairs, group * dv, tok), BF16),
        vmem((pairs, group * dv, tok), F32),
        vmem((heads, tok, dk), F32),
        vmem((heads, tok, dk), F32),
        vmem((heads, tok), F32),
        vmem((2, bits, heads, dk), F32),
        vmem((heads,) + block, F32),
        vmem((slots, heads) + block, F32),
        vmem((bits, heads) + block, F32),
        vmem((bits, half) + block, F32),
        vmem((bits, bits, half) + block, F32),
        vmem((bits, half) + block, F32),
        vmem((bits, bits, half) + block, F32),
        vmem((bits + 1, heads, dk), F32),
        vmem((bits, heads, dk), F32),
        vmem((seq_count, heads, tok), F32),
        vmem((head_count, 8, dk), F32),
        dma((bits, 2)),
        dma((bits, 2)),
        dma((bits,)),
        dma((bits,)),
        dma((bits,)),
        dma((bits,)),
        dma((bits, bits)),
        dma((bits, bits)),
        dma((bits,)),
        dma((bits,)),
        dma((seq_count,)),
        dma((seq_count,)),
        dma((head_count,)),
        dma((head_count,)),
    ]
    body = kernel
    chunks = half // group
    if bits == 3 and chunks * group == half:
        body = chunked_kernel
        scratch = scratch[:12] + [
            vmem((3, 2, heads, dk), F32),
            vmem((1 + slots, heads) + block, F32),
            vmem((half,) + block, F32),
            vmem((half,) + block, F32),
            vmem((half,) + block, F32),
            vmem((half,) + block, F32),
            vmem((half,) + block, F32),
            vmem((bits + 1, heads) + block, F32),
            vmem((seq_count, 1, dk), F32),
            vmem((seq_count, heads, tok), F32),
            vmem((head_count, 8, dk), F32),
            dma((chunks,)),
            dma((chunks,)),
            dma((chunks,)),
            dma((chunks,)),
            dma((1,)),
            dma((1,)),
            dma((chunks,)),
            dma((chunks,)),
            dma((chunks,)),
            dma((chunks,)),
            dma((chunks,)),
            dma((chunks,)),
            dma((2, chunks)),
            dma((2, chunks)),
            dma((seq_count,)),
            dma((seq_count,)),
            dma((seq_count,)),
            dma((seq_count,)),
            dma((head_count,)),
            dma((head_count,)),
        ]
    spec = pl.BlockSpec(memory_space=pltpu.VMEM)
    outs = [
        (queries.shape, BF16),
        (keys.shape, BF16),
        (values.shape, BF16),
        (level_weight.shape, F32),
        (log_gate.shape, F32),
    ]
    results = pl.pallas_call(
        functools.partial(body, seq_count, head_count),
        out_shape=tuple(vmem(shape, dtype) for shape, dtype in outs),
        in_specs=[spec] * 7,
        out_specs=(spec,) * 5,
        scratch_shapes=scratch,
        compiler_params=pltpu.CompilerParams(collective_id=0, has_side_effects=True),
    )(queries, keys, values, out_grad, log_gate, level_weight, doc_start.reshape(1, tok))
    count = len(outs)
    return pl.pallas_call(
        functools.partial(write_out, count),
        out_shape=tuple(jax.ShapeDtypeStruct(shape, dtype) for shape, dtype in outs),
        in_specs=[spec] * count,
        out_specs=(pl.BlockSpec(memory_space=pltpu.HBM),) * count,
        scratch_shapes=[dma((count,))],
    )(*[pltpu.with_memory_space_constraint(r, pltpu.VMEM) for r in results])


def solution(mesh):
    return jax.shard_map(
        functools.partial(shards, mesh.shape["seq"], mesh.shape["head"]),
        mesh=mesh,
        in_specs=(
            P("seq", "head"),
            P("seq", "head"),
            P("seq", "head"),
            P("seq", "head"),
            P("head", "seq"),
            P(None, "head", "seq"),
            P("seq"),
        ),
        out_specs=(
            P("seq", "head"),
            P("seq", "head"),
            P("seq", "head"),
            P(None, "head", "seq"),
            P("head", "seq"),
        ),
        check_vma=False,
    )
```

```python
import functools

import jax
import jax.numpy as jnp
from jax import lax
from jax.experimental import pallas as pl
from jax.experimental.pallas import tpu as pltpu
from jax.sharding import PartitionSpec as P

SPAN = 64
F32 = jnp.float32
BF16 = jnp.bfloat16
NN = (((1,), (0,)), ((), ()))
NT = (((1,), (1,)), ((), ()))
TN = (((0,), (0,)), ((), ()))
MESH = pl.DeviceIdType.MESH


def dot(a, b, dims):
    return lax.dot_general(a, b, dims, preferred_element_type=F32)


def split(x):
    high = x.astype(BF16)
    return high, (x - high.astype(F32)).astype(BF16)


def dot_fine(x, b, dims):
    high, low = split(x)
    return dot(high, b, dims) + dot(low, b, dims)


def span_level(a, b, levels):
    return 0 if a == b else min(levels - 1, (a ^ b).bit_length())


def kernel(
    seq_count,
    head_count,
    q_ref,
    k_ref,
    v_ref,
    g_ref,
    lg_ref,
    lw_ref,
    ds_ref,
    gq_ref,
    gk_ref,
    gv_ref,
    gl_ref,
    gg_ref,
    cum_s,
    col_s,
    lead_s,
    tail_s,
    bias_s,
    vt_s,
    gt_s,
    vg_s,
    gq_s,
    gk_s,
    drift_s,
    coef_s,
    state_s,
    back_s,
    lvl,
    got_s,
    got_u,
    sum_s,
    sum_u,
    dec,
    got_dec,
    tot,
    sq,
    lvl_send,
    lvl_recv,
    fwd_send,
    fwd_recv,
    s_send,
    s_recv,
    u_send,
    u_recv,
    d_send,
    d_recv,
    t_send,
    t_recv,
    q_send,
    q_recv,
):
    tok = q_ref.shape[0]
    heads = lg_ref.shape[0]
    levels = lw_ref.shape[0]
    dk = q_ref.shape[1] // heads
    dv = v_ref.shape[1] // heads
    group = dk // dv
    pairs = heads // group
    spans = tok // SPAN
    span_bits = spans.bit_length() - 1
    bits = seq_count.bit_length() - 1
    half = heads // 2
    cross = [min(span_bits + 1 + b, levels - 1) for b in range(bits)]
    slots = sorted(set(cross))
    place = lax.axis_index("seq")
    row = lax.axis_index("head")
    bit = [(place // (1 << b)) % 2 for b in range(bits)]
    peer = [place + (1 - 2 * bit[b]) * (1 << b) for b in range(bits)]
    want_s = [(place // (2 << b)) != (seq_count // (2 << b)) - 1 for b in range(bits)]
    mine = bit[0] * half
    theirs = (1 - bit[0]) * half

    barrier = pltpu.get_barrier_semaphore()
    for o in range(1, seq_count):
        pl.semaphore_signal(
            barrier, inc=1, device_id={"seq": (place + o) % seq_count}, device_id_type=MESH
        )
    for o in range(1, head_count):
        pl.semaphore_signal(
            barrier, inc=1, device_id={"head": (row + o) % head_count}, device_id_type=MESH
        )

    rows_i = lax.broadcasted_iota(jnp.int32, (tok, tok), 0)
    cols_i = lax.broadcasted_iota(jnp.int32, (tok, tok), 1)
    tri = (rows_i <= cols_i).astype(F32)
    starts = jnp.broadcast_to(ds_ref[...].astype(F32), (8, tok))
    both = jnp.concatenate([lg_ref[...], starts], axis=0)
    cum_all = lax.dot_general(
        both, tri, NN, precision=lax.Precision.HIGHEST, preferred_element_type=F32
    )
    cum_t = jnp.transpose(cum_all)
    cum = cum_all[:heads]
    reset = cum_all[heads : heads + 1]
    reset_col = cum_t[:, heads : heads + 1]
    bias_s[...] = jnp.where((rows_i <= cols_i) & (reset == reset_col), 0.0, -1e30)
    end = cum[:, tok - 1 : tok]
    reset_end = reset[:, tok - 1 : tok]
    cum_s[...] = cum
    lead_s[...] = jnp.where(reset == 0, jnp.exp(cum), 0.0)
    tail_s[...] = jnp.where(reset == reset_end, jnp.exp(end - cum), 0.0)
    dec[0] = jnp.broadcast_to(jnp.where(reset_end == 0, jnp.exp(end), 0.0), (heads, dk))
    for h in range(heads):
        col_s[h] = jnp.broadcast_to(cum_t[:, h : h + 1], (tok, tok))

    def states(p, _):
        lanes = pl.ds(pl.multiple_of(p * dk, dk), dk)
        vt = jnp.transpose(v_ref[:, lanes].astype(F32))
        gt = jnp.transpose(g_ref[:, lanes].astype(F32))
        vt_s[p] = vt.astype(BF16)
        gt_s[p] = gt.astype(BF16)
        for i in range(group):
            h = p * group + i
            wide = pl.ds(pl.multiple_of(h * dk, dk), dk)
            part = slice(i * dv, (i + 1) * dv)
            tail = tail_s[pl.ds(h, 1), :]
            lead = lead_s[pl.ds(h, 1), :]
            state_s[h] = dot_fine(vt[part] * tail, k_ref[:, wide], NN)
            gw = jnp.concatenate(
                [gt[part] * (lead * lw_ref[l, pl.ds(h, 1), :]) for l in slots], axis=0
            )
            back = dot_fine(gw, q_ref[:, wide], NN)
            for n in range(len(slots)):
                back_s[n, h] = back[n * dv : (n + 1) * dv]
        return 0

    lax.fori_loop(0, pairs, states, 0, unroll=2)
    pl.semaphore_wait(barrier, seq_count - 1 + head_count - 1)

    def slot(b):
        return slots.index(cross[b])

    def remote(src, dst, send, recv, b):
        return pltpu.make_async_remote_copy(
            src_ref=src,
            dst_ref=dst,
            send_sem=send,
            recv_sem=recv,
            device_id={"seq": peer[b]},
            device_id_type=MESH,
        )

    own = pl.ds(mine, half)
    other = pl.ds(theirs, half)

    def u_copy(b, j):
        src = back_s.at[slot(j), other] if b == 0 else sum_u.at[b, j]
        return remote(src, got_u.at[b, j], u_send.at[b, j], u_recv.at[b, j], b)

    def s_copy(b):
        src = state_s.at[other] if b == 0 else sum_s.at[b]
        return remote(src, got_s.at[b], s_send.at[b], s_recv.at[b], b)

    def d_copy(b):
        return remote(dec.at[b], got_dec.at[b], d_send.at[b], d_recv.at[b], b)

    def level_copy(b, low):
        if b == 0:
            src = state_s if low else back_s.at[slot(0)]
            return [
                remote(src.at[part], lvl.at[0, part], lvl_send.at[0, n], lvl_recv.at[0, n], 0)
                for n, part in enumerate((other, own))
            ]
        src = sum_s.at[b] if low else sum_u.at[b, b]
        return [remote(src, lvl.at[b, own], lvl_send.at[b, 0], lvl_recv.at[b, 0], b)]

    def level_wait(b, n):
        part = other if n == 1 else own
        return remote(
            lvl.at[b, part], lvl.at[b, part], lvl_send.at[b, n], lvl_recv.at[b, n], b
        )

    def forward_copy(b, part):
        return remote(lvl.at[b, part], lvl.at[b, part], fwd_send.at[b], fwd_recv.at[b], 0)

    def land(b):
        up_summed = (bit[b] == 1) & want_s[b]

        @pl.when(jnp.logical_not(up_summed))
        def _():
            level_wait(b, 0).wait_recv()

        if b > 0:
            forward_copy(b, own).start()

    def begin(b):
        d_copy(b).start()

        early = 0 if b in (0, bits - 1) else 1

        @pl.when((bit[b] == 0) & (want_s[b] | (early == 0)))
        def _():
            for c in level_copy(b, True):
                c.start()

        if b < bits - 1:

            @pl.when((bit[b] == 1) & want_s[b])
            def _():
                s_copy(b).start()

            for j in range(b + 1, bits):

                @pl.when(bit[j] == 1)
                def _(j=j):
                    u_copy(b, j).start()

        if early == 0:

            @pl.when(bit[b] == 1)
            def _():
                for c in level_copy(b, False):
                    c.start()

    def begin_late(b):
        if b in (0, bits - 1):
            return

        @pl.when((bit[b] == 0) & jnp.logical_not(want_s[b]))
        def _():
            for c in level_copy(b, True):
                c.start()

        @pl.when(bit[b] == 1)
        def _():
            for c in level_copy(b, False):
                c.start()

    def join(b):
        d_copy(b).wait_recv()
        up = bit[b].astype(F32)
        got = got_dec[b]
        now = dec[b]
        dec[b + 1] = got * now
        if b == bits - 1:
            return
        base_s = state_s.at[own] if b == 0 else sum_s.at[b]

        @pl.when(want_s[b])
        def _():
            @pl.when(bit[b] == 1)
            def _():
                level_wait(b, 0).wait_recv()

                def body(i, _):
                    d = dec[b, pl.ds(mine + i, 1), :]
                    sum_s[b + 1, i] = d * lvl[b, mine + i] + base_s[i]
                    return 0

                lax.fori_loop(0, half, body, 0, unroll=True)

            @pl.when(bit[b] == 0)
            def _():
                s_copy(b).wait_recv()

                def body(i, _):
                    d = got_dec[b, pl.ds(mine + i, 1), :]
                    sum_s[b + 1, i] = d * base_s[i] + got_s[b, i]
                    return 0

                lax.fori_loop(0, half, body, 0, unroll=True)

        for j in range(b + 1, bits):
            base_u = back_s.at[slot(j), own] if b == 0 else sum_u.at[b, j]

            @pl.when(bit[j] == 1)
            def _(j=j, base_u=base_u):
                u_copy(b, j).wait_recv()

                def body(i, _):
                    d0 = dec[b, pl.ds(mine + i, 1), :]
                    d1 = got_dec[b, pl.ds(mine + i, 1), :]
                    a = up * d1 + (1.0 - up)
                    c = (1.0 - up) * d0 + up
                    sum_u[b + 1, j, i] = a * base_u[i] + c * got_u[b, j, i]
                    return 0

                lax.fori_loop(0, half, body, 0, unroll=True)

    span_of = lax.broadcasted_iota(jnp.int32, (1, tok), 1) // SPAN

    def local(p, _):
        vt = vt_s[p]
        gt = gt_s[p]
        lanes = pl.ds(pl.multiple_of(p * dk, dk), dk)
        v_blk = v_ref[:, lanes]
        for i in range(group):
            h = p * group + i
            wide = pl.ds(pl.multiple_of(h * dk, dk), dk)
            part = slice(i * dv, (i + 1) * dv)
            q = q_ref[:, wide]
            k = k_ref[:, wide]
            score = dot(k, q, NT)
            pair = dot(v_blk[:, part], gt[part], NN)
            decay = jnp.exp((cum_s[pl.ds(h, 1), :] - col_s[h]) + bias_s[...])
            seen = decay * score
            both_p = seen * pair
            gains = [lw_ref[l, pl.ds(h, 1), :] for l in range(span_bits + 1)]
            level_rows = [jnp.zeros((1, tok), F32) for _ in range(span_bits + 1)]
            mixed, graded = [], []
            for cs in range(spans):
                rows = slice(cs * SPAN, (cs + 1) * SPAN)
                total = jnp.sum(both_p[rows], axis=0, keepdims=True)
                gain = jnp.zeros((1, tok), F32)
                for ct in range(cs, spans):
                    l = span_level(cs, ct, levels)
                    hit = span_of == ct
                    gain = jnp.where(hit, gains[l], gain)
                    level_rows[l] = level_rows[l] + jnp.where(hit, total, 0.0)
                mixed.append(seen[rows] * gain)
                graded.append(decay[rows] * gain * pair[rows])
            mix = jnp.concatenate(mixed, axis=0).astype(BF16)
            grade = jnp.concatenate(graded, axis=0).astype(BF16)
            for l in range(span_bits + 1):
                gl_ref[l, pl.ds(h, 1), :] = level_rows[l]
            drift_s[pl.ds(h, 1), :] = jnp.sum(mix.astype(F32) * pair, axis=0, keepdims=True)
            vg_s[p, part] = dot(gt[part], mix, NT)
            gk_s[h] = dot(grade, q, NN)
            gq_s[h] = dot(grade, k, TN)
        return 0

    begin(0)
    lax.fori_loop(0, pairs // 4, local, 0, unroll=2)
    join(0)
    if bits > 1:
        begin(1)
    lax.fori_loop(pairs // 4, pairs, local, 0, unroll=2)
    for b in range(1, bits):
        join(b)
        if b + 1 < bits:
            begin(b + 1)
        begin_late(b)
        land(b - 1)
    land(bits - 1)

    inner_f = jnp.ones((heads, dk), F32)
    inner_b = jnp.ones((heads, dk), F32)
    for b in range(bits):
        up = bit[b].astype(F32)
        got = got_dec[b]
        coef_s[0, b] = inner_f * up
        coef_s[1, b] = inner_b * (1.0 - up)
        inner_f = inner_f * (up * got + (1.0 - up))
        inner_b = inner_b * ((1.0 - up) * got + up)
    level_wait(0, 1).wait_recv()
    for b in range(1, bits):
        forward_copy(b, other).wait_recv()

    def finish(p, _):
        lanes = pl.ds(pl.multiple_of(p * dk, dk), dk)
        vt = vt_s[p].astype(F32)
        gt = gt_s[p].astype(F32)
        vg_all = []
        for i in range(group):
            h = p * group + i
            wide = pl.ds(pl.multiple_of(h * dk, dk), dk)
            part = slice(i * dv, (i + 1) * dv)
            q = q_ref[:, wide]
            k = k_ref[:, wide]
            tail = tail_s[pl.ds(h, 1), :]
            lead = lead_s[pl.ds(h, 1), :]
            blocks = [lvl[b, h] for b in range(bits)]
            entering = []
            for n in range(len(slots)):
                terms = [
                    coef_s[0, b, pl.ds(h, 1), :] * blocks[b] for b in range(bits) if slot(b) == n
                ]
                entering.append(functools.reduce(jnp.add, terms))
            entering = jnp.concatenate(entering, axis=0)
            after = functools.reduce(
                jnp.add, [coef_s[1, b, pl.ds(h, 1), :] * blocks[b] for b in range(bits)]
            )
            e_high, e_low = split(entering)
            seen = dot(e_high, q, NT) + dot(e_low, q, NT)
            drift = drift_s[pl.ds(h, 1), :]
            gws = []
            for n, l in enumerate(slots):
                gain = lw_ref[l, pl.ds(h, 1), :]
                level = lead * jnp.sum(
                    seen[n * dv : (n + 1) * dv] * gt[part], axis=0, keepdims=True
                )
                gl_ref[l, pl.ds(h, 1), :] = level
                drift = drift + gain * level
                gws.append(gt[part] * (lead * gain))
            gw, gw_low = split(jnp.concatenate(gws, axis=0))
            gq_in = dot(gw, e_high, TN) + dot(gw, e_low, TN) + dot(gw_low, e_high, TN)
            gq_ref[:, wide] = (gq_s[h] + gq_in).astype(BF16)
            a_high, a_low = split(after)
            tv, tv_low = split(vt[part] * tail)
            gk_in = dot(tv, a_high, TN) + dot(tv, a_low, TN) + dot(tv_low, a_high, TN)
            gk_ref[:, wide] = (gk_s[h] + gk_in).astype(BF16)
            vg = vg_s[p, part] + tail * (dot(a_high, k, NT) + dot(a_low, k, NT))
            drift_s[pl.ds(h, 1), :] = drift - jnp.sum(vg * vt[part], axis=0, keepdims=True)
            vg_all.append(vg)
        gv_ref[:, lanes] = jnp.transpose(jnp.concatenate(vg_all, axis=0)).astype(BF16)
        return 0

    lax.fori_loop(0, pairs, finish, 0, unroll=2)
    for l in range(levels):
        if l > span_bits and l not in slots:
            gl_ref[l] = jnp.zeros((heads, tok), F32)

    later = (rows_i >= cols_i).astype(F32)
    local_tail = lax.dot_general(
        drift_s[...], later, NN, precision=lax.Precision.HIGHEST, preferred_element_type=F32
    )
    lane = lax.broadcasted_iota(jnp.int32, (heads, tok), 1)
    first = local_tail[:, 0:1]
    plain = jnp.sum(local_tail, axis=1, keepdims=True)
    square = jnp.sum(local_tail * local_tail, axis=1, keepdims=True)
    tot[place] = jnp.where(lane == 0, first, jnp.where(lane == 1, plain, square))

    def tot_copy(o, slot_at):
        return pltpu.make_async_remote_copy(
            src_ref=tot.at[place],
            dst_ref=tot.at[slot_at],
            send_sem=t_send.at[o],
            recv_sem=t_recv.at[slot_at],
            device_id={"seq": (place + o) % seq_count},
            device_id_type=MESH,
        )

    for o in range(1, seq_count):
        tot_copy(o, place).start()
    for o in range(1, seq_count):
        tot_copy(o, (place + o) % seq_count).wait_recv()
    after_total = jnp.zeros((heads, 1), F32)
    my_later = jnp.zeros((heads, 1), F32)
    energy = jnp.zeros((heads, 1), F32)
    for d in reversed(range(seq_count)):
        piece = tot[d]
        my_later = my_later + jnp.where(place == d, 1.0, 0.0) * after_total
        energy = energy + (
            piece[:, 2:3] + after_total * (2.0 * piece[:, 1:2] + tok * after_total)
        )
        after_total = after_total + piece[:, 0:1]
    energy = jnp.sum(jnp.broadcast_to(energy, (heads, dk)), axis=0, keepdims=True)
    sq[row] = jnp.broadcast_to(energy, (8, dk))

    def sq_copy(o, slot_at):
        return pltpu.make_async_remote_copy(
            src_ref=sq.at[row],
            dst_ref=sq.at[slot_at],
            send_sem=q_send.at[o],
            recv_sem=q_recv.at[slot_at],
            device_id={"head": (row + o) % head_count},
            device_id_type=MESH,
        )

    for o in range(1, head_count):
        sq_copy(o, row).start()
    for o in range(1, head_count):
        sq_copy(o, (row + o) % head_count).wait_recv()
    whole = sq[0]
    for r in range(1, head_count):
        whole = whole + sq[r]
    count = heads * tok * seq_count * head_count
    factor = jnp.minimum(1.0, lax.rsqrt(whole[0:1] / count + 1e-6))
    gg_ref[...] = (local_tail + my_later) * factor

    for b in range(bits):
        d_copy(b).wait_send()
        for n in range(2 if b == 0 else 1):
            level_wait(b, n).wait_send()
        if b > 0:
            forward_copy(b, own).wait_send()
        if b < bits - 1:

            @pl.when((bit[b] == 1) & want_s[b])
            def _(b=b):
                s_copy(b).wait_send()

            for j in range(b + 1, bits):

                @pl.when(bit[j] == 1)
                def _(b=b, j=j):
                    u_copy(b, j).wait_send()

    for o in range(1, seq_count):
        tot_copy(o, place).wait_send()
    for o in range(1, head_count):
        sq_copy(o, row).wait_send()


def chunked_kernel(
    seq_count,
    head_count,
    q_hbm,
    k_hbm,
    v_hbm,
    g_hbm,
    lg_hbm,
    lw_hbm,
    ds_hbm,
    gq_ref,
    gk_ref,
    gv_ref,
    gl_ref,
    gg_ref,
    q_ref,
    k_ref,
    v_ref,
    g_ref,
    lg_ref,
    lw_ref,
    ds_ref,
    cum_s,
    col_s,
    lead_s,
    tail_s,
    bias_s,
    vt_s,
    gt_s,
    vg_s,
    gq_s,
    gk_s,
    drift_s,
    coef_s,
    mix_s,
    st,
    got_a,
    got_b,
    sum_a,
    sum_b,
    sum_q,
    lvl,
    decs,
    msg,
    i_sem,
    a_send,
    a_recv,
    b_send,
    b_recv,
    p_send,
    p_recv,
    xa_send,
    xa_recv,
    xb_send,
    xb_recv,
    y_send,
    y_recv,
    f_send,
    f_recv,
    d_send,
    d_recv,
    t_send,
    t_recv,
    round_sem,
    plane_sem,
):
    tok = q_ref.shape[0]
    heads = lg_ref.shape[0]
    levels = lw_ref.shape[0]
    dk = q_ref.shape[1] // heads
    dv = v_ref.shape[1] // heads
    group = dk // dv
    pairs = heads // group
    spans = tok // SPAN
    span_bits = spans.bit_length() - 1
    bits = seq_count.bit_length() - 1
    half = heads // 2
    chunks = half // group
    cross = [min(span_bits + 1 + b, levels - 1) for b in range(bits)]
    slots = sorted(set(cross))
    kind = [1 + slots.index(l) for l in cross]
    place = lax.axis_index("seq")
    row = lax.axis_index("head")
    core, x, y = [(place // (1 << b)) % 2 for b in range(bits)]
    peer = [place + (1 - 2 * u) * (1 << b) for b, u in enumerate((core, x, y))]
    first_chip = (1 - x) * (1 - y)
    second_chip = x * (1 - y)
    mine = core * half
    theirs = (1 - core) * half

    has_next = (row < head_count - 1).astype(jnp.int32)
    has_last = (row > 0).astype(jnp.int32)

    def greet(sem):
        @pl.when(has_next == 1)
        def _():
            pl.semaphore_signal(sem, inc=1, device_id={"head": row + 1}, device_id_type=MESH)

        @pl.when(has_last == 1)
        def _():
            pl.semaphore_signal(sem, inc=1, device_id={"head": row - 1}, device_id_type=MESH)

    barrier = pltpu.get_barrier_semaphore()
    for b in reversed(range(bits)):
        pl.semaphore_signal(barrier, inc=1, device_id={"seq": peer[b]}, device_id_type=MESH)
    greet(barrier)

    def load(n):
        src = (lg_hbm, ds_hbm, v_hbm, k_hbm, g_hbm, lw_hbm, q_hbm)[n]
        dst = (lg_ref, ds_ref, v_ref, k_ref, g_ref, lw_ref, q_ref)[n]
        return pltpu.make_async_copy(src, dst, i_sem.at[n])

    for n in range(7):
        load(n).start()
    for n in range(2):
        load(n).wait()

    rows_i = lax.broadcasted_iota(jnp.int32, (tok, tok), 0)
    cols_i = lax.broadcasted_iota(jnp.int32, (tok, tok), 1)
    tri = (rows_i <= cols_i).astype(F32)
    starts = jnp.broadcast_to(ds_ref[...].astype(F32), (8, tok))
    both = jnp.concatenate([lg_ref[...], starts], axis=0)
    cum_all = lax.dot_general(
        both, tri, NN, precision=lax.Precision.HIGHEST, preferred_element_type=F32
    )
    cum_t = jnp.transpose(
        jnp.concatenate([cum_all, jnp.zeros((dk - heads - 8, tok), F32)], axis=0)
    )
    cum = cum_all[:heads]
    reset = cum_all[heads : heads + 1]
    reset_col = cum_t[:, heads : heads + 1]
    bias_s[...] = jnp.where((rows_i <= cols_i) & (reset == reset_col), 0.0, -1e30)
    end = cum[:, tok - 1 : tok]
    reset_end = reset[:, tok - 1 : tok]
    cum_s[...] = cum
    lead_s[...] = jnp.where(reset == 0, jnp.exp(cum), 0.0)
    tail_s[...] = jnp.where(reset == reset_end, jnp.exp(end - cum), 0.0)
    lane_row = lax.broadcasted_iota(jnp.int32, (1, dk), 1)
    end_row = jnp.where(lane_row < heads, cum_t[tok - 1 : tok, :], 0.0)
    decs[0] = jnp.where(reset_end == 0, jnp.exp(end_row), 0.0)
    for h in range(heads):
        col_s[h] = jnp.broadcast_to(cum_t[:, h : h + 1], (tok, tok))

    def states(p, _):
        lanes = pl.ds(pl.multiple_of(p * dk, dk), dk)
        vt = jnp.transpose(v_ref[:, lanes].astype(F32))
        gt = jnp.transpose(g_ref[:, lanes].astype(F32))
        vt_s[p] = vt.astype(BF16)
        gt_s[p] = gt.astype(BF16)
        for i in range(group):
            h = p * group + i
            wide = pl.ds(pl.multiple_of(h * dk, dk), dk)
            part = slice(i * dv, (i + 1) * dv)
            tail = tail_s[pl.ds(h, 1), :]
            lead = lead_s[pl.ds(h, 1), :]
            st[0, h] = dot_fine(vt[part] * tail, k_ref[:, wide], NN)
            gw = jnp.concatenate(
                [gt[part] * (lead * lw_ref[l, pl.ds(h, 1), :]) for l in slots], axis=0
            )
            back = dot_fine(gw, q_ref[:, wide], NN)
            for n in range(len(slots)):
                st[1 + n, h] = back[n * dv : (n + 1) * dv]
        return 0

    for n in range(2, 7):
        load(n).wait()
    lax.fori_loop(0, pairs, states, 0, unroll=2)
    pl.semaphore_wait(barrier, bits + has_next + has_last)
    rounds = head_count - 2
    if rounds > 0:
        greet(round_sem.at[0])

    def remote(src, dst, send, recv, b):
        return pltpu.make_async_remote_copy(
            src_ref=src,
            dst_ref=dst,
            send_sem=send,
            recv_sem=recv,
            device_id={"seq": peer[b]},
            device_id_type=MESH,
        )

    def of(base, c):
        return pl.ds(base + c * group, group)

    def at(c):
        return pl.ds(c * group, group)

    kind_a = y * kind[2]
    kind_b = x * kind[1]
    slot_out = bits - (bits - 1) * first_chip
    slot_in = bits - (bits - 1) * second_chip

    def dec_copy(n):
        return remote(decs.at[2 * n], decs.at[2 * n + 1], d_send.at[n], d_recv.at[n], n)

    def a_copy(c):
        return remote(
            st.at[kind_a, of(theirs, c)], got_a.at[at(c)], a_send.at[c], a_recv.at[c], 0
        )

    def b_copy(c):
        return remote(
            st.at[kind_b, of(theirs, c)], got_b.at[at(c)], b_send.at[c], b_recv.at[c], 0
        )

    def p_copy():
        return remote(st.at[core * kind[0]], lvl.at[0], p_send.at[0], p_recv.at[0], 0)

    def xa_copy(c):
        return remote(
            sum_a.at[at(c)], lvl.at[slot_out, of(mine, c)], xa_send.at[c], xa_recv.at[c], 1
        )

    def xb_copy(c):
        return remote(sum_b.at[at(c)], lvl.at[1, of(mine, c)], xb_send.at[c], xb_recv.at[c], 1)

    def y_copy(c):
        return remote(sum_q.at[at(c)], lvl.at[2, of(mine, c)], y_send.at[c], y_recv.at[c], 2)

    def f_copy(j, base, c):
        part = lvl.at[j, of(base, c)]
        return remote(part, part, f_send.at[j - 1, c], f_recv.at[j - 1, c], 0)

    dec_copy(0).start()
    for c in range(chunks):
        a_copy(c).start()

    @pl.when(first_chip == 0)
    def _():
        for c in range(chunks):
            b_copy(c).start()

    p_copy().start()

    span_of = lax.broadcasted_iota(jnp.int32, (1, tok), 1) // SPAN

    def local(p, _):
        vt = vt_s[p]
        gt = gt_s[p]
        lanes = pl.ds(pl.multiple_of(p * dk, dk), dk)
        v_blk = v_ref[:, lanes]
        for i in range(group):
            h = p * group + i
            wide = pl.ds(pl.multiple_of(h * dk, dk), dk)
            part = slice(i * dv, (i + 1) * dv)
            q = q_ref[:, wide]
            k = k_ref[:, wide]
            score = dot(k, q, NT)
            pair = dot(v_blk[:, part], gt[part], NN)
            decay = jnp.exp((cum_s[pl.ds(h, 1), :] - col_s[h]) + bias_s[...])
            seen = decay * score
            both_p = seen * pair
            gains = [lw_ref[l, pl.ds(h, 1), :] for l in range(span_bits + 1)]
            level_rows = [jnp.zeros((1, tok), F32) for _ in range(span_bits + 1)]
            mixed, graded = [], []
            for cs in range(spans):
                rows = slice(cs * SPAN, (cs + 1) * SPAN)
                total = jnp.sum(both_p[rows], axis=0, keepdims=True)
                gain = jnp.zeros((1, tok), F32)
                for ct in range(cs, spans):
                    l = span_level(cs, ct, levels)
                    hit = span_of == ct
                    gain = jnp.where(hit, gains[l], gain)
                    level_rows[l] = level_rows[l] + jnp.where(hit, total, 0.0)
                mixed.append(seen[rows] * gain)
                graded.append(decay[rows] * gain * pair[rows])
            mix = jnp.concatenate(mixed, axis=0).astype(BF16)
            grade = jnp.concatenate(graded, axis=0).astype(BF16)
            for l in range(span_bits + 1):
                gl_ref[l, pl.ds(h, 1), :] = level_rows[l]
            drift_s[pl.ds(h, 1), :] = jnp.sum(mix.astype(F32) * pair, axis=0, keepdims=True)
            vg_s[p, part] = dot(gt[part], mix, NT)
            gk_s[h] = dot(grade, q, NN)
            gq_s[h] = dot(grade, k, TN)
        return 0

    def spread(device_rows):
        t = jnp.transpose(
            jnp.concatenate(
                device_rows + [jnp.zeros((8 - len(device_rows), dk), F32)], axis=0
            )
        )
        return [
            jnp.broadcast_to(t[:heads, n : n + 1], (heads, dk)) for n in range(len(device_rows))
        ]

    def weigh(n, swap, own, got):
        w = (swap % 2).astype(F32)
        mix_s[n, 0] = own * (1.0 - w) + w
        mix_s[n, 1] = got * w + (1.0 - w)

    def combine(n, c, own_at, got_at, put):
        for i in range(group):
            r = c * group + i
            ca = mix_s[n, 0, pl.ds(mine + r, 1), :]
            cb = mix_s[n, 1, pl.ds(mine + r, 1), :]
            put[r] = ca * own_at(r) + cb * got_at(r)

    lax.fori_loop(0, 2, local, 0, unroll=2)

    dec_copy(0).wait_recv()
    decs[2] = decs[0] * decs[1]
    d_self, d_pair = spread([decs[0], decs[1]])
    weigh(0, core + y, d_pair, d_self)
    weigh(1, core + x, d_pair, d_self)
    for c in range(chunks):
        a_copy(c).wait_recv()
        combine(0, c, lambda r: st[kind_a, mine + r], lambda r: got_a[r], sum_a)
        xa_copy(c).start()

    dec_copy(1).start()

    @pl.when(first_chip == 0)
    def _():
        for c in range(chunks):
            b_copy(c).wait_recv()
            combine(1, c, lambda r: st[kind_b, mine + r], lambda r: got_b[r], sum_b)
            xb_copy(c).start()

    lax.fori_loop(2, pairs - 2, local, 0, unroll=2)

    for r in range(1, rounds + 1):
        pl.semaphore_wait(round_sem.at[r - 1], has_next + has_last)
        if r < rounds:
            greet(round_sem.at[r])
    dec_copy(1).wait_recv()
    (d_side,) = spread([decs[3]])
    weigh(2, x + y, d_side, d_self * d_pair)
    inner_f = jnp.ones((heads, dk), F32)
    inner_b = jnp.ones((heads, dk), F32)
    for b, (u, got) in enumerate(((core, d_pair), (x, d_side), (y, None))):
        up = u.astype(F32)
        coef_s[0, b] = inner_f * up
        coef_s[1, b] = inner_b * (1.0 - up)
        if got is not None:
            inner_f = inner_f * (up * got + (1.0 - up))
            inner_b = inner_b * ((1.0 - up) * got + up)

    for c in range(chunks):
        xa_copy(c).wait_recv()
        combine(2, c, lambda r: sum_a[r], lambda r: lvl[slot_in, mine + r], sum_q)
        y_copy(c).start()

        @pl.when(second_chip == 1)
        def _(c=c):
            f_copy(1, mine, c).start()

        if c == 0:
            lax.fori_loop(pairs - 2, pairs, local, 0, unroll=2)

    def incoming(h):
        blocks = [lvl[b, h] for b in range(bits)]
        entering = []
        for n in range(len(slots)):
            terms = [
                coef_s[0, b, pl.ds(h, 1), :] * blocks[b]
                for b in range(bits)
                if kind[b] == 1 + n
            ]
            entering.append(functools.reduce(jnp.add, terms))
        after = functools.reduce(
            jnp.add, [coef_s[1, b, pl.ds(h, 1), :] * blocks[b] for b in range(bits)]
        )
        return split(jnp.concatenate(entering, axis=0)), split(after)

    def finish_drift(p):
        vt = vt_s[p].astype(F32)
        gt = gt_s[p].astype(F32)
        for i in range(group):
            h = p * group + i
            wide = pl.ds(pl.multiple_of(h * dk, dk), dk)
            part = slice(i * dv, (i + 1) * dv)
            q = q_ref[:, wide]
            k = k_ref[:, wide]
            tail = tail_s[pl.ds(h, 1), :]
            lead = lead_s[pl.ds(h, 1), :]
            (e_high, e_low), (a_high, a_low) = incoming(h)
            seen = dot(e_high, q, NT) + dot(e_low, q, NT)
            drift = drift_s[pl.ds(h, 1), :]
            for n, l in enumerate(slots):
                level = lead * jnp.sum(
                    seen[n * dv : (n + 1) * dv] * gt[part], axis=0, keepdims=True
                )
                gl_ref[l, pl.ds(h, 1), :] = level
                drift = drift + lw_ref[l, pl.ds(h, 1), :] * level
            vg = vg_s[p, part] + tail * (dot(a_high, k, NT) + dot(a_low, k, NT))
            drift_s[pl.ds(h, 1), :] = drift - jnp.sum(vg * vt[part], axis=0, keepdims=True)
            vg_s[p, part] = vg

    def finish_out(p):
        lanes = pl.ds(pl.multiple_of(p * dk, dk), dk)
        vt = vt_s[p].astype(F32)
        gt = gt_s[p].astype(F32)
        for i in range(group):
            h = p * group + i
            wide = pl.ds(pl.multiple_of(h * dk, dk), dk)
            part = slice(i * dv, (i + 1) * dv)
            tail = tail_s[pl.ds(h, 1), :]
            lead = lead_s[pl.ds(h, 1), :]
            (e_high, e_low), (a_high, a_low) = incoming(h)
            gws = [gt[part] * (lead * lw_ref[l, pl.ds(h, 1), :]) for l in slots]
            gw, gw_low = split(jnp.concatenate(gws, axis=0))
            gq_in = dot(gw, e_high, TN) + dot(gw, e_low, TN) + dot(gw_low, e_high, TN)
            gq_ref[:, wide] = (gq_s[h] + gq_in).astype(BF16)
            tv, tv_low = split(vt[part] * tail)
            gk_in = dot(tv, a_high, TN) + dot(tv, a_low, TN) + dot(tv_low, a_high, TN)
            gk_ref[:, wide] = (gk_s[h] + gk_in).astype(BF16)
        gv_ref[:, lanes] = jnp.transpose(vg_s[p]).astype(BF16)

    own_pair = core * chunks
    far_pair = (1 - core) * chunks
    p_copy().wait_recv()
    for c in range(chunks):

        @pl.when(second_chip == 0)
        def _(c=c):
            xb_copy(c).wait_recv()
            f_copy(1, mine, c).start()

        y_copy(c).wait_recv()
        f_copy(2, mine, c).start()
        if c == 0:
            for o in range(1, head_count):
                pl.semaphore_signal(
                    plane_sem,
                    inc=1,
                    device_id={"head": (row + o) % head_count},
                    device_id_type=MESH,
                )
        finish_drift(own_pair + c)
        if c < chunks - 1:
            finish_out(own_pair + c)
        for j in (1, 2):
            f_copy(j, theirs, c).wait_recv()
        finish_drift(far_pair + c)
        if c < chunks - 1:
            finish_out(far_pair + c)

    later = (rows_i >= cols_i).astype(F32)
    local_tail = lax.dot_general(
        drift_s[...], later, NN, precision=lax.Precision.HIGHEST, preferred_element_type=F32
    )
    lane = lax.broadcasted_iota(jnp.int32, (heads, tok), 1)
    head = lax.broadcasted_iota(jnp.int32, (heads, tok), 0)
    sums = [
        local_tail[:, 0:1],
        jnp.sum(local_tail, axis=1, keepdims=True),
        jnp.sum(local_tail * local_tail, axis=1, keepdims=True),
    ]
    packed = jnp.zeros((heads, tok), F32)
    for n, column in enumerate(sums):
        packed = jnp.where(lane == head + n * heads, column, packed)
    slot = row * seq_count + place
    total = seq_count * head_count
    msg[slot] = jnp.sum(packed, axis=0, keepdims=True)

    def tail_copy(to_row, to_place):
        return pltpu.make_async_remote_copy(
            src_ref=msg.at[slot],
            dst_ref=msg.at[slot],
            send_sem=t_send.at[0],
            recv_sem=t_recv.at[0],
            device_id={"seq": to_place, "head": to_row},
            device_id_type=MESH,
        )

    def tail_all():
        others = msg.at[pl.ds(0, total - 1)]
        return pltpu.make_async_remote_copy(
            src_ref=others,
            dst_ref=others,
            send_sem=t_send.at[0],
            recv_sem=t_recv.at[0],
            device_id={"seq": peer[0]},
            device_id_type=MESH,
        )

    pl.semaphore_wait(plane_sem, head_count - 1)
    for o in reversed(range(head_count)):
        for n in reversed(range(seq_count)):
            if (o, n) != (0, 0):
                tail_copy((row + o) % head_count, (place + n) % seq_count).start()

    finish_out(own_pair + chunks - 1)
    finish_out(far_pair + chunks - 1)
    for l in range(levels):
        if l > span_bits and l not in slots:
            gl_ref[l] = jnp.zeros((heads, tok), F32)

    for n in range(2):
        dec_copy(n).wait_send()
    p_copy().wait_send()
    for c in range(chunks):
        a_copy(c).wait_send()
        xa_copy(c).wait_send()
        y_copy(c).wait_send()
        for j in (1, 2):
            f_copy(j, mine, c).wait_send()

    @pl.when(first_chip == 0)
    def _():
        for c in range(chunks):
            b_copy(c).wait_send()
            xb_copy(c).wait_send()

    tail_all().wait_send()
    tail_all().wait_recv()
    rows = msg[:, 0, :]
    row_u = lax.broadcasted_iota(jnp.int32, (total, total), 0)
    row_v = lax.broadcasted_iota(jnp.int32, (total, total), 1)
    behind = (row_u // seq_count == row_v // seq_count) & (row_v > row_u)
    after_rows = lax.dot_general(
        behind.astype(F32), rows, NN, precision=lax.Precision.HIGHEST, preferred_element_type=F32
    )
    plain = pltpu.roll(rows, dk - heads, 1)
    square = pltpu.roll(rows, dk - 2 * heads, 1)
    energy = square + after_rows * (2.0 * plain + tok * after_rows)
    lane_all = lax.broadcasted_iota(jnp.int32, (total, dk), 1)
    slot_all = lax.broadcasted_iota(jnp.int32, (total, dk), 0)
    energy = jnp.sum(jnp.where(lane_all < heads, energy, 0.0), axis=0, keepdims=True)
    whole = jnp.sum(energy, axis=1, keepdims=True)
    my_row = jnp.sum(jnp.where(slot_all == slot, after_rows, 0.0), axis=0, keepdims=True)
    my_later = jnp.sum(jnp.where(lane == head, my_row, 0.0), axis=1, keepdims=True)
    count = heads * tok * total
    factor = jnp.minimum(1.0, lax.rsqrt(whole / count + 1e-6))
    gg_ref[...] = (local_tail + my_later) * factor


def write_out(count, *refs):
    sems = refs[-1]
    copies = [
        pltpu.make_async_copy(refs[i], refs[count + i], sems.at[i]) for i in range(count)
    ]
    for c in copies:
        c.start()
    for c in copies:
        c.wait()


def shards(seq_count, head_count, queries, keys, values, out_grad, log_gate, level_weight, doc_start):
    tok = queries.shape[0]
    heads = log_gate.shape[0]
    levels = level_weight.shape[0]
    dk = queries.shape[1] // heads
    dv = values.shape[1] // heads
    group = dk // dv
    pairs = heads // group
    bits = seq_count.bit_length() - 1
    half = heads // 2
    span_bits = (tok // SPAN).bit_length() - 1
    slots = len({min(span_bits + 1 + b, levels - 1) for b in range(bits)})
    dma = pltpu.SemaphoreType.DMA
    vmem = pltpu.VMEM
    block = (dv, dk)
    scratch = [
        vmem((heads, tok), F32),
        vmem((heads, tok, tok), F32),
        vmem((heads, tok), F32),
        vmem((heads, tok), F32),
        vmem((tok, tok), F32),
        vmem((pairs, group * dv, tok), BF16),
        vmem((pairs, group * dv, tok), BF16),
        vmem((pairs, group * dv, tok), F32),
        vmem((heads, tok, dk), F32),
        vmem((heads, tok, dk), F32),
        vmem((heads, tok), F32),
        vmem((2, bits, heads, dk), F32),
        vmem((heads,) + block, F32),
        vmem((slots, heads) + block, F32),
        vmem((bits, heads) + block, F32),
        vmem((bits, half) + block, F32),
        vmem((bits, bits, half) + block, F32),
        vmem((bits, half) + block, F32),
        vmem((bits, bits, half) + block, F32),
        vmem((bits + 1, heads, dk), F32),
        vmem((bits, heads, dk), F32),
        vmem((seq_count, heads, tok), F32),
        vmem((head_count, 8, dk), F32),
        dma((bits, 2)),
        dma((bits, 2)),
        dma((bits,)),
        dma((bits,)),
        dma((bits,)),
        dma((bits,)),
        dma((bits, bits)),
        dma((bits, bits)),
        dma((bits,)),
        dma((bits,)),
        dma((seq_count,)),
        dma((seq_count,)),
        dma((head_count,)),
        dma((head_count,)),
    ]
    args = (queries, keys, values, out_grad, log_gate, level_weight, doc_start.reshape(1, tok))
    spec = pl.BlockSpec(memory_space=pltpu.VMEM)
    in_spec = spec
    body = kernel
    chunks = half // group
    if bits == 3 and chunks * group == half and tok == dk and 3 * heads <= dk:
        body = chunked_kernel
        inputs = [(x.shape, x.dtype) for x in args]
        scratch = [vmem(*x) for x in inputs] + scratch[:12] + [
            vmem((3, 2, heads, dk), F32),
            vmem((1 + slots, heads) + block, F32),
            vmem((half,) + block, F32),
            vmem((half,) + block, F32),
            vmem((half,) + block, F32),
            vmem((half,) + block, F32),
            vmem((half,) + block, F32),
            vmem((bits + 1, heads) + block, F32),
            vmem((4, 1, dk), F32),
            vmem((seq_count * head_count, 1, dk), F32),
            dma((7,)),
            dma((chunks,)),
            dma((chunks,)),
            dma((chunks,)),
            dma((chunks,)),
            dma((1,)),
            dma((1,)),
            dma((chunks,)),
            dma((chunks,)),
            dma((chunks,)),
            dma((chunks,)),
            dma((chunks,)),
            dma((chunks,)),
            dma((2, chunks)),
            dma((2, chunks)),
            dma((2,)),
            dma((2,)),
            dma((1,)),
            dma((1,)),
            pltpu.SemaphoreType.REGULAR((max(1, head_count - 2),)),
            pltpu.SemaphoreType.REGULAR,
        ]
        in_spec = pl.BlockSpec(memory_space=pltpu.HBM)
    outs = [
        (queries.shape, BF16),
        (keys.shape, BF16),
        (values.shape, BF16),
        (level_weight.shape, F32),
        (log_gate.shape, F32),
    ]
    results = pl.pallas_call(
        functools.partial(body, seq_count, head_count),
        out_shape=tuple(vmem(shape, dtype) for shape, dtype in outs),
        in_specs=[in_spec] * 7,
        out_specs=(spec,) * 5,
        scratch_shapes=scratch,
        compiler_params=pltpu.CompilerParams(collective_id=0, has_side_effects=True),
    )(*args)
    count = len(outs)
    return pl.pallas_call(
        functools.partial(write_out, count),
        out_shape=tuple(jax.ShapeDtypeStruct(shape, dtype) for shape, dtype in outs),
        in_specs=[spec] * count,
        out_specs=(pl.BlockSpec(memory_space=pltpu.HBM),) * count,
        scratch_shapes=[dma((count,))],
    )(*[pltpu.with_memory_space_constraint(r, pltpu.VMEM) for r in results])


def solution(mesh):
    return jax.shard_map(
        functools.partial(shards, mesh.shape["seq"], mesh.shape["head"]),
        mesh=mesh,
        in_specs=(
            P("seq", "head"),
            P("seq", "head"),
            P("seq", "head"),
            P("seq", "head"),
            P("head", "seq"),
            P(None, "head", "seq"),
            P("seq"),
        ),
        out_specs=(
            P("seq", "head"),
            P("seq", "head"),
            P("seq", "head"),
            P(None, "head", "seq"),
            P("head", "seq"),
        ),
        check_vma=False,
    )
```

```python
import functools

import jax
import jax.numpy as jnp
from jax import lax
from jax.experimental import pallas as pl
from jax.experimental.pallas import tpu as pltpu
from jax.sharding import PartitionSpec as P

SPAN = 64
F32 = jnp.float32
BF16 = jnp.bfloat16
NN = (((1,), (0,)), ((), ()))
NT = (((1,), (1,)), ((), ()))
TN = (((0,), (0,)), ((), ()))
MESH = pl.DeviceIdType.MESH


def dot(a, b, dims):
    return lax.dot_general(a, b, dims, preferred_element_type=F32)


def split(x):
    high = x.astype(BF16)
    return high, (x - high.astype(F32)).astype(BF16)


def dot_fine(x, b, dims):
    high, low = split(x)
    return dot(high, b, dims) + dot(low, b, dims)


def span_level(a, b, levels):
    return 0 if a == b else min(levels - 1, (a ^ b).bit_length())


def kernel(
    seq_count,
    head_count,
    q_ref,
    k_ref,
    v_ref,
    g_ref,
    lg_ref,
    lw_ref,
    ds_ref,
    gq_ref,
    gk_ref,
    gv_ref,
    gl_ref,
    gg_ref,
    cum_s,
    col_s,
    lead_s,
    tail_s,
    bias_s,
    vt_s,
    gt_s,
    vg_s,
    gq_s,
    gk_s,
    drift_s,
    coef_s,
    state_s,
    back_s,
    lvl,
    got_s,
    got_u,
    sum_s,
    sum_u,
    dec,
    got_dec,
    tot,
    sq,
    lvl_send,
    lvl_recv,
    fwd_send,
    fwd_recv,
    s_send,
    s_recv,
    u_send,
    u_recv,
    d_send,
    d_recv,
    t_send,
    t_recv,
    q_send,
    q_recv,
):
    tok = q_ref.shape[0]
    heads = lg_ref.shape[0]
    levels = lw_ref.shape[0]
    dk = q_ref.shape[1] // heads
    dv = v_ref.shape[1] // heads
    group = dk // dv
    pairs = heads // group
    spans = tok // SPAN
    span_bits = spans.bit_length() - 1
    bits = seq_count.bit_length() - 1
    half = heads // 2
    cross = [min(span_bits + 1 + b, levels - 1) for b in range(bits)]
    slots = sorted(set(cross))
    place = lax.axis_index("seq")
    row = lax.axis_index("head")
    bit = [(place // (1 << b)) % 2 for b in range(bits)]
    peer = [place + (1 - 2 * bit[b]) * (1 << b) for b in range(bits)]
    want_s = [(place // (2 << b)) != (seq_count // (2 << b)) - 1 for b in range(bits)]
    mine = bit[0] * half
    theirs = (1 - bit[0]) * half

    barrier = pltpu.get_barrier_semaphore()
    for o in range(1, seq_count):
        pl.semaphore_signal(
            barrier, inc=1, device_id={"seq": (place + o) % seq_count}, device_id_type=MESH
        )
    for o in range(1, head_count):
        pl.semaphore_signal(
            barrier, inc=1, device_id={"head": (row + o) % head_count}, device_id_type=MESH
        )

    rows_i = lax.broadcasted_iota(jnp.int32, (tok, tok), 0)
    cols_i = lax.broadcasted_iota(jnp.int32, (tok, tok), 1)
    tri = (rows_i <= cols_i).astype(F32)
    starts = jnp.broadcast_to(ds_ref[...].astype(F32), (8, tok))
    both = jnp.concatenate([lg_ref[...], starts], axis=0)
    cum_all = lax.dot_general(
        both, tri, NN, precision=lax.Precision.HIGHEST, preferred_element_type=F32
    )
    cum_t = jnp.transpose(cum_all)
    cum = cum_all[:heads]
    reset = cum_all[heads : heads + 1]
    reset_col = cum_t[:, heads : heads + 1]
    bias_s[...] = jnp.where((rows_i <= cols_i) & (reset == reset_col), 0.0, -1e30)
    end = cum[:, tok - 1 : tok]
    reset_end = reset[:, tok - 1 : tok]
    cum_s[...] = cum
    lead_s[...] = jnp.where(reset == 0, jnp.exp(cum), 0.0)
    tail_s[...] = jnp.where(reset == reset_end, jnp.exp(end - cum), 0.0)
    dec[0] = jnp.broadcast_to(jnp.where(reset_end == 0, jnp.exp(end), 0.0), (heads, dk))
    for h in range(heads):
        col_s[h] = jnp.broadcast_to(cum_t[:, h : h + 1], (tok, tok))

    def states(p, _):
        lanes = pl.ds(pl.multiple_of(p * dk, dk), dk)
        vt = jnp.transpose(v_ref[:, lanes].astype(F32))
        gt = jnp.transpose(g_ref[:, lanes].astype(F32))
        vt_s[p] = vt.astype(BF16)
        gt_s[p] = gt.astype(BF16)
        for i in range(group):
            h = p * group + i
            wide = pl.ds(pl.multiple_of(h * dk, dk), dk)
            part = slice(i * dv, (i + 1) * dv)
            tail = tail_s[pl.ds(h, 1), :]
            lead = lead_s[pl.ds(h, 1), :]
            state_s[h] = dot_fine(vt[part] * tail, k_ref[:, wide], NN)
            gw = jnp.concatenate(
                [gt[part] * (lead * lw_ref[l, pl.ds(h, 1), :]) for l in slots], axis=0
            )
            back = dot_fine(gw, q_ref[:, wide], NN)
            for n in range(len(slots)):
                back_s[n, h] = back[n * dv : (n + 1) * dv]
        return 0

    lax.fori_loop(0, pairs, states, 0, unroll=2)
    pl.semaphore_wait(barrier, seq_count - 1 + head_count - 1)

    def slot(b):
        return slots.index(cross[b])

    def remote(src, dst, send, recv, b):
        return pltpu.make_async_remote_copy(
            src_ref=src,
            dst_ref=dst,
            send_sem=send,
            recv_sem=recv,
            device_id={"seq": peer[b]},
            device_id_type=MESH,
        )

    own = pl.ds(mine, half)
    other = pl.ds(theirs, half)

    def u_copy(b, j):
        src = back_s.at[slot(j), other] if b == 0 else sum_u.at[b, j]
        return remote(src, got_u.at[b, j], u_send.at[b, j], u_recv.at[b, j], b)

    def s_copy(b):
        src = state_s.at[other] if b == 0 else sum_s.at[b]
        return remote(src, got_s.at[b], s_send.at[b], s_recv.at[b], b)

    def d_copy(b):
        return remote(dec.at[b], got_dec.at[b], d_send.at[b], d_recv.at[b], b)

    def level_copy(b, low):
        if b == 0:
            src = state_s if low else back_s.at[slot(0)]
            return [
                remote(src.at[part], lvl.at[0, part], lvl_send.at[0, n], lvl_recv.at[0, n], 0)
                for n, part in enumerate((other, own))
            ]
        src = sum_s.at[b] if low else sum_u.at[b, b]
        return [remote(src, lvl.at[b, own], lvl_send.at[b, 0], lvl_recv.at[b, 0], b)]

    def level_wait(b, n):
        part = other if n == 1 else own
        return remote(
            lvl.at[b, part], lvl.at[b, part], lvl_send.at[b, n], lvl_recv.at[b, n], b
        )

    def forward_copy(b, part):
        return remote(lvl.at[b, part], lvl.at[b, part], fwd_send.at[b], fwd_recv.at[b], 0)

    def land(b):
        up_summed = (bit[b] == 1) & want_s[b]

        @pl.when(jnp.logical_not(up_summed))
        def _():
            level_wait(b, 0).wait_recv()

        if b > 0:
            forward_copy(b, own).start()

    def begin(b):
        d_copy(b).start()

        early = 0 if b in (0, bits - 1) else 1

        @pl.when((bit[b] == 0) & (want_s[b] | (early == 0)))
        def _():
            for c in level_copy(b, True):
                c.start()

        if b < bits - 1:

            @pl.when((bit[b] == 1) & want_s[b])
            def _():
                s_copy(b).start()

            for j in range(b + 1, bits):

                @pl.when(bit[j] == 1)
                def _(j=j):
                    u_copy(b, j).start()

        if early == 0:

            @pl.when(bit[b] == 1)
            def _():
                for c in level_copy(b, False):
                    c.start()

    def begin_late(b):
        if b in (0, bits - 1):
            return

        @pl.when((bit[b] == 0) & jnp.logical_not(want_s[b]))
        def _():
            for c in level_copy(b, True):
                c.start()

        @pl.when(bit[b] == 1)
        def _():
            for c in level_copy(b, False):
                c.start()

    def join(b):
        d_copy(b).wait_recv()
        up = bit[b].astype(F32)
        got = got_dec[b]
        now = dec[b]
        dec[b + 1] = got * now
        if b == bits - 1:
            return
        base_s = state_s.at[own] if b == 0 else sum_s.at[b]

        @pl.when(want_s[b])
        def _():
            @pl.when(bit[b] == 1)
            def _():
                level_wait(b, 0).wait_recv()

                def body(i, _):
                    d = dec[b, pl.ds(mine + i, 1), :]
                    sum_s[b + 1, i] = d * lvl[b, mine + i] + base_s[i]
                    return 0

                lax.fori_loop(0, half, body, 0, unroll=True)

            @pl.when(bit[b] == 0)
            def _():
                s_copy(b).wait_recv()

                def body(i, _):
                    d = got_dec[b, pl.ds(mine + i, 1), :]
                    sum_s[b + 1, i] = d * base_s[i] + got_s[b, i]
                    return 0

                lax.fori_loop(0, half, body, 0, unroll=True)

        for j in range(b + 1, bits):
            base_u = back_s.at[slot(j), own] if b == 0 else sum_u.at[b, j]

            @pl.when(bit[j] == 1)
            def _(j=j, base_u=base_u):
                u_copy(b, j).wait_recv()

                def body(i, _):
                    d0 = dec[b, pl.ds(mine + i, 1), :]
                    d1 = got_dec[b, pl.ds(mine + i, 1), :]
                    a = up * d1 + (1.0 - up)
                    c = (1.0 - up) * d0 + up
                    sum_u[b + 1, j, i] = a * base_u[i] + c * got_u[b, j, i]
                    return 0

                lax.fori_loop(0, half, body, 0, unroll=True)

    span_of = lax.broadcasted_iota(jnp.int32, (1, tok), 1) // SPAN

    def local(p, _):
        vt = vt_s[p]
        gt = gt_s[p]
        lanes = pl.ds(pl.multiple_of(p * dk, dk), dk)
        v_blk = v_ref[:, lanes]
        for i in range(group):
            h = p * group + i
            wide = pl.ds(pl.multiple_of(h * dk, dk), dk)
            part = slice(i * dv, (i + 1) * dv)
            q = q_ref[:, wide]
            k = k_ref[:, wide]
            score = dot(k, q, NT)
            pair = dot(v_blk[:, part], gt[part], NN)
            decay = jnp.exp((cum_s[pl.ds(h, 1), :] - col_s[h]) + bias_s[...])
            seen = decay * score
            both_p = seen * pair
            gains = [lw_ref[l, pl.ds(h, 1), :] for l in range(span_bits + 1)]
            level_rows = [jnp.zeros((1, tok), F32) for _ in range(span_bits + 1)]
            mixed, graded = [], []
            for cs in range(spans):
                rows = slice(cs * SPAN, (cs + 1) * SPAN)
                total = jnp.sum(both_p[rows], axis=0, keepdims=True)
                gain = jnp.zeros((1, tok), F32)
                for ct in range(cs, spans):
                    l = span_level(cs, ct, levels)
                    hit = span_of == ct
                    gain = jnp.where(hit, gains[l], gain)
                    level_rows[l] = level_rows[l] + jnp.where(hit, total, 0.0)
                mixed.append(seen[rows] * gain)
                graded.append(decay[rows] * gain * pair[rows])
            mix = jnp.concatenate(mixed, axis=0).astype(BF16)
            grade = jnp.concatenate(graded, axis=0).astype(BF16)
            for l in range(span_bits + 1):
                gl_ref[l, pl.ds(h, 1), :] = level_rows[l]
            drift_s[pl.ds(h, 1), :] = jnp.sum(mix.astype(F32) * pair, axis=0, keepdims=True)
            vg_s[p, part] = dot(gt[part], mix, NT)
            gk_s[h] = dot(grade, q, NN)
            gq_s[h] = dot(grade, k, TN)
        return 0

    begin(0)
    lax.fori_loop(0, pairs // 4, local, 0, unroll=2)
    join(0)
    if bits > 1:
        begin(1)
    lax.fori_loop(pairs // 4, pairs, local, 0, unroll=2)
    for b in range(1, bits):
        join(b)
        if b + 1 < bits:
            begin(b + 1)
        begin_late(b)
        land(b - 1)
    land(bits - 1)

    inner_f = jnp.ones((heads, dk), F32)
    inner_b = jnp.ones((heads, dk), F32)
    for b in range(bits):
        up = bit[b].astype(F32)
        got = got_dec[b]
        coef_s[0, b] = inner_f * up
        coef_s[1, b] = inner_b * (1.0 - up)
        inner_f = inner_f * (up * got + (1.0 - up))
        inner_b = inner_b * ((1.0 - up) * got + up)
    level_wait(0, 1).wait_recv()
    for b in range(1, bits):
        forward_copy(b, other).wait_recv()

    def finish(p, _):
        lanes = pl.ds(pl.multiple_of(p * dk, dk), dk)
        vt = vt_s[p].astype(F32)
        gt = gt_s[p].astype(F32)
        vg_all = []
        for i in range(group):
            h = p * group + i
            wide = pl.ds(pl.multiple_of(h * dk, dk), dk)
            part = slice(i * dv, (i + 1) * dv)
            q = q_ref[:, wide]
            k = k_ref[:, wide]
            tail = tail_s[pl.ds(h, 1), :]
            lead = lead_s[pl.ds(h, 1), :]
            blocks = [lvl[b, h] for b in range(bits)]
            entering = []
            for n in range(len(slots)):
                terms = [
                    coef_s[0, b, pl.ds(h, 1), :] * blocks[b] for b in range(bits) if slot(b) == n
                ]
                entering.append(functools.reduce(jnp.add, terms))
            entering = jnp.concatenate(entering, axis=0)
            after = functools.reduce(
                jnp.add, [coef_s[1, b, pl.ds(h, 1), :] * blocks[b] for b in range(bits)]
            )
            e_high, e_low = split(entering)
            seen = dot(e_high, q, NT) + dot(e_low, q, NT)
            drift = drift_s[pl.ds(h, 1), :]
            gws = []
            for n, l in enumerate(slots):
                gain = lw_ref[l, pl.ds(h, 1), :]
                level = lead * jnp.sum(
                    seen[n * dv : (n + 1) * dv] * gt[part], axis=0, keepdims=True
                )
                gl_ref[l, pl.ds(h, 1), :] = level
                drift = drift + gain * level
                gws.append(gt[part] * (lead * gain))
            gw, gw_low = split(jnp.concatenate(gws, axis=0))
            gq_in = dot(gw, e_high, TN) + dot(gw, e_low, TN) + dot(gw_low, e_high, TN)
            gq_ref[:, wide] = (gq_s[h] + gq_in).astype(BF16)
            a_high, a_low = split(after)
            tv, tv_low = split(vt[part] * tail)
            gk_in = dot(tv, a_high, TN) + dot(tv, a_low, TN) + dot(tv_low, a_high, TN)
            gk_ref[:, wide] = (gk_s[h] + gk_in).astype(BF16)
            vg = vg_s[p, part] + tail * (dot(a_high, k, NT) + dot(a_low, k, NT))
            drift_s[pl.ds(h, 1), :] = drift - jnp.sum(vg * vt[part], axis=0, keepdims=True)
            vg_all.append(vg)
        gv_ref[:, lanes] = jnp.transpose(jnp.concatenate(vg_all, axis=0)).astype(BF16)
        return 0

    lax.fori_loop(0, pairs, finish, 0, unroll=2)
    for l in range(levels):
        if l > span_bits and l not in slots:
            gl_ref[l] = jnp.zeros((heads, tok), F32)

    later = (rows_i >= cols_i).astype(F32)
    local_tail = lax.dot_general(
        drift_s[...], later, NN, precision=lax.Precision.HIGHEST, preferred_element_type=F32
    )
    lane = lax.broadcasted_iota(jnp.int32, (heads, tok), 1)
    first = local_tail[:, 0:1]
    plain = jnp.sum(local_tail, axis=1, keepdims=True)
    square = jnp.sum(local_tail * local_tail, axis=1, keepdims=True)
    tot[place] = jnp.where(lane == 0, first, jnp.where(lane == 1, plain, square))

    def tot_copy(o, slot_at):
        return pltpu.make_async_remote_copy(
            src_ref=tot.at[place],
            dst_ref=tot.at[slot_at],
            send_sem=t_send.at[o],
            recv_sem=t_recv.at[slot_at],
            device_id={"seq": (place + o) % seq_count},
            device_id_type=MESH,
        )

    for o in range(1, seq_count):
        tot_copy(o, place).start()
    for o in range(1, seq_count):
        tot_copy(o, (place + o) % seq_count).wait_recv()
    after_total = jnp.zeros((heads, 1), F32)
    my_later = jnp.zeros((heads, 1), F32)
    energy = jnp.zeros((heads, 1), F32)
    for d in reversed(range(seq_count)):
        piece = tot[d]
        my_later = my_later + jnp.where(place == d, 1.0, 0.0) * after_total
        energy = energy + (
            piece[:, 2:3] + after_total * (2.0 * piece[:, 1:2] + tok * after_total)
        )
        after_total = after_total + piece[:, 0:1]
    energy = jnp.sum(jnp.broadcast_to(energy, (heads, dk)), axis=0, keepdims=True)
    sq[row] = jnp.broadcast_to(energy, (8, dk))

    def sq_copy(o, slot_at):
        return pltpu.make_async_remote_copy(
            src_ref=sq.at[row],
            dst_ref=sq.at[slot_at],
            send_sem=q_send.at[o],
            recv_sem=q_recv.at[slot_at],
            device_id={"head": (row + o) % head_count},
            device_id_type=MESH,
        )

    for o in range(1, head_count):
        sq_copy(o, row).start()
    for o in range(1, head_count):
        sq_copy(o, (row + o) % head_count).wait_recv()
    whole = sq[0]
    for r in range(1, head_count):
        whole = whole + sq[r]
    count = heads * tok * seq_count * head_count
    factor = jnp.minimum(1.0, lax.rsqrt(whole[0:1] / count + 1e-6))
    gg_ref[...] = (local_tail + my_later) * factor

    for b in range(bits):
        d_copy(b).wait_send()
        for n in range(2 if b == 0 else 1):
            level_wait(b, n).wait_send()
        if b > 0:
            forward_copy(b, own).wait_send()
        if b < bits - 1:

            @pl.when((bit[b] == 1) & want_s[b])
            def _(b=b):
                s_copy(b).wait_send()

            for j in range(b + 1, bits):

                @pl.when(bit[j] == 1)
                def _(b=b, j=j):
                    u_copy(b, j).wait_send()

    for o in range(1, seq_count):
        tot_copy(o, place).wait_send()
    for o in range(1, head_count):
        sq_copy(o, row).wait_send()


def chunked_kernel(
    seq_count,
    head_count,
    q_hbm,
    k_hbm,
    v_hbm,
    g_hbm,
    lg_hbm,
    lw_hbm,
    ds_hbm,
    gq_ref,
    gk_ref,
    gv_ref,
    gl_ref,
    gg_ref,
    q_ref,
    k_ref,
    v_ref,
    g_ref,
    lg_ref,
    lw_ref,
    ds_ref,
    cum_s,
    col_s,
    lead_s,
    tail_s,
    bias_s,
    vt_s,
    gt_s,
    vg_s,
    gq_s,
    gk_s,
    drift_s,
    coef_s,
    mix_s,
    st,
    got_a,
    got_b,
    sum_a,
    sum_b,
    sum_q,
    lvl,
    decs,
    msg,
    i_sem,
    a_send,
    a_recv,
    b_send,
    b_recv,
    p_send,
    p_recv,
    xa_send,
    xa_recv,
    xb_send,
    xb_recv,
    y_send,
    y_recv,
    f_send,
    f_recv,
    d_send,
    d_recv,
    t_send,
    t_recv,
    round_sem,
    plane_sem,
):
    tok = q_ref.shape[0]
    heads = lg_ref.shape[0]
    levels = lw_ref.shape[0]
    dk = q_ref.shape[1] // heads
    dv = v_ref.shape[1] // heads
    group = dk // dv
    pairs = heads // group
    spans = tok // SPAN
    span_bits = spans.bit_length() - 1
    bits = seq_count.bit_length() - 1
    half = heads // 2
    chunks = half // group
    cross = [min(span_bits + 1 + b, levels - 1) for b in range(bits)]
    slots = sorted(set(cross))
    kind = [1 + slots.index(l) for l in cross]
    place = lax.axis_index("seq")
    row = lax.axis_index("head")
    core, x, y = [(place // (1 << b)) % 2 for b in range(bits)]
    peer = [place + (1 - 2 * u) * (1 << b) for b, u in enumerate((core, x, y))]
    first_chip = (1 - x) * (1 - y)
    second_chip = x * (1 - y)
    mine = core * half
    theirs = (1 - core) * half

    has_next = (row < head_count - 1).astype(jnp.int32)
    has_last = (row > 0).astype(jnp.int32)

    def greet(sem):
        @pl.when(has_next == 1)
        def _():
            pl.semaphore_signal(sem, inc=1, device_id={"head": row + 1}, device_id_type=MESH)

        @pl.when(has_last == 1)
        def _():
            pl.semaphore_signal(sem, inc=1, device_id={"head": row - 1}, device_id_type=MESH)

    barrier = pltpu.get_barrier_semaphore()
    for b in reversed(range(bits)):
        pl.semaphore_signal(barrier, inc=1, device_id={"seq": peer[b]}, device_id_type=MESH)
    greet(barrier)

    def load(n):
        src = (lg_hbm, ds_hbm, v_hbm, k_hbm, g_hbm, lw_hbm, q_hbm)[n]
        dst = (lg_ref, ds_ref, v_ref, k_ref, g_ref, lw_ref, q_ref)[n]
        return pltpu.make_async_copy(src, dst, i_sem.at[n])

    for n in range(7):
        load(n).start()
    for n in range(2):
        load(n).wait()

    rows_i = lax.broadcasted_iota(jnp.int32, (tok, tok), 0)
    cols_i = lax.broadcasted_iota(jnp.int32, (tok, tok), 1)
    tri = (rows_i <= cols_i).astype(F32)
    starts = jnp.broadcast_to(ds_ref[...].astype(F32), (8, tok))
    both = jnp.concatenate([lg_ref[...], starts], axis=0)
    cum_all = lax.dot_general(
        both, tri, NN, precision=lax.Precision.HIGHEST, preferred_element_type=F32
    )
    cum_t = jnp.transpose(
        jnp.concatenate([cum_all, jnp.zeros((dk - heads - 8, tok), F32)], axis=0)
    )
    cum = cum_all[:heads]
    reset = cum_all[heads : heads + 1]
    reset_col = cum_t[:, heads : heads + 1]
    bias_s[...] = jnp.where((rows_i <= cols_i) & (reset == reset_col), 0.0, -1e30)
    end = cum[:, tok - 1 : tok]
    reset_end = reset[:, tok - 1 : tok]
    cum_s[...] = cum
    lead_s[...] = jnp.where(reset == 0, jnp.exp(cum), 0.0)
    tail_s[...] = jnp.where(reset == reset_end, jnp.exp(end - cum), 0.0)
    lane_row = lax.broadcasted_iota(jnp.int32, (1, dk), 1)
    end_row = jnp.where(lane_row < heads, cum_t[tok - 1 : tok, :], 0.0)
    decs[0] = jnp.where(reset_end == 0, jnp.exp(end_row), 0.0)
    for h in range(heads):
        col_s[h] = jnp.broadcast_to(cum_t[:, h : h + 1], (tok, tok))

    def states(p, _):
        lanes = pl.ds(pl.multiple_of(p * dk, dk), dk)
        vt = jnp.transpose(v_ref[:, lanes].astype(F32))
        gt = jnp.transpose(g_ref[:, lanes].astype(F32))
        vt_s[p] = vt.astype(BF16)
        gt_s[p] = gt.astype(BF16)
        for i in range(group):
            h = p * group + i
            wide = pl.ds(pl.multiple_of(h * dk, dk), dk)
            part = slice(i * dv, (i + 1) * dv)
            tail = tail_s[pl.ds(h, 1), :]
            lead = lead_s[pl.ds(h, 1), :]
            st[0, h] = dot_fine(vt[part] * tail, k_ref[:, wide], NN)
            gw = jnp.concatenate(
                [gt[part] * (lead * lw_ref[l, pl.ds(h, 1), :]) for l in slots], axis=0
            )
            back = dot_fine(gw, q_ref[:, wide], NN)
            for n in range(len(slots)):
                st[1 + n, h] = back[n * dv : (n + 1) * dv]
        return 0

    for n in range(2, 7):
        load(n).wait()
    lax.fori_loop(0, pairs, states, 0, unroll=2)
    pl.semaphore_wait(barrier, bits + has_next + has_last)
    rounds = head_count - 2
    if rounds > 0:
        greet(round_sem.at[0])

    def remote(src, dst, send, recv, b):
        return pltpu.make_async_remote_copy(
            src_ref=src,
            dst_ref=dst,
            send_sem=send,
            recv_sem=recv,
            device_id={"seq": peer[b]},
            device_id_type=MESH,
        )

    def of(base, c):
        return pl.ds(base + c * group, group)

    def at(c):
        return pl.ds(c * group, group)

    kind_a = y * kind[2]
    kind_b = x * kind[1]
    slot_out = bits - (bits - 1) * first_chip
    slot_in = bits - (bits - 1) * second_chip

    def dec_copy(n):
        return remote(decs.at[2 * n], decs.at[2 * n + 1], d_send.at[n], d_recv.at[n], n)

    def a_copy(c):
        return remote(
            st.at[kind_a, of(theirs, c)], got_a.at[at(c)], a_send.at[c], a_recv.at[c], 0
        )

    def b_copy(c):
        return remote(
            st.at[kind_b, of(theirs, c)], got_b.at[at(c)], b_send.at[c], b_recv.at[c], 0
        )

    def p_copy(n):
        part = pl.ds(n * half, half)
        return remote(
            st.at[core * kind[0], part], lvl.at[0, part], p_send.at[n], p_recv.at[n], 0
        )

    def xa_copy(c):
        return remote(
            sum_a.at[at(c)], lvl.at[slot_out, of(mine, c)], xa_send.at[c], xa_recv.at[c], 1
        )

    def xb_copy(c):
        return remote(sum_b.at[at(c)], lvl.at[1, of(mine, c)], xb_send.at[c], xb_recv.at[c], 1)

    def y_copy(c):
        return remote(sum_q.at[at(c)], lvl.at[2, of(mine, c)], y_send.at[c], y_recv.at[c], 2)

    def f_copy(j, base, c):
        part = lvl.at[j, of(base, c)]
        return remote(part, part, f_send.at[j - 1, c], f_recv.at[j - 1, c], 0)

    dec_copy(0).start()
    for c in range(chunks):
        a_copy(c).start()

    span_of = lax.broadcasted_iota(jnp.int32, (1, tok), 1) // SPAN

    def local(p, _):
        vt = vt_s[p]
        gt = gt_s[p]
        lanes = pl.ds(pl.multiple_of(p * dk, dk), dk)
        v_blk = v_ref[:, lanes]
        for i in range(group):
            h = p * group + i
            wide = pl.ds(pl.multiple_of(h * dk, dk), dk)
            part = slice(i * dv, (i + 1) * dv)
            q = q_ref[:, wide]
            k = k_ref[:, wide]
            score = dot(k, q, NT)
            pair = dot(v_blk[:, part], gt[part], NN)
            decay = jnp.exp((cum_s[pl.ds(h, 1), :] - col_s[h]) + bias_s[...])
            seen = decay * score
            both_p = seen * pair
            gains = [lw_ref[l, pl.ds(h, 1), :] for l in range(span_bits + 1)]
            level_rows = [jnp.zeros((1, tok), F32) for _ in range(span_bits + 1)]
            mixed, graded = [], []
            for cs in range(spans):
                rows = slice(cs * SPAN, (cs + 1) * SPAN)
                total = jnp.sum(both_p[rows], axis=0, keepdims=True)
                gain = jnp.zeros((1, tok), F32)
                for ct in range(cs, spans):
                    l = span_level(cs, ct, levels)
                    hit = span_of == ct
                    gain = jnp.where(hit, gains[l], gain)
                    level_rows[l] = level_rows[l] + jnp.where(hit, total, 0.0)
                mixed.append(seen[rows] * gain)
                graded.append(decay[rows] * gain * pair[rows])
            mix = jnp.concatenate(mixed, axis=0).astype(BF16)
            grade = jnp.concatenate(graded, axis=0).astype(BF16)
            for l in range(span_bits + 1):
                gl_ref[l, pl.ds(h, 1), :] = level_rows[l]
            drift_s[pl.ds(h, 1), :] = jnp.sum(mix.astype(F32) * pair, axis=0, keepdims=True)
            vg_s[p, part] = dot(gt[part], mix, NT)
            gk_s[h] = dot(grade, q, NN)
            gq_s[h] = dot(grade, k, TN)
        return 0

    def spread(device_rows):
        t = jnp.transpose(
            jnp.concatenate(
                device_rows + [jnp.zeros((8 - len(device_rows), dk), F32)], axis=0
            )
        )
        return [
            jnp.broadcast_to(t[:heads, n : n + 1], (heads, dk)) for n in range(len(device_rows))
        ]

    def weigh(n, swap, own, got):
        w = (swap % 2).astype(F32)
        mix_s[n, 0] = own * (1.0 - w) + w
        mix_s[n, 1] = got * w + (1.0 - w)

    def combine(n, c, own_at, got_at, put):
        for i in range(group):
            r = c * group + i
            ca = mix_s[n, 0, pl.ds(mine + r, 1), :]
            cb = mix_s[n, 1, pl.ds(mine + r, 1), :]
            put[r] = ca * own_at(r) + cb * got_at(r)

    def local_pairs(first, last):
        lax.fori_loop(first, last, local, 0, unroll=2)

    def x_start(n):
        if n < chunks:
            xa_copy(n).start()
        else:

            @pl.when(first_chip == 0)
            def _():
                xb_copy(n - chunks).start()

    def x_sent(n):
        if n < chunks:
            xa_copy(n).wait_send()
        else:

            @pl.when(first_chip == 0)
            def _():
                xb_copy(n - chunks).wait_send()

    local_pairs(0, 2)
    dec_copy(0).wait_recv()
    decs[2] = decs[0] * decs[1]
    d_self, d_pair = spread([decs[0], decs[1]])
    weigh(0, core + y, d_pair, d_self)
    weigh(1, core + x, d_pair, d_self)
    for c in range(chunks):
        a_copy(c).wait_recv()
        combine(0, c, lambda r: st[kind_a, mine + r], lambda r: got_a[r], sum_a)
        if c < 2:
            x_start(c)
        if c == 1:
            dec_copy(1).start()

            @pl.when(first_chip == 0)
            def _():
                for n in range(chunks):
                    b_copy(n).start()

    local_pairs(2, 4)

    @pl.when(first_chip == 0)
    def _():
        for c in range(chunks):
            b_copy(c).wait_recv()
            combine(1, c, lambda r: st[kind_b, mine + r], lambda r: got_b[r], sum_b)

    for r in range(1, rounds + 1):
        pl.semaphore_wait(round_sem.at[r - 1], has_next + has_last)
        if r < rounds:
            greet(round_sem.at[r])
    x_sent(0)
    x_start(2)
    p_copy(0).start()
    local_pairs(4, 6)
    dec_copy(1).wait_recv()
    (d_side,) = spread([decs[3]])
    weigh(2, x + y, d_side, d_self * d_pair)
    inner_f = jnp.ones((heads, dk), F32)
    inner_b = jnp.ones((heads, dk), F32)
    for b, (u, got) in enumerate(((core, d_pair), (x, d_side), (y, None))):
        up = u.astype(F32)
        coef_s[0, b] = inner_f * up
        coef_s[1, b] = inner_b * (1.0 - up)
        if got is not None:
            inner_f = inner_f * (up * got + (1.0 - up))
            inner_b = inner_b * ((1.0 - up) * got + up)
    x_sent(1)
    x_start(3)
    p_copy(1).start()
    for c in range(chunks):
        xa_copy(c).wait_recv()
        combine(2, c, lambda r: sum_a[r], lambda r: lvl[slot_in, mine + r], sum_q)
        y_copy(c).start()

        @pl.when(second_chip == 1)
        def _(c=c):
            f_copy(1, mine, c).start()

        x_sent(c + 2)
        x_start(c + 4)
        if c == 0:
            local_pairs(6, pairs)

    def incoming(h):
        blocks = [lvl[b, h] for b in range(bits)]
        entering = []
        for n in range(len(slots)):
            terms = [
                coef_s[0, b, pl.ds(h, 1), :] * blocks[b]
                for b in range(bits)
                if kind[b] == 1 + n
            ]
            entering.append(functools.reduce(jnp.add, terms))
        after = functools.reduce(
            jnp.add, [coef_s[1, b, pl.ds(h, 1), :] * blocks[b] for b in range(bits)]
        )
        return split(jnp.concatenate(entering, axis=0)), split(after)

    def finish_drift(p):
        vt = vt_s[p].astype(F32)
        gt = gt_s[p].astype(F32)
        for i in range(group):
            h = p * group + i
            wide = pl.ds(pl.multiple_of(h * dk, dk), dk)
            part = slice(i * dv, (i + 1) * dv)
            q = q_ref[:, wide]
            k = k_ref[:, wide]
            tail = tail_s[pl.ds(h, 1), :]
            lead = lead_s[pl.ds(h, 1), :]
            (e_high, e_low), (a_high, a_low) = incoming(h)
            seen = dot(e_high, q, NT) + dot(e_low, q, NT)
            drift = drift_s[pl.ds(h, 1), :]
            for n, l in enumerate(slots):
                level = lead * jnp.sum(
                    seen[n * dv : (n + 1) * dv] * gt[part], axis=0, keepdims=True
                )
                gl_ref[l, pl.ds(h, 1), :] = level
                drift = drift + lw_ref[l, pl.ds(h, 1), :] * level
            vg = vg_s[p, part] + tail * (dot(a_high, k, NT) + dot(a_low, k, NT))
            drift_s[pl.ds(h, 1), :] = drift - jnp.sum(vg * vt[part], axis=0, keepdims=True)
            vg_s[p, part] = vg

    def finish_out(p):
        lanes = pl.ds(pl.multiple_of(p * dk, dk), dk)
        vt = vt_s[p].astype(F32)
        gt = gt_s[p].astype(F32)
        for i in range(group):
            h = p * group + i
            wide = pl.ds(pl.multiple_of(h * dk, dk), dk)
            part = slice(i * dv, (i + 1) * dv)
            tail = tail_s[pl.ds(h, 1), :]
            lead = lead_s[pl.ds(h, 1), :]
            (e_high, e_low), (a_high, a_low) = incoming(h)
            gws = [gt[part] * (lead * lw_ref[l, pl.ds(h, 1), :]) for l in slots]
            gw, gw_low = split(jnp.concatenate(gws, axis=0))
            gq_in = dot(gw, e_high, TN) + dot(gw, e_low, TN) + dot(gw_low, e_high, TN)
            gq_ref[:, wide] = (gq_s[h] + gq_in).astype(BF16)
            tv, tv_low = split(vt[part] * tail)
            gk_in = dot(tv, a_high, TN) + dot(tv, a_low, TN) + dot(tv_low, a_high, TN)
            gk_ref[:, wide] = (gk_s[h] + gk_in).astype(BF16)
        gv_ref[:, lanes] = jnp.transpose(vg_s[p]).astype(BF16)

    own_pair = core * chunks
    far_pair = (1 - core) * chunks
    for n in range(2):
        p_copy(n).wait_recv()
    for c in range(chunks):
        y_copy(c).wait_recv()
        f_copy(2, mine, c).start()

        @pl.when(second_chip == 0)
        def _(c=c):
            xb_copy(c).wait_recv()
            f_copy(1, mine, c).start()

        if c == 0:
            for o in range(1, head_count):
                pl.semaphore_signal(
                    plane_sem,
                    inc=1,
                    device_id={"head": (row + o) % head_count},
                    device_id_type=MESH,
                )
        finish_drift(own_pair + c)
        for j in (1, 2):
            f_copy(j, theirs, c).wait_recv()
        finish_drift(far_pair + c)

    later = (rows_i >= cols_i).astype(F32)
    local_tail = lax.dot_general(
        drift_s[...], later, NN, precision=lax.Precision.HIGHEST, preferred_element_type=F32
    )
    lane = lax.broadcasted_iota(jnp.int32, (heads, tok), 1)
    head = lax.broadcasted_iota(jnp.int32, (heads, tok), 0)
    sums = [
        local_tail[:, 0:1],
        jnp.sum(local_tail, axis=1, keepdims=True),
        jnp.sum(local_tail * local_tail, axis=1, keepdims=True),
    ]
    packed = jnp.zeros((heads, tok), F32)
    for n, column in enumerate(sums):
        packed = jnp.where(lane == head + n * heads, column, packed)
    slot = row * seq_count + place
    total = seq_count * head_count
    msg[slot] = jnp.sum(packed, axis=0, keepdims=True)

    def tail_copy(to_row, to_place):
        return pltpu.make_async_remote_copy(
            src_ref=msg.at[slot],
            dst_ref=msg.at[slot],
            send_sem=t_send.at[0],
            recv_sem=t_recv.at[0],
            device_id={"seq": to_place, "head": to_row},
            device_id_type=MESH,
        )

    def tail_all():
        others = msg.at[pl.ds(0, total - 1)]
        return pltpu.make_async_remote_copy(
            src_ref=others,
            dst_ref=others,
            send_sem=t_send.at[0],
            recv_sem=t_recv.at[0],
            device_id={"seq": peer[0]},
            device_id_type=MESH,
        )

    pl.semaphore_wait(plane_sem, head_count - 1)
    for o in reversed(range(head_count)):
        for n in reversed(range(seq_count)):
            if (o, n) != (0, 0):
                tail_copy((row + o) % head_count, (place + n) % seq_count).start()

    def outputs(p, _):
        finish_out(p)
        return 0

    lax.fori_loop(0, pairs, outputs, 0, unroll=2)
    for l in range(levels):
        if l > span_bits and l not in slots:
            gl_ref[l] = jnp.zeros((heads, tok), F32)

    for n in range(2):
        dec_copy(n).wait_send()
    for n in range(2):
        p_copy(n).wait_send()
    for n in range(chunks + 2, 2 * chunks):
        x_sent(n)
    for c in range(chunks):
        a_copy(c).wait_send()
        y_copy(c).wait_send()
        for j in (1, 2):
            f_copy(j, mine, c).wait_send()

    @pl.when(first_chip == 0)
    def _():
        for c in range(chunks):
            b_copy(c).wait_send()

    tail_all().wait_send()
    tail_all().wait_recv()
    rows = msg[:, 0, :]
    row_u = lax.broadcasted_iota(jnp.int32, (total, total), 0)
    row_v = lax.broadcasted_iota(jnp.int32, (total, total), 1)
    behind = (row_u // seq_count == row_v // seq_count) & (row_v > row_u)
    after_rows = lax.dot_general(
        behind.astype(F32), rows, NN, precision=lax.Precision.HIGHEST, preferred_element_type=F32
    )
    plain = pltpu.roll(rows, dk - heads, 1)
    square = pltpu.roll(rows, dk - 2 * heads, 1)
    energy = square + after_rows * (2.0 * plain + tok * after_rows)
    lane_all = lax.broadcasted_iota(jnp.int32, (total, dk), 1)
    slot_all = lax.broadcasted_iota(jnp.int32, (total, dk), 0)
    energy = jnp.sum(jnp.where(lane_all < heads, energy, 0.0), axis=0, keepdims=True)
    whole = jnp.sum(energy, axis=1, keepdims=True)
    my_row = jnp.sum(jnp.where(slot_all == slot, after_rows, 0.0), axis=0, keepdims=True)
    my_later = jnp.sum(jnp.where(lane == head, my_row, 0.0), axis=1, keepdims=True)
    count = heads * tok * total
    factor = jnp.minimum(1.0, lax.rsqrt(whole / count + 1e-6))
    gg_ref[...] = (local_tail + my_later) * factor


def write_out(count, *refs):
    sems = refs[-1]
    copies = [
        pltpu.make_async_copy(refs[i], refs[count + i], sems.at[i]) for i in range(count)
    ]
    for c in copies:
        c.start()
    for c in copies:
        c.wait()


def shards(seq_count, head_count, queries, keys, values, out_grad, log_gate, level_weight, doc_start):
    tok = queries.shape[0]
    heads = log_gate.shape[0]
    levels = level_weight.shape[0]
    dk = queries.shape[1] // heads
    dv = values.shape[1] // heads
    group = dk // dv
    pairs = heads // group
    bits = seq_count.bit_length() - 1
    half = heads // 2
    span_bits = (tok // SPAN).bit_length() - 1
    slots = len({min(span_bits + 1 + b, levels - 1) for b in range(bits)})
    dma = pltpu.SemaphoreType.DMA
    vmem = pltpu.VMEM
    block = (dv, dk)
    scratch = [
        vmem((heads, tok), F32),
        vmem((heads, tok, tok), F32),
        vmem((heads, tok), F32),
        vmem((heads, tok), F32),
        vmem((tok, tok), F32),
        vmem((pairs, group * dv, tok), BF16),
        vmem((pairs, group * dv, tok), BF16),
        vmem((pairs, group * dv, tok), F32),
        vmem((heads, tok, dk), F32),
        vmem((heads, tok, dk), F32),
        vmem((heads, tok), F32),
        vmem((2, bits, heads, dk), F32),
        vmem((heads,) + block, F32),
        vmem((slots, heads) + block, F32),
        vmem((bits, heads) + block, F32),
        vmem((bits, half) + block, F32),
        vmem((bits, bits, half) + block, F32),
        vmem((bits, half) + block, F32),
        vmem((bits, bits, half) + block, F32),
        vmem((bits + 1, heads, dk), F32),
        vmem((bits, heads, dk), F32),
        vmem((seq_count, heads, tok), F32),
        vmem((head_count, 8, dk), F32),
        dma((bits, 2)),
        dma((bits, 2)),
        dma((bits,)),
        dma((bits,)),
        dma((bits,)),
        dma((bits,)),
        dma((bits, bits)),
        dma((bits, bits)),
        dma((bits,)),
        dma((bits,)),
        dma((seq_count,)),
        dma((seq_count,)),
        dma((head_count,)),
        dma((head_count,)),
    ]
    args = (queries, keys, values, out_grad, log_gate, level_weight, doc_start.reshape(1, tok))
    spec = pl.BlockSpec(memory_space=pltpu.VMEM)
    in_spec = spec
    body = kernel
    chunks = half // group
    if bits == 3 and chunks == 4 and chunks * group == half and tok == dk and 3 * heads <= dk:
        body = chunked_kernel
        inputs = [(x.shape, x.dtype) for x in args]
        scratch = [vmem(*x) for x in inputs] + scratch[:12] + [
            vmem((3, 2, heads, dk), F32),
            vmem((1 + slots, heads) + block, F32),
            vmem((half,) + block, F32),
            vmem((half,) + block, F32),
            vmem((half,) + block, F32),
            vmem((half,) + block, F32),
            vmem((half,) + block, F32),
            vmem((bits + 1, heads) + block, F32),
            vmem((4, 1, dk), F32),
            vmem((seq_count * head_count, 1, dk), F32),
            dma((7,)),
            dma((chunks,)),
            dma((chunks,)),
            dma((chunks,)),
            dma((chunks,)),
            dma((2,)),
            dma((2,)),
            dma((chunks,)),
            dma((chunks,)),
            dma((chunks,)),
            dma((chunks,)),
            dma((chunks,)),
            dma((chunks,)),
            dma((2, chunks)),
            dma((2, chunks)),
            dma((2,)),
            dma((2,)),
            dma((1,)),
            dma((1,)),
            pltpu.SemaphoreType.REGULAR((max(1, head_count - 2),)),
            pltpu.SemaphoreType.REGULAR,
        ]
        in_spec = pl.BlockSpec(memory_space=pltpu.HBM)
    outs = [
        (queries.shape, BF16),
        (keys.shape, BF16),
        (values.shape, BF16),
        (level_weight.shape, F32),
        (log_gate.shape, F32),
    ]
    results = pl.pallas_call(
        functools.partial(body, seq_count, head_count),
        out_shape=tuple(vmem(shape, dtype) for shape, dtype in outs),
        in_specs=[in_spec] * 7,
        out_specs=(spec,) * 5,
        scratch_shapes=scratch,
        compiler_params=pltpu.CompilerParams(collective_id=0, has_side_effects=True),
    )(*args)
    count = len(outs)
    return pl.pallas_call(
        functools.partial(write_out, count),
        out_shape=tuple(jax.ShapeDtypeStruct(shape, dtype) for shape, dtype in outs),
        in_specs=[spec] * count,
        out_specs=(pl.BlockSpec(memory_space=pltpu.HBM),) * count,
        scratch_shapes=[dma((count,))],
    )(*[pltpu.with_memory_space_constraint(r, pltpu.VMEM) for r in results])


def solution(mesh):
    return jax.shard_map(
        functools.partial(shards, mesh.shape["seq"], mesh.shape["head"]),
        mesh=mesh,
        in_specs=(
            P("seq", "head"),
            P("seq", "head"),
            P("seq", "head"),
            P("seq", "head"),
            P("head", "seq"),
            P(None, "head", "seq"),
            P("seq"),
        ),
        out_specs=(
            P("seq", "head"),
            P("seq", "head"),
            P("seq", "head"),
            P(None, "head", "seq"),
            P("head", "seq"),
        ),
        check_vma=False,
    )
```

```python
import functools

import jax
import jax.numpy as jnp
from jax import lax
from jax.experimental import pallas as pl
from jax.experimental.pallas import tpu as pltpu
from jax.sharding import PartitionSpec as P

SPAN = 64
F32 = jnp.float32
BF16 = jnp.bfloat16
NN = (((1,), (0,)), ((), ()))
NT = (((1,), (1,)), ((), ()))
TN = (((0,), (0,)), ((), ()))
MESH = pl.DeviceIdType.MESH


def dot(a, b, dims):
    return lax.dot_general(a, b, dims, preferred_element_type=F32)


def split(x):
    high = x.astype(BF16)
    return high, (x - high.astype(F32)).astype(BF16)


def dot_fine(x, b, dims):
    high, low = split(x)
    return dot(high, b, dims) + dot(low, b, dims)


def span_level(a, b, levels):
    return 0 if a == b else min(levels - 1, (a ^ b).bit_length())


def kernel(
    seq_count,
    head_count,
    q_ref,
    k_ref,
    v_ref,
    g_ref,
    lg_ref,
    lw_ref,
    ds_ref,
    gq_ref,
    gk_ref,
    gv_ref,
    gl_ref,
    gg_ref,
    cum_s,
    col_s,
    lead_s,
    tail_s,
    bias_s,
    vt_s,
    gt_s,
    vg_s,
    gq_s,
    gk_s,
    drift_s,
    coef_s,
    state_s,
    back_s,
    lvl,
    got_s,
    got_u,
    sum_s,
    sum_u,
    dec,
    got_dec,
    tot,
    sq,
    lvl_send,
    lvl_recv,
    fwd_send,
    fwd_recv,
    s_send,
    s_recv,
    u_send,
    u_recv,
    d_send,
    d_recv,
    t_send,
    t_recv,
    q_send,
    q_recv,
):
    tok = q_ref.shape[0]
    heads = lg_ref.shape[0]
    levels = lw_ref.shape[0]
    dk = q_ref.shape[1] // heads
    dv = v_ref.shape[1] // heads
    group = dk // dv
    pairs = heads // group
    spans = tok // SPAN
    span_bits = spans.bit_length() - 1
    bits = seq_count.bit_length() - 1
    half = heads // 2
    cross = [min(span_bits + 1 + b, levels - 1) for b in range(bits)]
    slots = sorted(set(cross))
    place = lax.axis_index("seq")
    row = lax.axis_index("head")
    bit = [(place // (1 << b)) % 2 for b in range(bits)]
    peer = [place + (1 - 2 * bit[b]) * (1 << b) for b in range(bits)]
    want_s = [(place // (2 << b)) != (seq_count // (2 << b)) - 1 for b in range(bits)]
    mine = bit[0] * half
    theirs = (1 - bit[0]) * half

    barrier = pltpu.get_barrier_semaphore()
    for o in range(1, seq_count):
        pl.semaphore_signal(
            barrier, inc=1, device_id={"seq": (place + o) % seq_count}, device_id_type=MESH
        )
    for o in range(1, head_count):
        pl.semaphore_signal(
            barrier, inc=1, device_id={"head": (row + o) % head_count}, device_id_type=MESH
        )

    rows_i = lax.broadcasted_iota(jnp.int32, (tok, tok), 0)
    cols_i = lax.broadcasted_iota(jnp.int32, (tok, tok), 1)
    tri = (rows_i <= cols_i).astype(F32)
    starts = jnp.broadcast_to(ds_ref[...].astype(F32), (8, tok))
    both = jnp.concatenate([lg_ref[...], starts], axis=0)
    cum_all = lax.dot_general(
        both, tri, NN, precision=lax.Precision.HIGHEST, preferred_element_type=F32
    )
    cum_t = jnp.transpose(cum_all)
    cum = cum_all[:heads]
    reset = cum_all[heads : heads + 1]
    reset_col = cum_t[:, heads : heads + 1]
    bias_s[...] = jnp.where((rows_i <= cols_i) & (reset == reset_col), 0.0, -1e30)
    end = cum[:, tok - 1 : tok]
    reset_end = reset[:, tok - 1 : tok]
    cum_s[...] = cum
    lead_s[...] = jnp.where(reset == 0, jnp.exp(cum), 0.0)
    tail_s[...] = jnp.where(reset == reset_end, jnp.exp(end - cum), 0.0)
    dec[0] = jnp.broadcast_to(jnp.where(reset_end == 0, jnp.exp(end), 0.0), (heads, dk))
    for h in range(heads):
        col_s[h] = jnp.broadcast_to(cum_t[:, h : h + 1], (tok, tok))

    def states(p, _):
        lanes = pl.ds(pl.multiple_of(p * dk, dk), dk)
        vt = jnp.transpose(v_ref[:, lanes].astype(F32))
        gt = jnp.transpose(g_ref[:, lanes].astype(F32))
        vt_s[p] = vt.astype(BF16)
        gt_s[p] = gt.astype(BF16)
        for i in range(group):
            h = p * group + i
            wide = pl.ds(pl.multiple_of(h * dk, dk), dk)
            part = slice(i * dv, (i + 1) * dv)
            tail = tail_s[pl.ds(h, 1), :]
            lead = lead_s[pl.ds(h, 1), :]
            state_s[h] = dot_fine(vt[part] * tail, k_ref[:, wide], NN)
            gw = jnp.concatenate(
                [gt[part] * (lead * lw_ref[l, pl.ds(h, 1), :]) for l in slots], axis=0
            )
            back = dot_fine(gw, q_ref[:, wide], NN)
            for n in range(len(slots)):
                back_s[n, h] = back[n * dv : (n + 1) * dv]
        return 0

    lax.fori_loop(0, pairs, states, 0, unroll=2)
    pl.semaphore_wait(barrier, seq_count - 1 + head_count - 1)

    def slot(b):
        return slots.index(cross[b])

    def remote(src, dst, send, recv, b):
        return pltpu.make_async_remote_copy(
            src_ref=src,
            dst_ref=dst,
            send_sem=send,
            recv_sem=recv,
            device_id={"seq": peer[b]},
            device_id_type=MESH,
        )

    own = pl.ds(mine, half)
    other = pl.ds(theirs, half)

    def u_copy(b, j):
        src = back_s.at[slot(j), other] if b == 0 else sum_u.at[b, j]
        return remote(src, got_u.at[b, j], u_send.at[b, j], u_recv.at[b, j], b)

    def s_copy(b):
        src = state_s.at[other] if b == 0 else sum_s.at[b]
        return remote(src, got_s.at[b], s_send.at[b], s_recv.at[b], b)

    def d_copy(b):
        return remote(dec.at[b], got_dec.at[b], d_send.at[b], d_recv.at[b], b)

    def level_copy(b, low):
        if b == 0:
            src = state_s if low else back_s.at[slot(0)]
            return [
                remote(src.at[part], lvl.at[0, part], lvl_send.at[0, n], lvl_recv.at[0, n], 0)
                for n, part in enumerate((other, own))
            ]
        src = sum_s.at[b] if low else sum_u.at[b, b]
        return [remote(src, lvl.at[b, own], lvl_send.at[b, 0], lvl_recv.at[b, 0], b)]

    def level_wait(b, n):
        part = other if n == 1 else own
        return remote(
            lvl.at[b, part], lvl.at[b, part], lvl_send.at[b, n], lvl_recv.at[b, n], b
        )

    def forward_copy(b, part):
        return remote(lvl.at[b, part], lvl.at[b, part], fwd_send.at[b], fwd_recv.at[b], 0)

    def land(b):
        up_summed = (bit[b] == 1) & want_s[b]

        @pl.when(jnp.logical_not(up_summed))
        def _():
            level_wait(b, 0).wait_recv()

        if b > 0:
            forward_copy(b, own).start()

    def begin(b):
        d_copy(b).start()

        early = 0 if b in (0, bits - 1) else 1

        @pl.when((bit[b] == 0) & (want_s[b] | (early == 0)))
        def _():
            for c in level_copy(b, True):
                c.start()

        if b < bits - 1:

            @pl.when((bit[b] == 1) & want_s[b])
            def _():
                s_copy(b).start()

            for j in range(b + 1, bits):

                @pl.when(bit[j] == 1)
                def _(j=j):
                    u_copy(b, j).start()

        if early == 0:

            @pl.when(bit[b] == 1)
            def _():
                for c in level_copy(b, False):
                    c.start()

    def begin_late(b):
        if b in (0, bits - 1):
            return

        @pl.when((bit[b] == 0) & jnp.logical_not(want_s[b]))
        def _():
            for c in level_copy(b, True):
                c.start()

        @pl.when(bit[b] == 1)
        def _():
            for c in level_copy(b, False):
                c.start()

    def join(b):
        d_copy(b).wait_recv()
        up = bit[b].astype(F32)
        got = got_dec[b]
        now = dec[b]
        dec[b + 1] = got * now
        if b == bits - 1:
            return
        base_s = state_s.at[own] if b == 0 else sum_s.at[b]

        @pl.when(want_s[b])
        def _():
            @pl.when(bit[b] == 1)
            def _():
                level_wait(b, 0).wait_recv()

                def body(i, _):
                    d = dec[b, pl.ds(mine + i, 1), :]
                    sum_s[b + 1, i] = d * lvl[b, mine + i] + base_s[i]
                    return 0

                lax.fori_loop(0, half, body, 0, unroll=True)

            @pl.when(bit[b] == 0)
            def _():
                s_copy(b).wait_recv()

                def body(i, _):
                    d = got_dec[b, pl.ds(mine + i, 1), :]
                    sum_s[b + 1, i] = d * base_s[i] + got_s[b, i]
                    return 0

                lax.fori_loop(0, half, body, 0, unroll=True)

        for j in range(b + 1, bits):
            base_u = back_s.at[slot(j), own] if b == 0 else sum_u.at[b, j]

            @pl.when(bit[j] == 1)
            def _(j=j, base_u=base_u):
                u_copy(b, j).wait_recv()

                def body(i, _):
                    d0 = dec[b, pl.ds(mine + i, 1), :]
                    d1 = got_dec[b, pl.ds(mine + i, 1), :]
                    a = up * d1 + (1.0 - up)
                    c = (1.0 - up) * d0 + up
                    sum_u[b + 1, j, i] = a * base_u[i] + c * got_u[b, j, i]
                    return 0

                lax.fori_loop(0, half, body, 0, unroll=True)

    span_of = lax.broadcasted_iota(jnp.int32, (1, tok), 1) // SPAN

    def local(p, _):
        vt = vt_s[p]
        gt = gt_s[p]
        lanes = pl.ds(pl.multiple_of(p * dk, dk), dk)
        v_blk = v_ref[:, lanes]
        for i in range(group):
            h = p * group + i
            wide = pl.ds(pl.multiple_of(h * dk, dk), dk)
            part = slice(i * dv, (i + 1) * dv)
            q = q_ref[:, wide]
            k = k_ref[:, wide]
            score = dot(k, q, NT)
            pair = dot(v_blk[:, part], gt[part], NN)
            decay = jnp.exp((cum_s[pl.ds(h, 1), :] - col_s[h]) + bias_s[...])
            seen = decay * score
            both_p = seen * pair
            gains = [lw_ref[l, pl.ds(h, 1), :] for l in range(span_bits + 1)]
            level_rows = [jnp.zeros((1, tok), F32) for _ in range(span_bits + 1)]
            mixed, graded = [], []
            for cs in range(spans):
                rows = slice(cs * SPAN, (cs + 1) * SPAN)
                total = jnp.sum(both_p[rows], axis=0, keepdims=True)
                gain = jnp.zeros((1, tok), F32)
                for ct in range(cs, spans):
                    l = span_level(cs, ct, levels)
                    hit = span_of == ct
                    gain = jnp.where(hit, gains[l], gain)
                    level_rows[l] = level_rows[l] + jnp.where(hit, total, 0.0)
                mixed.append(seen[rows] * gain)
                graded.append(decay[rows] * gain * pair[rows])
            mix = jnp.concatenate(mixed, axis=0).astype(BF16)
            grade = jnp.concatenate(graded, axis=0).astype(BF16)
            for l in range(span_bits + 1):
                gl_ref[l, pl.ds(h, 1), :] = level_rows[l]
            drift_s[pl.ds(h, 1), :] = jnp.sum(mix.astype(F32) * pair, axis=0, keepdims=True)
            vg_s[p, part] = dot(gt[part], mix, NT)
            gk_s[h] = dot(grade, q, NN)
            gq_s[h] = dot(grade, k, TN)
        return 0

    begin(0)
    lax.fori_loop(0, pairs // 4, local, 0, unroll=2)
    join(0)
    if bits > 1:
        begin(1)
    lax.fori_loop(pairs // 4, pairs, local, 0, unroll=2)
    for b in range(1, bits):
        join(b)
        if b + 1 < bits:
            begin(b + 1)
        begin_late(b)
        land(b - 1)
    land(bits - 1)

    inner_f = jnp.ones((heads, dk), F32)
    inner_b = jnp.ones((heads, dk), F32)
    for b in range(bits):
        up = bit[b].astype(F32)
        got = got_dec[b]
        coef_s[0, b] = inner_f * up
        coef_s[1, b] = inner_b * (1.0 - up)
        inner_f = inner_f * (up * got + (1.0 - up))
        inner_b = inner_b * ((1.0 - up) * got + up)
    level_wait(0, 1).wait_recv()
    for b in range(1, bits):
        forward_copy(b, other).wait_recv()

    def finish(p, _):
        lanes = pl.ds(pl.multiple_of(p * dk, dk), dk)
        vt = vt_s[p].astype(F32)
        gt = gt_s[p].astype(F32)
        vg_all = []
        for i in range(group):
            h = p * group + i
            wide = pl.ds(pl.multiple_of(h * dk, dk), dk)
            part = slice(i * dv, (i + 1) * dv)
            q = q_ref[:, wide]
            k = k_ref[:, wide]
            tail = tail_s[pl.ds(h, 1), :]
            lead = lead_s[pl.ds(h, 1), :]
            blocks = [lvl[b, h] for b in range(bits)]
            entering = []
            for n in range(len(slots)):
                terms = [
                    coef_s[0, b, pl.ds(h, 1), :] * blocks[b] for b in range(bits) if slot(b) == n
                ]
                entering.append(functools.reduce(jnp.add, terms))
            entering = jnp.concatenate(entering, axis=0)
            after = functools.reduce(
                jnp.add, [coef_s[1, b, pl.ds(h, 1), :] * blocks[b] for b in range(bits)]
            )
            e_high, e_low = split(entering)
            seen = dot(e_high, q, NT) + dot(e_low, q, NT)
            drift = drift_s[pl.ds(h, 1), :]
            gws = []
            for n, l in enumerate(slots):
                gain = lw_ref[l, pl.ds(h, 1), :]
                level = lead * jnp.sum(
                    seen[n * dv : (n + 1) * dv] * gt[part], axis=0, keepdims=True
                )
                gl_ref[l, pl.ds(h, 1), :] = level
                drift = drift + gain * level
                gws.append(gt[part] * (lead * gain))
            gw, gw_low = split(jnp.concatenate(gws, axis=0))
            gq_in = dot(gw, e_high, TN) + dot(gw, e_low, TN) + dot(gw_low, e_high, TN)
            gq_ref[:, wide] = (gq_s[h] + gq_in).astype(BF16)
            a_high, a_low = split(after)
            tv, tv_low = split(vt[part] * tail)
            gk_in = dot(tv, a_high, TN) + dot(tv, a_low, TN) + dot(tv_low, a_high, TN)
            gk_ref[:, wide] = (gk_s[h] + gk_in).astype(BF16)
            vg = vg_s[p, part] + tail * (dot(a_high, k, NT) + dot(a_low, k, NT))
            drift_s[pl.ds(h, 1), :] = drift - jnp.sum(vg * vt[part], axis=0, keepdims=True)
            vg_all.append(vg)
        gv_ref[:, lanes] = jnp.transpose(jnp.concatenate(vg_all, axis=0)).astype(BF16)
        return 0

    lax.fori_loop(0, pairs, finish, 0, unroll=2)
    for l in range(levels):
        if l > span_bits and l not in slots:
            gl_ref[l] = jnp.zeros((heads, tok), F32)

    later = (rows_i >= cols_i).astype(F32)
    local_tail = lax.dot_general(
        drift_s[...], later, NN, precision=lax.Precision.HIGHEST, preferred_element_type=F32
    )
    lane = lax.broadcasted_iota(jnp.int32, (heads, tok), 1)
    first = local_tail[:, 0:1]
    plain = jnp.sum(local_tail, axis=1, keepdims=True)
    square = jnp.sum(local_tail * local_tail, axis=1, keepdims=True)
    tot[place] = jnp.where(lane == 0, first, jnp.where(lane == 1, plain, square))

    def tot_copy(o, slot_at):
        return pltpu.make_async_remote_copy(
            src_ref=tot.at[place],
            dst_ref=tot.at[slot_at],
            send_sem=t_send.at[o],
            recv_sem=t_recv.at[slot_at],
            device_id={"seq": (place + o) % seq_count},
            device_id_type=MESH,
        )

    for o in range(1, seq_count):
        tot_copy(o, place).start()
    for o in range(1, seq_count):
        tot_copy(o, (place + o) % seq_count).wait_recv()
    after_total = jnp.zeros((heads, 1), F32)
    my_later = jnp.zeros((heads, 1), F32)
    energy = jnp.zeros((heads, 1), F32)
    for d in reversed(range(seq_count)):
        piece = tot[d]
        my_later = my_later + jnp.where(place == d, 1.0, 0.0) * after_total
        energy = energy + (
            piece[:, 2:3] + after_total * (2.0 * piece[:, 1:2] + tok * after_total)
        )
        after_total = after_total + piece[:, 0:1]
    energy = jnp.sum(jnp.broadcast_to(energy, (heads, dk)), axis=0, keepdims=True)
    sq[row] = jnp.broadcast_to(energy, (8, dk))

    def sq_copy(o, slot_at):
        return pltpu.make_async_remote_copy(
            src_ref=sq.at[row],
            dst_ref=sq.at[slot_at],
            send_sem=q_send.at[o],
            recv_sem=q_recv.at[slot_at],
            device_id={"head": (row + o) % head_count},
            device_id_type=MESH,
        )

    for o in range(1, head_count):
        sq_copy(o, row).start()
    for o in range(1, head_count):
        sq_copy(o, (row + o) % head_count).wait_recv()
    whole = sq[0]
    for r in range(1, head_count):
        whole = whole + sq[r]
    count = heads * tok * seq_count * head_count
    factor = jnp.minimum(1.0, lax.rsqrt(whole[0:1] / count + 1e-6))
    gg_ref[...] = (local_tail + my_later) * factor

    for b in range(bits):
        d_copy(b).wait_send()
        for n in range(2 if b == 0 else 1):
            level_wait(b, n).wait_send()
        if b > 0:
            forward_copy(b, own).wait_send()
        if b < bits - 1:

            @pl.when((bit[b] == 1) & want_s[b])
            def _(b=b):
                s_copy(b).wait_send()

            for j in range(b + 1, bits):

                @pl.when(bit[j] == 1)
                def _(b=b, j=j):
                    u_copy(b, j).wait_send()

    for o in range(1, seq_count):
        tot_copy(o, place).wait_send()
    for o in range(1, head_count):
        sq_copy(o, row).wait_send()


def chunked_kernel(
    seq_count,
    head_count,
    q_hbm,
    k_hbm,
    v_hbm,
    g_hbm,
    lg_hbm,
    lw_hbm,
    ds_hbm,
    gq_ref,
    gk_ref,
    gv_ref,
    gl_ref,
    gg_ref,
    q_ref,
    k_ref,
    v_ref,
    g_ref,
    lg_ref,
    lw_ref,
    ds_ref,
    cum_s,
    col_s,
    lead_s,
    tail_s,
    bias_s,
    vt_s,
    gt_s,
    vg_s,
    gq_s,
    gk_s,
    drift_s,
    coef_s,
    mix_s,
    st,
    got_a,
    got_b,
    sum_a,
    sum_b,
    sum_q,
    lvl,
    decs,
    msg,
    i_sem,
    a_send,
    a_recv,
    b_send,
    b_recv,
    p_send,
    p_recv,
    xa_send,
    xa_recv,
    xb_send,
    xb_recv,
    y_send,
    y_recv,
    f_send,
    f_recv,
    d_send,
    d_recv,
    t_send,
    t_recv,
    round_sem,
    plane_sem,
):
    tok = q_ref.shape[0]
    heads = lg_ref.shape[0]
    levels = lw_ref.shape[0]
    dk = q_ref.shape[1] // heads
    dv = v_ref.shape[1] // heads
    group = dk // dv
    pairs = heads // group
    spans = tok // SPAN
    span_bits = spans.bit_length() - 1
    bits = seq_count.bit_length() - 1
    half = heads // 2
    chunks = half // group
    cross = [min(span_bits + 1 + b, levels - 1) for b in range(bits)]
    slots = sorted(set(cross))
    kind = [1 + slots.index(l) for l in cross]
    place = lax.axis_index("seq")
    row = lax.axis_index("head")
    core, x, y = [(place // (1 << b)) % 2 for b in range(bits)]
    peer = [place + (1 - 2 * u) * (1 << b) for b, u in enumerate((core, x, y))]
    first_chip = (1 - x) * (1 - y)
    second_chip = x * (1 - y)
    mine = core * half
    theirs = (1 - core) * half

    has_next = (row < head_count - 1).astype(jnp.int32)
    has_last = (row > 0).astype(jnp.int32)

    def greet(sem):
        @pl.when(has_next == 1)
        def _():
            pl.semaphore_signal(sem, inc=1, device_id={"head": row + 1}, device_id_type=MESH)

        @pl.when(has_last == 1)
        def _():
            pl.semaphore_signal(sem, inc=1, device_id={"head": row - 1}, device_id_type=MESH)

    barrier = pltpu.get_barrier_semaphore()
    for b in reversed(range(bits)):
        pl.semaphore_signal(barrier, inc=1, device_id={"seq": peer[b]}, device_id_type=MESH)
    greet(barrier)

    def load(n):
        src = (lg_hbm, ds_hbm, v_hbm, k_hbm, g_hbm, lw_hbm, q_hbm)[n]
        dst = (lg_ref, ds_ref, v_ref, k_ref, g_ref, lw_ref, q_ref)[n]
        return pltpu.make_async_copy(src, dst, i_sem.at[n])

    for n in range(7):
        load(n).start()
    for n in range(2):
        load(n).wait()

    rows_i = lax.broadcasted_iota(jnp.int32, (tok, tok), 0)
    cols_i = lax.broadcasted_iota(jnp.int32, (tok, tok), 1)
    tri = (rows_i <= cols_i).astype(F32)
    starts = jnp.broadcast_to(ds_ref[...].astype(F32), (8, tok))
    both = jnp.concatenate([lg_ref[...], starts], axis=0)
    cum_all = lax.dot_general(
        both, tri, NN, precision=lax.Precision.HIGHEST, preferred_element_type=F32
    )
    cum_t = jnp.transpose(
        jnp.concatenate([cum_all, jnp.zeros((dk - heads - 8, tok), F32)], axis=0)
    )
    cum = cum_all[:heads]
    reset = cum_all[heads : heads + 1]
    reset_col = cum_t[:, heads : heads + 1]
    bias_s[...] = jnp.where((rows_i <= cols_i) & (reset == reset_col), 0.0, -1e30)
    end = cum[:, tok - 1 : tok]
    reset_end = reset[:, tok - 1 : tok]
    cum_s[...] = cum
    lead_s[...] = jnp.where(reset == 0, jnp.exp(cum), 0.0)
    tail_s[...] = jnp.where(reset == reset_end, jnp.exp(end - cum), 0.0)
    lane_row = lax.broadcasted_iota(jnp.int32, (1, dk), 1)
    end_row = jnp.where(lane_row < heads, cum_t[tok - 1 : tok, :], 0.0)
    decs[0] = jnp.where(reset_end == 0, jnp.exp(end_row), 0.0)
    for h in range(heads):
        col_s[h] = jnp.broadcast_to(cum_t[:, h : h + 1], (tok, tok))

    def states(p, _):
        lanes = pl.ds(pl.multiple_of(p * dk, dk), dk)
        vt = jnp.transpose(v_ref[:, lanes].astype(F32))
        gt = jnp.transpose(g_ref[:, lanes].astype(F32))
        vt_s[p] = vt.astype(BF16)
        gt_s[p] = gt.astype(BF16)
        for i in range(group):
            h = p * group + i
            wide = pl.ds(pl.multiple_of(h * dk, dk), dk)
            part = slice(i * dv, (i + 1) * dv)
            tail = tail_s[pl.ds(h, 1), :]
            lead = lead_s[pl.ds(h, 1), :]
            st[0, h] = dot_fine(vt[part] * tail, k_ref[:, wide], NN)
            gw = jnp.concatenate(
                [gt[part] * (lead * lw_ref[l, pl.ds(h, 1), :]) for l in slots], axis=0
            )
            back = dot_fine(gw, q_ref[:, wide], NN)
            for n in range(len(slots)):
                st[1 + n, h] = back[n * dv : (n + 1) * dv]
        return 0

    for n in range(2, 7):
        load(n).wait()
    own_pair = core * chunks
    far_pair = (1 - core) * chunks
    def states_from(base):
        lax.fori_loop(0, 2, lambda n, _: states(base + n, 0), 0, unroll=2)

    states_from(far_pair)
    pl.semaphore_wait(barrier, bits + has_next + has_last)
    rounds = head_count - 2
    if rounds > 0:
        greet(round_sem.at[0])

    def remote(src, dst, send, recv, b):
        return pltpu.make_async_remote_copy(
            src_ref=src,
            dst_ref=dst,
            send_sem=send,
            recv_sem=recv,
            device_id={"seq": peer[b]},
            device_id_type=MESH,
        )

    def of(base, c):
        return pl.ds(base + c * group, group)

    def at(c):
        return pl.ds(c * group, group)

    kind_a = y * kind[2]
    kind_b = x * kind[1]
    slot_out = bits - (bits - 1) * first_chip
    slot_in = bits - (bits - 1) * second_chip

    def dec_copy(n):
        return remote(decs.at[2 * n], decs.at[2 * n + 1], d_send.at[n], d_recv.at[n], n)

    def a_copy(c):
        return remote(
            st.at[kind_a, of(theirs, c)], got_a.at[at(c)], a_send.at[c], a_recv.at[c], 0
        )

    def b_copy(c):
        return remote(
            st.at[kind_b, of(theirs, c)], got_b.at[at(c)], b_send.at[c], b_recv.at[c], 0
        )

    def p_copy(n):
        part = pl.ds(n * half, half)
        return remote(
            st.at[core * kind[0], part], lvl.at[0, part], p_send.at[n], p_recv.at[n], 0
        )

    piece = 2
    pieces = half // piece

    def xa_copy(n):
        here = pl.ds(n * piece, piece)
        there = pl.ds(mine + n * piece, piece)
        return remote(
            sum_a.at[here], lvl.at[slot_out, there], xa_send.at[n], xa_recv.at[n], 1
        )

    def xb_copy(n):
        here = pl.ds(n * piece, piece)
        there = pl.ds(mine + n * piece, piece)
        return remote(sum_b.at[here], lvl.at[1, there], xb_send.at[n], xb_recv.at[n], 1)

    def pieces_of(c):
        return range(c * group // piece, (c + 1) * group // piece)

    def y_copy(c):
        return remote(sum_q.at[at(c)], lvl.at[2, of(mine, c)], y_send.at[c], y_recv.at[c], 2)

    def f_copy(j, base, c):
        part = lvl.at[j, of(base, c)]
        return remote(part, part, f_send.at[j - 1, c], f_recv.at[j - 1, c], 0)

    dec_copy(0).start()
    for c in range(2):
        a_copy(c).start()
    states_from(far_pair + 2)
    for c in range(2, chunks):
        a_copy(c).start()
    states_from(own_pair)
    states_from(own_pair + 2)

    span_of = lax.broadcasted_iota(jnp.int32, (1, tok), 1) // SPAN

    def local(p, _):
        vt = vt_s[p]
        gt = gt_s[p]
        lanes = pl.ds(pl.multiple_of(p * dk, dk), dk)
        v_blk = v_ref[:, lanes]
        for i in range(group):
            h = p * group + i
            wide = pl.ds(pl.multiple_of(h * dk, dk), dk)
            part = slice(i * dv, (i + 1) * dv)
            q = q_ref[:, wide]
            k = k_ref[:, wide]
            score = dot(k, q, NT)
            pair = dot(v_blk[:, part], gt[part], NN)
            decay = jnp.exp((cum_s[pl.ds(h, 1), :] - col_s[h]) + bias_s[...])
            seen = decay * score
            both_p = seen * pair
            gains = [lw_ref[l, pl.ds(h, 1), :] for l in range(span_bits + 1)]
            level_rows = [jnp.zeros((1, tok), F32) for _ in range(span_bits + 1)]
            mixed, graded = [], []
            for cs in range(spans):
                rows = slice(cs * SPAN, (cs + 1) * SPAN)
                total = jnp.sum(both_p[rows], axis=0, keepdims=True)
                gain = jnp.zeros((1, tok), F32)
                for ct in range(cs, spans):
                    l = span_level(cs, ct, levels)
                    hit = span_of == ct
                    gain = jnp.where(hit, gains[l], gain)
                    level_rows[l] = level_rows[l] + jnp.where(hit, total, 0.0)
                mixed.append(seen[rows] * gain)
                graded.append(decay[rows] * gain * pair[rows])
            mix = jnp.concatenate(mixed, axis=0).astype(BF16)
            grade = jnp.concatenate(graded, axis=0).astype(BF16)
            for l in range(span_bits + 1):
                gl_ref[l, pl.ds(h, 1), :] = level_rows[l]
            drift_s[pl.ds(h, 1), :] = jnp.sum(mix.astype(F32) * pair, axis=0, keepdims=True)
            vg_s[p, part] = dot(gt[part], mix, NT)
            gk_s[h] = dot(grade, q, NN)
            gq_s[h] = dot(grade, k, TN)
        return 0

    def spread(device_rows):
        t = jnp.transpose(
            jnp.concatenate(
                device_rows + [jnp.zeros((8 - len(device_rows), dk), F32)], axis=0
            )
        )
        return [
            jnp.broadcast_to(t[:heads, n : n + 1], (heads, dk)) for n in range(len(device_rows))
        ]

    def weigh(n, swap, own, got):
        w = (swap % 2).astype(F32)
        mix_s[n, 0] = own * (1.0 - w) + w
        mix_s[n, 1] = got * w + (1.0 - w)

    def combine(n, c, own_at, got_at, put):
        for i in range(group):
            r = c * group + i
            ca = mix_s[n, 0, pl.ds(mine + r, 1), :]
            cb = mix_s[n, 1, pl.ds(mine + r, 1), :]
            put[r] = ca * own_at(r) + cb * got_at(r)

    def local_pairs(first, last):
        lax.fori_loop(first, last, local, 0, unroll=2)

    def x_start(n):
        if n < pieces:
            xa_copy(n).start()
        elif n < 2 * pieces:

            @pl.when(first_chip == 0)
            def _():
                xb_copy(n - pieces).start()

    def x_sent(n):
        if n < pieces:
            xa_copy(n).wait_send()
        else:

            @pl.when(first_chip == 0)
            def _():
                xb_copy(n - pieces).wait_send()

    ahead = 2

    def x_next(n):
        x_sent(n)
        x_start(n + ahead)

    dec_copy(0).wait_recv()
    decs[2] = decs[0] * decs[1]
    d_self, d_pair = spread([decs[0], decs[1]])
    weigh(0, core + y, d_pair, d_self)
    weigh(1, core + x, d_pair, d_self)
    for c in range(chunks):
        a_copy(c).wait_recv()
        combine(0, c, lambda r: st[kind_a, mine + r], lambda r: got_a[r], sum_a)
        for n in pieces_of(c):
            if n < ahead:
                x_start(n)
        if c == 1:
            dec_copy(1).start()

            @pl.when(first_chip == 0)
            def _():
                for n in range(chunks):
                    b_copy(n).start()

    local_pairs(0, 4)

    @pl.when(first_chip == 0)
    def _():
        for c in range(chunks):
            b_copy(c).wait_recv()
            combine(1, c, lambda r: st[kind_b, mine + r], lambda r: got_b[r], sum_b)

    for r in range(1, rounds + 1):
        pl.semaphore_wait(round_sem.at[r - 1], has_next + has_last)
        if r < rounds:
            greet(round_sem.at[r])
    x_next(0)
    p_copy(0).start()
    local_pairs(4, 6)
    dec_copy(1).wait_recv()
    (d_side,) = spread([decs[3]])
    weigh(2, x + y, d_side, d_self * d_pair)
    inner_f = jnp.ones((heads, dk), F32)
    inner_b = jnp.ones((heads, dk), F32)
    for b, (u, got) in enumerate(((core, d_pair), (x, d_side), (y, None))):
        up = u.astype(F32)
        coef_s[0, b] = inner_f * up
        coef_s[1, b] = inner_b * (1.0 - up)
        if got is not None:
            inner_f = inner_f * (up * got + (1.0 - up))
            inner_b = inner_b * ((1.0 - up) * got + up)
    x_next(1)
    p_copy(1).start()
    def turn(c):
        for n in pieces_of(c):
            xa_copy(n).wait_recv()
        combine(2, c, lambda r: sum_a[r], lambda r: lvl[slot_in, mine + r], sum_q)
        y_copy(c).start()

        @pl.when(second_chip == 1)
        def _():
            f_copy(1, mine, c).start()

    turn(0)
    local_pairs(6, pairs)
    x_next(2)
    turn(1)
    x_next(3)
    turn(2)
    x_next(4)
    turn(3)

    def incoming(h):
        blocks = [lvl[b, h] for b in range(bits)]
        entering = []
        for n in range(len(slots)):
            terms = [
                coef_s[0, b, pl.ds(h, 1), :] * blocks[b]
                for b in range(bits)
                if kind[b] == 1 + n
            ]
            entering.append(functools.reduce(jnp.add, terms))
        after = functools.reduce(
            jnp.add, [coef_s[1, b, pl.ds(h, 1), :] * blocks[b] for b in range(bits)]
        )
        return split(jnp.concatenate(entering, axis=0)), split(after)

    def finish_drift(p):
        vt = vt_s[p].astype(F32)
        gt = gt_s[p].astype(F32)
        for i in range(group):
            h = p * group + i
            wide = pl.ds(pl.multiple_of(h * dk, dk), dk)
            part = slice(i * dv, (i + 1) * dv)
            q = q_ref[:, wide]
            k = k_ref[:, wide]
            tail = tail_s[pl.ds(h, 1), :]
            lead = lead_s[pl.ds(h, 1), :]
            (e_high, e_low), (a_high, a_low) = incoming(h)
            seen = dot(e_high, q, NT) + dot(e_low, q, NT)
            drift = drift_s[pl.ds(h, 1), :]
            for n, l in enumerate(slots):
                level = lead * jnp.sum(
                    seen[n * dv : (n + 1) * dv] * gt[part], axis=0, keepdims=True
                )
                gl_ref[l, pl.ds(h, 1), :] = level
                drift = drift + lw_ref[l, pl.ds(h, 1), :] * level
            vg = vg_s[p, part] + tail * (dot(a_high, k, NT) + dot(a_low, k, NT))
            drift_s[pl.ds(h, 1), :] = drift - jnp.sum(vg * vt[part], axis=0, keepdims=True)
            vg_s[p, part] = vg

    def finish_out(p):
        lanes = pl.ds(pl.multiple_of(p * dk, dk), dk)
        vt = vt_s[p].astype(F32)
        gt = gt_s[p].astype(F32)
        for i in range(group):
            h = p * group + i
            wide = pl.ds(pl.multiple_of(h * dk, dk), dk)
            part = slice(i * dv, (i + 1) * dv)
            tail = tail_s[pl.ds(h, 1), :]
            lead = lead_s[pl.ds(h, 1), :]
            (e_high, e_low), (a_high, a_low) = incoming(h)
            gws = [gt[part] * (lead * lw_ref[l, pl.ds(h, 1), :]) for l in slots]
            gw, gw_low = split(jnp.concatenate(gws, axis=0))
            gq_in = dot(gw, e_high, TN) + dot(gw, e_low, TN) + dot(gw_low, e_high, TN)
            gq_ref[:, wide] = (gq_s[h] + gq_in).astype(BF16)
            tv, tv_low = split(vt[part] * tail)
            gk_in = dot(tv, a_high, TN) + dot(tv, a_low, TN) + dot(tv_low, a_high, TN)
            gk_ref[:, wide] = (gk_s[h] + gk_in).astype(BF16)
        gv_ref[:, lanes] = jnp.transpose(vg_s[p]).astype(BF16)

    for n in range(2):
        p_copy(n).wait_recv()
    for c in range(chunks):
        for n in ((5,), (), (), ())[c]:
            x_next(n)
        y_copy(c).wait_recv()
        f_copy(2, mine, c).start()

        @pl.when(second_chip == 0)
        def _(c=c):
            for n in pieces_of(c):
                xb_copy(n).wait_recv()
            f_copy(1, mine, c).start()

        if c == 0:
            for o in range(1, head_count):
                pl.semaphore_signal(
                    plane_sem,
                    inc=1,
                    device_id={"head": (row + o) % head_count},
                    device_id_type=MESH,
                )
        finish_drift(own_pair + c)
        for j in (1, 2):
            f_copy(j, theirs, c).wait_recv()
        finish_drift(far_pair + c)

    later = (rows_i >= cols_i).astype(F32)
    local_tail = lax.dot_general(
        drift_s[...], later, NN, precision=lax.Precision.HIGHEST, preferred_element_type=F32
    )
    lane = lax.broadcasted_iota(jnp.int32, (heads, tok), 1)
    head = lax.broadcasted_iota(jnp.int32, (heads, tok), 0)
    sums = [
        local_tail[:, 0:1],
        jnp.sum(local_tail, axis=1, keepdims=True),
        jnp.sum(local_tail * local_tail, axis=1, keepdims=True),
    ]
    packed = jnp.zeros((heads, tok), F32)
    for n, column in enumerate(sums):
        packed = jnp.where(lane == head + n * heads, column, packed)
    slot = row * seq_count + place
    total = seq_count * head_count
    msg[slot] = jnp.sum(packed, axis=0, keepdims=True)

    def tail_copy(to_row, to_place):
        return pltpu.make_async_remote_copy(
            src_ref=msg.at[slot],
            dst_ref=msg.at[slot],
            send_sem=t_send.at[0],
            recv_sem=t_recv.at[0],
            device_id={"seq": to_place, "head": to_row},
            device_id_type=MESH,
        )

    def tail_all():
        others = msg.at[pl.ds(0, total - 1)]
        return pltpu.make_async_remote_copy(
            src_ref=others,
            dst_ref=others,
            send_sem=t_send.at[0],
            recv_sem=t_recv.at[0],
            device_id={"seq": peer[0]},
            device_id_type=MESH,
        )

    pl.semaphore_wait(plane_sem, head_count - 1)
    for o in reversed(range(head_count)):
        for n in reversed(range(seq_count)):
            if (o, n) != (0, 0):
                tail_copy((row + o) % head_count, (place + n) % seq_count).start()

    def outputs(p, _):
        finish_out(p)
        return 0

    lax.fori_loop(0, pairs, outputs, 0, unroll=2)
    for l in range(levels):
        if l > span_bits and l not in slots:
            gl_ref[l] = jnp.zeros((heads, tok), F32)

    for n in range(2):
        dec_copy(n).wait_send()
    for n in range(2):
        p_copy(n).wait_send()
    for n in range(2 * pieces - ahead, 2 * pieces):
        x_sent(n)
    for c in range(chunks):
        a_copy(c).wait_send()
        y_copy(c).wait_send()
        for j in (1, 2):
            f_copy(j, mine, c).wait_send()

    @pl.when(first_chip == 0)
    def _():
        for c in range(chunks):
            b_copy(c).wait_send()

    tail_all().wait_send()
    tail_all().wait_recv()
    rows = msg[:, 0, :]
    row_u = lax.broadcasted_iota(jnp.int32, (total, total), 0)
    row_v = lax.broadcasted_iota(jnp.int32, (total, total), 1)
    behind = (row_u // seq_count == row_v // seq_count) & (row_v > row_u)
    after_rows = lax.dot_general(
        behind.astype(F32), rows, NN, precision=lax.Precision.HIGHEST, preferred_element_type=F32
    )
    plain = pltpu.roll(rows, dk - heads, 1)
    square = pltpu.roll(rows, dk - 2 * heads, 1)
    energy = square + after_rows * (2.0 * plain + tok * after_rows)
    lane_all = lax.broadcasted_iota(jnp.int32, (total, dk), 1)
    slot_all = lax.broadcasted_iota(jnp.int32, (total, dk), 0)
    energy = jnp.sum(jnp.where(lane_all < heads, energy, 0.0), axis=0, keepdims=True)
    whole = jnp.sum(energy, axis=1, keepdims=True)
    my_row = jnp.sum(jnp.where(slot_all == slot, after_rows, 0.0), axis=0, keepdims=True)
    my_later = jnp.sum(jnp.where(lane == head, my_row, 0.0), axis=1, keepdims=True)
    count = heads * tok * total
    factor = jnp.minimum(1.0, lax.rsqrt(whole / count + 1e-6))
    gg_ref[...] = (local_tail + my_later) * factor


def write_out(count, *refs):
    sems = refs[-1]
    copies = [
        pltpu.make_async_copy(refs[i], refs[count + i], sems.at[i]) for i in range(count)
    ]
    for c in copies:
        c.start()
    for c in copies:
        c.wait()


def shards(seq_count, head_count, queries, keys, values, out_grad, log_gate, level_weight, doc_start):
    tok = queries.shape[0]
    heads = log_gate.shape[0]
    levels = level_weight.shape[0]
    dk = queries.shape[1] // heads
    dv = values.shape[1] // heads
    group = dk // dv
    pairs = heads // group
    bits = seq_count.bit_length() - 1
    half = heads // 2
    span_bits = (tok // SPAN).bit_length() - 1
    slots = len({min(span_bits + 1 + b, levels - 1) for b in range(bits)})
    dma = pltpu.SemaphoreType.DMA
    vmem = pltpu.VMEM
    block = (dv, dk)
    scratch = [
        vmem((heads, tok), F32),
        vmem((heads, tok, tok), F32),
        vmem((heads, tok), F32),
        vmem((heads, tok), F32),
        vmem((tok, tok), F32),
        vmem((pairs, group * dv, tok), BF16),
        vmem((pairs, group * dv, tok), BF16),
        vmem((pairs, group * dv, tok), F32),
        vmem((heads, tok, dk), F32),
        vmem((heads, tok, dk), F32),
        vmem((heads, tok), F32),
        vmem((2, bits, heads, dk), F32),
        vmem((heads,) + block, F32),
        vmem((slots, heads) + block, F32),
        vmem((bits, heads) + block, F32),
        vmem((bits, half) + block, F32),
        vmem((bits, bits, half) + block, F32),
        vmem((bits, half) + block, F32),
        vmem((bits, bits, half) + block, F32),
        vmem((bits + 1, heads, dk), F32),
        vmem((bits, heads, dk), F32),
        vmem((seq_count, heads, tok), F32),
        vmem((head_count, 8, dk), F32),
        dma((bits, 2)),
        dma((bits, 2)),
        dma((bits,)),
        dma((bits,)),
        dma((bits,)),
        dma((bits,)),
        dma((bits, bits)),
        dma((bits, bits)),
        dma((bits,)),
        dma((bits,)),
        dma((seq_count,)),
        dma((seq_count,)),
        dma((head_count,)),
        dma((head_count,)),
    ]
    args = (queries, keys, values, out_grad, log_gate, level_weight, doc_start.reshape(1, tok))
    spec = pl.BlockSpec(memory_space=pltpu.VMEM)
    in_spec = spec
    body = kernel
    chunks = half // group
    if bits == 3 and chunks == 4 and chunks * group == half and tok == dk and 3 * heads <= dk:
        body = chunked_kernel
        inputs = [(x.shape, x.dtype) for x in args]
        scratch = [vmem(*x) for x in inputs] + scratch[:12] + [
            vmem((3, 2, heads, dk), F32),
            vmem((1 + slots, heads) + block, F32),
            vmem((half,) + block, F32),
            vmem((half,) + block, F32),
            vmem((half,) + block, F32),
            vmem((half,) + block, F32),
            vmem((half,) + block, F32),
            vmem((bits + 1, heads) + block, F32),
            vmem((4, 1, dk), F32),
            vmem((seq_count * head_count, 1, dk), F32),
            dma((7,)),
            dma((chunks,)),
            dma((chunks,)),
            dma((chunks,)),
            dma((chunks,)),
            dma((2,)),
            dma((2,)),
            dma((half,)),
            dma((half,)),
            dma((half,)),
            dma((half,)),
            dma((chunks,)),
            dma((chunks,)),
            dma((2, chunks)),
            dma((2, chunks)),
            dma((2,)),
            dma((2,)),
            dma((1,)),
            dma((1,)),
            pltpu.SemaphoreType.REGULAR((max(1, head_count - 2),)),
            pltpu.SemaphoreType.REGULAR,
        ]
        in_spec = pl.BlockSpec(memory_space=pltpu.HBM)
    outs = [
        (queries.shape, BF16),
        (keys.shape, BF16),
        (values.shape, BF16),
        (level_weight.shape, F32),
        (log_gate.shape, F32),
    ]
    results = pl.pallas_call(
        functools.partial(body, seq_count, head_count),
        out_shape=tuple(vmem(shape, dtype) for shape, dtype in outs),
        in_specs=[in_spec] * 7,
        out_specs=(spec,) * 5,
        scratch_shapes=scratch,
        compiler_params=pltpu.CompilerParams(collective_id=0, has_side_effects=True),
    )(*args)
    count = len(outs)
    return pl.pallas_call(
        functools.partial(write_out, count),
        out_shape=tuple(jax.ShapeDtypeStruct(shape, dtype) for shape, dtype in outs),
        in_specs=[spec] * count,
        out_specs=(pl.BlockSpec(memory_space=pltpu.HBM),) * count,
        scratch_shapes=[dma((count,))],
    )(*[pltpu.with_memory_space_constraint(r, pltpu.VMEM) for r in results])


def solution(mesh):
    return jax.shard_map(
        functools.partial(shards, mesh.shape["seq"], mesh.shape["head"]),
        mesh=mesh,
        in_specs=(
            P("seq", "head"),
            P("seq", "head"),
            P("seq", "head"),
            P("seq", "head"),
            P("head", "seq"),
            P(None, "head", "seq"),
            P("seq"),
        ),
        out_specs=(
            P("seq", "head"),
            P("seq", "head"),
            P("seq", "head"),
            P(None, "head", "seq"),
            P("head", "seq"),
        ),
        check_vma=False,
    )
```

```python
import functools

import jax
import jax.numpy as jnp
from jax import lax
from jax.experimental import pallas as pl
from jax.experimental.pallas import tpu as pltpu
from jax.sharding import PartitionSpec as P

SPAN = 64
F32 = jnp.float32
BF16 = jnp.bfloat16
NN = (((1,), (0,)), ((), ()))
NT = (((1,), (1,)), ((), ()))
TN = (((0,), (0,)), ((), ()))
MESH = pl.DeviceIdType.MESH


def dot(a, b, dims):
    return lax.dot_general(a, b, dims, preferred_element_type=F32)


def split(x):
    high = x.astype(BF16)
    return high, (x - high.astype(F32)).astype(BF16)


def pieces_exact(x):
    high = x.astype(BF16)
    rest = x - high.astype(F32)
    middle = rest.astype(BF16)
    return high, middle, (rest - middle.astype(F32)).astype(BF16)


def dot_exact(x, b):
    rows = x.shape[0]
    out = dot(jnp.concatenate(pieces_exact(x), axis=0), b, NN)
    return out[:rows] + out[rows : 2 * rows] + out[2 * rows :]


def dot_fine(x, b, dims):
    high, low = split(x)
    return dot(high, b, dims) + dot(low, b, dims)


def span_level(a, b, levels):
    return 0 if a == b else min(levels - 1, (a ^ b).bit_length())


def kernel(
    seq_count,
    head_count,
    q_ref,
    k_ref,
    v_ref,
    g_ref,
    lg_ref,
    lw_ref,
    ds_ref,
    gq_ref,
    gk_ref,
    gv_ref,
    gl_ref,
    gg_ref,
    cum_s,
    col_s,
    lead_s,
    tail_s,
    bias_s,
    vt_s,
    gt_s,
    vg_s,
    gq_s,
    gk_s,
    drift_s,
    coef_s,
    state_s,
    back_s,
    lvl,
    got_s,
    got_u,
    sum_s,
    sum_u,
    dec,
    got_dec,
    tot,
    sq,
    lvl_send,
    lvl_recv,
    fwd_send,
    fwd_recv,
    s_send,
    s_recv,
    u_send,
    u_recv,
    d_send,
    d_recv,
    t_send,
    t_recv,
    q_send,
    q_recv,
):
    tok = q_ref.shape[0]
    heads = lg_ref.shape[0]
    levels = lw_ref.shape[0]
    dk = q_ref.shape[1] // heads
    dv = v_ref.shape[1] // heads
    group = dk // dv
    pairs = heads // group
    spans = tok // SPAN
    span_bits = spans.bit_length() - 1
    bits = seq_count.bit_length() - 1
    half = heads // 2
    cross = [min(span_bits + 1 + b, levels - 1) for b in range(bits)]
    slots = sorted(set(cross))
    place = lax.axis_index("seq")
    row = lax.axis_index("head")
    bit = [(place // (1 << b)) % 2 for b in range(bits)]
    peer = [place + (1 - 2 * bit[b]) * (1 << b) for b in range(bits)]
    want_s = [(place // (2 << b)) != (seq_count // (2 << b)) - 1 for b in range(bits)]
    mine = bit[0] * half
    theirs = (1 - bit[0]) * half

    barrier = pltpu.get_barrier_semaphore()
    for o in range(1, seq_count):
        pl.semaphore_signal(
            barrier, inc=1, device_id={"seq": (place + o) % seq_count}, device_id_type=MESH
        )
    for o in range(1, head_count):
        pl.semaphore_signal(
            barrier, inc=1, device_id={"head": (row + o) % head_count}, device_id_type=MESH
        )

    rows_i = lax.broadcasted_iota(jnp.int32, (tok, tok), 0)
    cols_i = lax.broadcasted_iota(jnp.int32, (tok, tok), 1)
    tri = (rows_i <= cols_i).astype(F32)
    starts = jnp.broadcast_to(ds_ref[...].astype(F32), (8, tok))
    both = jnp.concatenate([lg_ref[...], starts], axis=0)
    cum_all = lax.dot_general(
        both, tri, NN, precision=lax.Precision.HIGHEST, preferred_element_type=F32
    )
    cum_t = jnp.transpose(cum_all)
    cum = cum_all[:heads]
    reset = cum_all[heads : heads + 1]
    reset_col = cum_t[:, heads : heads + 1]
    bias_s[...] = jnp.where((rows_i <= cols_i) & (reset == reset_col), 0.0, -1e30)
    end = cum[:, tok - 1 : tok]
    reset_end = reset[:, tok - 1 : tok]
    cum_s[...] = cum
    lead_s[...] = jnp.where(reset == 0, jnp.exp(cum), 0.0)
    tail_s[...] = jnp.where(reset == reset_end, jnp.exp(end - cum), 0.0)
    dec[0] = jnp.broadcast_to(jnp.where(reset_end == 0, jnp.exp(end), 0.0), (heads, dk))
    for h in range(heads):
        col_s[h] = jnp.broadcast_to(cum_t[:, h : h + 1], (tok, tok))

    def states(p, _):
        lanes = pl.ds(pl.multiple_of(p * dk, dk), dk)
        vt = jnp.transpose(v_ref[:, lanes].astype(F32))
        gt = jnp.transpose(g_ref[:, lanes].astype(F32))
        vt_s[p] = vt.astype(BF16)
        gt_s[p] = gt.astype(BF16)
        for i in range(group):
            h = p * group + i
            wide = pl.ds(pl.multiple_of(h * dk, dk), dk)
            part = slice(i * dv, (i + 1) * dv)
            tail = tail_s[pl.ds(h, 1), :]
            lead = lead_s[pl.ds(h, 1), :]
            state_s[h] = dot_fine(vt[part] * tail, k_ref[:, wide], NN)
            gw = jnp.concatenate(
                [gt[part] * (lead * lw_ref[l, pl.ds(h, 1), :]) for l in slots], axis=0
            )
            back = dot_fine(gw, q_ref[:, wide], NN)
            for n in range(len(slots)):
                back_s[n, h] = back[n * dv : (n + 1) * dv]
        return 0

    lax.fori_loop(0, pairs, states, 0, unroll=2)
    pl.semaphore_wait(barrier, seq_count - 1 + head_count - 1)

    def slot(b):
        return slots.index(cross[b])

    def remote(src, dst, send, recv, b):
        return pltpu.make_async_remote_copy(
            src_ref=src,
            dst_ref=dst,
            send_sem=send,
            recv_sem=recv,
            device_id={"seq": peer[b]},
            device_id_type=MESH,
        )

    own = pl.ds(mine, half)
    other = pl.ds(theirs, half)

    def u_copy(b, j):
        src = back_s.at[slot(j), other] if b == 0 else sum_u.at[b, j]
        return remote(src, got_u.at[b, j], u_send.at[b, j], u_recv.at[b, j], b)

    def s_copy(b):
        src = state_s.at[other] if b == 0 else sum_s.at[b]
        return remote(src, got_s.at[b], s_send.at[b], s_recv.at[b], b)

    def d_copy(b):
        return remote(dec.at[b], got_dec.at[b], d_send.at[b], d_recv.at[b], b)

    def level_copy(b, low):
        if b == 0:
            src = state_s if low else back_s.at[slot(0)]
            return [
                remote(src.at[part], lvl.at[0, part], lvl_send.at[0, n], lvl_recv.at[0, n], 0)
                for n, part in enumerate((other, own))
            ]
        src = sum_s.at[b] if low else sum_u.at[b, b]
        return [remote(src, lvl.at[b, own], lvl_send.at[b, 0], lvl_recv.at[b, 0], b)]

    def level_wait(b, n):
        part = other if n == 1 else own
        return remote(
            lvl.at[b, part], lvl.at[b, part], lvl_send.at[b, n], lvl_recv.at[b, n], b
        )

    def forward_copy(b, part):
        return remote(lvl.at[b, part], lvl.at[b, part], fwd_send.at[b], fwd_recv.at[b], 0)

    def land(b):
        up_summed = (bit[b] == 1) & want_s[b]

        @pl.when(jnp.logical_not(up_summed))
        def _():
            level_wait(b, 0).wait_recv()

        if b > 0:
            forward_copy(b, own).start()

    def begin(b):
        d_copy(b).start()

        early = 0 if b in (0, bits - 1) else 1

        @pl.when((bit[b] == 0) & (want_s[b] | (early == 0)))
        def _():
            for c in level_copy(b, True):
                c.start()

        if b < bits - 1:

            @pl.when((bit[b] == 1) & want_s[b])
            def _():
                s_copy(b).start()

            for j in range(b + 1, bits):

                @pl.when(bit[j] == 1)
                def _(j=j):
                    u_copy(b, j).start()

        if early == 0:

            @pl.when(bit[b] == 1)
            def _():
                for c in level_copy(b, False):
                    c.start()

    def begin_late(b):
        if b in (0, bits - 1):
            return

        @pl.when((bit[b] == 0) & jnp.logical_not(want_s[b]))
        def _():
            for c in level_copy(b, True):
                c.start()

        @pl.when(bit[b] == 1)
        def _():
            for c in level_copy(b, False):
                c.start()

    def join(b):
        d_copy(b).wait_recv()
        up = bit[b].astype(F32)
        got = got_dec[b]
        now = dec[b]
        dec[b + 1] = got * now
        if b == bits - 1:
            return
        base_s = state_s.at[own] if b == 0 else sum_s.at[b]

        @pl.when(want_s[b])
        def _():
            @pl.when(bit[b] == 1)
            def _():
                level_wait(b, 0).wait_recv()

                def body(i, _):
                    d = dec[b, pl.ds(mine + i, 1), :]
                    sum_s[b + 1, i] = d * lvl[b, mine + i] + base_s[i]
                    return 0

                lax.fori_loop(0, half, body, 0, unroll=True)

            @pl.when(bit[b] == 0)
            def _():
                s_copy(b).wait_recv()

                def body(i, _):
                    d = got_dec[b, pl.ds(mine + i, 1), :]
                    sum_s[b + 1, i] = d * base_s[i] + got_s[b, i]
                    return 0

                lax.fori_loop(0, half, body, 0, unroll=True)

        for j in range(b + 1, bits):
            base_u = back_s.at[slot(j), own] if b == 0 else sum_u.at[b, j]

            @pl.when(bit[j] == 1)
            def _(j=j, base_u=base_u):
                u_copy(b, j).wait_recv()

                def body(i, _):
                    d0 = dec[b, pl.ds(mine + i, 1), :]
                    d1 = got_dec[b, pl.ds(mine + i, 1), :]
                    a = up * d1 + (1.0 - up)
                    c = (1.0 - up) * d0 + up
                    sum_u[b + 1, j, i] = a * base_u[i] + c * got_u[b, j, i]
                    return 0

                lax.fori_loop(0, half, body, 0, unroll=True)

    span_of = lax.broadcasted_iota(jnp.int32, (1, tok), 1) // SPAN

    def local(p, _):
        vt = vt_s[p]
        gt = gt_s[p]
        lanes = pl.ds(pl.multiple_of(p * dk, dk), dk)
        v_blk = v_ref[:, lanes]
        for i in range(group):
            h = p * group + i
            wide = pl.ds(pl.multiple_of(h * dk, dk), dk)
            part = slice(i * dv, (i + 1) * dv)
            q = q_ref[:, wide]
            k = k_ref[:, wide]
            score = dot(k, q, NT)
            pair = dot(v_blk[:, part], gt[part], NN)
            decay = jnp.exp((cum_s[pl.ds(h, 1), :] - col_s[h]) + bias_s[...])
            seen = decay * score
            both_p = seen * pair
            gains = [lw_ref[l, pl.ds(h, 1), :] for l in range(span_bits + 1)]
            level_rows = [jnp.zeros((1, tok), F32) for _ in range(span_bits + 1)]
            mixed, graded = [], []
            for cs in range(spans):
                rows = slice(cs * SPAN, (cs + 1) * SPAN)
                total = jnp.sum(both_p[rows], axis=0, keepdims=True)
                gain = jnp.zeros((1, tok), F32)
                for ct in range(cs, spans):
                    l = span_level(cs, ct, levels)
                    hit = span_of == ct
                    gain = jnp.where(hit, gains[l], gain)
                    level_rows[l] = level_rows[l] + jnp.where(hit, total, 0.0)
                mixed.append(seen[rows] * gain)
                graded.append(decay[rows] * gain * pair[rows])
            mix = jnp.concatenate(mixed, axis=0).astype(BF16)
            grade = jnp.concatenate(graded, axis=0).astype(BF16)
            for l in range(span_bits + 1):
                gl_ref[l, pl.ds(h, 1), :] = level_rows[l]
            drift_s[pl.ds(h, 1), :] = jnp.sum(mix.astype(F32) * pair, axis=0, keepdims=True)
            vg_s[p, part] = dot(gt[part], mix, NT)
            gk_s[h] = dot(grade, q, NN)
            gq_s[h] = dot(grade, k, TN)
        return 0

    begin(0)
    lax.fori_loop(0, pairs // 4, local, 0, unroll=2)
    join(0)
    if bits > 1:
        begin(1)
    lax.fori_loop(pairs // 4, pairs, local, 0, unroll=2)
    for b in range(1, bits):
        join(b)
        if b + 1 < bits:
            begin(b + 1)
        begin_late(b)
        land(b - 1)
    land(bits - 1)

    inner_f = jnp.ones((heads, dk), F32)
    inner_b = jnp.ones((heads, dk), F32)
    for b in range(bits):
        up = bit[b].astype(F32)
        got = got_dec[b]
        coef_s[0, b] = inner_f * up
        coef_s[1, b] = inner_b * (1.0 - up)
        inner_f = inner_f * (up * got + (1.0 - up))
        inner_b = inner_b * ((1.0 - up) * got + up)
    level_wait(0, 1).wait_recv()
    for b in range(1, bits):
        forward_copy(b, other).wait_recv()

    def finish(p, _):
        lanes = pl.ds(pl.multiple_of(p * dk, dk), dk)
        vt = vt_s[p].astype(F32)
        gt = gt_s[p].astype(F32)
        vg_all = []
        for i in range(group):
            h = p * group + i
            wide = pl.ds(pl.multiple_of(h * dk, dk), dk)
            part = slice(i * dv, (i + 1) * dv)
            q = q_ref[:, wide]
            k = k_ref[:, wide]
            tail = tail_s[pl.ds(h, 1), :]
            lead = lead_s[pl.ds(h, 1), :]
            blocks = [lvl[b, h] for b in range(bits)]
            entering = []
            for n in range(len(slots)):
                terms = [
                    coef_s[0, b, pl.ds(h, 1), :] * blocks[b] for b in range(bits) if slot(b) == n
                ]
                entering.append(functools.reduce(jnp.add, terms))
            entering = jnp.concatenate(entering, axis=0)
            after = functools.reduce(
                jnp.add, [coef_s[1, b, pl.ds(h, 1), :] * blocks[b] for b in range(bits)]
            )
            e_high, e_low = split(entering)
            seen = dot(e_high, q, NT) + dot(e_low, q, NT)
            drift = drift_s[pl.ds(h, 1), :]
            gws = []
            for n, l in enumerate(slots):
                gain = lw_ref[l, pl.ds(h, 1), :]
                level = lead * jnp.sum(
                    seen[n * dv : (n + 1) * dv] * gt[part], axis=0, keepdims=True
                )
                gl_ref[l, pl.ds(h, 1), :] = level
                drift = drift + gain * level
                gws.append(gt[part] * (lead * gain))
            gw, gw_low = split(jnp.concatenate(gws, axis=0))
            gq_in = dot(gw, e_high, TN) + dot(gw, e_low, TN) + dot(gw_low, e_high, TN)
            gq_ref[:, wide] = (gq_s[h] + gq_in).astype(BF16)
            a_high, a_low = split(after)
            tv, tv_low = split(vt[part] * tail)
            gk_in = dot(tv, a_high, TN) + dot(tv, a_low, TN) + dot(tv_low, a_high, TN)
            gk_ref[:, wide] = (gk_s[h] + gk_in).astype(BF16)
            vg = vg_s[p, part] + tail * (dot(a_high, k, NT) + dot(a_low, k, NT))
            drift_s[pl.ds(h, 1), :] = drift - jnp.sum(vg * vt[part], axis=0, keepdims=True)
            vg_all.append(vg)
        gv_ref[:, lanes] = jnp.transpose(jnp.concatenate(vg_all, axis=0)).astype(BF16)
        return 0

    lax.fori_loop(0, pairs, finish, 0, unroll=2)
    for l in range(levels):
        if l > span_bits and l not in slots:
            gl_ref[l] = jnp.zeros((heads, tok), F32)

    later = (rows_i >= cols_i).astype(F32)
    local_tail = lax.dot_general(
        drift_s[...], later, NN, precision=lax.Precision.HIGHEST, preferred_element_type=F32
    )
    lane = lax.broadcasted_iota(jnp.int32, (heads, tok), 1)
    first = local_tail[:, 0:1]
    plain = jnp.sum(local_tail, axis=1, keepdims=True)
    square = jnp.sum(local_tail * local_tail, axis=1, keepdims=True)
    tot[place] = jnp.where(lane == 0, first, jnp.where(lane == 1, plain, square))

    def tot_copy(o, slot_at):
        return pltpu.make_async_remote_copy(
            src_ref=tot.at[place],
            dst_ref=tot.at[slot_at],
            send_sem=t_send.at[o],
            recv_sem=t_recv.at[slot_at],
            device_id={"seq": (place + o) % seq_count},
            device_id_type=MESH,
        )

    for o in range(1, seq_count):
        tot_copy(o, place).start()
    for o in range(1, seq_count):
        tot_copy(o, (place + o) % seq_count).wait_recv()
    after_total = jnp.zeros((heads, 1), F32)
    my_later = jnp.zeros((heads, 1), F32)
    energy = jnp.zeros((heads, 1), F32)
    for d in reversed(range(seq_count)):
        piece = tot[d]
        my_later = my_later + jnp.where(place == d, 1.0, 0.0) * after_total
        energy = energy + (
            piece[:, 2:3] + after_total * (2.0 * piece[:, 1:2] + tok * after_total)
        )
        after_total = after_total + piece[:, 0:1]
    energy = jnp.sum(jnp.broadcast_to(energy, (heads, dk)), axis=0, keepdims=True)
    sq[row] = jnp.broadcast_to(energy, (8, dk))

    def sq_copy(o, slot_at):
        return pltpu.make_async_remote_copy(
            src_ref=sq.at[row],
            dst_ref=sq.at[slot_at],
            send_sem=q_send.at[o],
            recv_sem=q_recv.at[slot_at],
            device_id={"head": (row + o) % head_count},
            device_id_type=MESH,
        )

    for o in range(1, head_count):
        sq_copy(o, row).start()
    for o in range(1, head_count):
        sq_copy(o, (row + o) % head_count).wait_recv()
    whole = sq[0]
    for r in range(1, head_count):
        whole = whole + sq[r]
    count = heads * tok * seq_count * head_count
    factor = jnp.minimum(1.0, lax.rsqrt(whole[0:1] / count + 1e-6))
    gg_ref[...] = (local_tail + my_later) * factor

    for b in range(bits):
        d_copy(b).wait_send()
        for n in range(2 if b == 0 else 1):
            level_wait(b, n).wait_send()
        if b > 0:
            forward_copy(b, own).wait_send()
        if b < bits - 1:

            @pl.when((bit[b] == 1) & want_s[b])
            def _(b=b):
                s_copy(b).wait_send()

            for j in range(b + 1, bits):

                @pl.when(bit[j] == 1)
                def _(b=b, j=j):
                    u_copy(b, j).wait_send()

    for o in range(1, seq_count):
        tot_copy(o, place).wait_send()
    for o in range(1, head_count):
        sq_copy(o, row).wait_send()


def chunked_kernel(
    seq_count,
    head_count,
    q_hbm,
    k_hbm,
    v_hbm,
    g_hbm,
    lg_hbm,
    lw_hbm,
    ds_hbm,
    gq_ref,
    gk_ref,
    gv_ref,
    gl_ref,
    tail_ref,
    msg,
    q_ref,
    k_ref,
    v_ref,
    g_ref,
    lg_ref,
    lw_ref,
    ds_ref,
    cum_s,
    col_s,
    lead_s,
    tail_s,
    bias_s,
    vt_s,
    gt_s,
    vg_s,
    gq_s,
    gk_s,
    drift_s,
    coef_s,
    mix_s,
    st,
    got_a,
    got_b,
    sum_a,
    sum_b,
    sum_q,
    lvl,
    decs,
    i_sem,
    a_send,
    a_recv,
    b_send,
    b_recv,
    p_send,
    p_recv,
    xa_send,
    xa_recv,
    xb_send,
    xb_recv,
    y_send,
    y_recv,
    f_send,
    f_recv,
    d_send,
    d_recv,
    t_send,
    t_recv,
    round_sem,
    plane_sem,
):
    tok = q_ref.shape[0]
    heads = lg_ref.shape[0]
    levels = lw_ref.shape[0]
    dk = q_ref.shape[1] // heads
    dv = v_ref.shape[1] // heads
    group = dk // dv
    pairs = heads // group
    spans = tok // SPAN
    span_bits = spans.bit_length() - 1
    bits = seq_count.bit_length() - 1
    half = heads // 2
    chunks = half // group
    cross = [min(span_bits + 1 + b, levels - 1) for b in range(bits)]
    slots = sorted(set(cross))
    kind = [1 + slots.index(l) for l in cross]
    place = lax.axis_index("seq")
    row = lax.axis_index("head")
    core, x, y = [(place // (1 << b)) % 2 for b in range(bits)]
    peer = [place + (1 - 2 * u) * (1 << b) for b, u in enumerate((core, x, y))]
    first_chip = (1 - x) * (1 - y)
    second_chip = x * (1 - y)
    mine = core * half
    theirs = (1 - core) * half

    has_next = (row < head_count - 1).astype(jnp.int32)
    has_last = (row > 0).astype(jnp.int32)

    def greet(sem):
        @pl.when(has_next == 1)
        def _():
            pl.semaphore_signal(sem, inc=1, device_id={"head": row + 1}, device_id_type=MESH)

        @pl.when(has_last == 1)
        def _():
            pl.semaphore_signal(sem, inc=1, device_id={"head": row - 1}, device_id_type=MESH)

    barrier = pltpu.get_barrier_semaphore()
    for b in reversed(range(bits)):
        pl.semaphore_signal(barrier, inc=1, device_id={"seq": peer[b]}, device_id_type=MESH)
    greet(barrier)

    def load(n):
        src = (lg_hbm, ds_hbm, v_hbm, k_hbm, g_hbm, lw_hbm, q_hbm)[n]
        dst = (lg_ref, ds_ref, v_ref, k_ref, g_ref, lw_ref, q_ref)[n]
        return pltpu.make_async_copy(src, dst, i_sem.at[n])

    for n in range(7):
        load(n).start()
    for n in range(2):
        load(n).wait()

    rows_i = lax.broadcasted_iota(jnp.int32, (tok, tok), 0)
    cols_i = lax.broadcasted_iota(jnp.int32, (tok, tok), 1)
    tri = (rows_i <= cols_i).astype(BF16)
    starts = jnp.broadcast_to(ds_ref[...].astype(F32), (8, tok))
    both = jnp.concatenate([lg_ref[...], starts], axis=0)
    cum_all = dot_exact(both, tri)
    cum_t = jnp.transpose(
        jnp.concatenate([cum_all, jnp.zeros((dk - heads - 8, tok), F32)], axis=0)
    )
    cum = cum_all[:heads]
    reset = cum_all[heads : heads + 1]
    reset_col = cum_t[:, heads : heads + 1]
    bias_s[...] = jnp.where((rows_i <= cols_i) & (reset == reset_col), 0.0, -1e30)
    end = cum[:, tok - 1 : tok]
    reset_end = reset[:, tok - 1 : tok]
    cum_s[...] = cum
    lead_s[...] = jnp.where(reset == 0, jnp.exp(cum), 0.0)
    tail_s[...] = jnp.where(reset == reset_end, jnp.exp(end - cum), 0.0)
    lane_row = lax.broadcasted_iota(jnp.int32, (1, dk), 1)
    end_row = jnp.where(lane_row < heads, cum_t[tok - 1 : tok, :], 0.0)
    decs[0] = jnp.where(reset_end == 0, jnp.exp(end_row), 0.0)
    for h in range(heads):
        col_s[h] = jnp.broadcast_to(cum_t[:, h : h + 1], (tok, tok))

    def states(p, _):
        lanes = pl.ds(pl.multiple_of(p * dk, dk), dk)
        vt = jnp.transpose(v_ref[:, lanes].astype(F32))
        gt = jnp.transpose(g_ref[:, lanes].astype(F32))
        vt_s[p] = vt.astype(BF16)
        gt_s[p] = gt.astype(BF16)
        for i in range(group):
            h = p * group + i
            wide = pl.ds(pl.multiple_of(h * dk, dk), dk)
            part = slice(i * dv, (i + 1) * dv)
            tail = tail_s[pl.ds(h, 1), :]
            lead = lead_s[pl.ds(h, 1), :]
            st[0, h] = dot_fine(vt[part] * tail, k_ref[:, wide], NN)
            gw = jnp.concatenate(
                [gt[part] * (lead * lw_ref[l, pl.ds(h, 1), :]) for l in slots], axis=0
            )
            back = dot_fine(gw, q_ref[:, wide], NN)
            for n in range(len(slots)):
                st[1 + n, h] = back[n * dv : (n + 1) * dv]
        return 0

    for n in range(2, 7):
        load(n).wait()
    own_pair = core * chunks
    far_pair = (1 - core) * chunks
    def states_from(base):
        lax.fori_loop(0, 2, lambda n, _: states(base + n, 0), 0, unroll=2)

    states_from(far_pair)
    pl.semaphore_wait(barrier, bits + has_next + has_last)
    rounds = head_count - 2
    if rounds > 0:
        greet(round_sem.at[0])

    def remote(src, dst, send, recv, b):
        return pltpu.make_async_remote_copy(
            src_ref=src,
            dst_ref=dst,
            send_sem=send,
            recv_sem=recv,
            device_id={"seq": peer[b]},
            device_id_type=MESH,
        )

    def of(base, c):
        return pl.ds(base + c * group, group)

    def at(c):
        return pl.ds(c * group, group)

    kind_a = y * kind[2]
    kind_b = x * kind[1]
    slot_out = bits - (bits - 1) * first_chip
    slot_in = bits - (bits - 1) * second_chip

    def dec_copy(n):
        return remote(decs.at[2 * n], decs.at[2 * n + 1], d_send.at[n], d_recv.at[n], n)

    def a_copy(c):
        return remote(
            st.at[kind_a, of(theirs, c)], got_a.at[at(c)], a_send.at[c], a_recv.at[c], 0
        )

    def b_copy(c):
        return remote(
            st.at[kind_b, of(theirs, c)], got_b.at[at(c)], b_send.at[c], b_recv.at[c], 0
        )

    def p_copy(n):
        part = pl.ds(n * half, half)
        return remote(
            st.at[core * kind[0], part], lvl.at[0, part], p_send.at[n], p_recv.at[n], 0
        )

    piece = 1
    pieces = half // piece

    def xa_copy(n):
        here = pl.ds(n * piece, piece)
        there = pl.ds(mine + n * piece, piece)
        return remote(
            sum_a.at[here], lvl.at[slot_out, there], xa_send.at[n], xa_recv.at[n], 1
        )

    def xb_copy(n):
        here = pl.ds(n * piece, piece)
        there = pl.ds(mine + n * piece, piece)
        return remote(sum_b.at[here], lvl.at[1, there], xb_send.at[n], xb_recv.at[n], 1)

    def pieces_of(c):
        return range(c * group // piece, (c + 1) * group // piece)

    def y_copy(n):
        here = pl.ds(n * piece, piece)
        there = pl.ds(mine + n * piece, piece)
        return remote(sum_q.at[here], lvl.at[2, there], y_send.at[n], y_recv.at[n], 2)

    def f_copy(j, base, c):
        part = lvl.at[j, of(base, c)]
        return remote(part, part, f_send.at[j - 1, c], f_recv.at[j - 1, c], 0)

    dec_copy(0).start()
    for c in range(2):
        a_copy(c).start()
    states_from(far_pair + 2)
    for c in range(2, chunks):
        a_copy(c).start()
    states_from(own_pair)
    states_from(own_pair + 2)

    span_of = lax.broadcasted_iota(jnp.int32, (1, tok), 1) // SPAN

    def local(p, _):
        vt = vt_s[p]
        gt = gt_s[p]
        lanes = pl.ds(pl.multiple_of(p * dk, dk), dk)
        v_blk = v_ref[:, lanes]
        for i in range(group):
            h = p * group + i
            wide = pl.ds(pl.multiple_of(h * dk, dk), dk)
            part = slice(i * dv, (i + 1) * dv)
            q = q_ref[:, wide]
            k = k_ref[:, wide]
            score = dot(k, q, NT)
            pair = dot(v_blk[:, part], gt[part], NN)
            decay = jnp.exp((cum_s[pl.ds(h, 1), :] - col_s[h]) + bias_s[...])
            seen = decay * score
            both_p = seen * pair
            gains = [lw_ref[l, pl.ds(h, 1), :] for l in range(span_bits + 1)]
            level_rows = [jnp.zeros((1, tok), F32) for _ in range(span_bits + 1)]
            mixed, graded = [], []
            for cs in range(spans):
                rows = slice(cs * SPAN, (cs + 1) * SPAN)
                total = jnp.sum(both_p[rows], axis=0, keepdims=True)
                gain = jnp.zeros((1, tok), F32)
                for ct in range(cs, spans):
                    l = span_level(cs, ct, levels)
                    hit = span_of == ct
                    gain = jnp.where(hit, gains[l], gain)
                    level_rows[l] = level_rows[l] + jnp.where(hit, total, 0.0)
                mixed.append(seen[rows] * gain)
                graded.append(decay[rows] * gain * pair[rows])
            mix = jnp.concatenate(mixed, axis=0).astype(BF16)
            grade = jnp.concatenate(graded, axis=0).astype(BF16)
            for l in range(span_bits + 1):
                gl_ref[l, pl.ds(h, 1), :] = level_rows[l]
            drift_s[pl.ds(h, 1), :] = jnp.sum(mix.astype(F32) * pair, axis=0, keepdims=True)
            vg_s[p, part] = dot(gt[part], mix, NT)
            gk_s[h] = dot(grade, q, NN)
            gq_s[h] = dot(grade, k, TN)
        return 0

    def spread(device_rows):
        t = jnp.transpose(
            jnp.concatenate(
                device_rows + [jnp.zeros((8 - len(device_rows), dk), F32)], axis=0
            )
        )
        return [
            jnp.broadcast_to(t[:heads, n : n + 1], (heads, dk)) for n in range(len(device_rows))
        ]

    def weigh(n, swap, own, got):
        w = (swap % 2).astype(F32)
        mix_s[n, 0] = own * (1.0 - w) + w
        mix_s[n, 1] = got * w + (1.0 - w)

    def combine(n, c, own_at, got_at, put):
        for i in range(group):
            r = c * group + i
            ca = mix_s[n, 0, pl.ds(mine + r, 1), :]
            cb = mix_s[n, 1, pl.ds(mine + r, 1), :]
            put[r] = ca * own_at(r) + cb * got_at(r)

    def local_pairs(first, last):
        lax.fori_loop(first, last, local, 0, unroll=2)

    def x_start(n):
        if n < pieces:
            xa_copy(n).start()
        elif n < 2 * pieces:

            @pl.when(first_chip == 0)
            def _():
                xb_copy(n - pieces).start()

    def x_sent(n):
        if n < pieces:
            xa_copy(n).wait_send()
        else:

            @pl.when(first_chip == 0)
            def _():
                xb_copy(n - pieces).wait_send()

    ahead = 5

    def x_next(n):
        x_sent(n)
        x_start(n + ahead)

    dec_copy(0).wait_recv()
    decs[2] = decs[0] * decs[1]
    d_self, d_pair = spread([decs[0], decs[1]])
    weigh(0, core + y, d_pair, d_self)
    weigh(1, core + x, d_pair, d_self)
    for c in range(chunks):
        a_copy(c).wait_recv()
        combine(0, c, lambda r: st[kind_a, mine + r], lambda r: got_a[r], sum_a)
        for n in pieces_of(c):
            if n < ahead:
                x_start(n)
        if c == 1:
            dec_copy(1).start()

            @pl.when(first_chip == 0)
            def _():
                for n in range(chunks):
                    b_copy(n).start()

    local_pairs(0, 4)

    @pl.when(first_chip == 0)
    def _():
        for c in range(chunks):
            b_copy(c).wait_recv()
            combine(1, c, lambda r: st[kind_b, mine + r], lambda r: got_b[r], sum_b)

    for r in range(1, rounds + 1):
        pl.semaphore_wait(round_sem.at[r - 1], has_next + has_last)
        if r < rounds:
            greet(round_sem.at[r])
    x_next(0)
    x_next(1)
    p_copy(0).start()
    local_pairs(4, 6)
    dec_copy(1).wait_recv()
    (d_side,) = spread([decs[3]])
    weigh(2, x + y, d_side, d_self * d_pair)
    inner_f = jnp.ones((heads, dk), F32)
    inner_b = jnp.ones((heads, dk), F32)
    for b, (u, got) in enumerate(((core, d_pair), (x, d_side), (y, None))):
        up = u.astype(F32)
        coef_s[0, b] = inner_f * up
        coef_s[1, b] = inner_b * (1.0 - up)
        if got is not None:
            inner_f = inner_f * (up * got + (1.0 - up))
            inner_b = inner_b * ((1.0 - up) * got + up)
    x_next(2)
    x_next(3)
    p_copy(1).start()
    def turn(n):
        xa_copy(n).wait_recv()
        for r in range(n * piece, (n + 1) * piece):
            ca = mix_s[2, 0, pl.ds(mine + r, 1), :]
            cb = mix_s[2, 1, pl.ds(mine + r, 1), :]
            sum_q[r] = ca * sum_a[r] + cb * lvl[slot_in, mine + r]
        y_copy(n).start()
        if (n + 1) * piece % group == 0:

            @pl.when(second_chip == 1)
            def _():
                f_copy(1, mine, n * piece // group).start()

    turn(0)
    local_pairs(6, pairs)
    x_next(4)
    turn(1)
    x_next(5)
    turn(2)
    x_next(6)
    turn(3)
    x_next(7)
    turn(4)
    x_next(8)
    turn(5)
    turn(6)
    x_next(9)
    x_next(10)
    turn(7)

    def incoming(h):
        blocks = [lvl[b, h] for b in range(bits)]
        entering = []
        for n in range(len(slots)):
            terms = [
                coef_s[0, b, pl.ds(h, 1), :] * blocks[b]
                for b in range(bits)
                if kind[b] == 1 + n
            ]
            entering.append(functools.reduce(jnp.add, terms))
        after = functools.reduce(
            jnp.add, [coef_s[1, b, pl.ds(h, 1), :] * blocks[b] for b in range(bits)]
        )
        return split(jnp.concatenate(entering, axis=0)), split(after)

    def finish_drift(p):
        vt = vt_s[p].astype(F32)
        gt = gt_s[p].astype(F32)
        for i in range(group):
            h = p * group + i
            wide = pl.ds(pl.multiple_of(h * dk, dk), dk)
            part = slice(i * dv, (i + 1) * dv)
            q = q_ref[:, wide]
            k = k_ref[:, wide]
            tail = tail_s[pl.ds(h, 1), :]
            lead = lead_s[pl.ds(h, 1), :]
            (e_high, e_low), (a_high, a_low) = incoming(h)
            seen = dot(e_high, q, NT) + dot(e_low, q, NT)
            drift = drift_s[pl.ds(h, 1), :]
            for n, l in enumerate(slots):
                level = lead * jnp.sum(
                    seen[n * dv : (n + 1) * dv] * gt[part], axis=0, keepdims=True
                )
                gl_ref[l, pl.ds(h, 1), :] = level
                drift = drift + lw_ref[l, pl.ds(h, 1), :] * level
            vg = vg_s[p, part] + tail * (dot(a_high, k, NT) + dot(a_low, k, NT))
            drift_s[pl.ds(h, 1), :] = drift - jnp.sum(vg * vt[part], axis=0, keepdims=True)
            vg_s[p, part] = vg

    def finish_out(p):
        lanes = pl.ds(pl.multiple_of(p * dk, dk), dk)
        vt = vt_s[p].astype(F32)
        gt = gt_s[p].astype(F32)
        for i in range(group):
            h = p * group + i
            wide = pl.ds(pl.multiple_of(h * dk, dk), dk)
            part = slice(i * dv, (i + 1) * dv)
            tail = tail_s[pl.ds(h, 1), :]
            lead = lead_s[pl.ds(h, 1), :]
            (e_high, e_low), (a_high, a_low) = incoming(h)
            gws = [gt[part] * (lead * lw_ref[l, pl.ds(h, 1), :]) for l in slots]
            gw, gw_low = split(jnp.concatenate(gws, axis=0))
            gq_in = dot(gw, e_high, TN) + dot(gw, e_low, TN) + dot(gw_low, e_high, TN)
            gq_ref[:, wide] = (gq_s[h] + gq_in).astype(BF16)
            tv, tv_low = split(vt[part] * tail)
            gk_in = dot(tv, a_high, TN) + dot(tv, a_low, TN) + dot(tv_low, a_high, TN)
            gk_ref[:, wide] = (gk_s[h] + gk_in).astype(BF16)
        gv_ref[:, lanes] = jnp.transpose(vg_s[p]).astype(BF16)

    for n in range(2):
        p_copy(n).wait_recv()
    for c in range(chunks):
        for n in ((), (), (), ())[c]:
            x_next(n)
        for n in pieces_of(c):
            y_copy(n).wait_recv()
        f_copy(2, mine, c).start()

        @pl.when(second_chip == 0)
        def _(c=c):
            for n in pieces_of(c):
                xb_copy(n).wait_recv()
            f_copy(1, mine, c).start()

        if c == 0:
            for o in range(1, head_count):
                pl.semaphore_signal(
                    plane_sem,
                    inc=1,
                    device_id={"head": (row + o) % head_count},
                    device_id_type=MESH,
                )
        finish_drift(own_pair + c)
        for j in (1, 2):
            f_copy(j, theirs, c).wait_recv()
        finish_drift(far_pair + c)

    later = (rows_i >= cols_i).astype(BF16)
    local_tail = dot_exact(drift_s[...], later)
    tail_ref[...] = local_tail
    lane = lax.broadcasted_iota(jnp.int32, (heads, tok), 1)
    head = lax.broadcasted_iota(jnp.int32, (heads, tok), 0)
    sums = [
        local_tail[:, 0:1],
        jnp.sum(local_tail, axis=1, keepdims=True),
        jnp.sum(local_tail * local_tail, axis=1, keepdims=True),
    ]
    packed = jnp.zeros((heads, tok), F32)
    for n, column in enumerate(sums):
        packed = jnp.where(lane == head + n * heads, column, packed)
    slot = row * seq_count + place
    total = seq_count * head_count
    msg[slot] = jnp.sum(packed, axis=0, keepdims=True)

    def tail_copy(to_row, to_place):
        return pltpu.make_async_remote_copy(
            src_ref=msg.at[slot],
            dst_ref=msg.at[slot],
            send_sem=t_send.at[0],
            recv_sem=t_recv.at[0],
            device_id={"seq": to_place, "head": to_row},
            device_id_type=MESH,
        )

    def tail_all():
        others = msg.at[pl.ds(0, total - 1)]
        return pltpu.make_async_remote_copy(
            src_ref=others,
            dst_ref=others,
            send_sem=t_send.at[0],
            recv_sem=t_recv.at[0],
            device_id={"seq": peer[0]},
            device_id_type=MESH,
        )

    pl.semaphore_wait(plane_sem, head_count - 1)
    for o in list(range(1, head_count)) + [0]:
        for n in list(range(1, seq_count)) + [0]:
            if (o, n) != (0, 0):
                tail_copy((row + o) % head_count, (place + n) % seq_count).start()

    def outputs(p, _):
        finish_out(p)
        return 0

    lax.fori_loop(0, pairs, outputs, 0, unroll=2)
    for l in range(levels):
        if l > span_bits and l not in slots:
            gl_ref[l] = jnp.zeros((heads, tok), F32)

    for n in range(2):
        dec_copy(n).wait_send()
    for n in range(2):
        p_copy(n).wait_send()
    for n in range(2 * pieces - ahead, 2 * pieces):
        x_sent(n)
    for c in range(chunks):
        a_copy(c).wait_send()
        for n in pieces_of(c):
            y_copy(n).wait_send()
        for j in (1, 2):
            f_copy(j, mine, c).wait_send()

    @pl.when(first_chip == 0)
    def _():
        for c in range(chunks):
            b_copy(c).wait_send()

    tail_all().wait_send()
    tail_all().wait_recv()


def finish_kernel(
    seq_count,
    head_count,
    gq_ref,
    gk_ref,
    gv_ref,
    gl_ref,
    tail_ref,
    msg,
    gq_out,
    gk_out,
    gv_out,
    gl_out,
    gg_out,
    gg_s,
    sems,
):
    copies = [
        pltpu.make_async_copy(src, dst, sems.at[n])
        for n, (src, dst) in enumerate(
            (
                (gq_ref, gq_out),
                (gk_ref, gk_out),
                (gv_ref, gv_out),
                (gl_ref, gl_out),
                (gg_s, gg_out),
            )
        )
    ]
    for c in copies[:4]:
        c.start()
    heads, tok = tail_ref.shape
    dk = msg.shape[2]
    total = seq_count * head_count
    slot = lax.axis_index("head") * seq_count + lax.axis_index("seq")
    rows = msg[:, 0, :]
    row_u = lax.broadcasted_iota(jnp.int32, (total, total), 0)
    row_v = lax.broadcasted_iota(jnp.int32, (total, total), 1)
    behind = ((row_u // seq_count == row_v // seq_count) & (row_v > row_u)).astype(BF16)
    after_rows = sum(dot(behind, piece, NN) for piece in pieces_exact(rows))
    plain = pltpu.roll(rows, dk - heads, 1)
    square = pltpu.roll(rows, dk - 2 * heads, 1)
    energy = square + after_rows * (2.0 * plain + tok * after_rows)
    lane_all = lax.broadcasted_iota(jnp.int32, (total, dk), 1)
    slot_all = lax.broadcasted_iota(jnp.int32, (total, dk), 0)
    energy = jnp.sum(jnp.where(lane_all < heads, energy, 0.0), axis=0, keepdims=True)
    whole = jnp.sum(energy, axis=1, keepdims=True)
    my_row = jnp.sum(jnp.where(slot_all == slot, after_rows, 0.0), axis=0, keepdims=True)
    lane = lax.broadcasted_iota(jnp.int32, (heads, dk), 1)
    head = lax.broadcasted_iota(jnp.int32, (heads, dk), 0)
    my_later = jnp.sum(jnp.where(lane == head, my_row, 0.0), axis=1, keepdims=True)
    count = heads * tok * total
    factor = jnp.minimum(1.0, lax.rsqrt(whole / count + 1e-6))
    gg_s[...] = (tail_ref[...] + my_later) * factor
    copies[4].start()
    for c in copies:
        c.wait()


def write_out(count, *refs):
    sems = refs[-1]
    copies = [
        pltpu.make_async_copy(refs[i], refs[count + i], sems.at[i]) for i in range(count)
    ]
    for c in copies:
        c.start()
    for c in copies:
        c.wait()


def shards(seq_count, head_count, queries, keys, values, out_grad, log_gate, level_weight, doc_start):
    tok = queries.shape[0]
    heads = log_gate.shape[0]
    levels = level_weight.shape[0]
    dk = queries.shape[1] // heads
    dv = values.shape[1] // heads
    group = dk // dv
    pairs = heads // group
    bits = seq_count.bit_length() - 1
    half = heads // 2
    span_bits = (tok // SPAN).bit_length() - 1
    slots = len({min(span_bits + 1 + b, levels - 1) for b in range(bits)})
    dma = pltpu.SemaphoreType.DMA
    vmem = pltpu.VMEM
    block = (dv, dk)
    scratch = [
        vmem((heads, tok), F32),
        vmem((heads, tok, tok), F32),
        vmem((heads, tok), F32),
        vmem((heads, tok), F32),
        vmem((tok, tok), F32),
        vmem((pairs, group * dv, tok), BF16),
        vmem((pairs, group * dv, tok), BF16),
        vmem((pairs, group * dv, tok), F32),
        vmem((heads, tok, dk), F32),
        vmem((heads, tok, dk), F32),
        vmem((heads, tok), F32),
        vmem((2, bits, heads, dk), F32),
        vmem((heads,) + block, F32),
        vmem((slots, heads) + block, F32),
        vmem((bits, heads) + block, F32),
        vmem((bits, half) + block, F32),
        vmem((bits, bits, half) + block, F32),
        vmem((bits, half) + block, F32),
        vmem((bits, bits, half) + block, F32),
        vmem((bits + 1, heads, dk), F32),
        vmem((bits, heads, dk), F32),
        vmem((seq_count, heads, tok), F32),
        vmem((head_count, 8, dk), F32),
        dma((bits, 2)),
        dma((bits, 2)),
        dma((bits,)),
        dma((bits,)),
        dma((bits,)),
        dma((bits,)),
        dma((bits, bits)),
        dma((bits, bits)),
        dma((bits,)),
        dma((bits,)),
        dma((seq_count,)),
        dma((seq_count,)),
        dma((head_count,)),
        dma((head_count,)),
    ]
    args = (queries, keys, values, out_grad, log_gate, level_weight, doc_start.reshape(1, tok))
    spec = pl.BlockSpec(memory_space=pltpu.VMEM)
    in_spec = spec
    body = kernel
    chunks = half // group
    if bits == 3 and chunks == 4 and chunks * group == half and tok == dk and 3 * heads <= dk:
        body = chunked_kernel
        inputs = [(x.shape, x.dtype) for x in args]
        scratch = [vmem(*x) for x in inputs] + scratch[:12] + [
            vmem((3, 2, heads, dk), F32),
            vmem((1 + slots, heads) + block, F32),
            vmem((half,) + block, F32),
            vmem((half,) + block, F32),
            vmem((half,) + block, F32),
            vmem((half,) + block, F32),
            vmem((half,) + block, F32),
            vmem((bits + 1, heads) + block, F32),
            vmem((4, 1, dk), F32),
            dma((7,)),
            dma((chunks,)),
            dma((chunks,)),
            dma((chunks,)),
            dma((chunks,)),
            dma((2,)),
            dma((2,)),
            dma((half,)),
            dma((half,)),
            dma((half,)),
            dma((half,)),
            dma((half,)),
            dma((half,)),
            dma((2, chunks)),
            dma((2, chunks)),
            dma((2,)),
            dma((2,)),
            dma((1,)),
            dma((1,)),
            pltpu.SemaphoreType.REGULAR((max(1, head_count - 2),)),
            pltpu.SemaphoreType.REGULAR,
        ]
        in_spec = pl.BlockSpec(memory_space=pltpu.HBM)
    outs = [
        (queries.shape, BF16),
        (keys.shape, BF16),
        (values.shape, BF16),
        (level_weight.shape, F32),
        (log_gate.shape, F32),
    ]
    held = list(outs)
    writer = (write_out, len(outs))
    writer_scratch = []
    if body is chunked_kernel:
        held.append(((seq_count * head_count, 1, dk), F32))
        writer = (finish_kernel, seq_count, head_count)
        writer_scratch = [vmem(*outs[-1])]
    results = pl.pallas_call(
        functools.partial(body, seq_count, head_count),
        out_shape=tuple(vmem(shape, dtype) for shape, dtype in held),
        in_specs=[in_spec] * 7,
        out_specs=(spec,) * len(held),
        scratch_shapes=scratch,
        compiler_params=pltpu.CompilerParams(collective_id=0, has_side_effects=True),
    )(*args)
    count = len(outs)
    return pl.pallas_call(
        functools.partial(*writer),
        out_shape=tuple(jax.ShapeDtypeStruct(shape, dtype) for shape, dtype in outs),
        in_specs=[spec] * len(held),
        out_specs=(pl.BlockSpec(memory_space=pltpu.HBM),) * count,
        scratch_shapes=writer_scratch + [dma((count,))],
    )(*[pltpu.with_memory_space_constraint(r, pltpu.VMEM) for r in results])


def solution(mesh):
    return jax.shard_map(
        functools.partial(shards, mesh.shape["seq"], mesh.shape["head"]),
        mesh=mesh,
        in_specs=(
            P("seq", "head"),
            P("seq", "head"),
            P("seq", "head"),
            P("seq", "head"),
            P("head", "seq"),
            P(None, "head", "seq"),
            P("seq"),
        ),
        out_specs=(
            P("seq", "head"),
            P("seq", "head"),
            P("seq", "head"),
            P(None, "head", "seq"),
            P("head", "seq"),
        ),
        check_vma=False,
    )
```

```python
import functools

import jax
import jax.numpy as jnp
from jax import lax
from jax.experimental import pallas as pl
from jax.experimental.pallas import tpu as pltpu
from jax.sharding import PartitionSpec as P

SPAN = 64
F32 = jnp.float32
BF16 = jnp.bfloat16
NN = (((1,), (0,)), ((), ()))
NT = (((1,), (1,)), ((), ()))
TN = (((0,), (0,)), ((), ()))
MESH = pl.DeviceIdType.MESH


def dot(a, b, dims):
    return lax.dot_general(a, b, dims, preferred_element_type=F32)


def split(x):
    high = x.astype(BF16)
    return high, (x - high.astype(F32)).astype(BF16)


def pieces_exact(x):
    high = x.astype(BF16)
    rest = x - high.astype(F32)
    middle = rest.astype(BF16)
    return high, middle, (rest - middle.astype(F32)).astype(BF16)


def dot_exact(x, b):
    rows = x.shape[0]
    out = dot(jnp.concatenate(pieces_exact(x), axis=0), b, NN)
    return out[:rows] + out[rows : 2 * rows] + out[2 * rows :]


def dot_fine(x, b, dims):
    high, low = split(x)
    return dot(high, b, dims) + dot(low, b, dims)


def span_level(a, b, levels):
    return 0 if a == b else min(levels - 1, (a ^ b).bit_length())


def kernel(
    seq_count,
    head_count,
    q_ref,
    k_ref,
    v_ref,
    g_ref,
    lg_ref,
    lw_ref,
    ds_ref,
    gq_ref,
    gk_ref,
    gv_ref,
    gl_ref,
    gg_ref,
    cum_s,
    col_s,
    lead_s,
    tail_s,
    bias_s,
    vt_s,
    gt_s,
    vg_s,
    gq_s,
    gk_s,
    drift_s,
    coef_s,
    state_s,
    back_s,
    lvl,
    got_s,
    got_u,
    sum_s,
    sum_u,
    dec,
    got_dec,
    tot,
    sq,
    lvl_send,
    lvl_recv,
    fwd_send,
    fwd_recv,
    s_send,
    s_recv,
    u_send,
    u_recv,
    d_send,
    d_recv,
    t_send,
    t_recv,
    q_send,
    q_recv,
):
    tok = q_ref.shape[0]
    heads = lg_ref.shape[0]
    levels = lw_ref.shape[0]
    dk = q_ref.shape[1] // heads
    dv = v_ref.shape[1] // heads
    group = dk // dv
    pairs = heads // group
    spans = tok // SPAN
    span_bits = spans.bit_length() - 1
    bits = seq_count.bit_length() - 1
    half = heads // 2
    cross = [min(span_bits + 1 + b, levels - 1) for b in range(bits)]
    slots = sorted(set(cross))
    place = lax.axis_index("seq")
    row = lax.axis_index("head")
    bit = [(place // (1 << b)) % 2 for b in range(bits)]
    peer = [place + (1 - 2 * bit[b]) * (1 << b) for b in range(bits)]
    want_s = [(place // (2 << b)) != (seq_count // (2 << b)) - 1 for b in range(bits)]
    mine = bit[0] * half
    theirs = (1 - bit[0]) * half

    barrier = pltpu.get_barrier_semaphore()
    for o in range(1, seq_count):
        pl.semaphore_signal(
            barrier, inc=1, device_id={"seq": (place + o) % seq_count}, device_id_type=MESH
        )
    for o in range(1, head_count):
        pl.semaphore_signal(
            barrier, inc=1, device_id={"head": (row + o) % head_count}, device_id_type=MESH
        )

    rows_i = lax.broadcasted_iota(jnp.int32, (tok, tok), 0)
    cols_i = lax.broadcasted_iota(jnp.int32, (tok, tok), 1)
    tri = (rows_i <= cols_i).astype(F32)
    starts = jnp.broadcast_to(ds_ref[...].astype(F32), (8, tok))
    both = jnp.concatenate([lg_ref[...], starts], axis=0)
    cum_all = lax.dot_general(
        both, tri, NN, precision=lax.Precision.HIGHEST, preferred_element_type=F32
    )
    cum_t = jnp.transpose(cum_all)
    cum = cum_all[:heads]
    reset = cum_all[heads : heads + 1]
    reset_col = cum_t[:, heads : heads + 1]
    bias_s[...] = jnp.where((rows_i <= cols_i) & (reset == reset_col), 0.0, -1e30)
    end = cum[:, tok - 1 : tok]
    reset_end = reset[:, tok - 1 : tok]
    cum_s[...] = cum
    lead_s[...] = jnp.where(reset == 0, jnp.exp(cum), 0.0)
    tail_s[...] = jnp.where(reset == reset_end, jnp.exp(end - cum), 0.0)
    dec[0] = jnp.broadcast_to(jnp.where(reset_end == 0, jnp.exp(end), 0.0), (heads, dk))
    for h in range(heads):
        col_s[h] = jnp.broadcast_to(cum_t[:, h : h + 1], (tok, tok))

    def states(p, _):
        lanes = pl.ds(pl.multiple_of(p * dk, dk), dk)
        vt = jnp.transpose(v_ref[:, lanes].astype(F32))
        gt = jnp.transpose(g_ref[:, lanes].astype(F32))
        vt_s[p] = vt.astype(BF16)
        gt_s[p] = gt.astype(BF16)
        for i in range(group):
            h = p * group + i
            wide = pl.ds(pl.multiple_of(h * dk, dk), dk)
            part = slice(i * dv, (i + 1) * dv)
            tail = tail_s[pl.ds(h, 1), :]
            lead = lead_s[pl.ds(h, 1), :]
            state_s[h] = dot_fine(vt[part] * tail, k_ref[:, wide], NN)
            gw = jnp.concatenate(
                [gt[part] * (lead * lw_ref[l, pl.ds(h, 1), :]) for l in slots], axis=0
            )
            back = dot_fine(gw, q_ref[:, wide], NN)
            for n in range(len(slots)):
                back_s[n, h] = back[n * dv : (n + 1) * dv]
        return 0

    lax.fori_loop(0, pairs, states, 0, unroll=2)
    pl.semaphore_wait(barrier, seq_count - 1 + head_count - 1)

    def slot(b):
        return slots.index(cross[b])

    def remote(src, dst, send, recv, b):
        return pltpu.make_async_remote_copy(
            src_ref=src,
            dst_ref=dst,
            send_sem=send,
            recv_sem=recv,
            device_id={"seq": peer[b]},
            device_id_type=MESH,
        )

    own = pl.ds(mine, half)
    other = pl.ds(theirs, half)

    def u_copy(b, j):
        src = back_s.at[slot(j), other] if b == 0 else sum_u.at[b, j]
        return remote(src, got_u.at[b, j], u_send.at[b, j], u_recv.at[b, j], b)

    def s_copy(b):
        src = state_s.at[other] if b == 0 else sum_s.at[b]
        return remote(src, got_s.at[b], s_send.at[b], s_recv.at[b], b)

    def d_copy(b):
        return remote(dec.at[b], got_dec.at[b], d_send.at[b], d_recv.at[b], b)

    def level_copy(b, low):
        if b == 0:
            src = state_s if low else back_s.at[slot(0)]
            return [
                remote(src.at[part], lvl.at[0, part], lvl_send.at[0, n], lvl_recv.at[0, n], 0)
                for n, part in enumerate((other, own))
            ]
        src = sum_s.at[b] if low else sum_u.at[b, b]
        return [remote(src, lvl.at[b, own], lvl_send.at[b, 0], lvl_recv.at[b, 0], b)]

    def level_wait(b, n):
        part = other if n == 1 else own
        return remote(
            lvl.at[b, part], lvl.at[b, part], lvl_send.at[b, n], lvl_recv.at[b, n], b
        )

    def forward_copy(b, part):
        return remote(lvl.at[b, part], lvl.at[b, part], fwd_send.at[b], fwd_recv.at[b], 0)

    def land(b):
        up_summed = (bit[b] == 1) & want_s[b]

        @pl.when(jnp.logical_not(up_summed))
        def _():
            level_wait(b, 0).wait_recv()

        if b > 0:
            forward_copy(b, own).start()

    def begin(b):
        d_copy(b).start()

        early = 0 if b in (0, bits - 1) else 1

        @pl.when((bit[b] == 0) & (want_s[b] | (early == 0)))
        def _():
            for c in level_copy(b, True):
                c.start()

        if b < bits - 1:

            @pl.when((bit[b] == 1) & want_s[b])
            def _():
                s_copy(b).start()

            for j in range(b + 1, bits):

                @pl.when(bit[j] == 1)
                def _(j=j):
                    u_copy(b, j).start()

        if early == 0:

            @pl.when(bit[b] == 1)
            def _():
                for c in level_copy(b, False):
                    c.start()

    def begin_late(b):
        if b in (0, bits - 1):
            return

        @pl.when((bit[b] == 0) & jnp.logical_not(want_s[b]))
        def _():
            for c in level_copy(b, True):
                c.start()

        @pl.when(bit[b] == 1)
        def _():
            for c in level_copy(b, False):
                c.start()

    def join(b):
        d_copy(b).wait_recv()
        up = bit[b].astype(F32)
        got = got_dec[b]
        now = dec[b]
        dec[b + 1] = got * now
        if b == bits - 1:
            return
        base_s = state_s.at[own] if b == 0 else sum_s.at[b]

        @pl.when(want_s[b])
        def _():
            @pl.when(bit[b] == 1)
            def _():
                level_wait(b, 0).wait_recv()

                def body(i, _):
                    d = dec[b, pl.ds(mine + i, 1), :]
                    sum_s[b + 1, i] = d * lvl[b, mine + i] + base_s[i]
                    return 0

                lax.fori_loop(0, half, body, 0, unroll=True)

            @pl.when(bit[b] == 0)
            def _():
                s_copy(b).wait_recv()

                def body(i, _):
                    d = got_dec[b, pl.ds(mine + i, 1), :]
                    sum_s[b + 1, i] = d * base_s[i] + got_s[b, i]
                    return 0

                lax.fori_loop(0, half, body, 0, unroll=True)

        for j in range(b + 1, bits):
            base_u = back_s.at[slot(j), own] if b == 0 else sum_u.at[b, j]

            @pl.when(bit[j] == 1)
            def _(j=j, base_u=base_u):
                u_copy(b, j).wait_recv()

                def body(i, _):
                    d0 = dec[b, pl.ds(mine + i, 1), :]
                    d1 = got_dec[b, pl.ds(mine + i, 1), :]
                    a = up * d1 + (1.0 - up)
                    c = (1.0 - up) * d0 + up
                    sum_u[b + 1, j, i] = a * base_u[i] + c * got_u[b, j, i]
                    return 0

                lax.fori_loop(0, half, body, 0, unroll=True)

    span_of = lax.broadcasted_iota(jnp.int32, (1, tok), 1) // SPAN

    def local(p, _):
        vt = vt_s[p]
        gt = gt_s[p]
        lanes = pl.ds(pl.multiple_of(p * dk, dk), dk)
        v_blk = v_ref[:, lanes]
        for i in range(group):
            h = p * group + i
            wide = pl.ds(pl.multiple_of(h * dk, dk), dk)
            part = slice(i * dv, (i + 1) * dv)
            q = q_ref[:, wide]
            k = k_ref[:, wide]
            score = dot(k, q, NT)
            pair = dot(v_blk[:, part], gt[part], NN)
            decay = jnp.exp((cum_s[pl.ds(h, 1), :] - col_s[h]) + bias_s[...])
            seen = decay * score
            both_p = seen * pair
            gains = [lw_ref[l, pl.ds(h, 1), :] for l in range(span_bits + 1)]
            level_rows = [jnp.zeros((1, tok), F32) for _ in range(span_bits + 1)]
            mixed, graded = [], []
            for cs in range(spans):
                rows = slice(cs * SPAN, (cs + 1) * SPAN)
                total = jnp.sum(both_p[rows], axis=0, keepdims=True)
                gain = jnp.zeros((1, tok), F32)
                for ct in range(cs, spans):
                    l = span_level(cs, ct, levels)
                    hit = span_of == ct
                    gain = jnp.where(hit, gains[l], gain)
                    level_rows[l] = level_rows[l] + jnp.where(hit, total, 0.0)
                mixed.append(seen[rows] * gain)
                graded.append(decay[rows] * gain * pair[rows])
            mix = jnp.concatenate(mixed, axis=0).astype(BF16)
            grade = jnp.concatenate(graded, axis=0).astype(BF16)
            for l in range(span_bits + 1):
                gl_ref[l, pl.ds(h, 1), :] = level_rows[l]
            drift_s[pl.ds(h, 1), :] = jnp.sum(mix.astype(F32) * pair, axis=0, keepdims=True)
            vg_s[p, part] = dot(gt[part], mix, NT)
            gk_s[h] = dot(grade, q, NN)
            gq_s[h] = dot(grade, k, TN)
        return 0

    begin(0)
    lax.fori_loop(0, pairs // 4, local, 0, unroll=2)
    join(0)
    if bits > 1:
        begin(1)
    lax.fori_loop(pairs // 4, pairs, local, 0, unroll=2)
    for b in range(1, bits):
        join(b)
        if b + 1 < bits:
            begin(b + 1)
        begin_late(b)
        land(b - 1)
    land(bits - 1)

    inner_f = jnp.ones((heads, dk), F32)
    inner_b = jnp.ones((heads, dk), F32)
    for b in range(bits):
        up = bit[b].astype(F32)
        got = got_dec[b]
        coef_s[0, b] = inner_f * up
        coef_s[1, b] = inner_b * (1.0 - up)
        inner_f = inner_f * (up * got + (1.0 - up))
        inner_b = inner_b * ((1.0 - up) * got + up)
    level_wait(0, 1).wait_recv()
    for b in range(1, bits):
        forward_copy(b, other).wait_recv()

    def finish(p, _):
        lanes = pl.ds(pl.multiple_of(p * dk, dk), dk)
        vt = vt_s[p].astype(F32)
        gt = gt_s[p].astype(F32)
        vg_all = []
        for i in range(group):
            h = p * group + i
            wide = pl.ds(pl.multiple_of(h * dk, dk), dk)
            part = slice(i * dv, (i + 1) * dv)
            q = q_ref[:, wide]
            k = k_ref[:, wide]
            tail = tail_s[pl.ds(h, 1), :]
            lead = lead_s[pl.ds(h, 1), :]
            blocks = [lvl[b, h] for b in range(bits)]
            entering = []
            for n in range(len(slots)):
                terms = [
                    coef_s[0, b, pl.ds(h, 1), :] * blocks[b] for b in range(bits) if slot(b) == n
                ]
                entering.append(functools.reduce(jnp.add, terms))
            entering = jnp.concatenate(entering, axis=0)
            after = functools.reduce(
                jnp.add, [coef_s[1, b, pl.ds(h, 1), :] * blocks[b] for b in range(bits)]
            )
            e_high, e_low = split(entering)
            seen = dot(e_high, q, NT) + dot(e_low, q, NT)
            drift = drift_s[pl.ds(h, 1), :]
            gws = []
            for n, l in enumerate(slots):
                gain = lw_ref[l, pl.ds(h, 1), :]
                level = lead * jnp.sum(
                    seen[n * dv : (n + 1) * dv] * gt[part], axis=0, keepdims=True
                )
                gl_ref[l, pl.ds(h, 1), :] = level
                drift = drift + gain * level
                gws.append(gt[part] * (lead * gain))
            gw, gw_low = split(jnp.concatenate(gws, axis=0))
            gq_in = dot(gw, e_high, TN) + dot(gw, e_low, TN) + dot(gw_low, e_high, TN)
            gq_ref[:, wide] = (gq_s[h] + gq_in).astype(BF16)
            a_high, a_low = split(after)
            tv, tv_low = split(vt[part] * tail)
            gk_in = dot(tv, a_high, TN) + dot(tv, a_low, TN) + dot(tv_low, a_high, TN)
            gk_ref[:, wide] = (gk_s[h] + gk_in).astype(BF16)
            vg = vg_s[p, part] + tail * (dot(a_high, k, NT) + dot(a_low, k, NT))
            drift_s[pl.ds(h, 1), :] = drift - jnp.sum(vg * vt[part], axis=0, keepdims=True)
            vg_all.append(vg)
        gv_ref[:, lanes] = jnp.transpose(jnp.concatenate(vg_all, axis=0)).astype(BF16)
        return 0

    lax.fori_loop(0, pairs, finish, 0, unroll=2)
    for l in range(levels):
        if l > span_bits and l not in slots:
            gl_ref[l] = jnp.zeros((heads, tok), F32)

    later = (rows_i >= cols_i).astype(F32)
    local_tail = lax.dot_general(
        drift_s[...], later, NN, precision=lax.Precision.HIGHEST, preferred_element_type=F32
    )
    lane = lax.broadcasted_iota(jnp.int32, (heads, tok), 1)
    first = local_tail[:, 0:1]
    plain = jnp.sum(local_tail, axis=1, keepdims=True)
    square = jnp.sum(local_tail * local_tail, axis=1, keepdims=True)
    tot[place] = jnp.where(lane == 0, first, jnp.where(lane == 1, plain, square))

    def tot_copy(o, slot_at):
        return pltpu.make_async_remote_copy(
            src_ref=tot.at[place],
            dst_ref=tot.at[slot_at],
            send_sem=t_send.at[o],
            recv_sem=t_recv.at[slot_at],
            device_id={"seq": (place + o) % seq_count},
            device_id_type=MESH,
        )

    for o in range(1, seq_count):
        tot_copy(o, place).start()
    for o in range(1, seq_count):
        tot_copy(o, (place + o) % seq_count).wait_recv()
    after_total = jnp.zeros((heads, 1), F32)
    my_later = jnp.zeros((heads, 1), F32)
    energy = jnp.zeros((heads, 1), F32)
    for d in reversed(range(seq_count)):
        piece = tot[d]
        my_later = my_later + jnp.where(place == d, 1.0, 0.0) * after_total
        energy = energy + (
            piece[:, 2:3] + after_total * (2.0 * piece[:, 1:2] + tok * after_total)
        )
        after_total = after_total + piece[:, 0:1]
    energy = jnp.sum(jnp.broadcast_to(energy, (heads, dk)), axis=0, keepdims=True)
    sq[row] = jnp.broadcast_to(energy, (8, dk))

    def sq_copy(o, slot_at):
        return pltpu.make_async_remote_copy(
            src_ref=sq.at[row],
            dst_ref=sq.at[slot_at],
            send_sem=q_send.at[o],
            recv_sem=q_recv.at[slot_at],
            device_id={"head": (row + o) % head_count},
            device_id_type=MESH,
        )

    for o in range(1, head_count):
        sq_copy(o, row).start()
    for o in range(1, head_count):
        sq_copy(o, (row + o) % head_count).wait_recv()
    whole = sq[0]
    for r in range(1, head_count):
        whole = whole + sq[r]
    count = heads * tok * seq_count * head_count
    factor = jnp.minimum(1.0, lax.rsqrt(whole[0:1] / count + 1e-6))
    gg_ref[...] = (local_tail + my_later) * factor

    for b in range(bits):
        d_copy(b).wait_send()
        for n in range(2 if b == 0 else 1):
            level_wait(b, n).wait_send()
        if b > 0:
            forward_copy(b, own).wait_send()
        if b < bits - 1:

            @pl.when((bit[b] == 1) & want_s[b])
            def _(b=b):
                s_copy(b).wait_send()

            for j in range(b + 1, bits):

                @pl.when(bit[j] == 1)
                def _(b=b, j=j):
                    u_copy(b, j).wait_send()

    for o in range(1, seq_count):
        tot_copy(o, place).wait_send()
    for o in range(1, head_count):
        sq_copy(o, row).wait_send()


def chunked_kernel(
    seq_count,
    head_count,
    q_hbm,
    k_hbm,
    v_hbm,
    g_hbm,
    lg_hbm,
    lw_hbm,
    ds_hbm,
    gq_ref,
    gk_ref,
    gv_ref,
    gl_ref,
    tail_ref,
    msg,
    q_ref,
    k_ref,
    v_ref,
    g_ref,
    lg_ref,
    lw_ref,
    ds_ref,
    cum_s,
    col_s,
    lead_s,
    tail_s,
    bias_s,
    vt_s,
    gt_s,
    vg_s,
    gq_s,
    gk_s,
    drift_s,
    coef_s,
    mix_s,
    st,
    got_a,
    got_b,
    sum_a,
    sum_b,
    sum_q,
    lvl,
    relay,
    decs,
    i_sem,
    a_send,
    a_recv,
    b_send,
    b_recv,
    p_send,
    p_recv,
    xa_send,
    xa_recv,
    xb_send,
    xb_recv,
    y_send,
    y_recv,
    f_send,
    f_recv,
    r_send,
    r_recv,
    d_send,
    d_recv,
    t_send,
    t_recv,
    round_sem,
    plane_sem,
):
    tok = q_ref.shape[0]
    heads = lg_ref.shape[0]
    levels = lw_ref.shape[0]
    dk = q_ref.shape[1] // heads
    dv = v_ref.shape[1] // heads
    group = dk // dv
    pairs = heads // group
    spans = tok // SPAN
    span_bits = spans.bit_length() - 1
    bits = seq_count.bit_length() - 1
    half = heads // 2
    chunks = half // group
    cross = [min(span_bits + 1 + b, levels - 1) for b in range(bits)]
    slots = sorted(set(cross))
    kind = [1 + slots.index(l) for l in cross]
    place = lax.axis_index("seq")
    row = lax.axis_index("head")
    core, x, y = [(place // (1 << b)) % 2 for b in range(bits)]
    peer = [place + (1 - 2 * u) * (1 << b) for b, u in enumerate((core, x, y))]
    first_chip = (1 - x) * (1 - y)
    second_chip = x * (1 - y)
    mine = core * half
    theirs = (1 - core) * half

    has_next = (row < head_count - 1).astype(jnp.int32)
    has_last = (row > 0).astype(jnp.int32)

    def greet(sem):
        @pl.when(has_next == 1)
        def _():
            pl.semaphore_signal(sem, inc=1, device_id={"head": row + 1}, device_id_type=MESH)

        @pl.when(has_last == 1)
        def _():
            pl.semaphore_signal(sem, inc=1, device_id={"head": row - 1}, device_id_type=MESH)

    barrier = pltpu.get_barrier_semaphore()
    for b in reversed(range(bits)):
        pl.semaphore_signal(barrier, inc=1, device_id={"seq": peer[b]}, device_id_type=MESH)
    greet(barrier)

    def load(n):
        src = (lg_hbm, ds_hbm, v_hbm, k_hbm, g_hbm, lw_hbm, q_hbm)[n]
        dst = (lg_ref, ds_ref, v_ref, k_ref, g_ref, lw_ref, q_ref)[n]
        return pltpu.make_async_copy(src, dst, i_sem.at[n])

    for n in range(7):
        load(n).start()
    for n in range(2):
        load(n).wait()

    rows_i = lax.broadcasted_iota(jnp.int32, (tok, tok), 0)
    cols_i = lax.broadcasted_iota(jnp.int32, (tok, tok), 1)
    tri = (rows_i <= cols_i).astype(BF16)
    starts = jnp.broadcast_to(ds_ref[...].astype(F32), (8, tok))
    both = jnp.concatenate([lg_ref[...], starts], axis=0)
    cum_all = dot_exact(both, tri)
    cum_t = jnp.transpose(
        jnp.concatenate([cum_all, jnp.zeros((dk - heads - 8, tok), F32)], axis=0)
    )
    cum = cum_all[:heads]
    reset = cum_all[heads : heads + 1]
    reset_col = cum_t[:, heads : heads + 1]
    bias_s[...] = jnp.where((rows_i <= cols_i) & (reset == reset_col), 0.0, -1e30)
    end = cum[:, tok - 1 : tok]
    reset_end = reset[:, tok - 1 : tok]
    cum_s[...] = cum
    lead_s[...] = jnp.where(reset == 0, jnp.exp(cum), 0.0)
    tail_s[...] = jnp.where(reset == reset_end, jnp.exp(end - cum), 0.0)
    lane_row = lax.broadcasted_iota(jnp.int32, (1, dk), 1)
    end_row = jnp.where(lane_row < heads, cum_t[tok - 1 : tok, :], 0.0)
    decs[0] = jnp.where(reset_end == 0, jnp.exp(end_row), 0.0)
    for h in range(heads):
        col_s[h] = jnp.broadcast_to(cum_t[:, h : h + 1], (tok, tok))

    def states(p, _):
        lanes = pl.ds(pl.multiple_of(p * dk, dk), dk)
        vt = jnp.transpose(v_ref[:, lanes].astype(F32))
        gt = jnp.transpose(g_ref[:, lanes].astype(F32))
        vt_s[p] = vt.astype(BF16)
        gt_s[p] = gt.astype(BF16)
        for i in range(group):
            h = p * group + i
            wide = pl.ds(pl.multiple_of(h * dk, dk), dk)
            part = slice(i * dv, (i + 1) * dv)
            tail = tail_s[pl.ds(h, 1), :]
            lead = lead_s[pl.ds(h, 1), :]
            st[0, h] = dot_fine(vt[part] * tail, k_ref[:, wide], NN)
            gw = jnp.concatenate(
                [gt[part] * (lead * lw_ref[l, pl.ds(h, 1), :]) for l in slots], axis=0
            )
            back = dot_fine(gw, q_ref[:, wide], NN)
            for n in range(len(slots)):
                st[1 + n, h] = back[n * dv : (n + 1) * dv]
        return 0

    for n in range(2, 7):
        load(n).wait()
    own_pair = core * chunks
    far_pair = (1 - core) * chunks
    def states_from(base):
        lax.fori_loop(0, 2, lambda n, _: states(base + n, 0), 0, unroll=2)

    states_from(far_pair)
    pl.semaphore_wait(barrier, bits + has_next + has_last)
    rounds = head_count - 2
    if rounds > 0:
        greet(round_sem.at[0])

    def remote(src, dst, send, recv, b):
        return pltpu.make_async_remote_copy(
            src_ref=src,
            dst_ref=dst,
            send_sem=send,
            recv_sem=recv,
            device_id={"seq": peer[b]},
            device_id_type=MESH,
        )

    def of(base, c):
        return pl.ds(base + c * group, group)

    def at(c):
        return pl.ds(c * group, group)

    kind_a = y * kind[2]
    kind_b = x * kind[1]
    slot_out = bits - (bits - 1) * first_chip
    slot_in = bits - (bits - 1) * second_chip

    def dec_copy(n):
        src = 3 if n == 2 else 2 * n
        return remote(decs.at[src], decs.at[2 * n + 1], d_send.at[n], d_recv.at[n], n)

    def a_copy(c):
        return remote(
            st.at[kind_a, of(theirs, c)], got_a.at[at(c)], a_send.at[c], a_recv.at[c], 0
        )

    def b_copy(c):
        return remote(
            st.at[kind_b, of(theirs, c)], got_b.at[at(c)], b_send.at[c], b_recv.at[c], 0
        )

    def p_copy(n):
        part = pl.ds(n * half, half)
        return remote(
            st.at[core * kind[0], part], lvl.at[0, part], p_send.at[n], p_recv.at[n], 0
        )

    piece = 1
    pieces = half // piece

    def xa_copy(n):
        here = pl.ds(n * piece, piece)
        there = pl.ds(mine + n * piece, piece)
        return remote(
            sum_a.at[here], lvl.at[slot_out, there], xa_send.at[n], xa_recv.at[n], 1
        )

    def xb_copy(n):
        here = pl.ds(n * piece, piece)
        there = pl.ds(mine + n * piece, piece)
        return remote(sum_b.at[here], lvl.at[1, there], xb_send.at[n], xb_recv.at[n], 1)

    def pieces_of(c):
        return range(c * group // piece, (c + 1) * group // piece)

    def y_copy(n):
        here = pl.ds(n * piece, piece)
        there = pl.ds(mine + n * piece, piece)
        return remote(sum_q.at[here], lvl.at[2, there], y_send.at[n], y_recv.at[n], 2)

    late = range(pieces - group // piece, pieces)

    def early_copy(n):
        return remote(
            sum_a.at[pl.ds(n * piece, piece)],
            relay.at[0, pl.ds((n - late[0]) * piece, piece)],
            y_send.at[n],
            y_recv.at[n],
            2,
        )

    def relay_copy(n):
        part = pl.ds((n - late[0]) * piece, piece)
        return remote(
            relay.at[0, part], relay.at[1, part], r_send.at[n - late[0]], r_recv.at[n - late[0]], 1
        )

    def f_copy(j, base, c):
        part = lvl.at[j, of(base, c)]
        return remote(part, part, f_send.at[j - 1, c], f_recv.at[j - 1, c], 0)

    dec_copy(0).start()
    for c in range(2):
        a_copy(c).start()
    states_from(far_pair + 2)
    for c in range(2, chunks):
        a_copy(c).start()
    states_from(own_pair)
    states_from(own_pair + 2)

    span_of = lax.broadcasted_iota(jnp.int32, (1, tok), 1) // SPAN

    def local(p, _):
        vt = vt_s[p]
        gt = gt_s[p]
        lanes = pl.ds(pl.multiple_of(p * dk, dk), dk)
        v_blk = v_ref[:, lanes]
        for i in range(group):
            h = p * group + i
            wide = pl.ds(pl.multiple_of(h * dk, dk), dk)
            part = slice(i * dv, (i + 1) * dv)
            q = q_ref[:, wide]
            k = k_ref[:, wide]
            score = dot(k, q, NT)
            pair = dot(v_blk[:, part], gt[part], NN)
            decay = jnp.exp((cum_s[pl.ds(h, 1), :] - col_s[h]) + bias_s[...])
            seen = decay * score
            both_p = seen * pair
            gains = [lw_ref[l, pl.ds(h, 1), :] for l in range(span_bits + 1)]
            level_rows = [jnp.zeros((1, tok), F32) for _ in range(span_bits + 1)]
            mixed, graded = [], []
            for cs in range(spans):
                rows = slice(cs * SPAN, (cs + 1) * SPAN)
                total = jnp.sum(both_p[rows], axis=0, keepdims=True)
                gain = jnp.zeros((1, tok), F32)
                for ct in range(cs, spans):
                    l = span_level(cs, ct, levels)
                    hit = span_of == ct
                    gain = jnp.where(hit, gains[l], gain)
                    level_rows[l] = level_rows[l] + jnp.where(hit, total, 0.0)
                mixed.append(seen[rows] * gain)
                graded.append(decay[rows] * gain * pair[rows])
            mix = jnp.concatenate(mixed, axis=0).astype(BF16)
            grade = jnp.concatenate(graded, axis=0).astype(BF16)
            for l in range(span_bits + 1):
                gl_ref[l, pl.ds(h, 1), :] = level_rows[l]
            drift_s[pl.ds(h, 1), :] = jnp.sum(mix.astype(F32) * pair, axis=0, keepdims=True)
            vg_s[p, part] = dot(gt[part], mix, NT)
            gk_s[h] = dot(grade, q, NN)
            gq_s[h] = dot(grade, k, TN)
        return 0

    def spread(device_rows):
        t = jnp.transpose(
            jnp.concatenate(
                device_rows + [jnp.zeros((8 - len(device_rows), dk), F32)], axis=0
            )
        )
        return [
            jnp.broadcast_to(t[:heads, n : n + 1], (heads, dk)) for n in range(len(device_rows))
        ]

    def weigh(n, swap, own, got):
        w = (swap % 2).astype(F32)
        mix_s[n, 0] = own * (1.0 - w) + w
        mix_s[n, 1] = got * w + (1.0 - w)

    def combine(n, c, own_at, got_at, put):
        for i in range(group):
            r = c * group + i
            ca = mix_s[n, 0, pl.ds(mine + r, 1), :]
            cb = mix_s[n, 1, pl.ds(mine + r, 1), :]
            put[r] = ca * own_at(r) + cb * got_at(r)

    def local_pairs(first, last):
        lax.fori_loop(first, last, local, 0, unroll=2)

    def x_start(n):
        if n in late:

            @pl.when(y == 0)
            def _():
                xa_copy(n).start()

        elif n < pieces:
            xa_copy(n).start()
        elif n - pieces in late:

            @pl.when((y == 1) & (first_chip == 0))
            def _():
                xb_copy(n - pieces).start()

        elif n < 2 * pieces:

            @pl.when(first_chip == 0)
            def _():
                xb_copy(n - pieces).start()

    def x_sent(n):
        if n in late:

            @pl.when(y == 0)
            def _():
                xa_copy(n).wait_send()

        elif n < pieces:
            xa_copy(n).wait_send()
        else:

            @pl.when(first_chip == 0)
            def _():
                xb_copy(n - pieces).wait_send()

    ahead = 5

    def x_next(n):
        x_sent(n)
        x_start(n + ahead)

    dec_copy(0).wait_recv()
    decs[2] = decs[0] * decs[1]
    d_self, d_pair = spread([decs[0], decs[1]])
    weigh(0, core + y, d_pair, d_self)
    weigh(1, core + x, d_pair, d_self)
    for c in range(chunks):
        a_copy(c).wait_recv()
        combine(0, c, lambda r: st[kind_a, mine + r], lambda r: got_a[r], sum_a)
        for n in pieces_of(c):
            if n < 3:
                x_start(n)
        if c == 1:
            dec_copy(1).start()

            @pl.when(first_chip == 0)
            def _():
                for n in range(chunks):
                    b_copy(n).start()

    @pl.when(y == 1)
    def _():
        for n in late:
            early_copy(n).start()

    for n in range(3, ahead):
        x_start(n)
    local_pairs(0, 4)

    @pl.when(first_chip == 0)
    def _():
        for c in range(chunks):
            b_copy(c).wait_recv()
            combine(1, c, lambda r: st[kind_b, mine + r], lambda r: got_b[r], sum_b)

    for r in range(1, rounds + 1):
        pl.semaphore_wait(round_sem.at[r - 1], has_next + has_last)
        if r < rounds:
            greet(round_sem.at[r])
    x_next(0)
    x_next(1)
    p_copy(0).start()
    local_pairs(4, 6)
    dec_copy(1).wait_recv()
    (d_side,) = spread([decs[3]])
    dec_copy(2).start()
    weigh(2, x + y, d_side, d_self * d_pair)
    inner_f = jnp.ones((heads, dk), F32)
    inner_b = jnp.ones((heads, dk), F32)
    for b, (u, got) in enumerate(((core, d_pair), (x, d_side), (y, None))):
        up = u.astype(F32)
        coef_s[0, b] = inner_f * up
        coef_s[1, b] = inner_b * (1.0 - up)
        if got is not None:
            inner_f = inner_f * (up * got + (1.0 - up))
            inner_b = inner_b * ((1.0 - up) * got + up)
    x_next(2)
    x_next(3)
    p_copy(1).start()
    def turn(n):
        if n in late:

            @pl.when(y == 0)
            def _():
                take_turn(n)

        else:
            take_turn(n)

    def take_turn(n):
        xa_copy(n).wait_recv()
        for r in range(n * piece, (n + 1) * piece):
            ca = mix_s[2, 0, pl.ds(mine + r, 1), :]
            cb = mix_s[2, 1, pl.ds(mine + r, 1), :]
            sum_q[r] = ca * sum_a[r] + cb * lvl[slot_in, mine + r]
        y_copy(n).start()
        if (n + 1) * piece % group == 0:

            @pl.when(second_chip == 1)
            def _():
                f_copy(1, mine, n * piece // group).start()

    turn(0)
    local_pairs(6, pairs)
    x_next(4)
    turn(1)
    x_next(5)
    turn(2)
    x_next(6)
    turn(3)
    x_next(7)
    turn(4)

    @pl.when(first_chip == 1)
    def _():
        for n in late:
            early_copy(n).wait_recv()
            relay_copy(n).start()
            for r in range(n * piece, (n + 1) * piece):
                lvl[2, mine + r] = jnp.zeros((dv, dk), F32)

    x_next(8)
    turn(5)
    turn(6)
    x_next(9)
    x_next(10)
    turn(7)

    def incoming(h):
        blocks = [lvl[b, h] for b in range(bits)]
        entering = []
        for n in range(len(slots)):
            terms = [
                coef_s[0, b, pl.ds(h, 1), :] * blocks[b]
                for b in range(bits)
                if kind[b] == 1 + n
            ]
            entering.append(functools.reduce(jnp.add, terms))
        after = functools.reduce(
            jnp.add, [coef_s[1, b, pl.ds(h, 1), :] * blocks[b] for b in range(bits)]
        )
        return split(jnp.concatenate(entering, axis=0)), split(after)

    def finish_drift(p):
        vt = vt_s[p].astype(F32)
        gt = gt_s[p].astype(F32)
        for i in range(group):
            h = p * group + i
            wide = pl.ds(pl.multiple_of(h * dk, dk), dk)
            part = slice(i * dv, (i + 1) * dv)
            q = q_ref[:, wide]
            k = k_ref[:, wide]
            tail = tail_s[pl.ds(h, 1), :]
            lead = lead_s[pl.ds(h, 1), :]
            (e_high, e_low), (a_high, a_low) = incoming(h)
            seen = dot(e_high, q, NT) + dot(e_low, q, NT)
            drift = drift_s[pl.ds(h, 1), :]
            for n, l in enumerate(slots):
                level = lead * jnp.sum(
                    seen[n * dv : (n + 1) * dv] * gt[part], axis=0, keepdims=True
                )
                gl_ref[l, pl.ds(h, 1), :] = level
                drift = drift + lw_ref[l, pl.ds(h, 1), :] * level
            vg = vg_s[p, part] + tail * (dot(a_high, k, NT) + dot(a_low, k, NT))
            drift_s[pl.ds(h, 1), :] = drift - jnp.sum(vg * vt[part], axis=0, keepdims=True)
            vg_s[p, part] = vg

    def finish_out(p):
        lanes = pl.ds(pl.multiple_of(p * dk, dk), dk)
        vt = vt_s[p].astype(F32)
        gt = gt_s[p].astype(F32)
        for i in range(group):
            h = p * group + i
            wide = pl.ds(pl.multiple_of(h * dk, dk), dk)
            part = slice(i * dv, (i + 1) * dv)
            tail = tail_s[pl.ds(h, 1), :]
            lead = lead_s[pl.ds(h, 1), :]
            (e_high, e_low), (a_high, a_low) = incoming(h)
            gws = [gt[part] * (lead * lw_ref[l, pl.ds(h, 1), :]) for l in slots]
            gw, gw_low = split(jnp.concatenate(gws, axis=0))
            gq_in = dot(gw, e_high, TN) + dot(gw, e_low, TN) + dot(gw_low, e_high, TN)
            gq_ref[:, wide] = (gq_s[h] + gq_in).astype(BF16)
            tv, tv_low = split(vt[part] * tail)
            gk_in = dot(tv, a_high, TN) + dot(tv, a_low, TN) + dot(tv_low, a_high, TN)
            gk_ref[:, wide] = (gk_s[h] + gk_in).astype(BF16)
        gv_ref[:, lanes] = jnp.transpose(vg_s[p]).astype(BF16)

    dec_copy(2).wait_recv()
    (d_cross,) = spread([decs[5]])
    mix_s[3, 0] = d_cross
    mix_s[3, 1] = d_self * d_pair

    def join_late():
        @pl.when(second_chip == 1)
        def _():
            for n in late:
                early_copy(n).wait_recv()
                relay_copy(n).wait_recv()
                for r in range(n * piece, (n + 1) * piece):
                    ca = mix_s[3, 0, pl.ds(mine + r, 1), :]
                    cb = mix_s[3, 1, pl.ds(mine + r, 1), :]
                    m = r - late[0] * piece
                    joined = ca * relay[0, m] + relay[1, m]
                    lvl[2, mine + r] = joined
                    sum_b[r] = sum_b[r] + cb * joined
                xb_copy(n).start()

    for n in range(2):
        p_copy(n).wait_recv()
    for c in range(chunks):
        for n in ((), (), (), ())[c]:
            x_next(n)
        if c == chunks - 1:

            @pl.when(y == 1)
            def _(c=c):
                for n in pieces_of(c):
                    y_copy(n).wait_recv()

        else:
            for n in pieces_of(c):
                y_copy(n).wait_recv()
        f_copy(2, mine, c).start()
        if c == 1:
            join_late()

        @pl.when(second_chip == 0)
        def _(c=c):
            for n in pieces_of(c):
                xb_copy(n).wait_recv()
            f_copy(1, mine, c).start()

        if c == 0:
            for o in range(1, head_count):
                pl.semaphore_signal(
                    plane_sem,
                    inc=1,
                    device_id={"head": (row + o) % head_count},
                    device_id_type=MESH,
                )
        finish_drift(own_pair + c)
        for j in (1, 2):
            f_copy(j, theirs, c).wait_recv()
        finish_drift(far_pair + c)

    later = (rows_i >= cols_i).astype(BF16)
    local_tail = dot_exact(drift_s[...], later)
    tail_ref[...] = local_tail
    lane = lax.broadcasted_iota(jnp.int32, (heads, tok), 1)
    head = lax.broadcasted_iota(jnp.int32, (heads, tok), 0)
    sums = [
        local_tail[:, 0:1],
        jnp.sum(local_tail, axis=1, keepdims=True),
        jnp.sum(local_tail * local_tail, axis=1, keepdims=True),
    ]
    packed = jnp.zeros((heads, tok), F32)
    for n, column in enumerate(sums):
        packed = jnp.where(lane == head + n * heads, column, packed)
    slot = row * seq_count + place
    total = seq_count * head_count
    msg[slot] = jnp.sum(packed, axis=0, keepdims=True)

    def tail_copy(to_row, to_place):
        return pltpu.make_async_remote_copy(
            src_ref=msg.at[slot],
            dst_ref=msg.at[slot],
            send_sem=t_send.at[0],
            recv_sem=t_recv.at[0],
            device_id={"seq": to_place, "head": to_row},
            device_id_type=MESH,
        )

    def tail_all():
        others = msg.at[pl.ds(0, total - 1)]
        return pltpu.make_async_remote_copy(
            src_ref=others,
            dst_ref=others,
            send_sem=t_send.at[0],
            recv_sem=t_recv.at[0],
            device_id={"seq": peer[0]},
            device_id_type=MESH,
        )

    pl.semaphore_wait(plane_sem, head_count - 1)
    for o in list(range(1, head_count)) + [0]:
        for n in list(range(1, seq_count)) + [0]:
            if (o, n) != (0, 0):
                tail_copy((row + o) % head_count, (place + n) % seq_count).start()

    def outputs(p, _):
        finish_out(p)
        return 0

    lax.fori_loop(0, pairs, outputs, 0, unroll=2)
    for l in range(levels):
        if l > span_bits and l not in slots:
            gl_ref[l] = jnp.zeros((heads, tok), F32)

    for n in range(3):
        dec_copy(n).wait_send()

    @pl.when(first_chip == 1)
    def _():
        for n in late:
            relay_copy(n).wait_send()

    for n in range(2):
        p_copy(n).wait_send()
    for n in range(2 * pieces - ahead, 2 * pieces):
        x_sent(n)
    for c in range(chunks):
        a_copy(c).wait_send()
        for n in pieces_of(c):
            y_copy(n).wait_send()
        for j in (1, 2):
            f_copy(j, mine, c).wait_send()

    @pl.when(first_chip == 0)
    def _():
        for c in range(chunks):
            b_copy(c).wait_send()

    tail_all().wait_send()
    tail_all().wait_recv()


def finish_kernel(
    seq_count,
    head_count,
    gq_ref,
    gk_ref,
    gv_ref,
    gl_ref,
    tail_ref,
    msg,
    gq_out,
    gk_out,
    gv_out,
    gl_out,
    gg_out,
    gg_s,
    sems,
):
    copies = [
        pltpu.make_async_copy(src, dst, sems.at[n])
        for n, (src, dst) in enumerate(
            (
                (gq_ref, gq_out),
                (gk_ref, gk_out),
                (gv_ref, gv_out),
                (gl_ref, gl_out),
                (gg_s, gg_out),
            )
        )
    ]
    for c in copies[:4]:
        c.start()
    heads, tok = tail_ref.shape
    dk = msg.shape[2]
    total = seq_count * head_count
    slot = lax.axis_index("head") * seq_count + lax.axis_index("seq")
    rows = msg[:, 0, :]
    row_u = lax.broadcasted_iota(jnp.int32, (total, total), 0)
    row_v = lax.broadcasted_iota(jnp.int32, (total, total), 1)
    behind = ((row_u // seq_count == row_v // seq_count) & (row_v > row_u)).astype(BF16)
    after_rows = sum(dot(behind, piece, NN) for piece in pieces_exact(rows))
    plain = pltpu.roll(rows, dk - heads, 1)
    square = pltpu.roll(rows, dk - 2 * heads, 1)
    energy = square + after_rows * (2.0 * plain + tok * after_rows)
    lane_all = lax.broadcasted_iota(jnp.int32, (total, dk), 1)
    slot_all = lax.broadcasted_iota(jnp.int32, (total, dk), 0)
    energy = jnp.sum(jnp.where(lane_all < heads, energy, 0.0), axis=0, keepdims=True)
    whole = jnp.sum(energy, axis=1, keepdims=True)
    my_row = jnp.sum(jnp.where(slot_all == slot, after_rows, 0.0), axis=0, keepdims=True)
    lane = lax.broadcasted_iota(jnp.int32, (heads, dk), 1)
    head = lax.broadcasted_iota(jnp.int32, (heads, dk), 0)
    my_later = jnp.sum(jnp.where(lane == head, my_row, 0.0), axis=1, keepdims=True)
    count = heads * tok * total
    factor = jnp.minimum(1.0, lax.rsqrt(whole / count + 1e-6))
    gg_s[...] = (tail_ref[...] + my_later) * factor
    copies[4].start()
    for c in copies:
        c.wait()


def write_out(count, *refs):
    sems = refs[-1]
    copies = [
        pltpu.make_async_copy(refs[i], refs[count + i], sems.at[i]) for i in range(count)
    ]
    for c in copies:
        c.start()
    for c in copies:
        c.wait()


def shards(seq_count, head_count, queries, keys, values, out_grad, log_gate, level_weight, doc_start):
    tok = queries.shape[0]
    heads = log_gate.shape[0]
    levels = level_weight.shape[0]
    dk = queries.shape[1] // heads
    dv = values.shape[1] // heads
    group = dk // dv
    pairs = heads // group
    bits = seq_count.bit_length() - 1
    half = heads // 2
    span_bits = (tok // SPAN).bit_length() - 1
    slots = len({min(span_bits + 1 + b, levels - 1) for b in range(bits)})
    dma = pltpu.SemaphoreType.DMA
    vmem = pltpu.VMEM
    block = (dv, dk)
    scratch = [
        vmem((heads, tok), F32),
        vmem((heads, tok, tok), F32),
        vmem((heads, tok), F32),
        vmem((heads, tok), F32),
        vmem((tok, tok), F32),
        vmem((pairs, group * dv, tok), BF16),
        vmem((pairs, group * dv, tok), BF16),
        vmem((pairs, group * dv, tok), F32),
        vmem((heads, tok, dk), F32),
        vmem((heads, tok, dk), F32),
        vmem((heads, tok), F32),
        vmem((2, bits, heads, dk), F32),
        vmem((heads,) + block, F32),
        vmem((slots, heads) + block, F32),
        vmem((bits, heads) + block, F32),
        vmem((bits, half) + block, F32),
        vmem((bits, bits, half) + block, F32),
        vmem((bits, half) + block, F32),
        vmem((bits, bits, half) + block, F32),
        vmem((bits + 1, heads, dk), F32),
        vmem((bits, heads, dk), F32),
        vmem((seq_count, heads, tok), F32),
        vmem((head_count, 8, dk), F32),
        dma((bits, 2)),
        dma((bits, 2)),
        dma((bits,)),
        dma((bits,)),
        dma((bits,)),
        dma((bits,)),
        dma((bits, bits)),
        dma((bits, bits)),
        dma((bits,)),
        dma((bits,)),
        dma((seq_count,)),
        dma((seq_count,)),
        dma((head_count,)),
        dma((head_count,)),
    ]
    args = (queries, keys, values, out_grad, log_gate, level_weight, doc_start.reshape(1, tok))
    spec = pl.BlockSpec(memory_space=pltpu.VMEM)
    in_spec = spec
    body = kernel
    chunks = half // group
    if bits == 3 and chunks == 4 and chunks * group == half and tok == dk and 3 * heads <= dk:
        body = chunked_kernel
        inputs = [(x.shape, x.dtype) for x in args]
        scratch = [vmem(*x) for x in inputs] + scratch[:12] + [
            vmem((4, 2, heads, dk), F32),
            vmem((1 + slots, heads) + block, F32),
            vmem((half,) + block, F32),
            vmem((half,) + block, F32),
            vmem((half,) + block, F32),
            vmem((half,) + block, F32),
            vmem((half,) + block, F32),
            vmem((bits + 1, heads) + block, F32),
            vmem((2, group) + block, F32),
            vmem((6, 1, dk), F32),
            dma((7,)),
            dma((chunks,)),
            dma((chunks,)),
            dma((chunks,)),
            dma((chunks,)),
            dma((2,)),
            dma((2,)),
            dma((half,)),
            dma((half,)),
            dma((half,)),
            dma((half,)),
            dma((half,)),
            dma((half,)),
            dma((2, chunks)),
            dma((2, chunks)),
            dma((group,)),
            dma((group,)),
            dma((3,)),
            dma((3,)),
            dma((1,)),
            dma((1,)),
            pltpu.SemaphoreType.REGULAR((max(1, head_count - 2),)),
            pltpu.SemaphoreType.REGULAR,
        ]
        in_spec = pl.BlockSpec(memory_space=pltpu.HBM)
    outs = [
        (queries.shape, BF16),
        (keys.shape, BF16),
        (values.shape, BF16),
        (level_weight.shape, F32),
        (log_gate.shape, F32),
    ]
    held = list(outs)
    writer = (write_out, len(outs))
    writer_scratch = []
    if body is chunked_kernel:
        held.append(((seq_count * head_count, 1, dk), F32))
        writer = (finish_kernel, seq_count, head_count)
        writer_scratch = [vmem(*outs[-1])]
    results = pl.pallas_call(
        functools.partial(body, seq_count, head_count),
        out_shape=tuple(vmem(shape, dtype) for shape, dtype in held),
        in_specs=[in_spec] * 7,
        out_specs=(spec,) * len(held),
        scratch_shapes=scratch,
        compiler_params=pltpu.CompilerParams(collective_id=0, has_side_effects=True),
    )(*args)
    count = len(outs)
    return pl.pallas_call(
        functools.partial(*writer),
        out_shape=tuple(jax.ShapeDtypeStruct(shape, dtype) for shape, dtype in outs),
        in_specs=[spec] * len(held),
        out_specs=(pl.BlockSpec(memory_space=pltpu.HBM),) * count,
        scratch_shapes=writer_scratch + [dma((count,))],
    )(*[pltpu.with_memory_space_constraint(r, pltpu.VMEM) for r in results])


def solution(mesh):
    return jax.shard_map(
        functools.partial(shards, mesh.shape["seq"], mesh.shape["head"]),
        mesh=mesh,
        in_specs=(
            P("seq", "head"),
            P("seq", "head"),
            P("seq", "head"),
            P("seq", "head"),
            P("head", "seq"),
            P(None, "head", "seq"),
            P("seq"),
        ),
        out_specs=(
            P("seq", "head"),
            P("seq", "head"),
            P("seq", "head"),
            P(None, "head", "seq"),
            P("head", "seq"),
        ),
        check_vma=False,
    )
```

```python
import functools

import jax
import jax.numpy as jnp
from jax import lax
from jax.experimental import pallas as pl
from jax.experimental.pallas import tpu as pltpu
from jax.sharding import PartitionSpec as P

SPAN = 64
F32 = jnp.float32
BF16 = jnp.bfloat16
NN = (((1,), (0,)), ((), ()))
NT = (((1,), (1,)), ((), ()))
TN = (((0,), (0,)), ((), ()))
MESH = pl.DeviceIdType.MESH


def dot(a, b, dims):
    return lax.dot_general(a, b, dims, preferred_element_type=F32)


def split(x):
    high = x.astype(BF16)
    return high, (x - high.astype(F32)).astype(BF16)


def pieces_exact(x):
    high = x.astype(BF16)
    rest = x - high.astype(F32)
    middle = rest.astype(BF16)
    return high, middle, (rest - middle.astype(F32)).astype(BF16)


def dot_exact(x, b):
    rows = x.shape[0]
    out = dot(jnp.concatenate(pieces_exact(x), axis=0), b, NN)
    return out[:rows] + out[rows : 2 * rows] + out[2 * rows :]


def dot_fine(x, b, dims):
    high, low = split(x)
    return dot(high, b, dims) + dot(low, b, dims)


def span_level(a, b, levels):
    return 0 if a == b else min(levels - 1, (a ^ b).bit_length())


def kernel(
    seq_count,
    head_count,
    q_ref,
    k_ref,
    v_ref,
    g_ref,
    lg_ref,
    lw_ref,
    ds_ref,
    gq_ref,
    gk_ref,
    gv_ref,
    gl_ref,
    gg_ref,
    cum_s,
    col_s,
    lead_s,
    tail_s,
    bias_s,
    vt_s,
    gt_s,
    vg_s,
    gq_s,
    gk_s,
    drift_s,
    coef_s,
    state_s,
    back_s,
    lvl,
    got_s,
    got_u,
    sum_s,
    sum_u,
    dec,
    got_dec,
    tot,
    sq,
    lvl_send,
    lvl_recv,
    fwd_send,
    fwd_recv,
    s_send,
    s_recv,
    u_send,
    u_recv,
    d_send,
    d_recv,
    t_send,
    t_recv,
    q_send,
    q_recv,
):
    tok = q_ref.shape[0]
    heads = lg_ref.shape[0]
    levels = lw_ref.shape[0]
    dk = q_ref.shape[1] // heads
    dv = v_ref.shape[1] // heads
    group = dk // dv
    pairs = heads // group
    spans = tok // SPAN
    span_bits = spans.bit_length() - 1
    bits = seq_count.bit_length() - 1
    half = heads // 2
    cross = [min(span_bits + 1 + b, levels - 1) for b in range(bits)]
    slots = sorted(set(cross))
    place = lax.axis_index("seq")
    row = lax.axis_index("head")
    bit = [(place // (1 << b)) % 2 for b in range(bits)]
    peer = [place + (1 - 2 * bit[b]) * (1 << b) for b in range(bits)]
    want_s = [(place // (2 << b)) != (seq_count // (2 << b)) - 1 for b in range(bits)]
    mine = bit[0] * half
    theirs = (1 - bit[0]) * half

    barrier = pltpu.get_barrier_semaphore()
    for o in range(1, seq_count):
        pl.semaphore_signal(
            barrier, inc=1, device_id={"seq": (place + o) % seq_count}, device_id_type=MESH
        )
    for o in range(1, head_count):
        pl.semaphore_signal(
            barrier, inc=1, device_id={"head": (row + o) % head_count}, device_id_type=MESH
        )

    rows_i = lax.broadcasted_iota(jnp.int32, (tok, tok), 0)
    cols_i = lax.broadcasted_iota(jnp.int32, (tok, tok), 1)
    tri = (rows_i <= cols_i).astype(F32)
    starts = jnp.broadcast_to(ds_ref[...].astype(F32), (8, tok))
    both = jnp.concatenate([lg_ref[...], starts], axis=0)
    cum_all = lax.dot_general(
        both, tri, NN, precision=lax.Precision.HIGHEST, preferred_element_type=F32
    )
    cum_t = jnp.transpose(cum_all)
    cum = cum_all[:heads]
    reset = cum_all[heads : heads + 1]
    reset_col = cum_t[:, heads : heads + 1]
    bias_s[...] = jnp.where((rows_i <= cols_i) & (reset == reset_col), 0.0, -1e30)
    end = cum[:, tok - 1 : tok]
    reset_end = reset[:, tok - 1 : tok]
    cum_s[...] = cum
    lead_s[...] = jnp.where(reset == 0, jnp.exp(cum), 0.0)
    tail_s[...] = jnp.where(reset == reset_end, jnp.exp(end - cum), 0.0)
    dec[0] = jnp.broadcast_to(jnp.where(reset_end == 0, jnp.exp(end), 0.0), (heads, dk))
    for h in range(heads):
        col_s[h] = jnp.broadcast_to(cum_t[:, h : h + 1], (tok, tok))

    def states(p, _):
        lanes = pl.ds(pl.multiple_of(p * dk, dk), dk)
        vt = jnp.transpose(v_ref[:, lanes].astype(F32))
        gt = jnp.transpose(g_ref[:, lanes].astype(F32))
        vt_s[p] = vt.astype(BF16)
        gt_s[p] = gt.astype(BF16)
        for i in range(group):
            h = p * group + i
            wide = pl.ds(pl.multiple_of(h * dk, dk), dk)
            part = slice(i * dv, (i + 1) * dv)
            tail = tail_s[pl.ds(h, 1), :]
            lead = lead_s[pl.ds(h, 1), :]
            state_s[h] = dot_fine(vt[part] * tail, k_ref[:, wide], NN)
            gw = jnp.concatenate(
                [gt[part] * (lead * lw_ref[l, pl.ds(h, 1), :]) for l in slots], axis=0
            )
            back = dot_fine(gw, q_ref[:, wide], NN)
            for n in range(len(slots)):
                back_s[n, h] = back[n * dv : (n + 1) * dv]
        return 0

    lax.fori_loop(0, pairs, states, 0, unroll=2)
    pl.semaphore_wait(barrier, seq_count - 1 + head_count - 1)

    def slot(b):
        return slots.index(cross[b])

    def remote(src, dst, send, recv, b):
        return pltpu.make_async_remote_copy(
            src_ref=src,
            dst_ref=dst,
            send_sem=send,
            recv_sem=recv,
            device_id={"seq": peer[b]},
            device_id_type=MESH,
        )

    own = pl.ds(mine, half)
    other = pl.ds(theirs, half)

    def u_copy(b, j):
        src = back_s.at[slot(j), other] if b == 0 else sum_u.at[b, j]
        return remote(src, got_u.at[b, j], u_send.at[b, j], u_recv.at[b, j], b)

    def s_copy(b):
        src = state_s.at[other] if b == 0 else sum_s.at[b]
        return remote(src, got_s.at[b], s_send.at[b], s_recv.at[b], b)

    def d_copy(b):
        return remote(dec.at[b], got_dec.at[b], d_send.at[b], d_recv.at[b], b)

    def level_copy(b, low):
        if b == 0:
            src = state_s if low else back_s.at[slot(0)]
            return [
                remote(src.at[part], lvl.at[0, part], lvl_send.at[0, n], lvl_recv.at[0, n], 0)
                for n, part in enumerate((other, own))
            ]
        src = sum_s.at[b] if low else sum_u.at[b, b]
        return [remote(src, lvl.at[b, own], lvl_send.at[b, 0], lvl_recv.at[b, 0], b)]

    def level_wait(b, n):
        part = other if n == 1 else own
        return remote(
            lvl.at[b, part], lvl.at[b, part], lvl_send.at[b, n], lvl_recv.at[b, n], b
        )

    def forward_copy(b, part):
        return remote(lvl.at[b, part], lvl.at[b, part], fwd_send.at[b], fwd_recv.at[b], 0)

    def land(b):
        up_summed = (bit[b] == 1) & want_s[b]

        @pl.when(jnp.logical_not(up_summed))
        def _():
            level_wait(b, 0).wait_recv()

        if b > 0:
            forward_copy(b, own).start()

    def begin(b):
        d_copy(b).start()

        early = 0 if b in (0, bits - 1) else 1

        @pl.when((bit[b] == 0) & (want_s[b] | (early == 0)))
        def _():
            for c in level_copy(b, True):
                c.start()

        if b < bits - 1:

            @pl.when((bit[b] == 1) & want_s[b])
            def _():
                s_copy(b).start()

            for j in range(b + 1, bits):

                @pl.when(bit[j] == 1)
                def _(j=j):
                    u_copy(b, j).start()

        if early == 0:

            @pl.when(bit[b] == 1)
            def _():
                for c in level_copy(b, False):
                    c.start()

    def begin_late(b):
        if b in (0, bits - 1):
            return

        @pl.when((bit[b] == 0) & jnp.logical_not(want_s[b]))
        def _():
            for c in level_copy(b, True):
                c.start()

        @pl.when(bit[b] == 1)
        def _():
            for c in level_copy(b, False):
                c.start()

    def join(b):
        d_copy(b).wait_recv()
        up = bit[b].astype(F32)
        got = got_dec[b]
        now = dec[b]
        dec[b + 1] = got * now
        if b == bits - 1:
            return
        base_s = state_s.at[own] if b == 0 else sum_s.at[b]

        @pl.when(want_s[b])
        def _():
            @pl.when(bit[b] == 1)
            def _():
                level_wait(b, 0).wait_recv()

                def body(i, _):
                    d = dec[b, pl.ds(mine + i, 1), :]
                    sum_s[b + 1, i] = d * lvl[b, mine + i] + base_s[i]
                    return 0

                lax.fori_loop(0, half, body, 0, unroll=True)

            @pl.when(bit[b] == 0)
            def _():
                s_copy(b).wait_recv()

                def body(i, _):
                    d = got_dec[b, pl.ds(mine + i, 1), :]
                    sum_s[b + 1, i] = d * base_s[i] + got_s[b, i]
                    return 0

                lax.fori_loop(0, half, body, 0, unroll=True)

        for j in range(b + 1, bits):
            base_u = back_s.at[slot(j), own] if b == 0 else sum_u.at[b, j]

            @pl.when(bit[j] == 1)
            def _(j=j, base_u=base_u):
                u_copy(b, j).wait_recv()

                def body(i, _):
                    d0 = dec[b, pl.ds(mine + i, 1), :]
                    d1 = got_dec[b, pl.ds(mine + i, 1), :]
                    a = up * d1 + (1.0 - up)
                    c = (1.0 - up) * d0 + up
                    sum_u[b + 1, j, i] = a * base_u[i] + c * got_u[b, j, i]
                    return 0

                lax.fori_loop(0, half, body, 0, unroll=True)

    span_of = lax.broadcasted_iota(jnp.int32, (1, tok), 1) // SPAN

    def local(p, _):
        vt = vt_s[p]
        gt = gt_s[p]
        lanes = pl.ds(pl.multiple_of(p * dk, dk), dk)
        v_blk = v_ref[:, lanes]
        for i in range(group):
            h = p * group + i
            wide = pl.ds(pl.multiple_of(h * dk, dk), dk)
            part = slice(i * dv, (i + 1) * dv)
            q = q_ref[:, wide]
            k = k_ref[:, wide]
            score = dot(k, q, NT)
            pair = dot(v_blk[:, part], gt[part], NN)
            decay = jnp.exp((cum_s[pl.ds(h, 1), :] - col_s[h]) + bias_s[...])
            seen = decay * score
            both_p = seen * pair
            gains = [lw_ref[l, pl.ds(h, 1), :] for l in range(span_bits + 1)]
            level_rows = [jnp.zeros((1, tok), F32) for _ in range(span_bits + 1)]
            mixed, graded = [], []
            for cs in range(spans):
                rows = slice(cs * SPAN, (cs + 1) * SPAN)
                total = jnp.sum(both_p[rows], axis=0, keepdims=True)
                gain = jnp.zeros((1, tok), F32)
                for ct in range(cs, spans):
                    l = span_level(cs, ct, levels)
                    hit = span_of == ct
                    gain = jnp.where(hit, gains[l], gain)
                    level_rows[l] = level_rows[l] + jnp.where(hit, total, 0.0)
                mixed.append(seen[rows] * gain)
                graded.append(decay[rows] * gain * pair[rows])
            mix = jnp.concatenate(mixed, axis=0).astype(BF16)
            grade = jnp.concatenate(graded, axis=0).astype(BF16)
            for l in range(span_bits + 1):
                gl_ref[l, pl.ds(h, 1), :] = level_rows[l]
            drift_s[pl.ds(h, 1), :] = jnp.sum(mix.astype(F32) * pair, axis=0, keepdims=True)
            vg_s[p, part] = dot(gt[part], mix, NT)
            gk_s[h] = dot(grade, q, NN)
            gq_s[h] = dot(grade, k, TN)
        return 0

    begin(0)
    lax.fori_loop(0, pairs // 4, local, 0, unroll=2)
    join(0)
    if bits > 1:
        begin(1)
    lax.fori_loop(pairs // 4, pairs, local, 0, unroll=2)
    for b in range(1, bits):
        join(b)
        if b + 1 < bits:
            begin(b + 1)
        begin_late(b)
        land(b - 1)
    land(bits - 1)

    inner_f = jnp.ones((heads, dk), F32)
    inner_b = jnp.ones((heads, dk), F32)
    for b in range(bits):
        up = bit[b].astype(F32)
        got = got_dec[b]
        coef_s[0, b] = inner_f * up
        coef_s[1, b] = inner_b * (1.0 - up)
        inner_f = inner_f * (up * got + (1.0 - up))
        inner_b = inner_b * ((1.0 - up) * got + up)
    level_wait(0, 1).wait_recv()
    for b in range(1, bits):
        forward_copy(b, other).wait_recv()

    def finish(p, _):
        lanes = pl.ds(pl.multiple_of(p * dk, dk), dk)
        vt = vt_s[p].astype(F32)
        gt = gt_s[p].astype(F32)
        vg_all = []
        for i in range(group):
            h = p * group + i
            wide = pl.ds(pl.multiple_of(h * dk, dk), dk)
            part = slice(i * dv, (i + 1) * dv)
            q = q_ref[:, wide]
            k = k_ref[:, wide]
            tail = tail_s[pl.ds(h, 1), :]
            lead = lead_s[pl.ds(h, 1), :]
            blocks = [lvl[b, h] for b in range(bits)]
            entering = []
            for n in range(len(slots)):
                terms = [
                    coef_s[0, b, pl.ds(h, 1), :] * blocks[b] for b in range(bits) if slot(b) == n
                ]
                entering.append(functools.reduce(jnp.add, terms))
            entering = jnp.concatenate(entering, axis=0)
            after = functools.reduce(
                jnp.add, [coef_s[1, b, pl.ds(h, 1), :] * blocks[b] for b in range(bits)]
            )
            e_high, e_low = split(entering)
            seen = dot(e_high, q, NT) + dot(e_low, q, NT)
            drift = drift_s[pl.ds(h, 1), :]
            gws = []
            for n, l in enumerate(slots):
                gain = lw_ref[l, pl.ds(h, 1), :]
                level = lead * jnp.sum(
                    seen[n * dv : (n + 1) * dv] * gt[part], axis=0, keepdims=True
                )
                gl_ref[l, pl.ds(h, 1), :] = level
                drift = drift + gain * level
                gws.append(gt[part] * (lead * gain))
            gw, gw_low = split(jnp.concatenate(gws, axis=0))
            gq_in = dot(gw, e_high, TN) + dot(gw, e_low, TN) + dot(gw_low, e_high, TN)
            gq_ref[:, wide] = (gq_s[h] + gq_in).astype(BF16)
            a_high, a_low = split(after)
            tv, tv_low = split(vt[part] * tail)
            gk_in = dot(tv, a_high, TN) + dot(tv, a_low, TN) + dot(tv_low, a_high, TN)
            gk_ref[:, wide] = (gk_s[h] + gk_in).astype(BF16)
            vg = vg_s[p, part] + tail * (dot(a_high, k, NT) + dot(a_low, k, NT))
            drift_s[pl.ds(h, 1), :] = drift - jnp.sum(vg * vt[part], axis=0, keepdims=True)
            vg_all.append(vg)
        gv_ref[:, lanes] = jnp.transpose(jnp.concatenate(vg_all, axis=0)).astype(BF16)
        return 0

    lax.fori_loop(0, pairs, finish, 0, unroll=2)
    for l in range(levels):
        if l > span_bits and l not in slots:
            gl_ref[l] = jnp.zeros((heads, tok), F32)

    later = (rows_i >= cols_i).astype(F32)
    local_tail = lax.dot_general(
        drift_s[...], later, NN, precision=lax.Precision.HIGHEST, preferred_element_type=F32
    )
    lane = lax.broadcasted_iota(jnp.int32, (heads, tok), 1)
    first = local_tail[:, 0:1]
    plain = jnp.sum(local_tail, axis=1, keepdims=True)
    square = jnp.sum(local_tail * local_tail, axis=1, keepdims=True)
    tot[place] = jnp.where(lane == 0, first, jnp.where(lane == 1, plain, square))

    def tot_copy(o, slot_at):
        return pltpu.make_async_remote_copy(
            src_ref=tot.at[place],
            dst_ref=tot.at[slot_at],
            send_sem=t_send.at[o],
            recv_sem=t_recv.at[slot_at],
            device_id={"seq": (place + o) % seq_count},
            device_id_type=MESH,
        )

    for o in range(1, seq_count):
        tot_copy(o, place).start()
    for o in range(1, seq_count):
        tot_copy(o, (place + o) % seq_count).wait_recv()
    after_total = jnp.zeros((heads, 1), F32)
    my_later = jnp.zeros((heads, 1), F32)
    energy = jnp.zeros((heads, 1), F32)
    for d in reversed(range(seq_count)):
        piece = tot[d]
        my_later = my_later + jnp.where(place == d, 1.0, 0.0) * after_total
        energy = energy + (
            piece[:, 2:3] + after_total * (2.0 * piece[:, 1:2] + tok * after_total)
        )
        after_total = after_total + piece[:, 0:1]
    energy = jnp.sum(jnp.broadcast_to(energy, (heads, dk)), axis=0, keepdims=True)
    sq[row] = jnp.broadcast_to(energy, (8, dk))

    def sq_copy(o, slot_at):
        return pltpu.make_async_remote_copy(
            src_ref=sq.at[row],
            dst_ref=sq.at[slot_at],
            send_sem=q_send.at[o],
            recv_sem=q_recv.at[slot_at],
            device_id={"head": (row + o) % head_count},
            device_id_type=MESH,
        )

    for o in range(1, head_count):
        sq_copy(o, row).start()
    for o in range(1, head_count):
        sq_copy(o, (row + o) % head_count).wait_recv()
    whole = sq[0]
    for r in range(1, head_count):
        whole = whole + sq[r]
    count = heads * tok * seq_count * head_count
    factor = jnp.minimum(1.0, lax.rsqrt(whole[0:1] / count + 1e-6))
    gg_ref[...] = (local_tail + my_later) * factor

    for b in range(bits):
        d_copy(b).wait_send()
        for n in range(2 if b == 0 else 1):
            level_wait(b, n).wait_send()
        if b > 0:
            forward_copy(b, own).wait_send()
        if b < bits - 1:

            @pl.when((bit[b] == 1) & want_s[b])
            def _(b=b):
                s_copy(b).wait_send()

            for j in range(b + 1, bits):

                @pl.when(bit[j] == 1)
                def _(b=b, j=j):
                    u_copy(b, j).wait_send()

    for o in range(1, seq_count):
        tot_copy(o, place).wait_send()
    for o in range(1, head_count):
        sq_copy(o, row).wait_send()


def chunked_kernel(
    seq_count,
    head_count,
    q_hbm,
    k_hbm,
    v_hbm,
    g_hbm,
    lg_hbm,
    lw_hbm,
    ds_hbm,
    gq_ref,
    gk_ref,
    gv_ref,
    gl_ref,
    tail_ref,
    msg,
    q_ref,
    k_ref,
    v_ref,
    g_ref,
    lg_ref,
    lw_ref,
    ds_ref,
    cum_s,
    col_s,
    lead_s,
    tail_s,
    bias_s,
    vt_s,
    gt_s,
    vg_s,
    gq_s,
    gk_s,
    drift_s,
    coef_s,
    mix_s,
    st,
    got_a,
    got_b,
    sum_a,
    sum_b,
    sum_q,
    lvl,
    relay,
    decs,
    i_sem,
    a_send,
    a_recv,
    b_send,
    b_recv,
    p_send,
    p_recv,
    xa_send,
    xa_recv,
    xb_send,
    xb_recv,
    y_send,
    y_recv,
    f_send,
    f_recv,
    r_send,
    r_recv,
    d_send,
    d_recv,
    t_send,
    t_recv,
    round_sem,
    plane_sem,
):
    tok = q_ref.shape[0]
    heads = lg_ref.shape[0]
    levels = lw_ref.shape[0]
    dk = q_ref.shape[1] // heads
    dv = v_ref.shape[1] // heads
    group = dk // dv
    pairs = heads // group
    spans = tok // SPAN
    span_bits = spans.bit_length() - 1
    bits = seq_count.bit_length() - 1
    half = heads // 2
    chunks = half // group
    cross = [min(span_bits + 1 + b, levels - 1) for b in range(bits)]
    slots = sorted(set(cross))
    kind = [1 + slots.index(l) for l in cross]
    place = lax.axis_index("seq")
    row = lax.axis_index("head")
    core, x, y = [(place // (1 << b)) % 2 for b in range(bits)]
    peer = [place + (1 - 2 * u) * (1 << b) for b, u in enumerate((core, x, y))]
    first_chip = (1 - x) * (1 - y)
    second_chip = x * (1 - y)
    mine = core * half
    theirs = (1 - core) * half

    has_next = (row < head_count - 1).astype(jnp.int32)
    has_last = (row > 0).astype(jnp.int32)

    def greet(sem):
        @pl.when(has_next == 1)
        def _():
            pl.semaphore_signal(sem, inc=1, device_id={"head": row + 1}, device_id_type=MESH)

        @pl.when(has_last == 1)
        def _():
            pl.semaphore_signal(sem, inc=1, device_id={"head": row - 1}, device_id_type=MESH)

    barrier = pltpu.get_barrier_semaphore()
    for b in reversed(range(bits)):
        pl.semaphore_signal(barrier, inc=1, device_id={"seq": peer[b]}, device_id_type=MESH)
    greet(barrier)

    def load(n):
        src = (lg_hbm, ds_hbm, v_hbm, k_hbm, g_hbm, lw_hbm, q_hbm)[n]
        dst = (lg_ref, ds_ref, v_ref, k_ref, g_ref, lw_ref, q_ref)[n]
        return pltpu.make_async_copy(src, dst, i_sem.at[n])

    for n in range(7):
        load(n).start()
    for n in range(2):
        load(n).wait()

    rows_i = lax.broadcasted_iota(jnp.int32, (tok, tok), 0)
    cols_i = lax.broadcasted_iota(jnp.int32, (tok, tok), 1)
    tri = (rows_i <= cols_i).astype(BF16)
    starts = jnp.broadcast_to(ds_ref[...].astype(F32), (8, tok))
    both = jnp.concatenate([lg_ref[...], starts], axis=0)
    cum_all = dot_exact(both, tri)
    cum = cum_all[:heads]
    reset = cum_all[heads : heads + 1]
    end_sum = cum[:, tok - 1 : tok]
    reset_end = reset[:, tok - 1 : tok]
    cum_s[...] = cum
    lead_s[...] = jnp.where(reset == 0, jnp.exp(cum), 0.0)
    tail_s[...] = jnp.where(reset == reset_end, jnp.exp(end_sum - cum), 0.0)
    def states(p, _):
        lanes = pl.ds(pl.multiple_of(p * dk, dk), dk)
        vt = jnp.transpose(v_ref[:, lanes].astype(F32))
        gt = jnp.transpose(g_ref[:, lanes].astype(F32))
        vt_s[p] = vt.astype(BF16)
        gt_s[p] = gt.astype(BF16)
        for i in range(group):
            h = p * group + i
            wide = pl.ds(pl.multiple_of(h * dk, dk), dk)
            part = slice(i * dv, (i + 1) * dv)
            tail = tail_s[pl.ds(h, 1), :]
            lead = lead_s[pl.ds(h, 1), :]
            st[0, h] = dot_fine(vt[part] * tail, k_ref[:, wide], NN)
            gw = jnp.concatenate(
                [gt[part] * (lead * lw_ref[l, pl.ds(h, 1), :]) for l in slots], axis=0
            )
            back = dot_fine(gw, q_ref[:, wide], NN)
            for n in range(len(slots)):
                st[1 + n, h] = back[n * dv : (n + 1) * dv]
        return 0

    for n in range(2, 7):
        load(n).wait()
    own_pair = core * chunks
    far_pair = (1 - core) * chunks
    def states_from(base):
        lax.fori_loop(0, 2, lambda n, _: states(base + n, 0), 0, unroll=2)

    states_from(far_pair)
    pl.semaphore_wait(barrier, bits + has_next + has_last)
    rounds = head_count - 2
    if rounds > 0:
        greet(round_sem.at[0])

    def remote(src, dst, send, recv, b):
        return pltpu.make_async_remote_copy(
            src_ref=src,
            dst_ref=dst,
            send_sem=send,
            recv_sem=recv,
            device_id={"seq": peer[b]},
            device_id_type=MESH,
        )

    def of(base, c):
        return pl.ds(base + c * group, group)

    def at(c):
        return pl.ds(c * group, group)

    kind_a = y * kind[2]
    kind_b = x * kind[1]
    slot_out = bits - (bits - 1) * first_chip
    slot_in = bits - (bits - 1) * second_chip

    def dec_copy(n):
        src = 3 if n == 2 else 2 * n
        return remote(decs.at[src], decs.at[2 * n + 1], d_send.at[n], d_recv.at[n], n)

    def a_copy(c):
        return remote(
            st.at[kind_a, of(theirs, c)], got_a.at[at(c)], a_send.at[c], a_recv.at[c], 0
        )

    def b_copy(c):
        return remote(
            st.at[kind_b, of(theirs, c)], got_b.at[at(c)], b_send.at[c], b_recv.at[c], 0
        )

    def p_copy(n):
        part = pl.ds(n * half, half)
        return remote(
            st.at[core * kind[0], part], lvl.at[0, part], p_send.at[n], p_recv.at[n], 0
        )

    piece = 1
    pieces = half // piece

    def xa_copy(n):
        here = pl.ds(n * piece, piece)
        there = pl.ds(mine + n * piece, piece)
        return remote(
            sum_a.at[here], lvl.at[slot_out, there], xa_send.at[n], xa_recv.at[n], 1
        )

    def xb_copy(n):
        here = pl.ds(n * piece, piece)
        there = pl.ds(mine + n * piece, piece)
        return remote(sum_b.at[here], lvl.at[1, there], xb_send.at[n], xb_recv.at[n], 1)

    def pieces_of(c):
        return range(c * group // piece, (c + 1) * group // piece)

    def y_copy(n):
        here = pl.ds(n * piece, piece)
        there = pl.ds(mine + n * piece, piece)
        return remote(sum_q.at[here], lvl.at[2, there], y_send.at[n], y_recv.at[n], 2)

    late = range(pieces - 2, pieces)

    def early_copy(n):
        return remote(
            sum_a.at[pl.ds(n * piece, piece)],
            relay.at[0, pl.ds((n - late[0]) * piece, piece)],
            y_send.at[n],
            y_recv.at[n],
            2,
        )

    def relay_copy(n):
        part = pl.ds((n - late[0]) * piece, piece)
        return remote(
            relay.at[0, part], relay.at[1, part], r_send.at[n - late[0]], r_recv.at[n - late[0]], 1
        )

    def f_copy(j, base, c):
        part = lvl.at[j, of(base, c)]
        return remote(part, part, f_send.at[j - 1, c], f_recv.at[j - 1, c], 0)

    for c in range(2):
        a_copy(c).start()
    lane_h = lax.broadcasted_iota(jnp.int32, (heads, dk), 1)
    head_h = lax.broadcasted_iota(jnp.int32, (heads, dk), 0)
    decay_all = jnp.where(reset_end == 0, jnp.exp(end_sum), 0.0)
    decs[0] = jnp.sum(jnp.where(lane_h == head_h, decay_all, 0.0), axis=0, keepdims=True)
    dec_copy(0).start()
    states_from(far_pair + 2)
    for c in range(2, chunks):
        a_copy(c).start()
    states_from(own_pair)
    states_from(own_pair + 2)
    cum_t = jnp.transpose(
        jnp.concatenate([cum_all, jnp.zeros((dk - heads - 8, tok), F32)], axis=0)
    )
    bias_s[...] = jnp.where(
        (rows_i <= cols_i) & (reset == cum_t[:, heads : heads + 1]), 0.0, -1e30
    )
    for h in range(heads):
        col_s[h] = jnp.broadcast_to(cum_t[:, h : h + 1], (tok, tok))


    span_of = lax.broadcasted_iota(jnp.int32, (1, tok), 1) // SPAN

    def local(p, _):
        vt = vt_s[p]
        gt = gt_s[p]
        lanes = pl.ds(pl.multiple_of(p * dk, dk), dk)
        v_blk = v_ref[:, lanes]
        for i in range(group):
            h = p * group + i
            wide = pl.ds(pl.multiple_of(h * dk, dk), dk)
            part = slice(i * dv, (i + 1) * dv)
            q = q_ref[:, wide]
            k = k_ref[:, wide]
            score = dot(k, q, NT)
            pair = dot(v_blk[:, part], gt[part], NN)
            decay = jnp.exp((cum_s[pl.ds(h, 1), :] - col_s[h]) + bias_s[...])
            seen = decay * score
            both_p = seen * pair
            gains = [lw_ref[l, pl.ds(h, 1), :] for l in range(span_bits + 1)]
            level_rows = [jnp.zeros((1, tok), F32) for _ in range(span_bits + 1)]
            mixed, graded = [], []
            for cs in range(spans):
                rows = slice(cs * SPAN, (cs + 1) * SPAN)
                total = jnp.sum(both_p[rows], axis=0, keepdims=True)
                gain = jnp.zeros((1, tok), F32)
                for ct in range(cs, spans):
                    l = span_level(cs, ct, levels)
                    hit = span_of == ct
                    gain = jnp.where(hit, gains[l], gain)
                    level_rows[l] = level_rows[l] + jnp.where(hit, total, 0.0)
                mixed.append(seen[rows] * gain)
                graded.append(decay[rows] * gain * pair[rows])
            mix = jnp.concatenate(mixed, axis=0).astype(BF16)
            grade = jnp.concatenate(graded, axis=0).astype(BF16)
            for l in range(span_bits + 1):
                gl_ref[l, pl.ds(h, 1), :] = level_rows[l]
            drift_s[pl.ds(h, 1), :] = jnp.sum(mix.astype(F32) * pair, axis=0, keepdims=True)
            vg_s[p, part] = dot(gt[part], mix, NT)
            gk_s[h] = dot(grade, q, NN)
            gq_s[h] = dot(grade, k, TN)
        return 0

    def spread(device_rows):
        t = jnp.transpose(
            jnp.concatenate(
                device_rows + [jnp.zeros((8 - len(device_rows), dk), F32)], axis=0
            )
        )
        return [
            jnp.broadcast_to(t[:heads, n : n + 1], (heads, dk)) for n in range(len(device_rows))
        ]

    def weigh(n, swap, own, got):
        w = (swap % 2).astype(F32)
        mix_s[n, 0] = own * (1.0 - w) + w
        mix_s[n, 1] = got * w + (1.0 - w)

    def combine(n, c, own_at, got_at, put):
        for i in range(group):
            r = c * group + i
            ca = mix_s[n, 0, pl.ds(mine + r, 1), :]
            cb = mix_s[n, 1, pl.ds(mine + r, 1), :]
            put[r] = ca * own_at(r) + cb * got_at(r)

    def local_pairs(first, last):
        lax.fori_loop(first, last, local, 0, unroll=2)

    def x_item(n, act):
        if n < late[0]:
            act(xa_copy(n))
            return

        @pl.when(y == 0)
        def _():
            if n < pieces:
                act(xa_copy(n))
            elif n < 2 * pieces and (n - pieces not in late or act is end):

                @pl.when(x == 1)
                def _():
                    act(xb_copy(n - pieces))

        if n - late[0] < pieces:

            @pl.when(y == 1)
            def _():
                act(xb_copy(n - late[0]))

    def begin(copy):
        copy.start()

    def end(copy):
        copy.wait_send()

    def x_start(n):
        x_item(n, begin)

    def x_sent(n):
        x_item(n, end)

    ahead = 5

    def x_next(n):
        x_sent(n)
        x_start(n + ahead)

    dec_copy(0).wait_recv()
    decs[2] = decs[0] * decs[1]
    d_self, d_pair = spread([decs[0], decs[1]])
    weigh(0, core + y, d_pair, d_self)
    weigh(1, core + x, d_pair, d_self)
    for c in range(chunks):
        a_copy(c).wait_recv()
        combine(0, c, lambda r: st[kind_a, mine + r], lambda r: got_a[r], sum_a)
        for n in pieces_of(c):
            if n < 2:
                x_start(n)
        if c == 1:
            dec_copy(1).start()

            @pl.when(first_chip == 0)
            def _():
                for n in range(chunks):
                    b_copy(n).start()

    for n in range(2, ahead):
        if n - 2 < len(late):

            @pl.when(y == 1)
            def _():
                early_copy(late[n - 2]).start()

        x_start(n)
    for n in late[ahead - 2 :]:

        @pl.when(y == 1)
        def _():
            early_copy(n).start()

    local_pairs(0, 4)

    @pl.when(first_chip == 0)
    def _():
        for c in range(chunks):
            b_copy(c).wait_recv()
            combine(1, c, lambda r: st[kind_b, mine + r], lambda r: got_b[r], sum_b)

    for r in range(1, rounds + 1):
        pl.semaphore_wait(round_sem.at[r - 1], has_next + has_last)
        if r < rounds:
            greet(round_sem.at[r])
    x_next(0)
    x_next(1)
    p_copy(0).start()
    local_pairs(4, 6)
    dec_copy(1).wait_recv()
    (d_side,) = spread([decs[3]])
    dec_copy(2).start()
    weigh(2, x + y, d_side, d_self * d_pair)
    inner_f = jnp.ones((heads, dk), F32)
    inner_b = jnp.ones((heads, dk), F32)
    for b, (u, got) in enumerate(((core, d_pair), (x, d_side), (y, None))):
        up = u.astype(F32)
        coef_s[0, b] = inner_f * up
        coef_s[1, b] = inner_b * (1.0 - up)
        if got is not None:
            inner_f = inner_f * (up * got + (1.0 - up))
            inner_b = inner_b * ((1.0 - up) * got + up)
    x_next(2)
    x_next(3)
    p_copy(1).start()
    def turn(n):
        if n in late:

            @pl.when(y == 0)
            def _():
                take_turn(n)

        else:
            take_turn(n)

    def take_turn(n):
        xa_copy(n).wait_recv()
        for r in range(n * piece, (n + 1) * piece):
            ca = mix_s[2, 0, pl.ds(mine + r, 1), :]
            cb = mix_s[2, 1, pl.ds(mine + r, 1), :]
            sum_q[r] = ca * sum_a[r] + cb * lvl[slot_in, mine + r]
        y_copy(n).start()
        if (n + 1) * piece % group == 0:

            @pl.when(second_chip == 1)
            def _():
                f_copy(1, mine, n * piece // group).start()

    def pass_on(ns):
        @pl.when(first_chip == 1)
        def _():
            for n in ns:
                early_copy(n).wait_recv()
                relay_copy(n).start()
                for r in range(n * piece, (n + 1) * piece):
                    lvl[2, mine + r] = jnp.zeros((dv, dk), F32)

    turn(0)
    local_pairs(6, pairs)
    x_next(4)
    turn(1)
    x_next(5)
    turn(2)
    x_next(6)
    turn(3)
    x_next(7)
    turn(4)
    pass_on(late[:1])

    x_next(8)
    turn(5)
    turn(6)
    pass_on(late[1:])
    x_next(9)
    x_next(10)
    turn(7)

    def incoming(h):
        blocks = [lvl[b, h] for b in range(bits)]
        entering = []
        for n in range(len(slots)):
            terms = [
                coef_s[0, b, pl.ds(h, 1), :] * blocks[b]
                for b in range(bits)
                if kind[b] == 1 + n
            ]
            entering.append(functools.reduce(jnp.add, terms))
        after = functools.reduce(
            jnp.add, [coef_s[1, b, pl.ds(h, 1), :] * blocks[b] for b in range(bits)]
        )
        return split(jnp.concatenate(entering, axis=0)), split(after)

    def finish_drift(p):
        vt = vt_s[p].astype(F32)
        gt = gt_s[p].astype(F32)
        for i in range(group):
            h = p * group + i
            wide = pl.ds(pl.multiple_of(h * dk, dk), dk)
            part = slice(i * dv, (i + 1) * dv)
            q = q_ref[:, wide]
            k = k_ref[:, wide]
            tail = tail_s[pl.ds(h, 1), :]
            lead = lead_s[pl.ds(h, 1), :]
            (e_high, e_low), (a_high, a_low) = incoming(h)
            seen = dot(e_high, q, NT) + dot(e_low, q, NT)
            drift = drift_s[pl.ds(h, 1), :]
            for n, l in enumerate(slots):
                level = lead * jnp.sum(
                    seen[n * dv : (n + 1) * dv] * gt[part], axis=0, keepdims=True
                )
                gl_ref[l, pl.ds(h, 1), :] = level
                drift = drift + lw_ref[l, pl.ds(h, 1), :] * level
            vg = vg_s[p, part] + tail * (dot(a_high, k, NT) + dot(a_low, k, NT))
            drift_s[pl.ds(h, 1), :] = drift - jnp.sum(vg * vt[part], axis=0, keepdims=True)
            vg_s[p, part] = vg

    def finish_out(p):
        lanes = pl.ds(pl.multiple_of(p * dk, dk), dk)
        vt = vt_s[p].astype(F32)
        gt = gt_s[p].astype(F32)
        for i in range(group):
            h = p * group + i
            wide = pl.ds(pl.multiple_of(h * dk, dk), dk)
            part = slice(i * dv, (i + 1) * dv)
            tail = tail_s[pl.ds(h, 1), :]
            lead = lead_s[pl.ds(h, 1), :]
            (e_high, e_low), (a_high, a_low) = incoming(h)
            gws = [gt[part] * (lead * lw_ref[l, pl.ds(h, 1), :]) for l in slots]
            gw, gw_low = split(jnp.concatenate(gws, axis=0))
            gq_in = dot(gw, e_high, TN) + dot(gw, e_low, TN) + dot(gw_low, e_high, TN)
            gq_ref[:, wide] = (gq_s[h] + gq_in).astype(BF16)
            tv, tv_low = split(vt[part] * tail)
            gk_in = dot(tv, a_high, TN) + dot(tv, a_low, TN) + dot(tv_low, a_high, TN)
            gk_ref[:, wide] = (gk_s[h] + gk_in).astype(BF16)
        gv_ref[:, lanes] = jnp.transpose(vg_s[p]).astype(BF16)

    dec_copy(2).wait_recv()
    (d_cross,) = spread([decs[5]])
    mix_s[3, 0] = d_cross
    mix_s[3, 1] = d_self * d_pair

    def join_late(ns):
        @pl.when(second_chip == 1)
        def _():
            for n in ns:
                early_copy(n).wait_recv()
                relay_copy(n).wait_recv()
                for r in range(n * piece, (n + 1) * piece):
                    ca = mix_s[3, 0, pl.ds(mine + r, 1), :]
                    cb = mix_s[3, 1, pl.ds(mine + r, 1), :]
                    m = r - late[0] * piece
                    joined = ca * relay[0, m] + relay[1, m]
                    lvl[2, mine + r] = joined
                    sum_b[r] = sum_b[r] + cb * joined
                xb_copy(n).start()

    for n in range(2):
        p_copy(n).wait_recv()
    def finish_far(c):
        for j in (1, 2):
            f_copy(j, theirs, c).wait_recv()
        finish_drift(far_pair + c)

    for c in range(chunks):
        for n in ((), (), (), ())[c]:
            x_next(n)
        if c == 0:
            join_late(late)
        for n in pieces_of(c):
            if n in late:

                @pl.when(y == 1)
                def _():
                    y_copy(n).wait_recv()

            else:
                y_copy(n).wait_recv()
        f_copy(2, mine, c).start()

        @pl.when(second_chip == 0)
        def _(c=c):
            for n in pieces_of(c):
                xb_copy(n).wait_recv()
            f_copy(1, mine, c).start()

        if c == 0:
            for o in range(1, head_count):
                pl.semaphore_signal(
                    plane_sem,
                    inc=1,
                    device_id={"head": (row + o) % head_count},
                    device_id_type=MESH,
                )
        finish_drift(own_pair + c)
        if c > 0:
            finish_far(c - 1)
    finish_far(chunks - 1)

    later = (rows_i >= cols_i).astype(BF16)
    local_tail = dot_exact(drift_s[...], later)
    tail_ref[...] = local_tail
    lane = lax.broadcasted_iota(jnp.int32, (heads, tok), 1)
    head = lax.broadcasted_iota(jnp.int32, (heads, tok), 0)
    sums = [
        local_tail[:, 0:1],
        jnp.sum(local_tail, axis=1, keepdims=True),
        jnp.sum(local_tail * local_tail, axis=1, keepdims=True),
    ]
    packed = jnp.zeros((heads, tok), F32)
    for n, column in enumerate(sums):
        packed = jnp.where(lane == head + n * heads, column, packed)
    slot = row * seq_count + place
    total = seq_count * head_count
    msg[slot] = jnp.sum(packed, axis=0, keepdims=True)

    def tail_copy(to_row, to_place):
        return pltpu.make_async_remote_copy(
            src_ref=msg.at[slot],
            dst_ref=msg.at[slot],
            send_sem=t_send.at[0],
            recv_sem=t_recv.at[0],
            device_id={"seq": to_place, "head": to_row},
            device_id_type=MESH,
        )

    def tail_all():
        others = msg.at[pl.ds(0, total - 1)]
        return pltpu.make_async_remote_copy(
            src_ref=others,
            dst_ref=others,
            send_sem=t_send.at[0],
            recv_sem=t_recv.at[0],
            device_id={"seq": peer[0]},
            device_id_type=MESH,
        )

    pl.semaphore_wait(plane_sem, head_count - 1)
    for o in list(range(1, head_count)) + [0]:
        for n in list(range(1, seq_count)) + [0]:
            if (o, n) != (0, 0):
                tail_copy((row + o) % head_count, (place + n) % seq_count).start()

    def outputs(p, _):
        finish_out(p)
        return 0

    lax.fori_loop(0, pairs, outputs, 0, unroll=2)
    for l in range(levels):
        if l > span_bits and l not in slots:
            gl_ref[l] = jnp.zeros((heads, tok), F32)

    for n in range(3):
        dec_copy(n).wait_send()

    @pl.when(first_chip == 1)
    def _():
        for n in late:
            relay_copy(n).wait_send()

    for n in range(2):
        p_copy(n).wait_send()
    for n in range(2 * pieces - ahead, 2 * pieces):
        x_sent(n)
    for c in range(chunks):
        a_copy(c).wait_send()
        for n in pieces_of(c):
            y_copy(n).wait_send()
        for j in (1, 2):
            f_copy(j, mine, c).wait_send()

    @pl.when(first_chip == 0)
    def _():
        for c in range(chunks):
            b_copy(c).wait_send()

    tail_all().wait_send()
    tail_all().wait_recv()


def finish_kernel(
    seq_count,
    head_count,
    gq_ref,
    gk_ref,
    gv_ref,
    gl_ref,
    tail_ref,
    msg,
    gq_out,
    gk_out,
    gv_out,
    gl_out,
    gg_out,
    gg_s,
    sems,
):
    copies = [
        pltpu.make_async_copy(src, dst, sems.at[n])
        for n, (src, dst) in enumerate(
            (
                (gq_ref, gq_out),
                (gk_ref, gk_out),
                (gv_ref, gv_out),
                (gl_ref, gl_out),
                (gg_s, gg_out),
            )
        )
    ]
    for c in copies[:4]:
        c.start()
    heads, tok = tail_ref.shape
    dk = msg.shape[2]
    total = seq_count * head_count
    slot = lax.axis_index("head") * seq_count + lax.axis_index("seq")
    rows = msg[:, 0, :]
    row_u = lax.broadcasted_iota(jnp.int32, (total, total), 0)
    row_v = lax.broadcasted_iota(jnp.int32, (total, total), 1)
    behind = ((row_u // seq_count == row_v // seq_count) & (row_v > row_u)).astype(BF16)
    after_rows = sum(dot(behind, piece, NN) for piece in pieces_exact(rows))
    plain = pltpu.roll(rows, dk - heads, 1)
    square = pltpu.roll(rows, dk - 2 * heads, 1)
    energy = square + after_rows * (2.0 * plain + tok * after_rows)
    lane_all = lax.broadcasted_iota(jnp.int32, (total, dk), 1)
    slot_all = lax.broadcasted_iota(jnp.int32, (total, dk), 0)
    energy = jnp.sum(jnp.where(lane_all < heads, energy, 0.0), axis=0, keepdims=True)
    whole = jnp.sum(energy, axis=1, keepdims=True)
    my_row = jnp.sum(jnp.where(slot_all == slot, after_rows, 0.0), axis=0, keepdims=True)
    lane = lax.broadcasted_iota(jnp.int32, (heads, dk), 1)
    head = lax.broadcasted_iota(jnp.int32, (heads, dk), 0)
    my_later = jnp.sum(jnp.where(lane == head, my_row, 0.0), axis=1, keepdims=True)
    count = heads * tok * total
    factor = jnp.minimum(1.0, lax.rsqrt(whole / count + 1e-6))
    gg_s[...] = (tail_ref[...] + my_later) * factor
    copies[4].start()
    for c in copies:
        c.wait()


def write_out(count, *refs):
    sems = refs[-1]
    copies = [
        pltpu.make_async_copy(refs[i], refs[count + i], sems.at[i]) for i in range(count)
    ]
    for c in copies:
        c.start()
    for c in copies:
        c.wait()


def shards(seq_count, head_count, queries, keys, values, out_grad, log_gate, level_weight, doc_start):
    tok = queries.shape[0]
    heads = log_gate.shape[0]
    levels = level_weight.shape[0]
    dk = queries.shape[1] // heads
    dv = values.shape[1] // heads
    group = dk // dv
    pairs = heads // group
    bits = seq_count.bit_length() - 1
    half = heads // 2
    span_bits = (tok // SPAN).bit_length() - 1
    slots = len({min(span_bits + 1 + b, levels - 1) for b in range(bits)})
    dma = pltpu.SemaphoreType.DMA
    vmem = pltpu.VMEM
    block = (dv, dk)
    scratch = [
        vmem((heads, tok), F32),
        vmem((heads, tok, tok), F32),
        vmem((heads, tok), F32),
        vmem((heads, tok), F32),
        vmem((tok, tok), F32),
        vmem((pairs, group * dv, tok), BF16),
        vmem((pairs, group * dv, tok), BF16),
        vmem((pairs, group * dv, tok), F32),
        vmem((heads, tok, dk), F32),
        vmem((heads, tok, dk), F32),
        vmem((heads, tok), F32),
        vmem((2, bits, heads, dk), F32),
        vmem((heads,) + block, F32),
        vmem((slots, heads) + block, F32),
        vmem((bits, heads) + block, F32),
        vmem((bits, half) + block, F32),
        vmem((bits, bits, half) + block, F32),
        vmem((bits, half) + block, F32),
        vmem((bits, bits, half) + block, F32),
        vmem((bits + 1, heads, dk), F32),
        vmem((bits, heads, dk), F32),
        vmem((seq_count, heads, tok), F32),
        vmem((head_count, 8, dk), F32),
        dma((bits, 2)),
        dma((bits, 2)),
        dma((bits,)),
        dma((bits,)),
        dma((bits,)),
        dma((bits,)),
        dma((bits, bits)),
        dma((bits, bits)),
        dma((bits,)),
        dma((bits,)),
        dma((seq_count,)),
        dma((seq_count,)),
        dma((head_count,)),
        dma((head_count,)),
    ]
    args = (queries, keys, values, out_grad, log_gate, level_weight, doc_start.reshape(1, tok))
    spec = pl.BlockSpec(memory_space=pltpu.VMEM)
    in_spec = spec
    body = kernel
    chunks = half // group
    if bits == 3 and chunks == 4 and chunks * group == half and tok == dk and 3 * heads <= dk:
        body = chunked_kernel
        inputs = [(x.shape, x.dtype) for x in args]
        scratch = [vmem(*x) for x in inputs] + scratch[:12] + [
            vmem((4, 2, heads, dk), F32),
            vmem((1 + slots, heads) + block, F32),
            vmem((half,) + block, F32),
            vmem((half,) + block, F32),
            vmem((half,) + block, F32),
            vmem((half,) + block, F32),
            vmem((half,) + block, F32),
            vmem((bits + 1, heads) + block, F32),
            vmem((2, 2) + block, F32),
            vmem((6, 1, dk), F32),
            dma((7,)),
            dma((chunks,)),
            dma((chunks,)),
            dma((chunks,)),
            dma((chunks,)),
            dma((2,)),
            dma((2,)),
            dma((half,)),
            dma((half,)),
            dma((half,)),
            dma((half,)),
            dma((half,)),
            dma((half,)),
            dma((2, chunks)),
            dma((2, chunks)),
            dma((2,)),
            dma((2,)),
            dma((3,)),
            dma((3,)),
            dma((1,)),
            dma((1,)),
            pltpu.SemaphoreType.REGULAR((max(1, head_count - 2),)),
            pltpu.SemaphoreType.REGULAR,
        ]
        in_spec = pl.BlockSpec(memory_space=pltpu.HBM)
    outs = [
        (queries.shape, BF16),
        (keys.shape, BF16),
        (values.shape, BF16),
        (level_weight.shape, F32),
        (log_gate.shape, F32),
    ]
    held = list(outs)
    writer = (write_out, len(outs))
    writer_scratch = []
    if body is chunked_kernel:
        held.append(((seq_count * head_count, 1, dk), F32))
        writer = (finish_kernel, seq_count, head_count)
        writer_scratch = [vmem(*outs[-1])]
    results = pl.pallas_call(
        functools.partial(body, seq_count, head_count),
        out_shape=tuple(vmem(shape, dtype) for shape, dtype in held),
        in_specs=[in_spec] * 7,
        out_specs=(spec,) * len(held),
        scratch_shapes=scratch,
        compiler_params=pltpu.CompilerParams(collective_id=0, has_side_effects=True),
    )(*args)
    count = len(outs)
    return pl.pallas_call(
        functools.partial(*writer),
        out_shape=tuple(jax.ShapeDtypeStruct(shape, dtype) for shape, dtype in outs),
        in_specs=[spec] * len(held),
        out_specs=(pl.BlockSpec(memory_space=pltpu.HBM),) * count,
        scratch_shapes=writer_scratch + [dma((count,))],
    )(*[pltpu.with_memory_space_constraint(r, pltpu.VMEM) for r in results])


def solution(mesh):
    return jax.shard_map(
        functools.partial(shards, mesh.shape["seq"], mesh.shape["head"]),
        mesh=mesh,
        in_specs=(
            P("seq", "head"),
            P("seq", "head"),
            P("seq", "head"),
            P("seq", "head"),
            P("head", "seq"),
            P(None, "head", "seq"),
            P("seq"),
        ),
        out_specs=(
            P("seq", "head"),
            P("seq", "head"),
            P("seq", "head"),
            P(None, "head", "seq"),
            P("head", "seq"),
        ),
        check_vma=False,
    )
```

```python
import functools

import jax
import jax.numpy as jnp
from jax import lax
from jax.experimental import pallas as pl
from jax.experimental.pallas import tpu as pltpu
from jax.sharding import PartitionSpec as P

SPAN = 64
F32 = jnp.float32
BF16 = jnp.bfloat16
NN = (((1,), (0,)), ((), ()))
NT = (((1,), (1,)), ((), ()))
TN = (((0,), (0,)), ((), ()))
MESH = pl.DeviceIdType.MESH


def dot(a, b, dims):
    return lax.dot_general(a, b, dims, preferred_element_type=F32)


def split(x):
    high = x.astype(BF16)
    return high, (x - high.astype(F32)).astype(BF16)


def pieces_exact(x):
    high = x.astype(BF16)
    rest = x - high.astype(F32)
    middle = rest.astype(BF16)
    return high, middle, (rest - middle.astype(F32)).astype(BF16)


def dot_exact(x, b):
    rows = x.shape[0]
    out = dot(jnp.concatenate(pieces_exact(x), axis=0), b, NN)
    return out[:rows] + out[rows : 2 * rows] + out[2 * rows :]


def dot_fine(x, b, dims):
    high, low = split(x)
    return dot(high, b, dims) + dot(low, b, dims)


def span_level(a, b, levels):
    return 0 if a == b else min(levels - 1, (a ^ b).bit_length())


def kernel(
    seq_count,
    head_count,
    q_ref,
    k_ref,
    v_ref,
    g_ref,
    lg_ref,
    lw_ref,
    ds_ref,
    gq_ref,
    gk_ref,
    gv_ref,
    gl_ref,
    gg_ref,
    cum_s,
    col_s,
    lead_s,
    tail_s,
    bias_s,
    vt_s,
    gt_s,
    vg_s,
    gq_s,
    gk_s,
    drift_s,
    coef_s,
    state_s,
    back_s,
    lvl,
    got_s,
    got_u,
    sum_s,
    sum_u,
    dec,
    got_dec,
    tot,
    sq,
    lvl_send,
    lvl_recv,
    fwd_send,
    fwd_recv,
    s_send,
    s_recv,
    u_send,
    u_recv,
    d_send,
    d_recv,
    t_send,
    t_recv,
    q_send,
    q_recv,
):
    tok = q_ref.shape[0]
    heads = lg_ref.shape[0]
    levels = lw_ref.shape[0]
    dk = q_ref.shape[1] // heads
    dv = v_ref.shape[1] // heads
    group = dk // dv
    pairs = heads // group
    spans = tok // SPAN
    span_bits = spans.bit_length() - 1
    bits = seq_count.bit_length() - 1
    half = heads // 2
    cross = [min(span_bits + 1 + b, levels - 1) for b in range(bits)]
    slots = sorted(set(cross))
    place = lax.axis_index("seq")
    row = lax.axis_index("head")
    bit = [(place // (1 << b)) % 2 for b in range(bits)]
    peer = [place + (1 - 2 * bit[b]) * (1 << b) for b in range(bits)]
    want_s = [(place // (2 << b)) != (seq_count // (2 << b)) - 1 for b in range(bits)]
    mine = bit[0] * half
    theirs = (1 - bit[0]) * half

    barrier = pltpu.get_barrier_semaphore()
    for o in range(1, seq_count):
        pl.semaphore_signal(
            barrier, inc=1, device_id={"seq": (place + o) % seq_count}, device_id_type=MESH
        )
    for o in range(1, head_count):
        pl.semaphore_signal(
            barrier, inc=1, device_id={"head": (row + o) % head_count}, device_id_type=MESH
        )

    rows_i = lax.broadcasted_iota(jnp.int32, (tok, tok), 0)
    cols_i = lax.broadcasted_iota(jnp.int32, (tok, tok), 1)
    tri = (rows_i <= cols_i).astype(F32)
    starts = jnp.broadcast_to(ds_ref[...].astype(F32), (8, tok))
    both = jnp.concatenate([lg_ref[...], starts], axis=0)
    cum_all = lax.dot_general(
        both, tri, NN, precision=lax.Precision.HIGHEST, preferred_element_type=F32
    )
    cum_t = jnp.transpose(cum_all)
    cum = cum_all[:heads]
    reset = cum_all[heads : heads + 1]
    reset_col = cum_t[:, heads : heads + 1]
    bias_s[...] = jnp.where((rows_i <= cols_i) & (reset == reset_col), 0.0, -1e30)
    end = cum[:, tok - 1 : tok]
    reset_end = reset[:, tok - 1 : tok]
    cum_s[...] = cum
    lead_s[...] = jnp.where(reset == 0, jnp.exp(cum), 0.0)
    tail_s[...] = jnp.where(reset == reset_end, jnp.exp(end - cum), 0.0)
    dec[0] = jnp.broadcast_to(jnp.where(reset_end == 0, jnp.exp(end), 0.0), (heads, dk))
    for h in range(heads):
        col_s[h] = jnp.broadcast_to(cum_t[:, h : h + 1], (tok, tok))

    def states(p, _):
        lanes = pl.ds(pl.multiple_of(p * dk, dk), dk)
        vt = jnp.transpose(v_ref[:, lanes].astype(F32))
        gt = jnp.transpose(g_ref[:, lanes].astype(F32))
        vt_s[p] = vt.astype(BF16)
        gt_s[p] = gt.astype(BF16)
        for i in range(group):
            h = p * group + i
            wide = pl.ds(pl.multiple_of(h * dk, dk), dk)
            part = slice(i * dv, (i + 1) * dv)
            tail = tail_s[pl.ds(h, 1), :]
            lead = lead_s[pl.ds(h, 1), :]
            state_s[h] = dot_fine(vt[part] * tail, k_ref[:, wide], NN)
            gw = jnp.concatenate(
                [gt[part] * (lead * lw_ref[l, pl.ds(h, 1), :]) for l in slots], axis=0
            )
            back = dot_fine(gw, q_ref[:, wide], NN)
            for n in range(len(slots)):
                back_s[n, h] = back[n * dv : (n + 1) * dv]
        return 0

    lax.fori_loop(0, pairs, states, 0, unroll=2)
    pl.semaphore_wait(barrier, seq_count - 1 + head_count - 1)

    def slot(b):
        return slots.index(cross[b])

    def remote(src, dst, send, recv, b):
        return pltpu.make_async_remote_copy(
            src_ref=src,
            dst_ref=dst,
            send_sem=send,
            recv_sem=recv,
            device_id={"seq": peer[b]},
            device_id_type=MESH,
        )

    own = pl.ds(mine, half)
    other = pl.ds(theirs, half)

    def u_copy(b, j):
        src = back_s.at[slot(j), other] if b == 0 else sum_u.at[b, j]
        return remote(src, got_u.at[b, j], u_send.at[b, j], u_recv.at[b, j], b)

    def s_copy(b):
        src = state_s.at[other] if b == 0 else sum_s.at[b]
        return remote(src, got_s.at[b], s_send.at[b], s_recv.at[b], b)

    def d_copy(b):
        return remote(dec.at[b], got_dec.at[b], d_send.at[b], d_recv.at[b], b)

    def level_copy(b, low):
        if b == 0:
            src = state_s if low else back_s.at[slot(0)]
            return [
                remote(src.at[part], lvl.at[0, part], lvl_send.at[0, n], lvl_recv.at[0, n], 0)
                for n, part in enumerate((other, own))
            ]
        src = sum_s.at[b] if low else sum_u.at[b, b]
        return [remote(src, lvl.at[b, own], lvl_send.at[b, 0], lvl_recv.at[b, 0], b)]

    def level_wait(b, n):
        part = other if n == 1 else own
        return remote(
            lvl.at[b, part], lvl.at[b, part], lvl_send.at[b, n], lvl_recv.at[b, n], b
        )

    def forward_copy(b, part):
        return remote(lvl.at[b, part], lvl.at[b, part], fwd_send.at[b], fwd_recv.at[b], 0)

    def land(b):
        up_summed = (bit[b] == 1) & want_s[b]

        @pl.when(jnp.logical_not(up_summed))
        def _():
            level_wait(b, 0).wait_recv()

        if b > 0:
            forward_copy(b, own).start()

    def begin(b):
        d_copy(b).start()

        early = 0 if b in (0, bits - 1) else 1

        @pl.when((bit[b] == 0) & (want_s[b] | (early == 0)))
        def _():
            for c in level_copy(b, True):
                c.start()

        if b < bits - 1:

            @pl.when((bit[b] == 1) & want_s[b])
            def _():
                s_copy(b).start()

            for j in range(b + 1, bits):

                @pl.when(bit[j] == 1)
                def _(j=j):
                    u_copy(b, j).start()

        if early == 0:

            @pl.when(bit[b] == 1)
            def _():
                for c in level_copy(b, False):
                    c.start()

    def begin_late(b):
        if b in (0, bits - 1):
            return

        @pl.when((bit[b] == 0) & jnp.logical_not(want_s[b]))
        def _():
            for c in level_copy(b, True):
                c.start()

        @pl.when(bit[b] == 1)
        def _():
            for c in level_copy(b, False):
                c.start()

    def join(b):
        d_copy(b).wait_recv()
        up = bit[b].astype(F32)
        got = got_dec[b]
        now = dec[b]
        dec[b + 1] = got * now
        if b == bits - 1:
            return
        base_s = state_s.at[own] if b == 0 else sum_s.at[b]

        @pl.when(want_s[b])
        def _():
            @pl.when(bit[b] == 1)
            def _():
                level_wait(b, 0).wait_recv()

                def body(i, _):
                    d = dec[b, pl.ds(mine + i, 1), :]
                    sum_s[b + 1, i] = d * lvl[b, mine + i] + base_s[i]
                    return 0

                lax.fori_loop(0, half, body, 0, unroll=True)

            @pl.when(bit[b] == 0)
            def _():
                s_copy(b).wait_recv()

                def body(i, _):
                    d = got_dec[b, pl.ds(mine + i, 1), :]
                    sum_s[b + 1, i] = d * base_s[i] + got_s[b, i]
                    return 0

                lax.fori_loop(0, half, body, 0, unroll=True)

        for j in range(b + 1, bits):
            base_u = back_s.at[slot(j), own] if b == 0 else sum_u.at[b, j]

            @pl.when(bit[j] == 1)
            def _(j=j, base_u=base_u):
                u_copy(b, j).wait_recv()

                def body(i, _):
                    d0 = dec[b, pl.ds(mine + i, 1), :]
                    d1 = got_dec[b, pl.ds(mine + i, 1), :]
                    a = up * d1 + (1.0 - up)
                    c = (1.0 - up) * d0 + up
                    sum_u[b + 1, j, i] = a * base_u[i] + c * got_u[b, j, i]
                    return 0

                lax.fori_loop(0, half, body, 0, unroll=True)

    span_of = lax.broadcasted_iota(jnp.int32, (1, tok), 1) // SPAN

    def local(p, _):
        vt = vt_s[p]
        gt = gt_s[p]
        lanes = pl.ds(pl.multiple_of(p * dk, dk), dk)
        v_blk = v_ref[:, lanes]
        for i in range(group):
            h = p * group + i
            wide = pl.ds(pl.multiple_of(h * dk, dk), dk)
            part = slice(i * dv, (i + 1) * dv)
            q = q_ref[:, wide]
            k = k_ref[:, wide]
            score = dot(k, q, NT)
            pair = dot(v_blk[:, part], gt[part], NN)
            decay = jnp.exp((cum_s[pl.ds(h, 1), :] - col_s[h]) + bias_s[...])
            seen = decay * score
            both_p = seen * pair
            gains = [lw_ref[l, pl.ds(h, 1), :] for l in range(span_bits + 1)]
            level_rows = [jnp.zeros((1, tok), F32) for _ in range(span_bits + 1)]
            mixed, graded = [], []
            for cs in range(spans):
                rows = slice(cs * SPAN, (cs + 1) * SPAN)
                total = jnp.sum(both_p[rows], axis=0, keepdims=True)
                gain = jnp.zeros((1, tok), F32)
                for ct in range(cs, spans):
                    l = span_level(cs, ct, levels)
                    hit = span_of == ct
                    gain = jnp.where(hit, gains[l], gain)
                    level_rows[l] = level_rows[l] + jnp.where(hit, total, 0.0)
                mixed.append(seen[rows] * gain)
                graded.append(decay[rows] * gain * pair[rows])
            mix = jnp.concatenate(mixed, axis=0).astype(BF16)
            grade = jnp.concatenate(graded, axis=0).astype(BF16)
            for l in range(span_bits + 1):
                gl_ref[l, pl.ds(h, 1), :] = level_rows[l]
            drift_s[pl.ds(h, 1), :] = jnp.sum(mix.astype(F32) * pair, axis=0, keepdims=True)
            vg_s[p, part] = dot(gt[part], mix, NT)
            gk_s[h] = dot(grade, q, NN)
            gq_s[h] = dot(grade, k, TN)
        return 0

    begin(0)
    lax.fori_loop(0, pairs // 4, local, 0, unroll=2)
    join(0)
    if bits > 1:
        begin(1)
    lax.fori_loop(pairs // 4, pairs, local, 0, unroll=2)
    for b in range(1, bits):
        join(b)
        if b + 1 < bits:
            begin(b + 1)
        begin_late(b)
        land(b - 1)
    land(bits - 1)

    inner_f = jnp.ones((heads, dk), F32)
    inner_b = jnp.ones((heads, dk), F32)
    for b in range(bits):
        up = bit[b].astype(F32)
        got = got_dec[b]
        coef_s[0, b] = inner_f * up
        coef_s[1, b] = inner_b * (1.0 - up)
        inner_f = inner_f * (up * got + (1.0 - up))
        inner_b = inner_b * ((1.0 - up) * got + up)
    level_wait(0, 1).wait_recv()
    for b in range(1, bits):
        forward_copy(b, other).wait_recv()

    def finish(p, _):
        lanes = pl.ds(pl.multiple_of(p * dk, dk), dk)
        vt = vt_s[p].astype(F32)
        gt = gt_s[p].astype(F32)
        vg_all = []
        for i in range(group):
            h = p * group + i
            wide = pl.ds(pl.multiple_of(h * dk, dk), dk)
            part = slice(i * dv, (i + 1) * dv)
            q = q_ref[:, wide]
            k = k_ref[:, wide]
            tail = tail_s[pl.ds(h, 1), :]
            lead = lead_s[pl.ds(h, 1), :]
            blocks = [lvl[b, h] for b in range(bits)]
            entering = []
            for n in range(len(slots)):
                terms = [
                    coef_s[0, b, pl.ds(h, 1), :] * blocks[b] for b in range(bits) if slot(b) == n
                ]
                entering.append(functools.reduce(jnp.add, terms))
            entering = jnp.concatenate(entering, axis=0)
            after = functools.reduce(
                jnp.add, [coef_s[1, b, pl.ds(h, 1), :] * blocks[b] for b in range(bits)]
            )
            e_high, e_low = split(entering)
            seen = dot(e_high, q, NT) + dot(e_low, q, NT)
            drift = drift_s[pl.ds(h, 1), :]
            gws = []
            for n, l in enumerate(slots):
                gain = lw_ref[l, pl.ds(h, 1), :]
                level = lead * jnp.sum(
                    seen[n * dv : (n + 1) * dv] * gt[part], axis=0, keepdims=True
                )
                gl_ref[l, pl.ds(h, 1), :] = level
                drift = drift + gain * level
                gws.append(gt[part] * (lead * gain))
            gw, gw_low = split(jnp.concatenate(gws, axis=0))
            gq_in = dot(gw, e_high, TN) + dot(gw, e_low, TN) + dot(gw_low, e_high, TN)
            gq_ref[:, wide] = (gq_s[h] + gq_in).astype(BF16)
            a_high, a_low = split(after)
            tv, tv_low = split(vt[part] * tail)
            gk_in = dot(tv, a_high, TN) + dot(tv, a_low, TN) + dot(tv_low, a_high, TN)
            gk_ref[:, wide] = (gk_s[h] + gk_in).astype(BF16)
            vg = vg_s[p, part] + tail * (dot(a_high, k, NT) + dot(a_low, k, NT))
            drift_s[pl.ds(h, 1), :] = drift - jnp.sum(vg * vt[part], axis=0, keepdims=True)
            vg_all.append(vg)
        gv_ref[:, lanes] = jnp.transpose(jnp.concatenate(vg_all, axis=0)).astype(BF16)
        return 0

    lax.fori_loop(0, pairs, finish, 0, unroll=2)
    for l in range(levels):
        if l > span_bits and l not in slots:
            gl_ref[l] = jnp.zeros((heads, tok), F32)

    later = (rows_i >= cols_i).astype(F32)
    local_tail = lax.dot_general(
        drift_s[...], later, NN, precision=lax.Precision.HIGHEST, preferred_element_type=F32
    )
    lane = lax.broadcasted_iota(jnp.int32, (heads, tok), 1)
    first = local_tail[:, 0:1]
    plain = jnp.sum(local_tail, axis=1, keepdims=True)
    square = jnp.sum(local_tail * local_tail, axis=1, keepdims=True)
    tot[place] = jnp.where(lane == 0, first, jnp.where(lane == 1, plain, square))

    def tot_copy(o, slot_at):
        return pltpu.make_async_remote_copy(
            src_ref=tot.at[place],
            dst_ref=tot.at[slot_at],
            send_sem=t_send.at[o],
            recv_sem=t_recv.at[slot_at],
            device_id={"seq": (place + o) % seq_count},
            device_id_type=MESH,
        )

    for o in range(1, seq_count):
        tot_copy(o, place).start()
    for o in range(1, seq_count):
        tot_copy(o, (place + o) % seq_count).wait_recv()
    after_total = jnp.zeros((heads, 1), F32)
    my_later = jnp.zeros((heads, 1), F32)
    energy = jnp.zeros((heads, 1), F32)
    for d in reversed(range(seq_count)):
        piece = tot[d]
        my_later = my_later + jnp.where(place == d, 1.0, 0.0) * after_total
        energy = energy + (
            piece[:, 2:3] + after_total * (2.0 * piece[:, 1:2] + tok * after_total)
        )
        after_total = after_total + piece[:, 0:1]
    energy = jnp.sum(jnp.broadcast_to(energy, (heads, dk)), axis=0, keepdims=True)
    sq[row] = jnp.broadcast_to(energy, (8, dk))

    def sq_copy(o, slot_at):
        return pltpu.make_async_remote_copy(
            src_ref=sq.at[row],
            dst_ref=sq.at[slot_at],
            send_sem=q_send.at[o],
            recv_sem=q_recv.at[slot_at],
            device_id={"head": (row + o) % head_count},
            device_id_type=MESH,
        )

    for o in range(1, head_count):
        sq_copy(o, row).start()
    for o in range(1, head_count):
        sq_copy(o, (row + o) % head_count).wait_recv()
    whole = sq[0]
    for r in range(1, head_count):
        whole = whole + sq[r]
    count = heads * tok * seq_count * head_count
    factor = jnp.minimum(1.0, lax.rsqrt(whole[0:1] / count + 1e-6))
    gg_ref[...] = (local_tail + my_later) * factor

    for b in range(bits):
        d_copy(b).wait_send()
        for n in range(2 if b == 0 else 1):
            level_wait(b, n).wait_send()
        if b > 0:
            forward_copy(b, own).wait_send()
        if b < bits - 1:

            @pl.when((bit[b] == 1) & want_s[b])
            def _(b=b):
                s_copy(b).wait_send()

            for j in range(b + 1, bits):

                @pl.when(bit[j] == 1)
                def _(b=b, j=j):
                    u_copy(b, j).wait_send()

    for o in range(1, seq_count):
        tot_copy(o, place).wait_send()
    for o in range(1, head_count):
        sq_copy(o, row).wait_send()


def chunked_kernel(
    seq_count,
    head_count,
    q_hbm,
    k_hbm,
    v_hbm,
    g_hbm,
    lg_hbm,
    lw_hbm,
    ds_hbm,
    gq_ref,
    gk_ref,
    gv_ref,
    gl_ref,
    tail_ref,
    msg,
    q_ref,
    k_ref,
    v_ref,
    g_ref,
    lg_ref,
    lw_ref,
    ds_ref,
    cum_s,
    col_s,
    lead_s,
    tail_s,
    bias_s,
    vt_s,
    gt_s,
    vg_s,
    gq_s,
    gk_s,
    drift_s,
    coef_s,
    mix_s,
    st,
    got_a,
    got_b,
    sum_a,
    sum_b,
    sum_q,
    lvl,
    relay,
    decs,
    i_sem,
    a_send,
    a_recv,
    b_send,
    b_recv,
    p_send,
    p_recv,
    xa_send,
    xa_recv,
    xb_send,
    xb_recv,
    y_send,
    y_recv,
    f_send,
    f_recv,
    r_send,
    r_recv,
    d_send,
    d_recv,
    t_send,
    t_recv,
    round_sem,
    plane_sem,
):
    tok = q_ref.shape[0]
    heads = lg_ref.shape[0]
    levels = lw_ref.shape[0]
    dk = q_ref.shape[1] // heads
    dv = v_ref.shape[1] // heads
    group = dk // dv
    pairs = heads // group
    spans = tok // SPAN
    span_bits = spans.bit_length() - 1
    bits = seq_count.bit_length() - 1
    half = heads // 2
    chunks = half // group
    cross = [min(span_bits + 1 + b, levels - 1) for b in range(bits)]
    slots = sorted(set(cross))
    kind = [1 + slots.index(l) for l in cross]
    place = lax.axis_index("seq")
    row = lax.axis_index("head")
    core, x, y = [(place // (1 << b)) % 2 for b in range(bits)]
    peer = [place + (1 - 2 * u) * (1 << b) for b, u in enumerate((core, x, y))]
    first_chip = (1 - x) * (1 - y)
    second_chip = x * (1 - y)
    mine = core * half
    theirs = (1 - core) * half

    has_next = (row < head_count - 1).astype(jnp.int32)
    has_last = (row > 0).astype(jnp.int32)

    def greet(sem):
        @pl.when(has_next == 1)
        def _():
            pl.semaphore_signal(sem, inc=1, device_id={"head": row + 1}, device_id_type=MESH)

        @pl.when(has_last == 1)
        def _():
            pl.semaphore_signal(sem, inc=1, device_id={"head": row - 1}, device_id_type=MESH)

    barrier = pltpu.get_barrier_semaphore()
    for b in reversed(range(bits)):
        pl.semaphore_signal(barrier, inc=1, device_id={"seq": peer[b]}, device_id_type=MESH)
    greet(barrier)

    def load(n):
        src = (lg_hbm, ds_hbm, v_hbm, k_hbm, g_hbm, lw_hbm, q_hbm)[n]
        dst = (lg_ref, ds_ref, v_ref, k_ref, g_ref, lw_ref, q_ref)[n]
        return pltpu.make_async_copy(src, dst, i_sem.at[n])

    for n in range(7):
        load(n).start()
    for n in range(2):
        load(n).wait()

    rows_i = lax.broadcasted_iota(jnp.int32, (tok, tok), 0)
    cols_i = lax.broadcasted_iota(jnp.int32, (tok, tok), 1)
    tri = (rows_i <= cols_i).astype(BF16)
    starts = jnp.broadcast_to(ds_ref[...].astype(F32), (8, tok))
    both = jnp.concatenate([lg_ref[...], starts], axis=0)
    cum_all = dot_exact(both, tri)
    cum = cum_all[:heads]
    reset = cum_all[heads : heads + 1]
    end_sum = cum[:, tok - 1 : tok]
    reset_end = reset[:, tok - 1 : tok]
    cum_s[...] = cum
    lead_s[...] = jnp.where(reset == 0, jnp.exp(cum), 0.0)
    tail_s[...] = jnp.where(reset == reset_end, jnp.exp(end_sum - cum), 0.0)
    def states(p, _):
        lanes = pl.ds(pl.multiple_of(p * dk, dk), dk)
        vt = jnp.transpose(v_ref[:, lanes].astype(F32))
        gt = jnp.transpose(g_ref[:, lanes].astype(F32))
        made = []
        for i in range(group):
            h = p * group + i
            wide = pl.ds(pl.multiple_of(h * dk, dk), dk)
            part = slice(i * dv, (i + 1) * dv)
            tail = tail_s[pl.ds(h, 1), :]
            lead = lead_s[pl.ds(h, 1), :]
            gw = jnp.concatenate(
                [gt[part] * (lead * lw_ref[l, pl.ds(h, 1), :]) for l in slots], axis=0
            )
            made.append(
                (
                    h,
                    dot_fine(vt[part] * tail, k_ref[:, wide], NN),
                    dot_fine(gw, q_ref[:, wide], NN),
                )
            )
        for h, front, back in made:
            st[0, h] = front
            for n in range(len(slots)):
                st[1 + n, h] = back[n * dv : (n + 1) * dv]
        vt_s[p] = vt.astype(BF16)
        gt_s[p] = gt.astype(BF16)
        return 0

    for n in range(2, 7):
        load(n).wait()
    own_pair = core * chunks
    far_pair = (1 - core) * chunks
    def states_from(base):
        lax.fori_loop(0, 2, lambda n, _: states(base + n, 0), 0, unroll=2)

    states_from(far_pair)
    pl.semaphore_wait(barrier, bits + has_next + has_last)
    rounds = head_count - 2
    if rounds > 0:
        greet(round_sem.at[0])

    def remote(src, dst, send, recv, b):
        return pltpu.make_async_remote_copy(
            src_ref=src,
            dst_ref=dst,
            send_sem=send,
            recv_sem=recv,
            device_id={"seq": peer[b]},
            device_id_type=MESH,
        )

    def of(base, c):
        return pl.ds(base + c * group, group)

    def at(c):
        return pl.ds(c * group, group)

    kind_a = y * kind[2]
    kind_b = x * kind[1]
    slot_out = bits - (bits - 1) * first_chip
    slot_in = bits - (bits - 1) * second_chip

    def dec_copy(n):
        src = 3 if n == 2 else 2 * n
        return remote(decs.at[src], decs.at[2 * n + 1], d_send.at[n], d_recv.at[n], n)

    def a_copy(c):
        return remote(
            st.at[kind_a, of(theirs, c)], got_a.at[at(c)], a_send.at[c], a_recv.at[c], 0
        )

    def b_copy(c):
        return remote(
            st.at[kind_b, of(theirs, c)], got_b.at[at(c)], b_send.at[c], b_recv.at[c], 0
        )

    def p_copy(n):
        part = pl.ds(n * half, half)
        return remote(
            st.at[core * kind[0], part], lvl.at[0, part], p_send.at[n], p_recv.at[n], 0
        )

    piece = 1
    pieces = half // piece

    def xa_copy(n):
        here = pl.ds(n * piece, piece)
        there = pl.ds(mine + n * piece, piece)
        return remote(
            sum_a.at[here], lvl.at[slot_out, there], xa_send.at[n], xa_recv.at[n], 1
        )

    def xb_copy(n):
        here = pl.ds(n * piece, piece)
        there = pl.ds(mine + n * piece, piece)
        return remote(sum_b.at[here], lvl.at[1, there], xb_send.at[n], xb_recv.at[n], 1)

    def pieces_of(c):
        return range(c * group // piece, (c + 1) * group // piece)

    def y_copy(n):
        here = pl.ds(n * piece, piece)
        there = pl.ds(mine + n * piece, piece)
        return remote(sum_q.at[here], lvl.at[2, there], y_send.at[n], y_recv.at[n], 2)

    late = range(pieces - 2, pieces)

    def early_copy(n):
        return remote(
            sum_a.at[pl.ds(n * piece, piece)],
            relay.at[0, pl.ds((n - late[0]) * piece, piece)],
            y_send.at[n],
            y_recv.at[n],
            2,
        )

    def relay_copy(n):
        part = pl.ds((n - late[0]) * piece, piece)
        return remote(
            relay.at[0, part], relay.at[1, part], r_send.at[n - late[0]], r_recv.at[n - late[0]], 1
        )

    def f_copy(j, base, c):
        part = lvl.at[j, of(base, c)]
        return remote(part, part, f_send.at[j - 1, c], f_recv.at[j - 1, c], 0)

    for c in range(2):
        a_copy(c).start()
    lane_h = lax.broadcasted_iota(jnp.int32, (heads, dk), 1)
    head_h = lax.broadcasted_iota(jnp.int32, (heads, dk), 0)
    decay_all = jnp.where(reset_end == 0, jnp.exp(end_sum), 0.0)
    decs[0] = jnp.sum(jnp.where(lane_h == head_h, decay_all, 0.0), axis=0, keepdims=True)
    dec_copy(0).start()
    states_from(far_pair + 2)
    for c in range(2, chunks):
        a_copy(c).start()
    states_from(own_pair)
    states_from(own_pair + 2)
    cum_t = jnp.transpose(
        jnp.concatenate([cum_all, jnp.zeros((dk - heads - 8, tok), F32)], axis=0)
    )
    bias_s[...] = jnp.where(
        (rows_i <= cols_i) & (reset == cum_t[:, heads : heads + 1]), 0.0, -1e30
    )
    for h in range(heads):
        col_s[h] = jnp.broadcast_to(cum_t[:, h : h + 1], (tok, tok))


    span_of = lax.broadcasted_iota(jnp.int32, (1, tok), 1) // SPAN

    def local(p, _):
        vt = vt_s[p]
        gt = gt_s[p]
        lanes = pl.ds(pl.multiple_of(p * dk, dk), dk)
        v_blk = v_ref[:, lanes]
        for i in range(group):
            h = p * group + i
            wide = pl.ds(pl.multiple_of(h * dk, dk), dk)
            part = slice(i * dv, (i + 1) * dv)
            q = q_ref[:, wide]
            k = k_ref[:, wide]
            score = dot(k, q, NT)
            pair = dot(v_blk[:, part], gt[part], NN)
            decay = jnp.exp((cum_s[pl.ds(h, 1), :] - col_s[h]) + bias_s[...])
            seen = decay * score
            both_p = seen * pair
            gains = [lw_ref[l, pl.ds(h, 1), :] for l in range(span_bits + 1)]
            level_rows = [jnp.zeros((1, tok), F32) for _ in range(span_bits + 1)]
            mixed, graded = [], []
            for cs in range(spans):
                rows = slice(cs * SPAN, (cs + 1) * SPAN)
                total = jnp.sum(both_p[rows], axis=0, keepdims=True)
                gain = jnp.zeros((1, tok), F32)
                for ct in range(cs, spans):
                    l = span_level(cs, ct, levels)
                    hit = span_of == ct
                    gain = jnp.where(hit, gains[l], gain)
                    level_rows[l] = level_rows[l] + jnp.where(hit, total, 0.0)
                mixed.append(seen[rows] * gain)
                graded.append(decay[rows] * gain * pair[rows])
            mix = jnp.concatenate(mixed, axis=0).astype(BF16)
            grade = jnp.concatenate(graded, axis=0).astype(BF16)
            for l in range(span_bits + 1):
                gl_ref[l, pl.ds(h, 1), :] = level_rows[l]
            drift_s[pl.ds(h, 1), :] = jnp.sum(mix.astype(F32) * pair, axis=0, keepdims=True)
            vg_s[p, part] = dot(gt[part], mix, NT)
            gk_s[h] = dot(grade, q, NN)
            gq_s[h] = dot(grade, k, TN)
        return 0

    def spread(device_rows):
        t = jnp.transpose(
            jnp.concatenate(
                device_rows + [jnp.zeros((8 - len(device_rows), dk), F32)], axis=0
            )
        )
        return [
            jnp.broadcast_to(t[:heads, n : n + 1], (heads, dk)) for n in range(len(device_rows))
        ]

    def weigh(n, swap, own, got):
        w = (swap % 2).astype(F32)
        mix_s[n, 0] = own * (1.0 - w) + w
        mix_s[n, 1] = got * w + (1.0 - w)

    def combine(n, c, own_at, got_at, put):
        for i in range(group):
            r = c * group + i
            ca = mix_s[n, 0, pl.ds(mine + r, 1), :]
            cb = mix_s[n, 1, pl.ds(mine + r, 1), :]
            put[r] = ca * own_at(r) + cb * got_at(r)

    def local_pairs(first, last):
        lax.fori_loop(first, last, local, 0, unroll=2)

    def x_item(n, act):
        if n < late[0]:
            act(xa_copy(n))
            return

        @pl.when(y == 0)
        def _():
            if n < pieces:
                act(xa_copy(n))
            elif n < 2 * pieces and (n - pieces not in late or act is end):

                @pl.when(x == 1)
                def _():
                    act(xb_copy(n - pieces))

        if n - late[0] < pieces:

            @pl.when(y == 1)
            def _():
                act(xb_copy(n - late[0]))

    def begin(copy):
        copy.start()

    def end(copy):
        copy.wait_send()

    def x_start(n):
        x_item(n, begin)

    def x_sent(n):
        x_item(n, end)

    ahead = 5

    def x_next(n):
        x_sent(n)
        x_start(n + ahead)

    dec_copy(0).wait_recv()
    decs[2] = decs[0] * decs[1]
    d_self, d_pair = spread([decs[0], decs[1]])
    weigh(0, core + y, d_pair, d_self)
    weigh(1, core + x, d_pair, d_self)
    for c in range(chunks):
        a_copy(c).wait_recv()
        combine(0, c, lambda r: st[kind_a, mine + r], lambda r: got_a[r], sum_a)
        for n in pieces_of(c):
            if n < 2:
                x_start(n)
        if c == 1:
            dec_copy(1).start()

            @pl.when(first_chip == 0)
            def _():
                for n in range(chunks):
                    b_copy(n).start()

    for n in range(2, ahead):
        if n - 2 < len(late):

            @pl.when(y == 1)
            def _():
                early_copy(late[n - 2]).start()

        x_start(n)
    for n in late[ahead - 2 :]:

        @pl.when(y == 1)
        def _():
            early_copy(n).start()

    local_pairs(0, 4)

    @pl.when(first_chip == 0)
    def _():
        for c in range(chunks):
            b_copy(c).wait_recv()
            combine(1, c, lambda r: st[kind_b, mine + r], lambda r: got_b[r], sum_b)

    for r in range(1, rounds + 1):
        pl.semaphore_wait(round_sem.at[r - 1], has_next + has_last)
        if r < rounds:
            greet(round_sem.at[r])
    x_next(0)
    x_next(1)

    @pl.when(core == 1)
    def _():
        p_copy(0).start()

    local_pairs(4, 6)
    dec_copy(1).wait_recv()
    (d_side,) = spread([decs[3]])
    dec_copy(2).start()
    weigh(2, x + y, d_side, d_self * d_pair)
    inner_f = jnp.ones((heads, dk), F32)
    inner_b = jnp.ones((heads, dk), F32)
    for b, (u, got) in enumerate(((core, d_pair), (x, d_side), (y, None))):
        up = u.astype(F32)
        coef_s[0, b] = inner_f * up
        coef_s[1, b] = inner_b * (1.0 - up)
        if got is not None:
            inner_f = inner_f * (up * got + (1.0 - up))
            inner_b = inner_b * ((1.0 - up) * got + up)
    x_next(2)
    x_next(3)

    @pl.when(core == 1)
    def _():
        p_copy(1).start()

    def turn(n):
        if n in late:

            @pl.when(y == 0)
            def _():
                take_turn(n)

        else:
            take_turn(n)

    def take_turn(n):
        xa_copy(n).wait_recv()
        for r in range(n * piece, (n + 1) * piece):
            ca = mix_s[2, 0, pl.ds(mine + r, 1), :]
            cb = mix_s[2, 1, pl.ds(mine + r, 1), :]
            sum_q[r] = ca * sum_a[r] + cb * lvl[slot_in, mine + r]
        y_copy(n).start()
        if (n + 1) * piece % group == 0:

            @pl.when(second_chip == 1)
            def _():
                f_copy(1, mine, n * piece // group).start()

    def pass_on(ns):
        @pl.when(first_chip == 1)
        def _():
            for n in ns:
                early_copy(n).wait_recv()
                relay_copy(n).start()
                for r in range(n * piece, (n + 1) * piece):
                    lvl[2, mine + r] = jnp.zeros((dv, dk), F32)

    turn(0)
    local_pairs(6, pairs)
    x_next(4)
    turn(1)
    x_next(5)

    @pl.when(core == 0)
    def _():
        p_copy(0).start()

    turn(2)
    x_next(6)
    turn(3)
    x_next(7)

    @pl.when(core == 0)
    def _():
        p_copy(1).start()

    turn(4)
    pass_on(late[:1])

    x_next(8)
    turn(5)
    turn(6)
    pass_on(late[1:])
    x_next(9)
    x_next(10)
    turn(7)

    def incoming(h):
        blocks = [lvl[b, h] for b in range(bits)]
        entering = []
        for n in range(len(slots)):
            terms = [
                coef_s[0, b, pl.ds(h, 1), :] * blocks[b]
                for b in range(bits)
                if kind[b] == 1 + n
            ]
            entering.append(functools.reduce(jnp.add, terms))
        after = functools.reduce(
            jnp.add, [coef_s[1, b, pl.ds(h, 1), :] * blocks[b] for b in range(bits)]
        )
        return split(jnp.concatenate(entering, axis=0)), split(after)

    def finish_drift(p):
        vt = vt_s[p].astype(F32)
        gt = gt_s[p].astype(F32)
        vg_old = vg_s[p]
        heads_of = [p * group + i for i in range(group)]
        held = [incoming(h) for h in heads_of]
        seen_all, out_all = [], []
        for h, ((e_high, e_low), (a_high, a_low)) in zip(heads_of, held):
            wide = pl.ds(pl.multiple_of(h * dk, dk), dk)
            q = q_ref[:, wide]
            k = k_ref[:, wide]
            seen_all.append(dot(e_high, q, NT) + dot(e_low, q, NT))
            out_all.append(dot(a_high, k, NT) + dot(a_low, k, NT))
        stores = []
        for i, h in enumerate(heads_of):
            part = slice(i * dv, (i + 1) * dv)
            lead = lead_s[pl.ds(h, 1), :]
            drift = drift_s[pl.ds(h, 1), :]
            rows = []
            for n, l in enumerate(slots):
                level = lead * jnp.sum(
                    seen_all[i][n * dv : (n + 1) * dv] * gt[part], axis=0, keepdims=True
                )
                rows.append(level)
                drift = drift + lw_ref[l, pl.ds(h, 1), :] * level
            vg = vg_old[part] + tail_s[pl.ds(h, 1), :] * out_all[i]
            drift = drift - jnp.sum(vg * vt[part], axis=0, keepdims=True)
            stores.append((drift, vg, rows))
        for h, (drift, vg, rows) in zip(heads_of, stores):
            drift_s[pl.ds(h, 1), :] = drift
            for l, level in zip(slots, rows):
                gl_ref[l, pl.ds(h, 1), :] = level
        vg_s[p] = jnp.concatenate([vg for _, vg, _ in stores], axis=0)

    def finish_out(p):
        lanes = pl.ds(pl.multiple_of(p * dk, dk), dk)
        vt = vt_s[p].astype(F32)
        gt = gt_s[p].astype(F32)
        for i in range(group):
            h = p * group + i
            wide = pl.ds(pl.multiple_of(h * dk, dk), dk)
            part = slice(i * dv, (i + 1) * dv)
            tail = tail_s[pl.ds(h, 1), :]
            lead = lead_s[pl.ds(h, 1), :]
            (e_high, e_low), (a_high, a_low) = incoming(h)
            gws = [gt[part] * (lead * lw_ref[l, pl.ds(h, 1), :]) for l in slots]
            gw, gw_low = split(jnp.concatenate(gws, axis=0))
            gq_in = dot(gw, e_high, TN) + dot(gw, e_low, TN) + dot(gw_low, e_high, TN)
            gq_ref[:, wide] = (gq_s[h] + gq_in).astype(BF16)
            tv, tv_low = split(vt[part] * tail)
            gk_in = dot(tv, a_high, TN) + dot(tv, a_low, TN) + dot(tv_low, a_high, TN)
            gk_ref[:, wide] = (gk_s[h] + gk_in).astype(BF16)
        gv_ref[:, lanes] = jnp.transpose(vg_s[p]).astype(BF16)

    dec_copy(2).wait_recv()
    (d_cross,) = spread([decs[5]])
    mix_s[3, 0] = d_cross
    mix_s[3, 1] = d_self * d_pair

    def join_late(ns):
        @pl.when(second_chip == 1)
        def _():
            for n in ns:
                early_copy(n).wait_recv()
                relay_copy(n).wait_recv()
                for r in range(n * piece, (n + 1) * piece):
                    ca = mix_s[3, 0, pl.ds(mine + r, 1), :]
                    cb = mix_s[3, 1, pl.ds(mine + r, 1), :]
                    m = r - late[0] * piece
                    joined = ca * relay[0, m] + relay[1, m]
                    lvl[2, mine + r] = joined
                    sum_b[r] = sum_b[r] + cb * joined
                xb_copy(n).start()

    for n in range(2):
        p_copy(n).wait_recv()
    def finish_far(c):
        for j in (1, 2):
            f_copy(j, theirs, c).wait_recv()
        finish_drift(far_pair + c)

    for c in range(chunks):
        for n in ((), (), (), ())[c]:
            x_next(n)
        if c == 0:
            join_late(late)
        for n in pieces_of(c):
            if n in late:

                @pl.when(y == 1)
                def _():
                    y_copy(n).wait_recv()

            else:
                y_copy(n).wait_recv()
        f_copy(2, mine, c).start()

        @pl.when(second_chip == 0)
        def _(c=c):
            for n in pieces_of(c):
                xb_copy(n).wait_recv()
            f_copy(1, mine, c).start()

        if c == 0:
            for o in range(1, head_count):
                pl.semaphore_signal(
                    plane_sem,
                    inc=1,
                    device_id={"head": (row + o) % head_count},
                    device_id_type=MESH,
                )
        finish_drift(own_pair + c)
        if c > 0:
            finish_far(c - 1)
    finish_far(chunks - 1)

    later = (rows_i >= cols_i).astype(BF16)
    local_tail = dot_exact(drift_s[...], later)
    tail_ref[...] = local_tail
    lane = lax.broadcasted_iota(jnp.int32, (heads, tok), 1)
    head = lax.broadcasted_iota(jnp.int32, (heads, tok), 0)
    sums = [
        local_tail[:, 0:1],
        jnp.sum(local_tail, axis=1, keepdims=True),
        jnp.sum(local_tail * local_tail, axis=1, keepdims=True),
    ]
    packed = jnp.zeros((heads, tok), F32)
    for n, column in enumerate(sums):
        packed = jnp.where(lane == head + n * heads, column, packed)
    slot = row * seq_count + place
    total = seq_count * head_count
    msg[slot] = jnp.sum(packed, axis=0, keepdims=True)

    def tail_copy(to_row, to_place):
        return pltpu.make_async_remote_copy(
            src_ref=msg.at[slot],
            dst_ref=msg.at[slot],
            send_sem=t_send.at[0],
            recv_sem=t_recv.at[0],
            device_id={"seq": to_place, "head": to_row},
            device_id_type=MESH,
        )

    def tail_all():
        others = msg.at[pl.ds(0, total - 1)]
        return pltpu.make_async_remote_copy(
            src_ref=others,
            dst_ref=others,
            send_sem=t_send.at[0],
            recv_sem=t_recv.at[0],
            device_id={"seq": peer[0]},
            device_id_type=MESH,
        )

    pl.semaphore_wait(plane_sem, head_count - 1)
    for o in list(range(1, head_count)) + [0]:
        for n in list(range(1, seq_count)) + [0]:
            if (o, n) != (0, 0):
                tail_copy((row + o) % head_count, (place + n) % seq_count).start()

    def outputs(p, _):
        finish_out(p)
        return 0

    lax.fori_loop(0, pairs, outputs, 0, unroll=2)
    for l in range(levels):
        if l > span_bits and l not in slots:
            gl_ref[l] = jnp.zeros((heads, tok), F32)

    for n in range(3):
        dec_copy(n).wait_send()

    @pl.when(first_chip == 1)
    def _():
        for n in late:
            relay_copy(n).wait_send()

    for n in range(2):
        p_copy(n).wait_send()
    for n in range(2 * pieces - ahead, 2 * pieces):
        x_sent(n)
    for c in range(chunks):
        a_copy(c).wait_send()
        for n in pieces_of(c):
            y_copy(n).wait_send()
        for j in (1, 2):
            f_copy(j, mine, c).wait_send()

    @pl.when(first_chip == 0)
    def _():
        for c in range(chunks):
            b_copy(c).wait_send()

    tail_all().wait_send()
    tail_all().wait_recv()


def finish_kernel(
    seq_count,
    head_count,
    gq_ref,
    gk_ref,
    gv_ref,
    gl_ref,
    tail_ref,
    msg,
    gq_out,
    gk_out,
    gv_out,
    gl_out,
    gg_out,
    gg_s,
    sems,
):
    copies = [
        pltpu.make_async_copy(src, dst, sems.at[n])
        for n, (src, dst) in enumerate(
            (
                (gq_ref, gq_out),
                (gk_ref, gk_out),
                (gv_ref, gv_out),
                (gl_ref, gl_out),
                (gg_s, gg_out),
            )
        )
    ]
    for c in copies[:4]:
        c.start()
    heads, tok = tail_ref.shape
    dk = msg.shape[2]
    total = seq_count * head_count
    slot = lax.axis_index("head") * seq_count + lax.axis_index("seq")
    rows = msg[:, 0, :]
    row_u = lax.broadcasted_iota(jnp.int32, (total, total), 0)
    row_v = lax.broadcasted_iota(jnp.int32, (total, total), 1)
    behind = ((row_u // seq_count == row_v // seq_count) & (row_v > row_u)).astype(BF16)
    after_rows = sum(dot(behind, piece, NN) for piece in pieces_exact(rows))
    plain = pltpu.roll(rows, dk - heads, 1)
    square = pltpu.roll(rows, dk - 2 * heads, 1)
    energy = square + after_rows * (2.0 * plain + tok * after_rows)
    lane_all = lax.broadcasted_iota(jnp.int32, (total, dk), 1)
    slot_all = lax.broadcasted_iota(jnp.int32, (total, dk), 0)
    energy = jnp.sum(jnp.where(lane_all < heads, energy, 0.0), axis=0, keepdims=True)
    whole = jnp.sum(energy, axis=1, keepdims=True)
    my_row = jnp.sum(jnp.where(slot_all == slot, after_rows, 0.0), axis=0, keepdims=True)
    lane = lax.broadcasted_iota(jnp.int32, (heads, dk), 1)
    head = lax.broadcasted_iota(jnp.int32, (heads, dk), 0)
    my_later = jnp.sum(jnp.where(lane == head, my_row, 0.0), axis=1, keepdims=True)
    count = heads * tok * total
    factor = jnp.minimum(1.0, lax.rsqrt(whole / count + 1e-6))
    gg_s[...] = (tail_ref[...] + my_later) * factor
    copies[4].start()
    for c in copies:
        c.wait()


def write_out(count, *refs):
    sems = refs[-1]
    copies = [
        pltpu.make_async_copy(refs[i], refs[count + i], sems.at[i]) for i in range(count)
    ]
    for c in copies:
        c.start()
    for c in copies:
        c.wait()


def shards(seq_count, head_count, queries, keys, values, out_grad, log_gate, level_weight, doc_start):
    tok = queries.shape[0]
    heads = log_gate.shape[0]
    levels = level_weight.shape[0]
    dk = queries.shape[1] // heads
    dv = values.shape[1] // heads
    group = dk // dv
    pairs = heads // group
    bits = seq_count.bit_length() - 1
    half = heads // 2
    span_bits = (tok // SPAN).bit_length() - 1
    slots = len({min(span_bits + 1 + b, levels - 1) for b in range(bits)})
    dma = pltpu.SemaphoreType.DMA
    vmem = pltpu.VMEM
    block = (dv, dk)
    scratch = [
        vmem((heads, tok), F32),
        vmem((heads, tok, tok), F32),
        vmem((heads, tok), F32),
        vmem((heads, tok), F32),
        vmem((tok, tok), F32),
        vmem((pairs, group * dv, tok), BF16),
        vmem((pairs, group * dv, tok), BF16),
        vmem((pairs, group * dv, tok), F32),
        vmem((heads, tok, dk), F32),
        vmem((heads, tok, dk), F32),
        vmem((heads, tok), F32),
        vmem((2, bits, heads, dk), F32),
        vmem((heads,) + block, F32),
        vmem((slots, heads) + block, F32),
        vmem((bits, heads) + block, F32),
        vmem((bits, half) + block, F32),
        vmem((bits, bits, half) + block, F32),
        vmem((bits, half) + block, F32),
        vmem((bits, bits, half) + block, F32),
        vmem((bits + 1, heads, dk), F32),
        vmem((bits, heads, dk), F32),
        vmem((seq_count, heads, tok), F32),
        vmem((head_count, 8, dk), F32),
        dma((bits, 2)),
        dma((bits, 2)),
        dma((bits,)),
        dma((bits,)),
        dma((bits,)),
        dma((bits,)),
        dma((bits, bits)),
        dma((bits, bits)),
        dma((bits,)),
        dma((bits,)),
        dma((seq_count,)),
        dma((seq_count,)),
        dma((head_count,)),
        dma((head_count,)),
    ]
    args = (queries, keys, values, out_grad, log_gate, level_weight, doc_start.reshape(1, tok))
    spec = pl.BlockSpec(memory_space=pltpu.VMEM)
    in_spec = spec
    body = kernel
    chunks = half // group
    if bits == 3 and chunks == 4 and chunks * group == half and tok == dk and 3 * heads <= dk:
        body = chunked_kernel
        inputs = [(x.shape, x.dtype) for x in args]
        scratch = [vmem(*x) for x in inputs] + scratch[:12] + [
            vmem((4, 2, heads, dk), F32),
            vmem((1 + slots, heads) + block, F32),
            vmem((half,) + block, F32),
            vmem((half,) + block, F32),
            vmem((half,) + block, F32),
            vmem((half,) + block, F32),
            vmem((half,) + block, F32),
            vmem((bits + 1, heads) + block, F32),
            vmem((2, 2) + block, F32),
            vmem((6, 1, dk), F32),
            dma((7,)),
            dma((chunks,)),
            dma((chunks,)),
            dma((chunks,)),
            dma((chunks,)),
            dma((2,)),
            dma((2,)),
            dma((half,)),
            dma((half,)),
            dma((half,)),
            dma((half,)),
            dma((half,)),
            dma((half,)),
            dma((2, chunks)),
            dma((2, chunks)),
            dma((2,)),
            dma((2,)),
            dma((3,)),
            dma((3,)),
            dma((1,)),
            dma((1,)),
            pltpu.SemaphoreType.REGULAR((max(1, head_count - 2),)),
            pltpu.SemaphoreType.REGULAR,
        ]
        in_spec = pl.BlockSpec(memory_space=pltpu.HBM)
    outs = [
        (queries.shape, BF16),
        (keys.shape, BF16),
        (values.shape, BF16),
        (level_weight.shape, F32),
        (log_gate.shape, F32),
    ]
    held = list(outs)
    writer = (write_out, len(outs))
    writer_scratch = []
    if body is chunked_kernel:
        held.append(((seq_count * head_count, 1, dk), F32))
        writer = (finish_kernel, seq_count, head_count)
        writer_scratch = [vmem(*outs[-1])]
    results = pl.pallas_call(
        functools.partial(body, seq_count, head_count),
        out_shape=tuple(vmem(shape, dtype) for shape, dtype in held),
        in_specs=[in_spec] * 7,
        out_specs=(spec,) * len(held),
        scratch_shapes=scratch,
        compiler_params=pltpu.CompilerParams(collective_id=0, has_side_effects=True),
    )(*args)
    count = len(outs)
    return pl.pallas_call(
        functools.partial(*writer),
        out_shape=tuple(jax.ShapeDtypeStruct(shape, dtype) for shape, dtype in outs),
        in_specs=[spec] * len(held),
        out_specs=(pl.BlockSpec(memory_space=pltpu.HBM),) * count,
        scratch_shapes=writer_scratch + [dma((count,))],
    )(*[pltpu.with_memory_space_constraint(r, pltpu.VMEM) for r in results])


def solution(mesh):
    return jax.shard_map(
        functools.partial(shards, mesh.shape["seq"], mesh.shape["head"]),
        mesh=mesh,
        in_specs=(
            P("seq", "head"),
            P("seq", "head"),
            P("seq", "head"),
            P("seq", "head"),
            P("head", "seq"),
            P(None, "head", "seq"),
            P("seq"),
        ),
        out_specs=(
            P("seq", "head"),
            P("seq", "head"),
            P("seq", "head"),
            P(None, "head", "seq"),
            P("head", "seq"),
        ),
        check_vma=False,
    )
```
